32 devices in a mesh: dp: 4 (over z), row: 4 (over y, x), col: 2 (over core).
Axes of the slice: x: 2, y: 2, z: 4, core: 2. Of those that a mesh axis runs over, the one named last changes fastest.
Arguments:
- inputs: bfloat16 [4096, 1024], P(('dp', 'row'), 'col'), may hold values from -53 to 53
- prefix: int32 [4], P('dp'), may hold values from 102 to 512
- picks: int32 [4096, 4, 32], P(('dp', 'col')), may hold values from 0 to 65535, as said below
- gain_attn: bfloat16 [1024], replicated, may hold values from 0.25 to 1.75
- w_qkv: bfloat16 [3, 1024, 1024], P(None, 'col', 'row'), may hold values from -0.1875 to 0.1875
- w_attn_out: bfloat16 [1024, 1024], P('row', 'col'), may hold values from -1.5 to 1.5
- gain_mem: bfloat16 [1024], replicated, may hold values from 0.25 to 1.75
- w_query: bfloat16 [1024, 4096], P('col', 'row'), may hold values from -0.1875 to 0.1875
- w_gate: bfloat16 [1024, 1024], P('col', 'row'), may hold values from -0.1875 to 0.1875
- w_proj: bfloat16 [1024, 1024], P('row', 'col'), may hold values from -0.5 to 0.5
- subkeys: bfloat16 [4, 2, 256, 512], replicated, may hold values from -0.1875 to 0.1875
- values: bfloat16 [65536, 1024], P(('dp', 'row', 'col')), may hold values from -6 to 6
- cotangent: bfloat16 [4096, 1024], P(('dp', 'row'), 'col'), may hold values from -6 to 6
Outputs:
- output: bfloat16 [4096, 1024], P(('dp', 'row'), 'col')
- grad_inputs: float32 [4096, 1024], P(('dp', 'row'), 'col')
- grad_gain_attn: float32 [1024], replicated
- grad_w_qkv: float32 [3, 1024, 1024], P(None, 'col', 'row')
- grad_w_attn_out: float32 [1024, 1024], P('row', 'col')
- grad_gain_mem: float32 [1024], replicated
- grad_w_query: float32 [1024, 4096], P('col', 'row')
- grad_w_gate: float32 [1024, 1024], P('col', 'row')
- grad_w_proj: float32 [1024, 1024], P('row', 'col')
- grad_subkeys: float32 [4, 2, 256, 512], replicated
- grad_values: float32 [65536, 1024], P(('dp', 'row', 'col'))
The draws below stay inside these ranges and needn't reach their ends.
Inputs may be any that keep to these rules, and one draw needn't show every extreme that they name: `picks`: for each memory head and each aligned block of 128 tokens, each device's run of 2048 value rows is picked exactly 128 times.
All inputs are finite; a program needn't handle non-finite values.
Results may differ from the reference program's by a relative error of at most 0.018.
Values may be sent and summed in bfloat16 or wider, within the bound.
A program may use at most 256 MiB of HBM per device.

```python
import math
import jax
import jax.numpy as jnp
from jax import lax

D = 1024
HEADS = 16
HDIM = 64
MH = 4
HALF = 512
SUBKEYS = 256
VDIM = 1024
TOPK = 32
FBLK = 128
SEQ = 1024
TOKENS = 4096
VROWS = 65536
ROWS_DEV = 2048
CAP = 128
N_DP = 4


def draw_inputs(key, part):
    key_base, key_rows, key_cols = jax.random.split(key, 3)
    base_values = jnp.clip(jax.random.normal(key_base, (TOKENS, D), jnp.float32), -5.0, 5.0)
    col_scale = jnp.exp(jax.random.uniform(key_cols, (1, D), jnp.float32, math.log(0.3), math.log(3.0)))
    row_scale = jnp.exp(jax.random.uniform(key_rows, (TOKENS, 1), jnp.float32, math.log(0.3), math.log(3.0)))
    return (base_values * row_scale * col_scale).astype(jnp.bfloat16)


def draw_picks(key, part):
    block_count = TOKENS // FBLK * MH
    pick_count = FBLK * TOPK
    perm_keys = jax.random.split(jax.random.fold_in(key, 11), block_count)
    orders = jax.vmap(lambda one_key: jax.random.permutation(one_key, pick_count))(perm_keys)
    owners = orders // CAP
    offsets = jax.random.randint(jax.random.fold_in(key, 12), (block_count, pick_count), 0, ROWS_DEV)
    rows_all = (owners * ROWS_DEV + offsets).reshape(TOKENS // FBLK, MH, FBLK, TOPK)
    return jnp.transpose(rows_all, (0, 2, 1, 3)).reshape(TOKENS, MH, TOPK).astype(jnp.int32)


def set_ends(values, stream_key, smallest, high):
    longest = values.shape.index(max(values.shape))
    spots = []
    for shift in (0, 1):
        where = [jax.random.randint(jax.random.fold_in(stream_key, axis), (), 0, length) for axis, length in enumerate(values.shape)]
        where[longest] = (where[longest] + shift) % values.shape[longest]
        spots.append(tuple(where))
    return values.at[spots[0]].set(smallest).at[spots[1]].set(high)


def levels(rng, extent, cuts, least, high):
    def one(dim, parts):
        heights = jax.random.uniform(jax.random.fold_in(jax.random.fold_in(rng, 6), dim), (parts,), jnp.float32, least / len(cuts), high / len(cuts))
        return jnp.repeat(jnp.exp(heights), extent[dim] // parts).reshape((-1,) + (1,) * (len(extent) - dim - 1))

    factor_of = one(*cuts[0])
    for cut in cuts[1:]:
        factor_of = factor_of * one(*cut)
    return factor_of


def noise(own_key, shape, deviation, reach, shards=(), held_as=jnp.bfloat16):
    values = jax.random.normal(own_key, shape, jnp.float32) * deviation
    if len(shards) > 0:
        values = levels(own_key, shape, shards, -0.22, 0.18) * values
    return jnp.clip(values, min=-reach, max=reach).astype(held_as)


def setup_inputs(seed: int = 0) -> dict:
    streams_of = jax.random.split(jax.random.key(seed), 14)
    return {
        "inputs": draw_inputs(jax.random.fold_in(streams_of[13], 71), 0),
        "prefix": set_ends(jax.random.randint(streams_of[1], (N_DP,), SEQ // 10, SEQ // 2 + 1), jax.random.fold_in(streams_of[1], 1), SEQ // 10, (SEQ // 2 + 1) - 1).astype(jnp.int32),
        "picks": draw_picks(jax.random.fold_in(streams_of[13], 71), 0),
        "gain_attn": jnp.clip(1.0 + 0.15 * jax.random.normal(streams_of[3], (D,), jnp.float32), 0.25, 1.75).astype(jnp.bfloat16),
        "w_qkv": noise(streams_of[4], (3, D, HEADS * HDIM), D ** -0.5, 0.1875, ((1, 2), (2, 4))),
        "w_attn_out": noise(streams_of[5], (HEADS * HDIM, D), (HEADS * HDIM // 64) ** -0.5, 1.5, ((0, 4), (1, 2))),
        "gain_mem": jnp.clip(1.0 + 0.15 * jax.random.normal(streams_of[6], (D,), jnp.float32), 0.25, 1.75).astype(jnp.bfloat16),
        "w_query": noise(streams_of[7], (D, MH * 2 * HALF), D ** -0.5, 0.1875, ((0, 2), (1, 4))),
        "w_gate": noise(streams_of[8], (D, VDIM), D ** -0.5, 0.1875, ((0, 2), (1, 4))),
        "w_proj": noise(streams_of[9], (VDIM, D), (VDIM // 8) ** -0.5, 0.5, ((0, 4), (1, 2))),
        "subkeys": noise(streams_of[10], (MH, 2, SUBKEYS, HALF), (2 * HALF) ** -0.5, 0.1875),
        "values": noise(streams_of[11], (VROWS, VDIM), 1.0, 6.0, ((0, 32),)),
        "cotangent": noise(streams_of[12], (TOKENS, D), 1.0, 6.0, ((0, 16), (1, 2))),
    }


EPSILON = 1e-06

@jax.custom_vjp
def low(v):
    return lax.optimization_barrier(v.astype(jnp.bfloat16)).astype(jnp.float32)

@jax.custom_vjp
def low_back(v):
    return v

def low_keep(v):
    return (low(v), None)

def low_pass(kept, grad):
    return (grad,)

def back_keep(v):
    return (v, None)

def back_low(kept, grad):
    return (low(grad),)
low.defvjp(low_keep, low_pass)
low_back.defvjp(back_keep, back_low)

def rms_scale(values_in, gain):
    return values_in * lax.rsqrt(lax.optimization_barrier(jnp.mean(values_in * values_in, axis=-1, keepdims=True)) + EPSILON) * gain

def attention_block(qkv, prefix_len):
    length = qkv.shape[1]
    queries = qkv[0].reshape(length, HEADS, HDIM)
    key_rows = qkv[1].reshape(length, HEADS, HDIM)
    value_rows = qkv[2].reshape(length, HEADS, HDIM)
    scores = jnp.einsum('qhd,khd->hqk', queries, key_rows, precision=lax.Precision.HIGHEST) * HDIM ** (-0.5)
    scores = low_back(scores)
    position = jnp.arange(length, dtype=jnp.int32)
    allowed = (position[None, :] <= position[:, None]) | (position[None, :] < prefix_len)
    scores = jnp.where(allowed[None], scores, -jnp.inf)
    probabilities = jax.nn.softmax(scores, axis=-1)
    mixed_rows = jnp.einsum('hqk,khd->qhd', low(probabilities), value_rows, precision=lax.Precision.HIGHEST)
    return mixed_rows.reshape(length, HEADS * HDIM)

@jax.checkpoint
def head_read(weights, picks_head, values):
    picked_rows = jnp.take(values, picks_head, axis=0)
    return jnp.einsum('sk,skf->sf', weights, picked_rows, precision=lax.Precision.HIGHEST)

def memory_read(weights, picks_seq, values):
    memory_sum = head_read(weights[:, 0], picks_seq[:, 0], values)
    for head_index in range(1, MH):
        memory_sum = memory_sum + head_read(weights[:, head_index], picks_seq[:, head_index], values)
    return memory_sum

def layer_forward(seq_inputs, prefix_len, picks_seq, gain_attn, w_qkv, w_attn_out, gain_mem, w_query, w_gate, w_proj, subkeys, values):
    normed = low(rms_scale(seq_inputs, gain_attn))
    qkv = low(low_back(jnp.einsum('sd,jdf->jsf', normed, w_qkv, precision=lax.Precision.HIGHEST)))
    attended = low(low_back(attention_block(qkv, prefix_len)))
    hidden = seq_inputs + low_back(jnp.dot(attended, w_attn_out, precision=lax.Precision.HIGHEST))
    normed_mem = low(rms_scale(hidden, gain_mem))
    query_rows = low(low_back(jnp.dot(normed_mem, w_query, precision=lax.Precision.HIGHEST)))
    gate_value = low_back(jnp.dot(normed_mem, w_gate, precision=lax.Precision.HIGHEST))
    query_rows = query_rows.reshape(-1, MH, 2, HALF)
    first_scores = low_back(jnp.einsum('shd,had->sha', query_rows[:, :, 0], subkeys[:, 0], precision=lax.Precision.HIGHEST))
    second_scores = low_back(jnp.einsum('shd,had->sha', query_rows[:, :, 1], subkeys[:, 1], precision=lax.Precision.HIGHEST))
    upper_index = picks_seq // SUBKEYS
    lower_index = picks_seq % SUBKEYS
    pick_scores = jnp.take_along_axis(first_scores, upper_index, axis=2) + jnp.take_along_axis(second_scores, lower_index, axis=2)
    weights = low(jax.nn.softmax(pick_scores, axis=-1))
    memory = low_back(memory_read(weights, picks_seq, values))
    gated_value = low(memory * jax.nn.silu(gate_value))
    return hidden + low_back(jnp.dot(gated_value, w_proj, precision=lax.Precision.HIGHEST))

def reference(inputs, prefix, picks, gain_attn, w_qkv, w_attn_out, gain_mem, w_query, w_gate, w_proj, subkeys, values, cotangent):
    floats = [array.astype(jnp.float32) for array in (inputs, gain_attn, w_qkv, w_attn_out, gain_mem, w_query, w_gate, w_proj, subkeys, values)]
    seq_picks = picks.reshape(N_DP, SEQ, MH, TOPK)
    layer_step = jax.checkpoint(layer_forward)

    def forward(seq_all, gain_attn, w_qkv, w_attn_out, gain_mem, w_query, w_gate, w_proj, subkeys, values):

        def visit_seq(scan_carry, seq_item):
            seq_inputs, prefix_len, picks_seq = seq_item
            result = layer_step(seq_inputs, prefix_len, picks_seq, gain_attn, w_qkv, w_attn_out, gain_mem, w_query, w_gate, w_proj, subkeys, values)
            return (scan_carry, result)
        _, outputs = lax.scan(visit_seq, 0, (seq_all.reshape(N_DP, SEQ, D), prefix, seq_picks))
        return outputs.reshape(N_DP * SEQ, D)
    output, pull_back = jax.vjp(forward, *floats)
    gradients = pull_back(cotangent.astype(jnp.float32))
    return (output.astype(jnp.bfloat16), gradients[0], gradients[1], gradients[2], gradients[3], gradients[4], gradients[5], gradients[6], gradients[7], gradients[8], gradients[9])
```

```python
import functools

import jax
import jax.numpy as jnp
from jax import lax
from jax.experimental import pallas as pl
from jax.sharding import PartitionSpec as P

D = 1024
HDIM = 64
HALF = 512
SUBKEYS = 256
TOPK = 32
FBLK = 128


EPSILON = 1e-06


def row_gather(operand):
    return lax.all_gather(operand, "row", axis=0, tiled=True)


def col_gather(operand):
    return lax.all_gather(operand, "col", axis=0, tiled=True)


def feature_total(operand):
    return lax.psum(operand, "col")


def col_reduce(gathered, product):
    return lax.psum_scatter(product(gathered), "col", scatter_dimension=0, tiled=True)


def row_reduce(gathered, product):
    return lax.psum_scatter(product(gathered), "row", scatter_dimension=0, tiled=True)


def norm_forward(residual, gain_slice):
    sum_squares = feature_total(jnp.sum(residual * residual, axis=1))
    inv_scale = lax.rsqrt(sum_squares / D + EPSILON)
    unit_rows = residual * inv_scale[:, None]
    return (unit_rows, inv_scale, (unit_rows * gain_slice).astype(jnp.bfloat16))


def norm_backward(grad_normed, unit_rows, inv_scale, gain_slice):
    grad_unit = grad_normed * gain_slice
    inner_mean = feature_total(jnp.sum(grad_unit * unit_rows, axis=1)) / D
    grad_input = inv_scale[:, None] * (grad_unit - unit_rows * inner_mean[:, None])
    return (grad_input, jnp.sum(grad_normed * unit_rows, axis=0))


def allowed_mask(query_count, key_count, first_pos, prefix_len):
    query_pos = first_pos + lax.iota(jnp.int32, query_count)
    key_pos = lax.iota(jnp.int32, key_count)
    return (key_pos[None, :] <= query_pos[:, None]) | (key_pos[None, :] < prefix_len)


def head_scores(query_head, key_head, allowed):
    raw_scores = jnp.einsum(
        "qd,kd->qk", query_head, key_head, preferred_element_type=jnp.float32
    ) * HDIM ** (-0.5)
    return jnp.where(allowed, raw_scores, -jnp.inf)


def attend_forward(own_qkv, kv_rows, allowed):
    head_count = own_qkv.shape[2] // HDIM
    outputs = []
    log_sums = []
    for head_index in range(head_count):
        columns = slice(head_index * HDIM, (head_index + 1) * HDIM)
        scores = head_scores(own_qkv[:, 0, columns], kv_rows[:, 0, columns], allowed)
        peak_score = jnp.max(scores, axis=1, keepdims=True)
        exp_scores = jnp.exp(scores - peak_score)
        row_sum = jnp.sum(exp_scores, axis=1, keepdims=True)
        probabilities = (exp_scores / row_sum).astype(jnp.bfloat16)
        outputs.append(
            jnp.dot(probabilities, kv_rows[:, 1, columns], preferred_element_type=jnp.float32)
        )
        log_sums.append(peak_score[:, 0] + jnp.log(row_sum[:, 0]))
    return (jnp.concatenate(outputs, axis=1), jnp.stack(log_sums))


def attend_backward(own_qkv, kv_rows, allowed, log_sums, grad_out):
    head_count = own_qkv.shape[2] // HDIM
    grad_queries = []
    grad_keys = []
    grad_values = []
    for head_index in range(head_count):
        columns = slice(head_index * HDIM, (head_index + 1) * HDIM)
        query_head = own_qkv[:, 0, columns]
        key_head = kv_rows[:, 0, columns]
        value_head = kv_rows[:, 1, columns]
        grad_head = grad_out[:, columns]
        scores = head_scores(query_head, key_head, allowed)
        probabilities = jnp.exp(scores - log_sums[head_index][:, None])
        grad_probs = jnp.einsum(
            "qd,kd->qk", grad_head, value_head, preferred_element_type=jnp.float32
        )
        inner_sum = jnp.sum(probabilities * grad_probs, axis=1, keepdims=True)
        grad_scores = (probabilities * (grad_probs - inner_sum)).astype(jnp.bfloat16)
        grad_queries.append(
            jnp.dot(grad_scores, key_head, preferred_element_type=jnp.float32) * HDIM ** (-0.5)
        )
        grad_keys.append(
            jnp.einsum("qk,qd->kd", grad_scores, query_head, preferred_element_type=jnp.float32)
            * HDIM ** (-0.5)
        )
        grad_values.append(
            jnp.einsum(
                "qk,qd->kd",
                probabilities.astype(jnp.bfloat16),
                grad_head,
                preferred_element_type=jnp.float32,
            )
        )
    stacked = jnp.stack(
        [jnp.concatenate(grad_keys, axis=1), jnp.concatenate(grad_values, axis=1)], axis=1
    )
    return (jnp.concatenate(grad_queries, axis=1), stacked)


def flat_picks(picks_head):
    blocks = picks_head.shape[0] // FBLK
    return jnp.swapaxes(picks_head.reshape(blocks, FBLK, TOPK), 1, 2).reshape(blocks, TOPK * FBLK)


def one_hot(row_values, size):
    hot = lax.broadcasted_iota(jnp.int32, (size, row_values.shape[1]), 0) == row_values
    return jnp.where(hot, 1.0, 0.0).astype(jnp.bfloat16)


def route_kernel(rows_dev, owners, cap, picks_ref, rank_ref, meta_ref):
    lane = lax.broadcasted_iota(jnp.int32, (FBLK, FBLK), 0)
    before = jnp.where(lane < lax.broadcasted_iota(jnp.int32, (FBLK, FBLK), 1), 1.0, 0.0).astype(
        jnp.bfloat16
    )
    picks = picks_ref[0]
    owner = picks // rows_dev
    local = picks % rows_dev
    hot = one_hot(owner, owners)
    running = jnp.zeros((owners, 1), jnp.float32)
    ranks = []
    for chunk in range(picks.shape[1] // FBLK):
        part = hot[:, chunk * FBLK : (chunk + 1) * FBLK]
        earlier = jnp.dot(part, before, preferred_element_type=jnp.float32)
        wide = part.astype(jnp.float32)
        ranks.append(jnp.sum(wide * (earlier + running), axis=0, keepdims=True))
        running = running + jnp.sum(wide, axis=1, keepdims=True)
    rank = jnp.concatenate(ranks, axis=1).astype(jnp.int32)
    rank_ref[0] = rank
    slot_hot = one_hot(rank, cap)
    token = lax.broadcasted_iota(jnp.int32, picks.shape, 1) % FBLK
    outs = []
    for payload in (local % SUBKEYS, local // SUBKEYS, token):
        scaled = hot * payload.astype(jnp.float32).astype(jnp.bfloat16)
        outs.append(
            lax.dot_general(
                scaled, slot_hot, (((1,), (1,)), ((), ())), preferred_element_type=jnp.float32
            ).astype(jnp.int32)
        )
    meta_ref[0] = (outs[1] * FBLK + outs[2]) * SUBKEYS + outs[0]


def route(flat, rows_dev, owners, cap):
    blocks, count = flat.shape
    rank, meta = pl.pallas_call(
        functools.partial(route_kernel, rows_dev, owners, cap),
        grid=(blocks,),
        in_specs=[pl.BlockSpec((1, 1, count), lambda i: (i, 0, 0))],
        out_specs=[
            pl.BlockSpec((1, 1, count), lambda i: (i, 0, 0)),
            pl.BlockSpec((1, owners, cap), lambda i: (i, 0, 0)),
        ],
        out_shape=[
            jax.ShapeDtypeStruct((blocks, 1, count), jnp.int32),
            jax.ShapeDtypeStruct((blocks, owners, cap), jnp.int32),
        ],
        name="route",
    )(flat[:, None, :])
    return rank, meta


def weigh_kernel(rows_dev, owners, cap, query_ref, keys_ref, picks_ref, rank_ref, weights_ref, slots_ref):
    picks = picks_ref[0]
    first = lax.dot_general(
        keys_ref[0], query_ref[:, :HALF], (((1,), (1,)), ((), ())), preferred_element_type=jnp.float32
    )
    second = lax.dot_general(
        keys_ref[1], query_ref[:, HALF:], (((1,), (1,)), ((), ())), preferred_element_type=jnp.float32
    )
    upper = picks // SUBKEYS
    lower = picks % SUBKEYS
    key_id = lax.broadcasted_iota(jnp.int32, (SUBKEYS, FBLK), 0)
    rows = []
    for pick in range(TOPK):
        columns = slice(pick * FBLK, (pick + 1) * FBLK)
        chosen = jnp.where(key_id == upper[:, columns], first, 0.0) + jnp.where(
            key_id == lower[:, columns], second, 0.0
        )
        rows.append(jnp.sum(chosen, axis=0, keepdims=True))
    scores = jnp.concatenate(rows, axis=0)
    powers = jnp.exp(scores - jnp.max(scores, axis=0, keepdims=True))
    weights = powers / jnp.sum(powers, axis=0, keepdims=True)
    weights_ref[0] = weights
    flat = jnp.concatenate([weights[pick : pick + 1] for pick in range(TOPK)], axis=1)
    scaled = one_hot(picks // rows_dev, owners) * flat.astype(jnp.bfloat16)
    slots_ref[0] = lax.dot_general(
        scaled,
        one_hot(rank_ref[0], cap),
        (((1,), (1,)), ((), ())),
        preferred_element_type=jnp.float32,
    ).astype(jnp.bfloat16)


def weigh(query_rows, keys_head, flat, rank, rows_dev, owners, cap):
    blocks, count = flat.shape
    return pl.pallas_call(
        functools.partial(weigh_kernel, rows_dev, owners, cap),
        grid=(blocks,),
        in_specs=[
            pl.BlockSpec((FBLK, 2 * HALF), lambda i: (i, 0)),
            pl.BlockSpec((2, SUBKEYS, HALF), lambda i: (0, 0, 0)),
            pl.BlockSpec((1, 1, count), lambda i: (i, 0, 0)),
            pl.BlockSpec((1, 1, count), lambda i: (i, 0, 0)),
        ],
        out_specs=[
            pl.BlockSpec((1, TOPK, FBLK), lambda i: (i, 0, 0)),
            pl.BlockSpec((1, owners, cap), lambda i: (i, 0, 0)),
        ],
        out_shape=[
            jax.ShapeDtypeStruct((blocks, TOPK, FBLK), jnp.float32),
            jax.ShapeDtypeStruct((blocks, owners, cap), jnp.bfloat16),
        ],
        name="weigh",
    )(query_rows, keys_head, flat[:, None, :], rank)


def spread_kernel(areas, key_ref, low_ref, weight_ref, out_ref):
    key = key_ref[0]
    at_key = lax.broadcasted_iota(jnp.int32, (areas * FBLK, key.shape[1]), 0) == key
    left = jnp.where(at_key, weight_ref[0].astype(jnp.float32), 0.0).astype(jnp.bfloat16)
    stacked = lax.dot_general(
        left,
        one_hot(low_ref[0], SUBKEYS),
        (((1,), (1,)), ((), ())),
        preferred_element_type=jnp.float32,
    ).astype(jnp.bfloat16)
    for area in range(areas):
        out_ref[:, area * SUBKEYS : (area + 1) * SUBKEYS] = stacked[area * FBLK : (area + 1) * FBLK]


def spread(key, low, weight, rows_dev):
    blocks, slots = key.shape
    areas = rows_dev // SUBKEYS
    row = pl.BlockSpec((1, 1, slots), lambda i: (i, 0, 0))
    return pl.pallas_call(
        functools.partial(spread_kernel, areas),
        grid=(blocks,),
        in_specs=[row, row, row],
        out_specs=pl.BlockSpec((FBLK, rows_dev), lambda i: (i, 0)),
        out_shape=jax.ShapeDtypeStruct((blocks * FBLK, rows_dev), jnp.bfloat16),
        name="spread",
    )(key[:, None], low[:, None], weight[:, None])


def collect_kernel(areas, grid_ref, key_ref, low_ref, out_ref):
    key = key_ref[0]
    low_hot = one_hot(low_ref[0], SUBKEYS)
    total = jnp.zeros(key.shape, jnp.float32)
    for area in range(areas):
        product = jnp.dot(
            grid_ref[:, area * SUBKEYS : (area + 1) * SUBKEYS],
            low_hot,
            preferred_element_type=jnp.float32,
        )
        spot = lax.broadcasted_iota(jnp.int32, product.shape, 0) + area * FBLK
        total = total + jnp.sum(jnp.where(spot == key, product, 0.0), axis=0, keepdims=True)
    out_ref[0] = total


def collect(grid_products, key, low, rows_dev):
    blocks, slots = key.shape
    row = pl.BlockSpec((1, 1, slots), lambda i: (i, 0, 0))
    return pl.pallas_call(
        functools.partial(collect_kernel, rows_dev // SUBKEYS),
        grid=(blocks,),
        in_specs=[pl.BlockSpec((FBLK, rows_dev), lambda i: (i, 0)), row, row],
        out_specs=row,
        out_shape=jax.ShapeDtypeStruct((blocks, 1, slots), jnp.float32),
        name="collect",
    )(grid_products, key[:, None], low[:, None])[:, 0]


def unweigh_kernel(rows_dev, owners, back_ref, picks_ref, rank_ref, weights_ref, first_ref, second_ref):
    picks = picks_ref[0]
    hot = one_hot(picks // rows_dev, owners)
    back = back_ref[0]
    high = back.astype(jnp.bfloat16)
    rest = back - high.astype(jnp.float32)
    middle = rest.astype(jnp.bfloat16)
    lowest = (rest - middle.astype(jnp.float32)).astype(jnp.bfloat16)
    spread_back = (
        jnp.dot(high, hot, preferred_element_type=jnp.float32)
        + jnp.dot(middle, hot, preferred_element_type=jnp.float32)
        + jnp.dot(lowest, hot, preferred_element_type=jnp.float32)
    )
    slot = lax.broadcasted_iota(jnp.int32, spread_back.shape, 0)
    flat = jnp.sum(jnp.where(slot == rank_ref[0], spread_back, 0.0), axis=0, keepdims=True)
    grads = jnp.concatenate(
        [flat[:, pick * FBLK : (pick + 1) * FBLK] for pick in range(TOPK)], axis=0
    )
    weights = weights_ref[0]
    grads = weights * (grads - jnp.sum(weights * grads, axis=0, keepdims=True))
    upper = picks // SUBKEYS
    lower = picks % SUBKEYS
    key_id = lax.broadcasted_iota(jnp.int32, (SUBKEYS, FBLK), 0)
    first = jnp.zeros((SUBKEYS, FBLK), jnp.float32)
    second = jnp.zeros((SUBKEYS, FBLK), jnp.float32)
    for pick in range(TOPK):
        columns = slice(pick * FBLK, (pick + 1) * FBLK)
        value = grads[pick : pick + 1]
        first = first + jnp.where(key_id == upper[:, columns], value, 0.0)
        second = second + jnp.where(key_id == lower[:, columns], value, 0.0)
    first_ref[...] = first.astype(jnp.bfloat16)
    second_ref[...] = second.astype(jnp.bfloat16)


def unweigh(back, flat, rank, weights, rows_dev, owners):
    blocks, count = flat.shape
    cap = back.shape[1]
    return pl.pallas_call(
        functools.partial(unweigh_kernel, rows_dev, owners),
        grid=(blocks,),
        in_specs=[
            pl.BlockSpec((1, cap, owners), lambda i: (i, 0, 0)),
            pl.BlockSpec((1, 1, count), lambda i: (i, 0, 0)),
            pl.BlockSpec((1, 1, count), lambda i: (i, 0, 0)),
            pl.BlockSpec((1, TOPK, FBLK), lambda i: (i, 0, 0)),
        ],
        out_specs=[
            pl.BlockSpec((SUBKEYS, FBLK), lambda i: (0, i)),
            pl.BlockSpec((SUBKEYS, FBLK), lambda i: (0, i)),
        ],
        out_shape=[jax.ShapeDtypeStruct((SUBKEYS, blocks * FBLK), jnp.bfloat16)] * 2,
        name="unweigh",
    )(back, flat[:, None, :], rank, weights)


EVERYONE = ("dp", "row", "col")


def exchange(operand):
    return lax.all_to_all(operand, EVERYONE, split_axis=0, concat_axis=0, tiled=True)


def by_block(arrived, dp_count, row_count, col_count):
    _, blocks, cap = arrived.shape
    wide = arrived.reshape(dp_count, row_count, col_count, blocks, cap)
    return jnp.transpose(wide, (0, 2, 3, 1, 4)).reshape(
        dp_count * col_count * blocks, row_count * cap
    )


def by_source(blocked, dp_count, row_count, col_count, blocks, cap):
    wide = blocked.reshape(dp_count, col_count, blocks, row_count, cap)
    return jnp.transpose(wide, (0, 3, 1, 2, 4)).reshape(
        dp_count * row_count * col_count, blocks, cap
    )


def memory_all(query_rows, grad_memory, picks, subkeys, values):
    dp_count = lax.axis_size("dp")
    row_count = lax.axis_size("row")
    col_count = lax.axis_size("col")
    owners = dp_count * row_count * col_count
    rows_dev = values.shape[0]
    cap = FBLK * TOPK // owners
    own_tokens = query_rows.shape[0]
    blocks = own_tokens // FBLK
    head_id = lax.axis_index("row")
    keys_head = lax.dynamic_index_in_dim(subkeys, head_id, 0, keepdims=False)
    picks_head = lax.dynamic_index_in_dim(picks, head_id, 1, keepdims=False)
    flat = flat_picks(picks_head)
    rank, meta = route(flat, rows_dev, owners, cap)
    sizes = (dp_count, row_count, col_count)
    meta_in = by_block(exchange(jnp.swapaxes(meta, 0, 1)), *sizes)
    key = meta_in // SUBKEYS
    low = meta_in % SUBKEYS
    weights, slots = weigh(query_rows, keys_head, flat, rank, rows_dev, owners, cap)
    weight_in = by_block(exchange(jnp.swapaxes(slots, 0, 1)), *sizes)
    table = spread(key, low, weight_in, rows_dev)
    partial = jnp.dot(table, values, preferred_element_type=jnp.float32).astype(jnp.bfloat16)
    grid = partial.reshape(dp_count, col_count, own_tokens, row_count, -1)
    grid = jnp.transpose(grid, (0, 3, 1, 2, 4)).reshape(owners, own_tokens, -1)
    memory = lax.psum_scatter(grid, EVERYONE, scatter_dimension=0, tiled=True)[0]
    memory = memory.astype(jnp.float32)
    wide = lax.all_gather(grad_memory, "row", axis=1, tiled=True)
    grad_all = lax.all_gather(wide, ("dp", "col"), axis=0, tiled=True)
    grad_values = lax.dot_general(
        table, grad_all, (((0,), (0,)), ((), ())), preferred_element_type=jnp.float32
    )
    products = lax.dot_general(
        grad_all, values, (((1,), (1,)), ((), ())), preferred_element_type=jnp.float32
    ).astype(jnp.bfloat16)
    found = collect(products, key, low, rows_dev)
    back = exchange(by_source(found, *sizes, blocks, cap))
    first_t, second_t = unweigh(
        jnp.transpose(back, (1, 2, 0)), flat, rank, weights, rows_dev, owners
    )
    grad_query = jnp.concatenate(
        [
            lax.dot_general(
                part, keys_head[i], (((0,), (0,)), ((), ())), preferred_element_type=jnp.float32
            )
            for i, part in enumerate((first_t, second_t))
        ],
        axis=1,
    ).astype(jnp.bfloat16)
    grad_keys = jnp.stack(
        [
            jnp.dot(first_t, query_rows[:, :HALF], preferred_element_type=jnp.float32),
            jnp.dot(second_t, query_rows[:, HALF:], preferred_element_type=jnp.float32),
        ]
    )
    return memory, grad_query, grad_values, grad_keys


def per_device(
    inputs,
    prefix,
    picks,
    gain_attn,
    w_qkv,
    w_attn_out,
    gain_mem,
    w_query,
    w_gate,
    w_proj,
    subkeys,
    values,
    cotangent,
):
    width_part = inputs.shape[1]
    own_tokens = picks.shape[0]
    seq_tokens = own_tokens * lax.axis_size("col")
    query_width = w_query.shape[1]
    col_first = lax.axis_index("col") * width_part
    gain_one = lax.dynamic_slice_in_dim(gain_attn, col_first, width_part).astype(jnp.float32)
    gain_two = lax.dynamic_slice_in_dim(gain_mem, col_first, width_part).astype(jnp.float32)

    def project_qkv(piece_rows):
        return jnp.einsum("tc,jcf->tjf", piece_rows, w_qkv, preferred_element_type=jnp.float32)

    def proj_attn(piece_rows):
        return jnp.dot(piece_rows, w_attn_out, preferred_element_type=jnp.float32)

    def project_memory(piece_rows):
        return jnp.concatenate(
            [
                jnp.dot(piece_rows, w_query, preferred_element_type=jnp.float32),
                jnp.dot(piece_rows, w_gate, preferred_element_type=jnp.float32),
            ],
            axis=1,
        )

    def proj_mem(piece_rows):
        return jnp.dot(piece_rows, w_proj, preferred_element_type=jnp.float32)

    def back_proj(piece_rows):
        return jnp.einsum("tc,fc->tf", piece_rows, w_proj, preferred_element_type=jnp.float32)

    def back_memory_in(piece_rows):
        return jnp.einsum(
            "tq,cq->tc", piece_rows[:, :query_width], w_query, preferred_element_type=jnp.float32
        ) + jnp.einsum(
            "tf,cf->tc", piece_rows[:, query_width:], w_gate, preferred_element_type=jnp.float32
        )

    def back_attn(piece_rows):
        return jnp.einsum("tc,fc->tf", piece_rows, w_attn_out, preferred_element_type=jnp.float32)

    def back_qkv(piece_rows):
        return jnp.einsum("tjf,jcf->tc", piece_rows, w_qkv, preferred_element_type=jnp.float32)

    residual = inputs.astype(jnp.float32)
    unit_one, scale_one, normed_one = norm_forward(residual, gain_one)
    gathered_one = row_gather(normed_one)
    own_qkv = col_reduce(gathered_one, project_qkv).astype(jnp.bfloat16)
    kv_rows = col_gather(own_qkv[:, 1:])
    allowed = allowed_mask(own_tokens, seq_tokens, lax.axis_index("col") * own_tokens, prefix[0])
    attended_sum, log_sums = attend_forward(own_qkv, kv_rows, allowed)
    attended = attended_sum.astype(jnp.bfloat16)
    attended_all = col_gather(attended)
    hidden = residual + row_reduce(attended_all, proj_attn)
    unit_two, scale_two, normed_two = norm_forward(hidden, gain_two)
    gathered_two = row_gather(normed_two)
    mixed_sum = col_reduce(gathered_two, project_memory)
    query_rows = mixed_sum[:, :query_width].astype(jnp.bfloat16)
    gate_value = mixed_sum[:, query_width:]
    sigmoid_gate = jax.nn.sigmoid(gate_value)
    silu_gate = gate_value * sigmoid_gate
    grad_rows = row_gather(cotangent)
    grad_gated = col_reduce(grad_rows, back_proj)
    grad_memory = (grad_gated * silu_gate).astype(jnp.bfloat16)
    memory, grad_query, grad_values, grad_keys = memory_all(
        query_rows, grad_memory, picks, subkeys, values
    )
    gated_value = (memory * silu_gate).astype(jnp.bfloat16)
    gated_all = col_gather(gated_value)
    output = (hidden + row_reduce(gated_all, proj_mem)).astype(jnp.bfloat16)
    grad_w_proj = jnp.einsum("tf,tc->fc", gated_all, grad_rows, preferred_element_type=jnp.float32)
    grad_gate = (
        grad_gated * memory * sigmoid_gate * (1.0 + gate_value * (1.0 - sigmoid_gate))
    ).astype(jnp.bfloat16)
    grad_keys = lax.psum_scatter(grad_keys.reshape(-1, HALF), ("dp", "col"), scatter_dimension=0, tiled=True)
    grad_subkeys = lax.all_gather(
        grad_keys.astype(jnp.bfloat16), ("row", "dp", "col"), axis=0, tiled=True
    ).astype(jnp.float32).reshape(subkeys.shape)
    grad_mixed = col_gather(jnp.concatenate([grad_query, grad_gate], axis=1))
    grad_w_query = jnp.einsum(
        "tc,tq->cq", gathered_two, grad_mixed[:, :query_width], preferred_element_type=jnp.float32
    )
    grad_w_gate = jnp.einsum(
        "tc,tf->cf", gathered_two, grad_mixed[:, query_width:], preferred_element_type=jnp.float32
    )
    grad_normed_two = row_reduce(grad_mixed, back_memory_in)
    grad_from_two, grad_gain_two = norm_backward(grad_normed_two, unit_two, scale_two, gain_two)
    grad_hidden = cotangent.astype(jnp.float32) + grad_from_two
    grad_hidden_all = row_gather(grad_hidden.astype(jnp.bfloat16))
    grad_w_attn_out = jnp.einsum(
        "tf,tc->fc", attended_all, grad_hidden_all, preferred_element_type=jnp.float32
    )
    grad_attended = col_reduce(grad_hidden_all, back_attn).astype(jnp.bfloat16)
    grad_query_own, grad_kv_all = attend_backward(
        own_qkv, kv_rows, allowed, log_sums, grad_attended
    )
    grad_kv_own = lax.psum_scatter(grad_kv_all, "col", scatter_dimension=0, tiled=True)
    grad_qkv = jnp.concatenate([grad_query_own[:, None], grad_kv_own], axis=1).astype(jnp.bfloat16)
    grad_qkv_all = col_gather(grad_qkv)
    grad_w_qkv = jnp.einsum(
        "tc,tjf->jcf", gathered_one, grad_qkv_all, preferred_element_type=jnp.float32
    )
    grad_normed_one = row_reduce(grad_qkv_all, back_qkv)
    grad_from_one, grad_gain_one = norm_backward(grad_normed_one, unit_one, scale_one, gain_one)
    grad_inputs = grad_hidden + grad_from_one
    weight_sums = (
        lax.psum(grad_w_qkv.astype(jnp.bfloat16), "dp").astype(jnp.float32),
        lax.psum(grad_w_attn_out.astype(jnp.bfloat16), "dp").astype(jnp.float32),
        lax.psum(grad_w_query.astype(jnp.bfloat16), "dp").astype(jnp.float32),
        lax.psum(grad_w_gate.astype(jnp.bfloat16), "dp").astype(jnp.float32),
        lax.psum(grad_w_proj.astype(jnp.bfloat16), "dp").astype(jnp.float32),
    )
    gain_full_one = lax.dynamic_update_slice_in_dim(
        jnp.zeros(gain_attn.shape, jnp.float32), grad_gain_one, col_first, 0
    )
    gain_full_two = lax.dynamic_update_slice_in_dim(
        jnp.zeros(gain_mem.shape, jnp.float32), grad_gain_two, col_first, 0
    )
    small_sums = lax.psum((gain_full_one, gain_full_two), ("dp", "row", "col"))
    return (
        output,
        grad_inputs,
        small_sums[0],
        weight_sums[0],
        weight_sums[1],
        small_sums[1],
        weight_sums[2],
        weight_sums[3],
        weight_sums[4],
        grad_subkeys,
        grad_values,
    )


def solution(mesh):
    placed = (
        P(("dp", "row"), "col"),
        P("dp"),
        P(("dp", "col"), None, None),
        P(),
        P(None, "col", "row"),
        P("row", "col"),
        P(),
        P("col", "row"),
        P("col", "row"),
        P("row", "col"),
        P(),
        P(("dp", "row", "col"), None),
        P(("dp", "row"), "col"),
    )
    return jax.shard_map(
        per_device,
        mesh=mesh,
        in_specs=placed,
        out_specs=(
            P(("dp", "row"), "col"),
            P(("dp", "row"), "col"),
            P(),
            P(None, "col", "row"),
            P("row", "col"),
            P(),
            P("col", "row"),
            P("col", "row"),
            P("row", "col"),
            P(),
            P(("dp", "row", "col"), None),
        ),
        check_vma=False,
    )
```

```python
import functools

import jax
import jax.numpy as jnp
from jax import lax
from jax.experimental import pallas as pl
from jax.experimental.pallas import tpu as pltpu
from jax.sharding import PartitionSpec as P

D = 1024
HDIM = 64
HALF = 512
SUBKEYS = 256
TOPK = 32
FBLK = 128


EPSILON = 1e-06


MESH = pl.DeviceIdType.MESH
VMEM = pl.BlockSpec(memory_space=pltpu.VMEM)
ANY = pl.BlockSpec(memory_space=pl.ANY)
DMA = pltpu.SemaphoreType.DMA


def here():
    return lax.axis_index("dp"), lax.axis_index("row"), lax.axis_index("col")


def grid_sizes():
    return lax.axis_size("dp"), lax.axis_size("row"), lax.axis_size("col")


def remote(src, dst, send_sem, recv_sem, device):
    return pltpu.make_async_remote_copy(
        src_ref=src,
        dst_ref=dst,
        send_sem=send_sem,
        recv_sem=recv_sem,
        device_id=device,
        device_id_type=MESH,
    )


def arrived(dst, sem):
    pltpu.make_async_copy(dst, dst, sem).wait()


def greet_plane(spot, sizes):
    barrier = pltpu.get_barrier_semaphore()
    dp, row, col = spot
    _, rows, cols = sizes
    for j in range(rows):
        for k in range(cols):
            if j + k > 0:
                pl.semaphore_signal(
                    barrier,
                    inc=1,
                    device_id=(dp, lax.rem(row + j, rows), lax.rem(col + k, cols)),
                    device_id_type=MESH,
                )
    pl.semaphore_wait(barrier, rows * cols - 1)


def greet_partner(spot, sizes):
    barrier = pltpu.get_barrier_semaphore()
    dp, row, col = spot
    pl.semaphore_signal(barrier, inc=1, device_id=(dp, row, 1 - col), device_id_type=MESH)
    pl.semaphore_wait(barrier, 1)


def device_of(index, sizes):
    _, rows, cols = sizes
    return (
        lax.div(index, rows * cols),
        lax.rem(lax.div(index, cols), rows),
        lax.rem(index, cols),
    )


def index_of(spot, sizes):
    return (spot[0] * sizes[1] + spot[1]) * sizes[2] + spot[2]


def greet_all(spot, sizes):
    barrier = pltpu.get_barrier_semaphore()
    count = sizes[0] * sizes[1] * sizes[2]
    me = index_of(spot, sizes)

    def greet(step, carry):
        pl.semaphore_signal(
            barrier,
            inc=1,
            device_id=device_of(lax.rem(me + step, count), sizes),
            device_id_type=MESH,
        )
        return carry

    lax.fori_loop(1, count, greet, 0)
    pl.semaphore_wait(barrier, count - 1)


class Gather:
    def __init__(self, spot, sizes, src, dst, send, recv):
        self.spot, self.sizes, self.src, self.dst = spot, sizes, src, dst
        self.send, self.recv = send, recv
        self.tokens, self.width = src.shape
        dp, row, col = spot
        _, rows, cols = sizes
        self.half = rows // cols
        self.target = lax.div(row, self.half)
        self.slot = lax.rem(row, self.half) * cols + col
        first = pl.multiple_of(lax.rem(row, self.half) * self.tokens, self.tokens)
        left = pl.multiple_of(col * self.width, self.width)
        self.there = dst.at[pl.ds(first, self.tokens), pl.ds(left, self.width)]

    def copy(self, step):
        dp, row, _ = self.spot
        device = (dp, lax.rem(row + step, self.sizes[1]), self.target)
        return remote(self.src, self.there, self.send.at[step], self.recv.at[self.slot], device)

    def start(self):
        col = self.spot[2]

        for step in range(1, self.sizes[1]):
            self.copy(step).start()

        @pl.when(self.target == col)
        def _():
            pltpu.make_async_copy(self.src, self.there, self.recv.at[self.slot]).start()

        @pl.when(self.target != col)
        def _():
            self.copy(0).start()

    def wait(self):
        cols = self.sizes[2]
        for i in range(self.half):
            for k in range(cols):
                arrived(
                    self.dst.at[pl.ds(i * self.tokens, self.tokens), pl.ds(k * self.width, self.width)],
                    self.recv.at[i * cols + k],
                )
        for step in range(1, self.sizes[1]):
            self.copy(step).wait_send()

        @pl.when(self.target != self.spot[2])
        def _():
            self.copy(0).wait_send()


class Scatter:
    def __init__(self, spot, sizes, src, landing, send, recv):
        self.spot, self.sizes, self.src, self.landing = spot, sizes, src, landing
        self.send, self.recv = send, recv
        _, self.tokens, self.width = landing.shape
        self.half = sizes[1] // sizes[2]

    def parts(self):
        dp, row, col = self.spot
        cols = self.sizes[2]
        for i in range(self.half):
            for k in range(cols):
                piece = self.src.at[
                    pl.ds(i * self.tokens, self.tokens), pl.ds(k * self.width, self.width)
                ]
                target = col * self.half + i
                mine = jnp.logical_and(target == row, col == k)
                there = self.landing.at[row]
                copy = remote(
                    piece, there, self.send.at[i * cols + k], self.recv.at[row], (dp, target, k)
                )
                yield mine, copy, pltpu.make_async_copy(piece, there, self.recv.at[row])

    def start(self):
        for mine, copy, own in self.parts():
            pl.when(jnp.logical_not(mine))(copy.start)
            pl.when(mine)(own.start)

    def wait(self):
        for q in range(self.sizes[1]):
            arrived(self.landing.at[q], self.recv.at[q])

    def wait_send(self):
        for mine, copy, _ in self.parts():
            pl.when(jnp.logical_not(mine))(copy.wait_send)


def plane_sems(sizes):
    rows, cols = sizes[1], sizes[2]
    return [DMA((rows,)), DMA((rows,))]


def start_kernel(sizes, *refs):
    x, dy, wqkv, wquery, wgate, wproj, wattn = refs[:7]
    xs, dys, wqkv_all, wquery_all, wgate_all, wproj_all, wattn_all = refs[7:14]
    xsend, xrecv, ysend, yrecv, wsend, wrecv, wlocal = refs[14:]
    spot = here()
    dp, row, col = spot
    greet_plane(spot, sizes)
    gather_x = Gather(spot, sizes, x, xs, xsend, xrecv)
    gather_y = Gather(spot, sizes, dy, dys, ysend, yrecv)
    gather_x.start()
    gather_y.start()
    copies = []
    for n, (src, dst, dim) in enumerate(
        (
            (wqkv, wqkv_all, 1),
            (wquery, wquery_all, 0),
            (wgate, wgate_all, 0),
            (wproj, wproj_all, 1),
            (wattn, wattn_all, 1),
        )
    ):
        size = src.shape[dim]
        window = [slice(None)] * len(src.shape)
        window[dim] = pl.ds(pl.multiple_of(col * size, size), size)
        there = dst.at[tuple(window)]
        away = remote(src, there, wsend.at[n], wrecv.at[n], (dp, row, 1 - col))
        own = pltpu.make_async_copy(src, there, wlocal.at[n])
        away.start()
        own.start()
        copies += [away, own]
    for copy in copies:
        copy.wait()
    gather_x.wait()
    gather_y.wait()


def start_all(sizes, x, dy, wqkv, wquery, wgate, wproj, wattn):
    tokens, width = x.shape
    half = sizes[1] // sizes[2]
    cols = sizes[2]
    low = jnp.bfloat16

    def twice(operand, dim):
        shape = list(operand.shape)
        shape[dim] *= cols
        return jax.ShapeDtypeStruct(tuple(shape), low)

    whole = jax.ShapeDtypeStruct((half * tokens, cols * width), low)
    return pl.pallas_call(
        functools.partial(start_kernel, sizes),
        in_specs=[VMEM] * 7,
        out_specs=[ANY] * 7,
        out_shape=[
            whole,
            whole,
            twice(wqkv, 1),
            twice(wquery, 0),
            twice(wgate, 0),
            twice(wproj, 1),
            twice(wattn, 1),
        ],
        scratch_shapes=plane_sems(sizes) * 2 + [DMA((5,))] * 3,
        compiler_params=pltpu.CompilerParams(collective_id=0, has_side_effects=True),
        name="start_all",
    )(x, dy, wqkv, wquery, wgate, wproj, wattn)


def swap_kernel(sizes, src, dst, send, recv, own):
    spot = here()
    dp, row, col = spot
    greet_partner(spot, sizes)
    size = src.shape[1]
    there = dst.at[:, pl.ds(pl.multiple_of(col * size, size), size)]
    away = remote(src, there, send, recv, (dp, row, 1 - col))
    local = pltpu.make_async_copy(src, there, own)
    away.start()
    local.start()
    away.wait()
    local.wait()


def swap_tokens(sizes, src):
    shape = (src.shape[0], src.shape[1] * sizes[2], src.shape[2])
    return pl.pallas_call(
        functools.partial(swap_kernel, sizes),
        in_specs=[VMEM],
        out_specs=VMEM,
        out_shape=jax.ShapeDtypeStruct(shape, src.dtype),
        scratch_shapes=[DMA, DMA, DMA],
        compiler_params=pltpu.CompilerParams(collective_id=1, has_side_effects=True),
        name="swap_tokens",
    )(src)


def pair_sum_kernel(sizes, src, out, landing, send, recv):
    spot = here()
    dp, row, col = spot
    greet_partner(spot, sizes)
    size = landing.shape[1]
    other = pl.multiple_of((1 - col) * size, size)
    away = remote(src.at[:, pl.ds(other, size)], landing, send, recv, (dp, row, 1 - col))
    away.start()
    away.wait()
    own = src[:, pl.ds(pl.multiple_of(col * size, size), size)]
    out[...] = (own + landing[...]).astype(out.dtype)


def pair_sum(sizes, src):
    shape = (src.shape[0], src.shape[1] // sizes[2], src.shape[2])
    return pl.pallas_call(
        functools.partial(pair_sum_kernel, sizes),
        in_specs=[VMEM],
        out_specs=VMEM,
        out_shape=jax.ShapeDtypeStruct(shape, jnp.bfloat16),
        scratch_shapes=[pltpu.VMEM(shape, src.dtype), DMA, DMA],
        compiler_params=pltpu.CompilerParams(collective_id=2, has_side_effects=True),
        name="pair_sum",
    )(src)


def fold(column):
    return jnp.broadcast_to(column, (column.shape[0], 128))


def join_kernel(
    sizes, part, x, gain, hidden, normed_all, landing, mine, theirs, block,
    ssend, srecv, gsend, grecv, psend, precv,
):
    spot = here()
    dp, row, col = spot
    greet_plane(spot, sizes)
    scatter = Scatter(spot, sizes, part, landing, ssend, srecv)
    scatter.start()
    scatter.wait()
    total = x[...].astype(jnp.float32)
    for q in range(sizes[1]):
        total = total + landing[q].astype(jnp.float32)
    hidden[...] = total
    mine[...] = fold(jnp.sum(total * total, axis=1, keepdims=True))
    pair = remote(mine, theirs, psend, precv, (dp, row, 1 - col))
    pair.start()
    pair.wait()
    squares = mine[:, :1] + theirs[:, :1]
    scale = lax.rsqrt(squares / D + EPSILON)
    block[...] = (hidden[...] * scale * gain[...].astype(jnp.float32)).astype(jnp.bfloat16)
    gather = Gather(spot, sizes, block, normed_all, gsend, grecv)
    gather.start()
    scatter.wait_send()
    gather.wait()


def join(sizes, part, x, gain):
    tokens, width = x.shape
    rows = sizes[1]
    return pl.pallas_call(
        functools.partial(join_kernel, sizes),
        in_specs=[VMEM] * 3,
        out_specs=[VMEM, VMEM],
        out_shape=[
            jax.ShapeDtypeStruct((tokens, width), jnp.float32),
            jax.ShapeDtypeStruct(part.shape, jnp.bfloat16),
        ],
        scratch_shapes=[
            pltpu.VMEM((rows, tokens, width), jnp.bfloat16),
            pltpu.VMEM((tokens, 128), jnp.float32),
            pltpu.VMEM((tokens, 128), jnp.float32),
            pltpu.VMEM((tokens, width), jnp.bfloat16),
        ]
        + plane_sems(sizes) * 2
        + [DMA, DMA],
        compiler_params=pltpu.CompilerParams(collective_id=3, has_side_effects=True),
        name="join",
    )(part, x, gain[None])


def norm_back(sizes, spot, landing, base, above, gain, mine, theirs, psend, precv):
    dp, row, col = spot
    normed_grad = landing[0].astype(jnp.float32)
    for q in range(1, sizes[1]):
        normed_grad = normed_grad + landing[q].astype(jnp.float32)
    values = base[...].astype(jnp.float32)
    unit_grad = normed_grad * gain[...].astype(jnp.float32)
    mine[0] = fold(jnp.sum(values * values, axis=1, keepdims=True))
    mine[1] = fold(jnp.sum(unit_grad * values, axis=1, keepdims=True))
    pair = remote(mine, theirs, psend, precv, (dp, row, 1 - col))
    pair.start()
    pair.wait()
    scale = lax.rsqrt((mine[0, :, :1] + theirs[0, :, :1]) / D + EPSILON)
    inner = scale * (mine[1, :, :1] + theirs[1, :, :1]) / D
    unit = values * scale
    grad = above[...].astype(jnp.float32) + scale * (unit_grad - unit * inner)
    return grad, jnp.sum(normed_grad * unit, axis=0, keepdims=True)


def middle_kernel(
    sizes, part, out_part, hidden, dy, gain, output, grad, grad_all, gain_grad,
    landing, out_landing, mine, theirs, block, ssend, srecv, osend, orecv, gsend, grecv, psend, precv,
):
    spot = here()
    greet_plane(spot, sizes)
    scatter = Scatter(spot, sizes, part, landing, ssend, srecv)
    scatter.start()
    out_scatter = Scatter(spot, sizes, out_part, out_landing, osend, orecv)
    out_scatter.start()
    scatter.wait()
    total, gains = norm_back(sizes, spot, landing, hidden, dy, gain, mine, theirs, psend, precv)
    gain_grad[...] = gains
    grad[...] = total
    block[...] = total.astype(jnp.bfloat16)
    gather = Gather(spot, sizes, block, grad_all, gsend, grecv)
    gather.start()
    out_scatter.wait()
    result = hidden[...]
    for q in range(sizes[1]):
        result = result + out_landing[q].astype(jnp.float32)
    output[...] = result.astype(jnp.bfloat16)
    scatter.wait_send()
    out_scatter.wait_send()
    gather.wait()


def middle(sizes, part, out_part, hidden, dy, gain):
    tokens, width = hidden.shape
    rows = sizes[1]
    low, wide = jnp.bfloat16, jnp.float32
    return pl.pallas_call(
        functools.partial(middle_kernel, sizes),
        in_specs=[VMEM] * 5,
        out_specs=[VMEM] * 4,
        out_shape=[
            jax.ShapeDtypeStruct((tokens, width), low),
            jax.ShapeDtypeStruct((tokens, width), wide),
            jax.ShapeDtypeStruct(part.shape, low),
            jax.ShapeDtypeStruct((1, width), wide),
        ],
        scratch_shapes=[
            pltpu.VMEM((rows, tokens, width), low),
            pltpu.VMEM((rows, tokens, width), low),
            pltpu.VMEM((2, tokens, 128), wide),
            pltpu.VMEM((2, tokens, 128), wide),
            pltpu.VMEM((tokens, width), low),
        ]
        + plane_sems(sizes) * 3
        + [DMA, DMA],
        compiler_params=pltpu.CompilerParams(collective_id=4, has_side_effects=True),
        name="middle",
    )(part, out_part, hidden, dy, gain[None])


def last_kernel(
    sizes, part, x, above, gain, other_gain, grad, gain_sums,
    landing, mine, theirs, own_gain, gain_landing, ssend, srecv, psend, precv, bsend, brecv,
):
    spot = here()
    count = sizes[0] * sizes[1] * sizes[2]
    me = index_of(spot, sizes)
    greet_all(spot, sizes)
    scatter = Scatter(spot, sizes, part, landing, ssend, srecv)
    scatter.start()
    scatter.wait()
    total, gains = norm_back(sizes, spot, landing, x, above, gain, mine, theirs, psend, precv)
    lines = gains.shape[1] // 128
    for line in range(lines):
        columns = slice(line * 128, (line + 1) * 128)
        own_gain[line : line + 1] = gains[:, columns]
        own_gain[lines + line : lines + line + 1] = other_gain[:, columns]

    def tell(step, carry):
        device = device_of(lax.rem(me + step, count), sizes)
        remote(own_gain, gain_landing.at[me], bsend, brecv, device).start()
        return carry

    lax.fori_loop(1, count, tell, 0)
    gain_landing[me] = own_gain[...]
    grad[...] = total
    scatter.wait_send()
    arrived(gain_landing.at[pl.ds(0, count - 1)], brecv)
    for col in range(sizes[2]):

        def add(index, sums):
            return sums + gain_landing[index * sizes[2] + col]

        gain_sums[col] = lax.fori_loop(
            0, sizes[0] * sizes[1], add, jnp.zeros(own_gain.shape, jnp.float32)
        )
    arrived(gain_landing.at[pl.ds(0, count - 1)], bsend)


def last(sizes, part, x, above, gain, other_gain):
    tokens, width = x.shape
    rows = sizes[1]
    lines = 2 * width // 128
    count = sizes[0] * sizes[1] * sizes[2]
    wide = jnp.float32
    return pl.pallas_call(
        functools.partial(last_kernel, sizes),
        in_specs=[VMEM] * 5,
        out_specs=[VMEM] * 2,
        out_shape=[
            jax.ShapeDtypeStruct((tokens, width), wide),
            jax.ShapeDtypeStruct((sizes[2], lines, 128), wide),
        ],
        scratch_shapes=[
            pltpu.VMEM((rows, tokens, width), jnp.bfloat16),
            pltpu.VMEM((2, tokens, 128), wide),
            pltpu.VMEM((2, tokens, 128), wide),
            pltpu.VMEM((lines, 128), wide),
            pltpu.VMEM((count, lines, 128), wide),
        ]
        + plane_sems(sizes)
        + [DMA, DMA, DMA, DMA],
        compiler_params=pltpu.CompilerParams(collective_id=5, has_side_effects=True),
        name="last",
    )(part, x, above, gain[None], other_gain)


def allowed_mask(query_count, key_count, first_pos, prefix_len):
    query_pos = first_pos + lax.iota(jnp.int32, query_count)
    key_pos = lax.iota(jnp.int32, key_count)
    return (key_pos[None, :] <= query_pos[:, None]) | (key_pos[None, :] < prefix_len)


def flat_picks(picks_head):
    blocks = picks_head.shape[0] // FBLK
    return jnp.swapaxes(picks_head.reshape(blocks, FBLK, TOPK), 1, 2).reshape(blocks, TOPK * FBLK)


def one_hot(row_values, size):
    hot = lax.broadcasted_iota(jnp.int32, (size, row_values.shape[1]), 0) == row_values
    return jnp.where(hot, 1.0, 0.0).astype(jnp.bfloat16)


def route_kernel(rows_dev, owners, cap, picks_ref, rank_ref, meta_ref):
    lane = lax.broadcasted_iota(jnp.int32, (FBLK, FBLK), 0)
    before = jnp.where(lane < lax.broadcasted_iota(jnp.int32, (FBLK, FBLK), 1), 1.0, 0.0).astype(
        jnp.bfloat16
    )
    picks = picks_ref[0]
    owner = picks // rows_dev
    local = picks % rows_dev
    hot = one_hot(owner, owners)
    running = jnp.zeros((owners, 1), jnp.float32)
    ranks = []
    for chunk in range(picks.shape[1] // FBLK):
        part = hot[:, chunk * FBLK : (chunk + 1) * FBLK]
        earlier = jnp.dot(part, before, preferred_element_type=jnp.float32)
        wide = part.astype(jnp.float32)
        ranks.append(jnp.sum(wide * (earlier + running), axis=0, keepdims=True))
        running = running + jnp.sum(wide, axis=1, keepdims=True)
    rank = jnp.concatenate(ranks, axis=1).astype(jnp.int32)
    rank_ref[0] = rank
    slot_hot = one_hot(rank, cap)
    token = lax.broadcasted_iota(jnp.int32, picks.shape, 1) % FBLK
    outs = []
    for payload in (local % SUBKEYS, local // SUBKEYS, token):
        scaled = hot * payload.astype(jnp.float32).astype(jnp.bfloat16)
        outs.append(
            lax.dot_general(
                scaled, slot_hot, (((1,), (1,)), ((), ())), preferred_element_type=jnp.float32
            ).astype(jnp.int32)
        )
    meta_ref[0] = (outs[1] * FBLK + outs[2]) * SUBKEYS + outs[0]


def route(flat, rows_dev, owners, cap):
    blocks, count = flat.shape
    rank, meta = pl.pallas_call(
        functools.partial(route_kernel, rows_dev, owners, cap),
        grid=(blocks,),
        in_specs=[pl.BlockSpec((1, 1, count), lambda i: (i, 0, 0))],
        out_specs=[
            pl.BlockSpec((1, 1, count), lambda i: (i, 0, 0)),
            pl.BlockSpec((1, owners, cap), lambda i: (i, 0, 0)),
        ],
        out_shape=[
            jax.ShapeDtypeStruct((blocks, 1, count), jnp.int32),
            jax.ShapeDtypeStruct((blocks, owners, cap), jnp.int32),
        ],
        name="route",
    )(flat[:, None, :])
    return rank, meta


def weigh_kernel(rows_dev, owners, cap, query_ref, keys_ref, picks_ref, rank_ref, weights_ref, slots_ref):
    picks = picks_ref[0]
    first = lax.dot_general(
        keys_ref[0], query_ref[:, :HALF], (((1,), (1,)), ((), ())), preferred_element_type=jnp.float32
    )
    second = lax.dot_general(
        keys_ref[1], query_ref[:, HALF:], (((1,), (1,)), ((), ())), preferred_element_type=jnp.float32
    )
    upper = picks // SUBKEYS
    lower = picks % SUBKEYS
    key_id = lax.broadcasted_iota(jnp.int32, (SUBKEYS, FBLK), 0)
    rows = []
    for pick in range(TOPK):
        columns = slice(pick * FBLK, (pick + 1) * FBLK)
        chosen = jnp.where(key_id == upper[:, columns], first, 0.0) + jnp.where(
            key_id == lower[:, columns], second, 0.0
        )
        rows.append(jnp.sum(chosen, axis=0, keepdims=True))
    scores = jnp.concatenate(rows, axis=0)
    powers = jnp.exp(scores - jnp.max(scores, axis=0, keepdims=True))
    weights = powers / jnp.sum(powers, axis=0, keepdims=True)
    weights_ref[0] = weights
    flat = jnp.concatenate([weights[pick : pick + 1] for pick in range(TOPK)], axis=1)
    scaled = one_hot(picks // rows_dev, owners) * flat.astype(jnp.bfloat16)
    slots_ref[0] = lax.dot_general(
        scaled,
        one_hot(rank_ref[0], cap),
        (((1,), (1,)), ((), ())),
        preferred_element_type=jnp.float32,
    ).astype(jnp.bfloat16)


def weigh(query_rows, keys_head, flat, rank, rows_dev, owners, cap):
    blocks, count = flat.shape
    return pl.pallas_call(
        functools.partial(weigh_kernel, rows_dev, owners, cap),
        grid=(blocks,),
        in_specs=[
            pl.BlockSpec((FBLK, 2 * HALF), lambda i: (i, 0)),
            pl.BlockSpec((2, SUBKEYS, HALF), lambda i: (0, 0, 0)),
            pl.BlockSpec((1, 1, count), lambda i: (i, 0, 0)),
            pl.BlockSpec((1, 1, count), lambda i: (i, 0, 0)),
        ],
        out_specs=[
            pl.BlockSpec((1, TOPK, FBLK), lambda i: (i, 0, 0)),
            pl.BlockSpec((1, owners, cap), lambda i: (i, 0, 0)),
        ],
        out_shape=[
            jax.ShapeDtypeStruct((blocks, TOPK, FBLK), jnp.float32),
            jax.ShapeDtypeStruct((blocks, owners, cap), jnp.bfloat16),
        ],
        name="weigh",
    )(query_rows, keys_head, flat[:, None, :], rank)


def spread_kernel(areas, key_ref, low_ref, weight_ref, out_ref):
    key = key_ref[0]
    at_key = lax.broadcasted_iota(jnp.int32, (areas * FBLK, key.shape[1]), 0) == key
    left = jnp.where(at_key, weight_ref[0].astype(jnp.float32), 0.0).astype(jnp.bfloat16)
    stacked = lax.dot_general(
        left,
        one_hot(low_ref[0], SUBKEYS),
        (((1,), (1,)), ((), ())),
        preferred_element_type=jnp.float32,
    ).astype(jnp.bfloat16)
    for area in range(areas):
        out_ref[:, area * SUBKEYS : (area + 1) * SUBKEYS] = stacked[area * FBLK : (area + 1) * FBLK]


def spread(key, low, weight, rows_dev):
    blocks, slots = key.shape
    areas = rows_dev // SUBKEYS
    row = pl.BlockSpec((1, 1, slots), lambda i: (i, 0, 0))
    return pl.pallas_call(
        functools.partial(spread_kernel, areas),
        grid=(blocks,),
        in_specs=[row, row, row],
        out_specs=pl.BlockSpec((FBLK, rows_dev), lambda i: (i, 0)),
        out_shape=jax.ShapeDtypeStruct((blocks * FBLK, rows_dev), jnp.bfloat16),
        name="spread",
    )(key[:, None], low[:, None], weight[:, None])


def collect_kernel(areas, grid_ref, key_ref, low_ref, out_ref):
    key = key_ref[0]
    low_hot = one_hot(low_ref[0], SUBKEYS)
    total = jnp.zeros(key.shape, jnp.float32)
    for area in range(areas):
        product = jnp.dot(
            grid_ref[:, area * SUBKEYS : (area + 1) * SUBKEYS],
            low_hot,
            preferred_element_type=jnp.float32,
        )
        spot = lax.broadcasted_iota(jnp.int32, product.shape, 0) + area * FBLK
        total = total + jnp.sum(jnp.where(spot == key, product, 0.0), axis=0, keepdims=True)
    out_ref[0] = total


def collect(grid_products, key, low, rows_dev):
    blocks, slots = key.shape
    row = pl.BlockSpec((1, 1, slots), lambda i: (i, 0, 0))
    return pl.pallas_call(
        functools.partial(collect_kernel, rows_dev // SUBKEYS),
        grid=(blocks,),
        in_specs=[pl.BlockSpec((FBLK, rows_dev), lambda i: (i, 0)), row, row],
        out_specs=row,
        out_shape=jax.ShapeDtypeStruct((blocks, 1, slots), jnp.float32),
        name="collect",
    )(grid_products, key[:, None], low[:, None])[:, 0]


def unweigh_kernel(rows_dev, owners, back_ref, picks_ref, rank_ref, weights_ref, first_ref, second_ref):
    picks = picks_ref[0]
    hot = one_hot(picks // rows_dev, owners)
    back = back_ref[0]
    high = back.astype(jnp.bfloat16)
    rest = back - high.astype(jnp.float32)
    middle = rest.astype(jnp.bfloat16)
    lowest = (rest - middle.astype(jnp.float32)).astype(jnp.bfloat16)
    spread_back = (
        jnp.dot(high, hot, preferred_element_type=jnp.float32)
        + jnp.dot(middle, hot, preferred_element_type=jnp.float32)
        + jnp.dot(lowest, hot, preferred_element_type=jnp.float32)
    )
    slot = lax.broadcasted_iota(jnp.int32, spread_back.shape, 0)
    flat = jnp.sum(jnp.where(slot == rank_ref[0], spread_back, 0.0), axis=0, keepdims=True)
    grads = jnp.concatenate(
        [flat[:, pick * FBLK : (pick + 1) * FBLK] for pick in range(TOPK)], axis=0
    )
    weights = weights_ref[0]
    grads = weights * (grads - jnp.sum(weights * grads, axis=0, keepdims=True))
    upper = picks // SUBKEYS
    lower = picks % SUBKEYS
    key_id = lax.broadcasted_iota(jnp.int32, (SUBKEYS, FBLK), 0)
    first = jnp.zeros((SUBKEYS, FBLK), jnp.float32)
    second = jnp.zeros((SUBKEYS, FBLK), jnp.float32)
    for pick in range(TOPK):
        columns = slice(pick * FBLK, (pick + 1) * FBLK)
        value = grads[pick : pick + 1]
        first = first + jnp.where(key_id == upper[:, columns], value, 0.0)
        second = second + jnp.where(key_id == lower[:, columns], value, 0.0)
    first_ref[...] = first.astype(jnp.bfloat16)
    second_ref[...] = second.astype(jnp.bfloat16)


def unweigh(back, flat, rank, weights, rows_dev, owners):
    blocks, count = flat.shape
    cap = back.shape[1]
    return pl.pallas_call(
        functools.partial(unweigh_kernel, rows_dev, owners),
        grid=(blocks,),
        in_specs=[
            pl.BlockSpec((1, cap, owners), lambda i: (i, 0, 0)),
            pl.BlockSpec((1, 1, count), lambda i: (i, 0, 0)),
            pl.BlockSpec((1, 1, count), lambda i: (i, 0, 0)),
            pl.BlockSpec((1, TOPK, FBLK), lambda i: (i, 0, 0)),
        ],
        out_specs=[
            pl.BlockSpec((SUBKEYS, FBLK), lambda i: (0, i)),
            pl.BlockSpec((SUBKEYS, FBLK), lambda i: (0, i)),
        ],
        out_shape=[jax.ShapeDtypeStruct((SUBKEYS, blocks * FBLK), jnp.bfloat16)] * 2,
        name="unweigh",
    )(back, flat[:, None, :], rank, weights)


EVERYONE = ("dp", "row", "col")


def exchange(operand):
    return lax.all_to_all(operand, EVERYONE, split_axis=0, concat_axis=0, tiled=True)


def by_block(arrived, dp_count, row_count, col_count):
    _, blocks, cap = arrived.shape
    wide = arrived.reshape(dp_count, row_count, col_count, blocks, cap)
    return jnp.transpose(wide, (0, 2, 3, 1, 4)).reshape(
        dp_count * col_count * blocks, row_count * cap
    )


def by_source(blocked, dp_count, row_count, col_count, blocks, cap):
    wide = blocked.reshape(dp_count, col_count, blocks, row_count, cap)
    return jnp.transpose(wide, (0, 3, 1, 2, 4)).reshape(
        dp_count * row_count * col_count, blocks, cap
    )


def memory_all(query_rows, grad_memory, picks, subkeys, values):
    dp_count = lax.axis_size("dp")
    row_count = lax.axis_size("row")
    col_count = lax.axis_size("col")
    owners = dp_count * row_count * col_count
    rows_dev = values.shape[0]
    cap = FBLK * TOPK // owners
    own_tokens = query_rows.shape[0]
    blocks = own_tokens // FBLK
    head_id = lax.axis_index("row")
    keys_head = lax.dynamic_index_in_dim(subkeys, head_id, 0, keepdims=False)
    picks_head = lax.dynamic_index_in_dim(picks, head_id, 1, keepdims=False)
    flat = flat_picks(picks_head)
    rank, meta = route(flat, rows_dev, owners, cap)
    sizes = (dp_count, row_count, col_count)
    meta_in = by_block(exchange(jnp.swapaxes(meta, 0, 1)), *sizes)
    key = meta_in // SUBKEYS
    low = meta_in % SUBKEYS
    weights, slots = weigh(query_rows, keys_head, flat, rank, rows_dev, owners, cap)
    weight_in = by_block(exchange(jnp.swapaxes(slots, 0, 1)), *sizes)
    table = spread(key, low, weight_in, rows_dev)
    partial = jnp.dot(table, values, preferred_element_type=jnp.float32).astype(jnp.bfloat16)
    grid = partial.reshape(dp_count, col_count, own_tokens, row_count, -1)
    grid = jnp.transpose(grid, (0, 3, 1, 2, 4)).reshape(owners, own_tokens, -1)
    memory = lax.psum_scatter(grid, EVERYONE, scatter_dimension=0, tiled=True)[0]
    memory = memory.astype(jnp.float32)
    wide = lax.all_gather(grad_memory, "row", axis=1, tiled=True)
    grad_all = lax.all_gather(wide, ("dp", "col"), axis=0, tiled=True)
    grad_values = lax.dot_general(
        table, grad_all, (((0,), (0,)), ((), ())), preferred_element_type=jnp.float32
    )
    products = lax.dot_general(
        grad_all, values, (((1,), (1,)), ((), ())), preferred_element_type=jnp.float32
    ).astype(jnp.bfloat16)
    found = collect(products, key, low, rows_dev)
    back = exchange(by_source(found, *sizes, blocks, cap))
    first_t, second_t = unweigh(
        jnp.transpose(back, (1, 2, 0)), flat, rank, weights, rows_dev, owners
    )
    grad_query = jnp.concatenate(
        [
            lax.dot_general(
                part, keys_head[i], (((0,), (0,)), ((), ())), preferred_element_type=jnp.float32
            )
            for i, part in enumerate((first_t, second_t))
        ],
        axis=1,
    ).astype(jnp.bfloat16)
    grad_keys = jnp.stack(
        [
            jnp.dot(first_t, query_rows[:, :HALF], preferred_element_type=jnp.float32),
            jnp.dot(second_t, query_rows[:, HALF:], preferred_element_type=jnp.float32),
        ]
    )
    return memory, grad_query, grad_values, grad_keys


def head_scores(query_head, key_head, allowed):
    raw_scores = jnp.einsum(
        "qd,kd->qk", query_head, key_head, preferred_element_type=jnp.float32
    ) * HDIM ** (-0.5)
    return jnp.where(allowed, raw_scores, -jnp.inf)


def attend_forward(queries, keys, values, allowed):
    outputs = []
    log_sums = []
    for head_index in range(queries.shape[1] // HDIM):
        columns = slice(head_index * HDIM, (head_index + 1) * HDIM)
        scores = head_scores(queries[:, columns], keys[:, columns], allowed)
        peak_score = jnp.max(scores, axis=1, keepdims=True)
        exp_scores = jnp.exp(scores - peak_score)
        row_sum = jnp.sum(exp_scores, axis=1, keepdims=True)
        probabilities = (exp_scores / row_sum).astype(jnp.bfloat16)
        outputs.append(
            jnp.dot(probabilities, values[:, columns], preferred_element_type=jnp.float32)
        )
        log_sums.append(peak_score[:, 0] + jnp.log(row_sum[:, 0]))
    return (jnp.concatenate(outputs, axis=1), jnp.stack(log_sums))


def attend_backward(queries, keys, values, allowed, log_sums, grad_out):
    grad_queries = []
    grad_keys = []
    grad_values = []
    for head_index in range(queries.shape[1] // HDIM):
        columns = slice(head_index * HDIM, (head_index + 1) * HDIM)
        query_head = queries[:, columns]
        key_head = keys[:, columns]
        value_head = values[:, columns]
        grad_head = grad_out[:, columns]
        scores = head_scores(query_head, key_head, allowed)
        probabilities = jnp.exp(scores - log_sums[head_index][:, None])
        grad_probs = jnp.einsum(
            "qd,kd->qk", grad_head, value_head, preferred_element_type=jnp.float32
        )
        inner_sum = jnp.sum(probabilities * grad_probs, axis=1, keepdims=True)
        grad_scores = (probabilities * (grad_probs - inner_sum)).astype(jnp.bfloat16)
        grad_queries.append(
            jnp.dot(grad_scores, key_head, preferred_element_type=jnp.float32) * HDIM ** (-0.5)
        )
        grad_keys.append(
            jnp.einsum("qk,qd->kd", grad_scores, query_head, preferred_element_type=jnp.float32)
            * HDIM ** (-0.5)
        )
        grad_values.append(
            jnp.einsum(
                "qk,qd->kd",
                probabilities.astype(jnp.bfloat16),
                grad_head,
                preferred_element_type=jnp.float32,
            )
        )
    stacked = jnp.stack([jnp.concatenate(grad_keys, axis=1), jnp.concatenate(grad_values, axis=1)])
    return (jnp.concatenate(grad_queries, axis=1), stacked)


def dense(left, right):
    return jnp.dot(left, right, preferred_element_type=jnp.float32)


def dense_nt(left, right):
    return lax.dot_general(left, right, (((1,), (1,)), ((), ())), preferred_element_type=jnp.float32)


def dense_tn(left, right):
    return lax.dot_general(left, right, (((0,), (0,)), ((), ())), preferred_element_type=jnp.float32)


def per_device(
    inputs,
    prefix,
    picks,
    gain_attn,
    w_qkv,
    w_attn_out,
    gain_mem,
    w_query,
    w_gate,
    w_proj,
    subkeys,
    values,
    cotangent,
):
    low = jnp.bfloat16
    sizes = grid_sizes()
    width_part = inputs.shape[1]
    own_tokens = picks.shape[0]
    seq_tokens = own_tokens * sizes[2]
    col = lax.axis_index("col")
    col_first = col * width_part
    gain_one = lax.dynamic_slice_in_dim(gain_attn, col_first, width_part)
    gain_two = lax.dynamic_slice_in_dim(gain_mem, col_first, width_part)

    x_own, dy_own, qkv_w, query_w, gate_w, proj_w, attn_w = start_all(
        sizes, inputs, cotangent, w_qkv, w_query, w_gate, w_proj, w_attn_out
    )
    residual = x_own.astype(jnp.float32)
    scale_one = lax.rsqrt(jnp.sum(residual * residual, axis=1, keepdims=True) / D + EPSILON)
    normed_one = (residual * scale_one * gain_attn.astype(jnp.float32)).astype(low)
    qkv = jnp.einsum("tc,jcf->jtf", normed_one, qkv_w, preferred_element_type=jnp.float32).astype(low)
    kv_all = swap_tokens(sizes, qkv[1:])
    allowed = allowed_mask(own_tokens, seq_tokens, col * own_tokens, prefix[0])
    attended_sum, log_sums = attend_forward(qkv[0], kv_all[0], kv_all[1], allowed)
    attended = attended_sum.astype(low)
    hidden, normed_two = join(sizes, dense(attended, attn_w).astype(low), inputs, gain_two)
    query_rows = dense(normed_two, query_w).astype(low)
    gate_value = dense(normed_two, gate_w)
    sigmoid_gate = jax.nn.sigmoid(gate_value)
    silu_gate = gate_value * sigmoid_gate
    grad_gated = dense_nt(dy_own, proj_w)
    grad_memory = (grad_gated * silu_gate).astype(low)
    memory, grad_query, grad_values, grad_keys = memory_all(
        query_rows, grad_memory, picks, subkeys, values
    )
    gated_value = (memory * silu_gate).astype(low)
    out_part = dense(gated_value, proj_w).astype(low)
    grad_gate = (
        grad_gated * memory * sigmoid_gate * (1.0 + gate_value * (1.0 - sigmoid_gate))
    ).astype(low)
    grad_part = (dense_nt(grad_query, query_w) + dense_nt(grad_gate, gate_w)).astype(low)
    output, grad_hidden, grad_hidden_all, gain_two_grad = middle(
        sizes, grad_part, out_part, hidden, cotangent, gain_two
    )
    grad_attended = dense_nt(grad_hidden_all, attn_w).astype(low)
    grad_query_own, grad_kv_part = attend_backward(
        qkv[0], kv_all[0], kv_all[1], allowed, log_sums, grad_attended
    )
    grad_kv = pair_sum(sizes, grad_kv_part)
    grad_q = grad_query_own.astype(low)
    x_part = (
        dense_nt(grad_q, qkv_w[0]) + dense_nt(grad_kv[0], qkv_w[1]) + dense_nt(grad_kv[1], qkv_w[2])
    ).astype(low)
    grad_inputs, gain_sums = last(sizes, x_part, inputs, grad_hidden, gain_one, gain_two_grad)
    gain_rows = gain_sums.reshape(sizes[2], 2, width_part)
    grad_gain_one = gain_rows[:, 0].reshape(-1)
    grad_gain_two = gain_rows[:, 1].reshape(-1)

    def col_sum(grad, dim):
        return lax.psum_scatter(grad.astype(low), "col", scatter_dimension=dim, tiled=True)

    def weight_sum(grad, dim):
        return lax.psum(col_sum(grad, dim), "dp").astype(jnp.float32)

    grad_w_proj = weight_sum(dense_tn(gated_value, dy_own), 1)
    grad_w_query = weight_sum(dense_tn(normed_two, grad_query), 0)
    grad_w_gate = weight_sum(dense_tn(normed_two, grad_gate), 0)
    grad_w_attn_out = weight_sum(dense_tn(attended, grad_hidden_all), 1)
    grad_w_qkv = weight_sum(
        jnp.stack([dense_tn(normed_one, part) for part in (grad_q, grad_kv[0], grad_kv[1])]), 1
    )
    grad_keys = lax.psum_scatter(
        grad_keys.astype(low).reshape(-1, HALF), ("dp", "col"), scatter_dimension=0, tiled=True
    )
    grad_subkeys = (
        lax.all_gather(grad_keys, ("row", "dp", "col"), axis=0, tiled=True)
        .astype(jnp.float32)
        .reshape(subkeys.shape)
    )
    return (
        output,
        grad_inputs,
        grad_gain_one,
        grad_w_qkv,
        grad_w_attn_out,
        grad_gain_two,
        grad_w_query,
        grad_w_gate,
        grad_w_proj,
        grad_subkeys,
        grad_values,
    )


def solution(mesh):
    placed = (
        P(("dp", "row"), "col"),
        P("dp"),
        P(("dp", "col"), None, None),
        P(),
        P(None, "col", "row"),
        P("row", "col"),
        P(),
        P("col", "row"),
        P("col", "row"),
        P("row", "col"),
        P(),
        P(("dp", "row", "col"), None),
        P(("dp", "row"), "col"),
    )
    return jax.shard_map(
        per_device,
        mesh=mesh,
        in_specs=placed,
        out_specs=(
            P(("dp", "row"), "col"),
            P(("dp", "row"), "col"),
            P(),
            P(None, "col", "row"),
            P("row", "col"),
            P(),
            P("col", "row"),
            P("col", "row"),
            P("row", "col"),
            P(),
            P(("dp", "row", "col"), None),
        ),
        check_vma=False,
    )
```

```python
import functools

import jax
import jax.numpy as jnp
from jax import lax
from jax.experimental import pallas as pl
from jax.experimental.pallas import tpu as pltpu
from jax.sharding import PartitionSpec as P

D = 1024
HDIM = 64
HALF = 512
SUBKEYS = 256
TOPK = 32
FBLK = 128


EPSILON = 1e-06


MESH = pl.DeviceIdType.MESH
VMEM = pl.BlockSpec(memory_space=pltpu.VMEM)
ANY = pl.BlockSpec(memory_space=pl.ANY)
DMA = pltpu.SemaphoreType.DMA


def here():
    return lax.axis_index("dp"), lax.axis_index("row"), lax.axis_index("col")


def grid_sizes():
    return lax.axis_size("dp"), lax.axis_size("row"), lax.axis_size("col")


def remote(src, dst, send_sem, recv_sem, device):
    return pltpu.make_async_remote_copy(
        src_ref=src,
        dst_ref=dst,
        send_sem=send_sem,
        recv_sem=recv_sem,
        device_id=device,
        device_id_type=MESH,
    )


def arrived(dst, sem):
    pltpu.make_async_copy(dst, dst, sem).wait()


def greet_plane(spot, sizes):
    barrier = pltpu.get_barrier_semaphore()
    dp, row, col = spot
    _, rows, cols = sizes
    for j in range(rows):
        for k in range(cols):
            if j + k > 0:
                pl.semaphore_signal(
                    barrier,
                    inc=1,
                    device_id=(dp, lax.rem(row + j, rows), lax.rem(col + k, cols)),
                    device_id_type=MESH,
                )
    pl.semaphore_wait(barrier, rows * cols - 1)


def greet_partner(spot, sizes):
    barrier = pltpu.get_barrier_semaphore()
    dp, row, col = spot
    pl.semaphore_signal(barrier, inc=1, device_id=(dp, row, 1 - col), device_id_type=MESH)
    pl.semaphore_wait(barrier, 1)


def device_of(index, sizes):
    _, rows, cols = sizes
    return (
        lax.div(index, rows * cols),
        lax.rem(lax.div(index, cols), rows),
        lax.rem(index, cols),
    )


def index_of(spot, sizes):
    return (spot[0] * sizes[1] + spot[1]) * sizes[2] + spot[2]


def greet_all(spot, sizes):
    barrier = pltpu.get_barrier_semaphore()
    count = sizes[0] * sizes[1] * sizes[2]
    me = index_of(spot, sizes)

    def greet(step, carry):
        pl.semaphore_signal(
            barrier,
            inc=1,
            device_id=device_of(lax.rem(me + step, count), sizes),
            device_id_type=MESH,
        )
        return carry

    lax.fori_loop(1, count, greet, 0)
    pl.semaphore_wait(barrier, count - 1)


class Gather:
    def __init__(self, spot, sizes, src, dst, send, recv):
        self.spot, self.sizes, self.src, self.dst = spot, sizes, src, dst
        self.send, self.recv = send, recv
        self.tokens, self.width = src.shape
        dp, row, col = spot
        _, rows, cols = sizes
        self.half = rows // cols
        self.target = lax.div(row, self.half)
        self.slot = lax.rem(row, self.half) * cols + col
        first = pl.multiple_of(lax.rem(row, self.half) * self.tokens, self.tokens)
        left = pl.multiple_of(col * self.width, self.width)
        self.there = dst.at[pl.ds(first, self.tokens), pl.ds(left, self.width)]

    def copy(self, step):
        dp, row, _ = self.spot
        device = (dp, lax.rem(row + step, self.sizes[1]), self.target)
        return remote(self.src, self.there, self.send.at[step], self.recv.at[self.slot], device)

    def start(self):
        col = self.spot[2]

        for step in range(1, self.sizes[1]):
            self.copy(step).start()

        @pl.when(self.target == col)
        def _():
            pltpu.make_async_copy(self.src, self.there, self.recv.at[self.slot]).start()

        @pl.when(self.target != col)
        def _():
            self.copy(0).start()

    def wait(self):
        cols = self.sizes[2]
        for i in range(self.half):
            for k in range(cols):
                arrived(
                    self.dst.at[pl.ds(i * self.tokens, self.tokens), pl.ds(k * self.width, self.width)],
                    self.recv.at[i * cols + k],
                )
        for step in range(1, self.sizes[1]):
            self.copy(step).wait_send()

        @pl.when(self.target != self.spot[2])
        def _():
            self.copy(0).wait_send()


class Scatter:
    def __init__(self, spot, sizes, src, landing, send, recv):
        self.spot, self.sizes, self.src, self.landing = spot, sizes, src, landing
        self.send, self.recv = send, recv
        _, self.tokens, self.width = landing.shape
        self.half = sizes[1] // sizes[2]

    def parts(self):
        dp, row, col = self.spot
        cols = self.sizes[2]
        for i in range(self.half):
            for k in range(cols):
                piece = self.src.at[
                    pl.ds(i * self.tokens, self.tokens), pl.ds(k * self.width, self.width)
                ]
                target = col * self.half + i
                mine = jnp.logical_and(target == row, col == k)
                there = self.landing.at[row]
                copy = remote(
                    piece, there, self.send.at[i * cols + k], self.recv.at[row], (dp, target, k)
                )
                yield mine, copy, pltpu.make_async_copy(piece, there, self.recv.at[row])

    def start(self):
        for mine, copy, own in self.parts():
            pl.when(jnp.logical_not(mine))(copy.start)
            pl.when(mine)(own.start)

    def wait(self):
        for q in range(self.sizes[1]):
            arrived(self.landing.at[q], self.recv.at[q])

    def wait_send(self):
        for mine, copy, _ in self.parts():
            pl.when(jnp.logical_not(mine))(copy.wait_send)


def plane_sems(sizes):
    rows, cols = sizes[1], sizes[2]
    return [DMA((rows,)), DMA((rows,))]


def start_kernel(sizes, *refs):
    x, dy, wqkv, wquery, wgate, wproj, wattn = refs[:7]
    xs, dys, wqkv_all, wquery_all, wgate_all, wproj_all, wattn_all = refs[7:14]
    xsend, xrecv, ysend, yrecv, wsend, wrecv, wlocal = refs[14:]
    spot = here()
    dp, row, col = spot
    greet_plane(spot, sizes)
    gather_x = Gather(spot, sizes, x, xs, xsend, xrecv)
    gather_y = Gather(spot, sizes, dy, dys, ysend, yrecv)
    gather_x.start()
    gather_y.start()
    copies = []
    for n, (src, dst, dim) in enumerate(
        (
            (wqkv, wqkv_all, 1),
            (wquery, wquery_all, 0),
            (wgate, wgate_all, 0),
            (wproj, wproj_all, 1),
            (wattn, wattn_all, 1),
        )
    ):
        size = src.shape[dim]
        window = [slice(None)] * len(src.shape)
        window[dim] = pl.ds(pl.multiple_of(col * size, size), size)
        there = dst.at[tuple(window)]
        away = remote(src, there, wsend.at[n], wrecv.at[n], (dp, row, 1 - col))
        own = pltpu.make_async_copy(src, there, wlocal.at[n])
        away.start()
        own.start()
        copies += [away, own]
    for copy in copies:
        copy.wait()
    gather_x.wait()
    gather_y.wait()


def start_all(sizes, x, dy, wqkv, wquery, wgate, wproj, wattn):
    tokens, width = x.shape
    half = sizes[1] // sizes[2]
    cols = sizes[2]
    low = jnp.bfloat16

    def twice(operand, dim):
        shape = list(operand.shape)
        shape[dim] *= cols
        return jax.ShapeDtypeStruct(tuple(shape), low)

    whole = jax.ShapeDtypeStruct((half * tokens, cols * width), low)
    return pl.pallas_call(
        functools.partial(start_kernel, sizes),
        in_specs=[VMEM] * 7,
        out_specs=[ANY] * 7,
        out_shape=[
            whole,
            whole,
            twice(wqkv, 1),
            twice(wquery, 0),
            twice(wgate, 0),
            twice(wproj, 1),
            twice(wattn, 1),
        ],
        scratch_shapes=plane_sems(sizes) * 2 + [DMA((5,))] * 3,
        compiler_params=pltpu.CompilerParams(collective_id=0, has_side_effects=True),
        name="start_all",
    )(x, dy, wqkv, wquery, wgate, wproj, wattn)


def swap_kernel(sizes, src, dst, send, recv, own):
    spot = here()
    dp, row, col = spot
    greet_partner(spot, sizes)
    size = src.shape[1]
    there = dst.at[:, pl.ds(pl.multiple_of(col * size, size), size)]
    away = remote(src, there, send, recv, (dp, row, 1 - col))
    local = pltpu.make_async_copy(src, there, own)
    away.start()
    local.start()
    away.wait()
    local.wait()


def swap_tokens(sizes, src):
    shape = (src.shape[0], src.shape[1] * sizes[2], src.shape[2])
    return pl.pallas_call(
        functools.partial(swap_kernel, sizes),
        in_specs=[VMEM],
        out_specs=VMEM,
        out_shape=jax.ShapeDtypeStruct(shape, src.dtype),
        scratch_shapes=[DMA, DMA, DMA],
        compiler_params=pltpu.CompilerParams(collective_id=1, has_side_effects=True),
        name="swap_tokens",
    )(src)


def pair_sum_kernel(sizes, src, out, landing, send, recv):
    spot = here()
    dp, row, col = spot
    greet_partner(spot, sizes)
    size = landing.shape[1]
    other = pl.multiple_of((1 - col) * size, size)
    away = remote(src.at[:, pl.ds(other, size)], landing, send, recv, (dp, row, 1 - col))
    away.start()
    away.wait()
    own = src[:, pl.ds(pl.multiple_of(col * size, size), size)]
    out[...] = (own + landing[...]).astype(out.dtype)


def pair_sum(sizes, src):
    shape = (src.shape[0], src.shape[1] // sizes[2], src.shape[2])
    return pl.pallas_call(
        functools.partial(pair_sum_kernel, sizes),
        in_specs=[VMEM],
        out_specs=VMEM,
        out_shape=jax.ShapeDtypeStruct(shape, jnp.bfloat16),
        scratch_shapes=[pltpu.VMEM(shape, src.dtype), DMA, DMA],
        compiler_params=pltpu.CompilerParams(collective_id=2, has_side_effects=True),
        name="pair_sum",
    )(src)


def fold(column):
    return jnp.broadcast_to(column, (column.shape[0], 128))


def join_kernel(
    sizes, part, x, gain, hidden, normed_all, landing, mine, theirs, block,
    ssend, srecv, gsend, grecv, psend, precv,
):
    spot = here()
    dp, row, col = spot
    greet_plane(spot, sizes)
    scatter = Scatter(spot, sizes, part, landing, ssend, srecv)
    scatter.start()
    scatter.wait()
    total = x[...].astype(jnp.float32)
    for q in range(sizes[1]):
        total = total + landing[q].astype(jnp.float32)
    hidden[...] = total
    mine[...] = fold(jnp.sum(total * total, axis=1, keepdims=True))
    pair = remote(mine, theirs, psend, precv, (dp, row, 1 - col))
    pair.start()
    pair.wait()
    squares = mine[:, :1] + theirs[:, :1]
    scale = lax.rsqrt(squares / D + EPSILON)
    block[...] = (hidden[...] * scale * gain[...].astype(jnp.float32)).astype(jnp.bfloat16)
    gather = Gather(spot, sizes, block, normed_all, gsend, grecv)
    gather.start()
    scatter.wait_send()
    gather.wait()


def join(sizes, part, x, gain):
    tokens, width = x.shape
    rows = sizes[1]
    return pl.pallas_call(
        functools.partial(join_kernel, sizes),
        in_specs=[VMEM] * 3,
        out_specs=[VMEM, VMEM],
        out_shape=[
            jax.ShapeDtypeStruct((tokens, width), jnp.float32),
            jax.ShapeDtypeStruct(part.shape, jnp.bfloat16),
        ],
        scratch_shapes=[
            pltpu.VMEM((rows, tokens, width), jnp.bfloat16),
            pltpu.VMEM((tokens, 128), jnp.float32),
            pltpu.VMEM((tokens, 128), jnp.float32),
            pltpu.VMEM((tokens, width), jnp.bfloat16),
        ]
        + plane_sems(sizes) * 2
        + [DMA, DMA],
        compiler_params=pltpu.CompilerParams(collective_id=3, has_side_effects=True),
        name="join",
    )(part, x, gain[None])


def norm_back(sizes, spot, landing, base, above, gain, mine, theirs, psend, precv):
    dp, row, col = spot
    normed_grad = landing[0].astype(jnp.float32)
    for q in range(1, sizes[1]):
        normed_grad = normed_grad + landing[q].astype(jnp.float32)
    values = base[...].astype(jnp.float32)
    unit_grad = normed_grad * gain[...].astype(jnp.float32)
    mine[0] = fold(jnp.sum(values * values, axis=1, keepdims=True))
    mine[1] = fold(jnp.sum(unit_grad * values, axis=1, keepdims=True))
    pair = remote(mine, theirs, psend, precv, (dp, row, 1 - col))
    pair.start()
    pair.wait()
    scale = lax.rsqrt((mine[0, :, :1] + theirs[0, :, :1]) / D + EPSILON)
    inner = scale * (mine[1, :, :1] + theirs[1, :, :1]) / D
    unit = values * scale
    grad = above[...].astype(jnp.float32) + scale * (unit_grad - unit * inner)
    return grad, jnp.sum(normed_grad * unit, axis=0, keepdims=True)


def middle_kernel(
    sizes, part, out_part, hidden, dy, gain, output, grad, grad_all, gain_grad,
    landing, out_landing, mine, theirs, block, ssend, srecv, osend, orecv, gsend, grecv, psend, precv,
):
    spot = here()
    greet_plane(spot, sizes)
    scatter = Scatter(spot, sizes, part, landing, ssend, srecv)
    scatter.start()
    out_scatter = Scatter(spot, sizes, out_part, out_landing, osend, orecv)
    out_scatter.start()
    scatter.wait()
    total, gains = norm_back(sizes, spot, landing, hidden, dy, gain, mine, theirs, psend, precv)
    gain_grad[...] = gains
    grad[...] = total
    block[...] = total.astype(jnp.bfloat16)
    gather = Gather(spot, sizes, block, grad_all, gsend, grecv)
    gather.start()
    out_scatter.wait()
    result = hidden[...]
    for q in range(sizes[1]):
        result = result + out_landing[q].astype(jnp.float32)
    output[...] = result.astype(jnp.bfloat16)
    scatter.wait_send()
    out_scatter.wait_send()
    gather.wait()


def middle(sizes, part, out_part, hidden, dy, gain):
    tokens, width = hidden.shape
    rows = sizes[1]
    low, wide = jnp.bfloat16, jnp.float32
    return pl.pallas_call(
        functools.partial(middle_kernel, sizes),
        in_specs=[VMEM] * 5,
        out_specs=[VMEM] * 4,
        out_shape=[
            jax.ShapeDtypeStruct((tokens, width), low),
            jax.ShapeDtypeStruct((tokens, width), wide),
            jax.ShapeDtypeStruct(part.shape, low),
            jax.ShapeDtypeStruct((1, width), wide),
        ],
        scratch_shapes=[
            pltpu.VMEM((rows, tokens, width), low),
            pltpu.VMEM((rows, tokens, width), low),
            pltpu.VMEM((2, tokens, 128), wide),
            pltpu.VMEM((2, tokens, 128), wide),
            pltpu.VMEM((tokens, width), low),
        ]
        + plane_sems(sizes) * 3
        + [DMA, DMA],
        compiler_params=pltpu.CompilerParams(collective_id=4, has_side_effects=True),
        name="middle",
    )(part, out_part, hidden, dy, gain[None])


def last_kernel(
    sizes, part, x, above, gain, other_gain, grad, gain_sums,
    landing, mine, theirs, own_gain, gain_landing, ssend, srecv, psend, precv, bsend, brecv,
):
    spot = here()
    count = sizes[0] * sizes[1] * sizes[2]
    me = index_of(spot, sizes)
    greet_all(spot, sizes)
    scatter = Scatter(spot, sizes, part, landing, ssend, srecv)
    scatter.start()
    scatter.wait()
    total, gains = norm_back(sizes, spot, landing, x, above, gain, mine, theirs, psend, precv)
    lines = gains.shape[1] // 128
    for line in range(lines):
        columns = slice(line * 128, (line + 1) * 128)
        own_gain[line : line + 1] = gains[:, columns]
        own_gain[lines + line : lines + line + 1] = other_gain[:, columns]

    def tell(step, carry):
        device = device_of(lax.rem(me + step, count), sizes)
        remote(own_gain, gain_landing.at[me], bsend, brecv, device).start()
        return carry

    lax.fori_loop(1, count, tell, 0)
    gain_landing[me] = own_gain[...]
    grad[...] = total
    scatter.wait_send()
    arrived(gain_landing.at[pl.ds(0, count - 1)], brecv)
    for col in range(sizes[2]):

        def add(index, sums):
            return sums + gain_landing[index * sizes[2] + col]

        gain_sums[col] = lax.fori_loop(
            0, sizes[0] * sizes[1], add, jnp.zeros(own_gain.shape, jnp.float32)
        )
    arrived(gain_landing.at[pl.ds(0, count - 1)], bsend)


def last(sizes, part, x, above, gain, other_gain):
    tokens, width = x.shape
    rows = sizes[1]
    lines = 2 * width // 128
    count = sizes[0] * sizes[1] * sizes[2]
    wide = jnp.float32
    return pl.pallas_call(
        functools.partial(last_kernel, sizes),
        in_specs=[VMEM] * 5,
        out_specs=[VMEM] * 2,
        out_shape=[
            jax.ShapeDtypeStruct((tokens, width), wide),
            jax.ShapeDtypeStruct((sizes[2], lines, 128), wide),
        ],
        scratch_shapes=[
            pltpu.VMEM((rows, tokens, width), jnp.bfloat16),
            pltpu.VMEM((2, tokens, 128), wide),
            pltpu.VMEM((2, tokens, 128), wide),
            pltpu.VMEM((lines, 128), wide),
            pltpu.VMEM((count, lines, 128), wide),
        ]
        + plane_sems(sizes)
        + [DMA, DMA, DMA, DMA],
        compiler_params=pltpu.CompilerParams(collective_id=5, has_side_effects=True),
        name="last",
    )(part, x, above, gain[None], other_gain)


def allowed_mask(query_count, key_count, first_pos, prefix_len):
    query_pos = first_pos + lax.iota(jnp.int32, query_count)
    key_pos = lax.iota(jnp.int32, key_count)
    return (key_pos[None, :] <= query_pos[:, None]) | (key_pos[None, :] < prefix_len)


def flat_picks(picks_head):
    blocks = picks_head.shape[0] // FBLK
    return jnp.swapaxes(picks_head.reshape(blocks, FBLK, TOPK), 1, 2).reshape(blocks, TOPK * FBLK)


def one_hot(row_values, size):
    hot = lax.broadcasted_iota(jnp.int32, (size, row_values.shape[1]), 0) == row_values
    return jnp.where(hot, 1.0, 0.0).astype(jnp.bfloat16)


def route_kernel(rows_dev, owners, cap, picks_ref, rank_ref, meta_ref):
    lane = lax.broadcasted_iota(jnp.int32, (FBLK, FBLK), 0)
    before = jnp.where(lane < lax.broadcasted_iota(jnp.int32, (FBLK, FBLK), 1), 1.0, 0.0).astype(
        jnp.bfloat16
    )
    picks = picks_ref[0]
    owner = picks // rows_dev
    local = picks % rows_dev
    hot = one_hot(owner, owners)
    running = jnp.zeros((owners, 1), jnp.float32)
    ranks = []
    for chunk in range(picks.shape[1] // FBLK):
        part = hot[:, chunk * FBLK : (chunk + 1) * FBLK]
        earlier = jnp.dot(part, before, preferred_element_type=jnp.float32)
        wide = part.astype(jnp.float32)
        ranks.append(jnp.sum(wide * (earlier + running), axis=0, keepdims=True))
        running = running + jnp.sum(wide, axis=1, keepdims=True)
    rank = jnp.concatenate(ranks, axis=1).astype(jnp.int32)
    rank_ref[0] = rank
    slot_hot = one_hot(rank, cap)
    token = lax.broadcasted_iota(jnp.int32, picks.shape, 1) % FBLK
    outs = []
    for payload in (local % SUBKEYS, local // SUBKEYS, token):
        scaled = hot * payload.astype(jnp.float32).astype(jnp.bfloat16)
        outs.append(
            lax.dot_general(
                scaled, slot_hot, (((1,), (1,)), ((), ())), preferred_element_type=jnp.float32
            ).astype(jnp.int32)
        )
    meta_ref[0] = (outs[1] * FBLK + outs[2]) * SUBKEYS + outs[0]


def route(flat, rows_dev, owners, cap):
    blocks, count = flat.shape
    rank, meta = pl.pallas_call(
        functools.partial(route_kernel, rows_dev, owners, cap),
        grid=(blocks,),
        in_specs=[pl.BlockSpec((1, 1, count), lambda i: (i, 0, 0))],
        out_specs=[
            pl.BlockSpec((1, 1, count), lambda i: (i, 0, 0)),
            pl.BlockSpec((1, owners, cap), lambda i: (i, 0, 0)),
        ],
        out_shape=[
            jax.ShapeDtypeStruct((blocks, 1, count), jnp.int32),
            jax.ShapeDtypeStruct((blocks, owners, cap), jnp.int32),
        ],
        name="route",
    )(flat[:, None, :])
    return rank, meta


def weigh_kernel(rows_dev, owners, cap, query_ref, keys_ref, picks_ref, rank_ref, weights_ref, slots_ref):
    picks = picks_ref[0]
    first = lax.dot_general(
        keys_ref[0], query_ref[:, :HALF], (((1,), (1,)), ((), ())), preferred_element_type=jnp.float32
    )
    second = lax.dot_general(
        keys_ref[1], query_ref[:, HALF:], (((1,), (1,)), ((), ())), preferred_element_type=jnp.float32
    )
    upper = picks // SUBKEYS
    lower = picks % SUBKEYS
    key_id = lax.broadcasted_iota(jnp.int32, (SUBKEYS, FBLK), 0)
    rows = []
    for pick in range(TOPK):
        columns = slice(pick * FBLK, (pick + 1) * FBLK)
        chosen = jnp.where(key_id == upper[:, columns], first, 0.0) + jnp.where(
            key_id == lower[:, columns], second, 0.0
        )
        rows.append(jnp.sum(chosen, axis=0, keepdims=True))
    scores = jnp.concatenate(rows, axis=0)
    powers = jnp.exp(scores - jnp.max(scores, axis=0, keepdims=True))
    weights = powers / jnp.sum(powers, axis=0, keepdims=True)
    weights_ref[0] = weights
    flat = jnp.concatenate([weights[pick : pick + 1] for pick in range(TOPK)], axis=1)
    scaled = one_hot(picks // rows_dev, owners) * flat.astype(jnp.bfloat16)
    slots_ref[0] = lax.dot_general(
        scaled,
        one_hot(rank_ref[0], cap),
        (((1,), (1,)), ((), ())),
        preferred_element_type=jnp.float32,
    ).astype(jnp.bfloat16)


def weigh(query_rows, keys_head, flat, rank, rows_dev, owners, cap):
    blocks, count = flat.shape
    return pl.pallas_call(
        functools.partial(weigh_kernel, rows_dev, owners, cap),
        grid=(blocks,),
        in_specs=[
            pl.BlockSpec((FBLK, 2 * HALF), lambda i: (i, 0)),
            pl.BlockSpec((2, SUBKEYS, HALF), lambda i: (0, 0, 0)),
            pl.BlockSpec((1, 1, count), lambda i: (i, 0, 0)),
            pl.BlockSpec((1, 1, count), lambda i: (i, 0, 0)),
        ],
        out_specs=[
            pl.BlockSpec((1, TOPK, FBLK), lambda i: (i, 0, 0)),
            pl.BlockSpec((1, owners, cap), lambda i: (i, 0, 0)),
        ],
        out_shape=[
            jax.ShapeDtypeStruct((blocks, TOPK, FBLK), jnp.float32),
            jax.ShapeDtypeStruct((blocks, owners, cap), jnp.bfloat16),
        ],
        name="weigh",
    )(query_rows, keys_head, flat[:, None, :], rank)


def own_block(tokens_ref, dp, col, row, width):
    left = pl.multiple_of(row * width, width)
    return tokens_ref.at[dp, col, :, pl.ds(left, width)]


def send_rows(spot, sizes, src, landing, send, recv):
    count = sizes[0] * sizes[1] * sizes[2]
    me = index_of(spot, sizes)

    def one(step, carry):
        other = lax.rem(me + step, count)
        remote(src.at[other], landing.at[me], send, recv, device_of(other, sizes)).start()
        return carry

    lax.fori_loop(1, count, one, 0)
    landing[me] = src[me]


def all_rows(landing, sem):
    return arrived(landing.at[pl.ds(0, landing.shape[0] - 1)], sem)


def slot_row(sizes, table, dp, col, block):
    pieces = []
    for row in range(sizes[1]):
        index = (dp * sizes[1] + row) * sizes[2] + col
        pieces.append(table[index, block : block + 1, :])
    return jnp.concatenate(pieces, axis=1)


def read_kernel(
    sizes, blocks, grads, meta, slots, values,
    grads_all, table, own_part, other_part, meta_in,
    slots_in, tables, parts, msend, mrecv, ssend, srecv, zsend, zrecv, xsend, xrecv, csend, crecv,
    local, tsem, psem, qsend, qrecv,
):
    spot = here()
    dp, row, col = spot
    dps, rows, cols = sizes
    tokens, width = grads.shape
    areas = values.shape[0] // SUBKEYS
    greet_all(spot, sizes)
    send_rows(spot, sizes, meta, meta_in, msend, mrecv)
    send_rows(spot, sizes, slots, slots_in, ssend, srecv)

    def block_at(j, k, c):
        return own_block(grads_all, lax.rem(dp + j, dps), c, lax.rem(row + k, rows), width)

    def cross(src, j, k):
        remote(src, block_at(j, k, col), csend, crecv, (dp, row, 1 - col)).start()

    def sideways(src, j):
        for k in range(1, rows):
            remote(
                src, block_at(j, 0, col), xsend, xrecv.at[j, rows - k],
                (dp, lax.rem(row + k, rows), col),
            ).start()

    for k in range(1, dps):
        remote(
            grads, block_at(0, 0, col), zsend, zrecv.at[dps - k], (lax.rem(dp + k, dps), row, col)
        ).start()
    sideways(grads, 0)
    cross(grads, 0, 0)
    keep = pltpu.make_async_copy(grads, block_at(0, 0, col), local)
    keep.start()

    def from_above(j):
        src = block_at(j, 0, col)
        arrived(src, zrecv.at[j])
        sideways(src, j)
        cross(src, j, 0)

    def from_side(j):
        for k in range(1, rows):
            src = block_at(j, k, col)
            arrived(src, xrecv.at[j, k])
            cross(src, j, k)

    all_rows(meta_in, mrecv)
    all_rows(slots_in, srecv)

    def chunk(turn, kk):
        source_dp = lax.rem(dp + 1 + turn, dps)
        source_col = 1 - col if kk == 0 else col
        table_out = pltpu.make_async_copy(
            tables.at[kk], table.at[source_dp, source_col], tsem.at[kk]
        )

        @pl.when(turn > 0)
        def _():
            table_out.wait()

        for block in range(blocks):
            row_meta = slot_row(sizes, meta_in, source_dp, source_col, block)
            key = row_meta // SUBKEYS
            low = row_meta % SUBKEYS
            weight = slot_row(sizes, slots_in, source_dp, source_col, block)
            at_key = lax.broadcasted_iota(jnp.int32, (areas * FBLK, key.shape[1]), 0) == key
            left = jnp.where(at_key, weight, 0.0).astype(jnp.bfloat16)
            stacked = lax.dot_general(
                left,
                one_hot(low, SUBKEYS),
                (((1,), (1,)), ((), ())),
                preferred_element_type=jnp.float32,
            ).astype(jnp.bfloat16)
            for area in range(areas):
                tables[
                    kk,
                    block * FBLK : (block + 1) * FBLK,
                    area * SUBKEYS : (area + 1) * SUBKEYS,
                ] = stacked[area * FBLK : (area + 1) * FBLK]
        table_out.start()
        if kk == 0:
            part_out = remote(
                parts.at[0], other_part.at[source_dp], qsend, qrecv, (dp, row, 1 - col)
            )
        else:
            part_out = pltpu.make_async_copy(parts.at[1], own_part.at[source_dp], psem)

        @pl.when(turn > 0)
        def _():
            if kk == 0:
                part_out.wait_send()
            else:
                part_out.wait()

        def strip(n, carry):
            columns = pl.ds(pl.multiple_of(n * 256, 256), 256)
            parts[kk, :, columns] = jnp.dot(
                tables[kk], values[:, columns], preferred_element_type=jnp.float32
            ).astype(jnp.bfloat16)
            return carry

        lax.fori_loop(0, values.shape[1] // 256, strip, 0)
        part_out.start()

    def step(turn, carry):
        chunk(turn, 0)

        @pl.when(jnp.logical_and(turn > 0, 2 * turn < dps))
        def _():
            from_above(2 * turn)

        @pl.when(turn > 0)
        def _():
            from_side(turn - 1)

        chunk(turn, 1)

        @pl.when(2 * turn + 1 < dps)
        def _():
            from_above(2 * turn + 1)

        return carry

    lax.fori_loop(0, dps, step, 0)
    from_side(dps - 1)
    keep.wait()
    for kk in range(2):
        pltpu.make_async_copy(tables.at[kk], table.at[0, 0], tsem.at[kk]).wait()
    pltpu.make_async_copy(parts.at[1], own_part.at[0], psem).wait()
    remote(parts.at[0], other_part.at[0], qsend, qrecv, (dp, row, 1 - col)).wait_send()
    arrived(other_part, qrecv)
    arrived(grads_all.at[:, 0], crecv)
    arrived(grads_all.at[:, 0], csend)
    arrived(grads_all.at[pl.ds(0, dps - 1), 0, :, pl.ds(0, width)], zsend)
    arrived(grads_all.at[:, 0, :, pl.ds(0, (rows - 1) * width)], xsend)
    all_rows(meta_in, msend)
    all_rows(slots_in, ssend)


def read_memory(sizes, grads, meta, slots, values):
    dps, rows, cols = sizes
    tokens, width = grads.shape
    rows_dev, features = values.shape
    blocks = tokens // FBLK
    low = jnp.bfloat16
    shape = jax.ShapeDtypeStruct
    return pl.pallas_call(
        functools.partial(read_kernel, sizes, blocks),
        in_specs=[VMEM] * 4,
        out_specs=[ANY, ANY, ANY, ANY, VMEM],
        out_shape=[
            shape((dps, cols, tokens, rows * width), low),
            shape((dps, cols, tokens, rows_dev), low),
            shape((dps, tokens, features), low),
            shape((dps, tokens, features), low),
            shape(meta.shape, meta.dtype),
        ],
        scratch_shapes=[
            pltpu.VMEM(slots.shape, slots.dtype),
            pltpu.VMEM((2, tokens, rows_dev), low),
            pltpu.VMEM((2, tokens, features), low),
            DMA, DMA, DMA, DMA,
            DMA, DMA((dps,)),
            DMA, DMA((dps, rows)),
            DMA, DMA,
            DMA, DMA((2,)), DMA, DMA, DMA,
        ],
        compiler_params=pltpu.CompilerParams(collective_id=6, has_side_effects=True),
        name="read_memory",
    )(grads, meta, slots, values)


def back_kernel(
    sizes, blocks, grads_all, own_part, other_part, meta_in, values_t,
    memory, back, side_land, deep_land,
    chunks, found, hots, mine, theirs, acc, side, total, deep,
    gsem, osem, tsem, xsend, xrecv, zsend, zrecv, fsend, frecv, flocal, ssem, dsem,
):
    spot = here()
    dp, row, col = spot
    dps, rows, cols = sizes
    tokens, width = memory.shape
    areas = values_t.shape[1] // SUBKEYS
    count = dps * rows * cols
    me = index_of(spot, sizes)
    greet_all(spot, sizes)

    def source(turn):
        return lax.rem(dp + 1 + turn, dps)

    def load_parts(turn):
        return (
            pltpu.make_async_copy(own_part.at[source(turn)], mine, osem),
            pltpu.make_async_copy(other_part.at[source(turn)], theirs, tsem),
        )

    def load_chunk(turn, kk):
        return pltpu.make_async_copy(
            grads_all.at[source(turn), 1 - col if kk == 0 else col], chunks.at[kk], gsem.at[kk]
        )

    def piece(turn, k):
        left = pl.multiple_of(lax.rem(row + k, rows) * width, width)
        return acc.at[turn, :, pl.ds(left, width)]

    def combine(turn):
        for copy in load_parts(turn):
            copy.wait()
        acc[turn] = (mine[...].astype(jnp.float32) + theirs[...].astype(jnp.float32)).astype(
            jnp.bfloat16
        )

        @pl.when(turn + 1 < dps)
        def _():
            for copy in load_parts(turn + 1):
                copy.start()

        for k in range(1, rows):
            remote(
                piece(turn, k), side_land.at[turn, rows - k], xsend, xrecv.at[turn, rows - k],
                (dp, lax.rem(row + k, rows), col),
            ).start()

    def row_total(turn):
        copies = []
        for k in range(1, rows):
            arrived(side_land.at[turn, k], xrecv.at[turn, k])
            copies.append(pltpu.make_async_copy(side_land.at[turn, k], side.at[k], ssem.at[k]))
            copies[-1].start()
        result = acc[turn, :, pl.ds(pl.multiple_of(row * width, width), width)].astype(jnp.float32)
        for k in range(1, rows):
            copies[k - 1].wait()
            result = result + side[k].astype(jnp.float32)
        return result

    def deeper(turn):
        total[turn] = row_total(turn).astype(jnp.bfloat16)
        remote(
            total.at[turn], deep_land.at[dps - 2 - turn], zsend, zrecv.at[dps - 2 - turn],
            (source(turn), row, col),
        ).start()

    for copy in load_parts(0):
        copy.start()
    for kk in range(2):
        load_chunk(0, kk).start()

    def chunk(turn, kk):
        source_dp = source(turn)
        source_col = 1 - col if kk == 0 else col
        keys = []
        for block in range(blocks):
            row_meta = slot_row(sizes, meta_in, source_dp, source_col, block)
            keys.append(row_meta // SUBKEYS)
            hots[block] = one_hot(row_meta % SUBKEYS, SUBKEYS)
        load_chunk(turn, kk).wait()

        def area_step(area, sums):
            columns = pl.ds(pl.multiple_of(area * SUBKEYS, SUBKEYS), SUBKEYS)
            grid = jnp.dot(
                chunks[kk], values_t[:, columns], preferred_element_type=jnp.float32
            ).astype(jnp.bfloat16)
            new = []
            for block in range(blocks):
                product = jnp.dot(
                    grid[block * FBLK : (block + 1) * FBLK],
                    hots[block],
                    preferred_element_type=jnp.float32,
                )
                spot_id = lax.broadcasted_iota(jnp.int32, product.shape, 0) + area * FBLK
                new.append(
                    sums[block]
                    + jnp.sum(
                        jnp.where(spot_id == keys[block], product, 0.0), axis=0, keepdims=True
                    )
                )
            return tuple(new)

        sums = lax.fori_loop(
            0, areas, area_step, tuple(jnp.zeros(keys[0].shape, jnp.float32) for _ in range(blocks))
        )

        @pl.when(turn + 1 < dps)
        def _():
            load_chunk(turn + 1, kk).start()

        for r in range(rows):
            index = (source_dp * rows + r) * cols + source_col
            for block in range(blocks):
                found[index, block : block + 1, :] = sums[block][:, r * 128 : (r + 1) * 128]
            away = remote(found.at[index], back.at[me], fsend, frecv, (source_dp, r, source_col))
            own = jnp.logical_and(jnp.logical_and(source_dp == dp, row == r), source_col == col)
            if kk == 0:
                away.start()
            else:
                pl.when(jnp.logical_not(own))(away.start)
                pl.when(own)(pltpu.make_async_copy(found.at[index], back.at[me], flocal).start)

    def step(turn, carry):
        @pl.when(2 * turn < dps)
        def _():
            combine(2 * turn)

        @pl.when(turn > 0)
        def _():
            deeper(turn - 1)

        chunk(turn, 0)

        @pl.when(2 * turn + 1 < dps)
        def _():
            combine(2 * turn + 1)

        chunk(turn, 1)
        return carry

    lax.fori_loop(0, dps, step, 0)
    result = row_total(dps - 1)
    for k in range(dps - 1):
        arrived(deep_land.at[k], zrecv.at[k])
        copy = pltpu.make_async_copy(deep_land.at[k], deep.at[k % 2], dsem.at[k % 2])
        copy.start()
        copy.wait()
        result = result + deep[k % 2].astype(jnp.float32)
    memory[...] = result
    arrived(back.at[pl.ds(0, count - 1)], frecv)
    arrived(back.at[0], flocal)
    arrived(back.at[pl.ds(0, count - 1)], fsend)
    arrived(side_land.at[:, pl.ds(0, rows - 1)], xsend)
    arrived(deep_land.at[pl.ds(0, dps - 1)], zsend)


def back_memory(sizes, grads_all, own_part, other_part, meta_in, values_t):
    dps, rows, cols = sizes
    _, _, tokens, features = grads_all.shape
    width = features // rows
    blocks = tokens // FBLK
    count = dps * rows * cols
    low, wide = jnp.bfloat16, jnp.float32
    shape = jax.ShapeDtypeStruct
    memory, back, _, _ = pl.pallas_call(
        functools.partial(back_kernel, sizes, blocks),
        in_specs=[ANY, ANY, ANY, VMEM, VMEM],
        out_specs=[VMEM, VMEM, ANY, ANY],
        out_shape=[
            shape((tokens, width), wide),
            shape((count, blocks, 128), wide),
            shape((dps, rows, tokens, width), low),
            shape((dps, tokens, width), low),
        ],
        scratch_shapes=[
            pltpu.VMEM((2, tokens, features), low),
            pltpu.VMEM((count, blocks, 128), wide),
            pltpu.VMEM((blocks, SUBKEYS, rows * 128), low),
            pltpu.VMEM((tokens, features), low),
            pltpu.VMEM((tokens, features), low),
            pltpu.VMEM((dps, tokens, features), low),
            pltpu.VMEM((rows, tokens, width), low),
            pltpu.VMEM((dps, tokens, width), low),
            pltpu.VMEM((2, tokens, width), low),
            DMA((2,)), DMA, DMA,
            DMA, DMA((dps, rows)),
            DMA, DMA((dps,)),
            DMA, DMA, DMA, DMA((rows,)), DMA((2,)),
        ],
        compiler_params=pltpu.CompilerParams(collective_id=7, has_side_effects=True),
        name="back_memory",
    )(grads_all, own_part, other_part, meta_in, values_t)
    return memory, back


def unweigh_kernel(rows_dev, owners, back_ref, picks_ref, rank_ref, weights_ref, first_ref, second_ref):
    picks = picks_ref[0]
    hot = one_hot(picks // rows_dev, owners)
    back = back_ref[0]
    high = back.astype(jnp.bfloat16)
    rest = back - high.astype(jnp.float32)
    middle = rest.astype(jnp.bfloat16)
    lowest = (rest - middle.astype(jnp.float32)).astype(jnp.bfloat16)
    spread_back = (
        jnp.dot(high, hot, preferred_element_type=jnp.float32)
        + jnp.dot(middle, hot, preferred_element_type=jnp.float32)
        + jnp.dot(lowest, hot, preferred_element_type=jnp.float32)
    )
    slot = lax.broadcasted_iota(jnp.int32, spread_back.shape, 0)
    flat = jnp.sum(jnp.where(slot == rank_ref[0], spread_back, 0.0), axis=0, keepdims=True)
    grads = jnp.concatenate(
        [flat[:, pick * FBLK : (pick + 1) * FBLK] for pick in range(TOPK)], axis=0
    )
    weights = weights_ref[0]
    grads = weights * (grads - jnp.sum(weights * grads, axis=0, keepdims=True))
    upper = picks // SUBKEYS
    lower = picks % SUBKEYS
    key_id = lax.broadcasted_iota(jnp.int32, (SUBKEYS, FBLK), 0)
    first = jnp.zeros((SUBKEYS, FBLK), jnp.float32)
    second = jnp.zeros((SUBKEYS, FBLK), jnp.float32)
    for pick in range(TOPK):
        columns = slice(pick * FBLK, (pick + 1) * FBLK)
        value = grads[pick : pick + 1]
        first = first + jnp.where(key_id == upper[:, columns], value, 0.0)
        second = second + jnp.where(key_id == lower[:, columns], value, 0.0)
    first_ref[...] = first.astype(jnp.bfloat16)
    second_ref[...] = second.astype(jnp.bfloat16)


def unweigh(back, flat, rank, weights, rows_dev, owners):
    blocks, count = flat.shape
    cap = back.shape[1]
    return pl.pallas_call(
        functools.partial(unweigh_kernel, rows_dev, owners),
        grid=(blocks,),
        in_specs=[
            pl.BlockSpec((1, cap, owners), lambda i: (i, 0, 0)),
            pl.BlockSpec((1, 1, count), lambda i: (i, 0, 0)),
            pl.BlockSpec((1, 1, count), lambda i: (i, 0, 0)),
            pl.BlockSpec((1, TOPK, FBLK), lambda i: (i, 0, 0)),
        ],
        out_specs=[
            pl.BlockSpec((SUBKEYS, FBLK), lambda i: (0, i)),
            pl.BlockSpec((SUBKEYS, FBLK), lambda i: (0, i)),
        ],
        out_shape=[jax.ShapeDtypeStruct((SUBKEYS, blocks * FBLK), jnp.bfloat16)] * 2,
        name="unweigh",
    )(back, flat[:, None, :], rank, weights)


def memory_all(query_rows, grad_memory, picks, subkeys, values):
    sizes = grid_sizes()
    owners = sizes[0] * sizes[1] * sizes[2]
    rows_dev = values.shape[0]
    cap = FBLK * TOPK // owners
    head_id = lax.axis_index("row")
    keys_head = lax.dynamic_index_in_dim(subkeys, head_id, 0, keepdims=False)
    picks_head = lax.dynamic_index_in_dim(picks, head_id, 1, keepdims=False)
    flat = flat_picks(picks_head)
    rank, meta = route(flat, rows_dev, owners, cap)
    weights, slots = weigh(query_rows, keys_head, flat, rank, rows_dev, owners, cap)
    spare = ((0, 0), (0, 0), (0, 128 - cap))
    meta = jnp.pad(jnp.swapaxes(meta, 0, 1), spare, constant_values=-1)
    slots = jnp.pad(jnp.swapaxes(slots, 0, 1).astype(jnp.float32), spare)
    grads_all, table, own_part, other_part, meta_in = read_memory(
        sizes, grad_memory, meta, slots, values
    )
    memory, back = back_memory(sizes, grads_all, own_part, other_part, meta_in, values.T)
    grad_values = dense_tn(
        table.reshape(-1, rows_dev), grads_all.reshape(-1, grads_all.shape[-1])
    )
    first_t, second_t = unweigh(
        jnp.transpose(back, (1, 2, 0))[:, :cap], flat, rank, weights, rows_dev, owners
    )
    grad_query = jnp.concatenate(
        [
            lax.dot_general(
                part, keys_head[i], (((0,), (0,)), ((), ())), preferred_element_type=jnp.float32
            )
            for i, part in enumerate((first_t, second_t))
        ],
        axis=1,
    ).astype(jnp.bfloat16)
    grad_keys = jnp.stack(
        [
            jnp.dot(first_t, query_rows[:, :HALF], preferred_element_type=jnp.float32),
            jnp.dot(second_t, query_rows[:, HALF:], preferred_element_type=jnp.float32),
        ]
    )
    return memory, grad_query, grad_values, grad_keys


def head_scores(query_head, key_head, allowed):
    raw_scores = jnp.einsum(
        "qd,kd->qk", query_head, key_head, preferred_element_type=jnp.float32
    ) * HDIM ** (-0.5)
    return jnp.where(allowed, raw_scores, -jnp.inf)


def attend_forward(queries, keys, values, allowed):
    outputs = []
    log_sums = []
    for head_index in range(queries.shape[1] // HDIM):
        columns = slice(head_index * HDIM, (head_index + 1) * HDIM)
        scores = head_scores(queries[:, columns], keys[:, columns], allowed)
        peak_score = jnp.max(scores, axis=1, keepdims=True)
        exp_scores = jnp.exp(scores - peak_score)
        row_sum = jnp.sum(exp_scores, axis=1, keepdims=True)
        probabilities = (exp_scores / row_sum).astype(jnp.bfloat16)
        outputs.append(
            jnp.dot(probabilities, values[:, columns], preferred_element_type=jnp.float32)
        )
        log_sums.append(peak_score[:, 0] + jnp.log(row_sum[:, 0]))
    return (jnp.concatenate(outputs, axis=1), jnp.stack(log_sums))


def attend_backward(queries, keys, values, allowed, log_sums, grad_out):
    grad_queries = []
    grad_keys = []
    grad_values = []
    for head_index in range(queries.shape[1] // HDIM):
        columns = slice(head_index * HDIM, (head_index + 1) * HDIM)
        query_head = queries[:, columns]
        key_head = keys[:, columns]
        value_head = values[:, columns]
        grad_head = grad_out[:, columns]
        scores = head_scores(query_head, key_head, allowed)
        probabilities = jnp.exp(scores - log_sums[head_index][:, None])
        grad_probs = jnp.einsum(
            "qd,kd->qk", grad_head, value_head, preferred_element_type=jnp.float32
        )
        inner_sum = jnp.sum(probabilities * grad_probs, axis=1, keepdims=True)
        grad_scores = (probabilities * (grad_probs - inner_sum)).astype(jnp.bfloat16)
        grad_queries.append(
            jnp.dot(grad_scores, key_head, preferred_element_type=jnp.float32) * HDIM ** (-0.5)
        )
        grad_keys.append(
            jnp.einsum("qk,qd->kd", grad_scores, query_head, preferred_element_type=jnp.float32)
            * HDIM ** (-0.5)
        )
        grad_values.append(
            jnp.einsum(
                "qk,qd->kd",
                probabilities.astype(jnp.bfloat16),
                grad_head,
                preferred_element_type=jnp.float32,
            )
        )
    stacked = jnp.stack([jnp.concatenate(grad_keys, axis=1), jnp.concatenate(grad_values, axis=1)])
    return (jnp.concatenate(grad_queries, axis=1), stacked)


def dense(left, right):
    return jnp.dot(left, right, preferred_element_type=jnp.float32)


def dense_nt(left, right):
    return lax.dot_general(left, right, (((1,), (1,)), ((), ())), preferred_element_type=jnp.float32)


def dense_tn(left, right):
    return lax.dot_general(left, right, (((0,), (0,)), ((), ())), preferred_element_type=jnp.float32)


def per_device(
    inputs,
    prefix,
    picks,
    gain_attn,
    w_qkv,
    w_attn_out,
    gain_mem,
    w_query,
    w_gate,
    w_proj,
    subkeys,
    values,
    cotangent,
):
    low = jnp.bfloat16
    sizes = grid_sizes()
    width_part = inputs.shape[1]
    own_tokens = picks.shape[0]
    seq_tokens = own_tokens * sizes[2]
    col = lax.axis_index("col")
    col_first = col * width_part
    gain_one = lax.dynamic_slice_in_dim(gain_attn, col_first, width_part)
    gain_two = lax.dynamic_slice_in_dim(gain_mem, col_first, width_part)

    x_own, dy_own, qkv_w, query_w, gate_w, proj_w, attn_w = start_all(
        sizes, inputs, cotangent, w_qkv, w_query, w_gate, w_proj, w_attn_out
    )
    residual = x_own.astype(jnp.float32)
    scale_one = lax.rsqrt(jnp.sum(residual * residual, axis=1, keepdims=True) / D + EPSILON)
    normed_one = (residual * scale_one * gain_attn.astype(jnp.float32)).astype(low)
    qkv = jnp.einsum("tc,jcf->jtf", normed_one, qkv_w, preferred_element_type=jnp.float32).astype(low)
    kv_all = swap_tokens(sizes, qkv[1:])
    allowed = allowed_mask(own_tokens, seq_tokens, col * own_tokens, prefix[0])
    attended_sum, log_sums = attend_forward(qkv[0], kv_all[0], kv_all[1], allowed)
    attended = attended_sum.astype(low)
    hidden, normed_two = join(sizes, dense(attended, attn_w).astype(low), inputs, gain_two)
    query_rows = dense(normed_two, query_w).astype(low)
    gate_value = dense(normed_two, gate_w)
    sigmoid_gate = jax.nn.sigmoid(gate_value)
    silu_gate = gate_value * sigmoid_gate
    grad_gated = dense_nt(dy_own, proj_w)
    grad_memory = (grad_gated * silu_gate).astype(low)
    memory, grad_query, grad_values, grad_keys = memory_all(
        query_rows, grad_memory, picks, subkeys, values
    )
    gated_value = (memory * silu_gate).astype(low)
    out_part = dense(gated_value, proj_w).astype(low)
    grad_gate = (
        grad_gated * memory * sigmoid_gate * (1.0 + gate_value * (1.0 - sigmoid_gate))
    ).astype(low)
    grad_part = (dense_nt(grad_query, query_w) + dense_nt(grad_gate, gate_w)).astype(low)
    output, grad_hidden, grad_hidden_all, gain_two_grad = middle(
        sizes, grad_part, out_part, hidden, cotangent, gain_two
    )
    grad_attended = dense_nt(grad_hidden_all, attn_w).astype(low)
    grad_query_own, grad_kv_part = attend_backward(
        qkv[0], kv_all[0], kv_all[1], allowed, log_sums, grad_attended
    )
    grad_kv = pair_sum(sizes, grad_kv_part)
    grad_q = grad_query_own.astype(low)
    x_part = (
        dense_nt(grad_q, qkv_w[0]) + dense_nt(grad_kv[0], qkv_w[1]) + dense_nt(grad_kv[1], qkv_w[2])
    ).astype(low)
    grad_inputs, gain_sums = last(sizes, x_part, inputs, grad_hidden, gain_one, gain_two_grad)
    gain_rows = gain_sums.reshape(sizes[2], 2, width_part)
    grad_gain_one = gain_rows[:, 0].reshape(-1)
    grad_gain_two = gain_rows[:, 1].reshape(-1)

    def col_sum(grad, dim):
        return lax.psum_scatter(grad.astype(low), "col", scatter_dimension=dim, tiled=True)

    def weight_sum(grad, dim):
        return lax.psum(col_sum(grad, dim), "dp").astype(jnp.float32)

    grad_w_proj = weight_sum(dense_tn(gated_value, dy_own), 1)
    grad_w_query = weight_sum(dense_tn(normed_two, grad_query), 0)
    grad_w_gate = weight_sum(dense_tn(normed_two, grad_gate), 0)
    grad_w_attn_out = weight_sum(dense_tn(attended, grad_hidden_all), 1)
    grad_w_qkv = weight_sum(
        jnp.stack([dense_tn(normed_one, part) for part in (grad_q, grad_kv[0], grad_kv[1])]), 1
    )
    grad_keys = lax.psum_scatter(
        grad_keys.astype(low).reshape(-1, HALF), ("dp", "col"), scatter_dimension=0, tiled=True
    )
    grad_subkeys = (
        lax.all_gather(grad_keys, ("row", "dp", "col"), axis=0, tiled=True)
        .astype(jnp.float32)
        .reshape(subkeys.shape)
    )
    return (
        output,
        grad_inputs,
        grad_gain_one,
        grad_w_qkv,
        grad_w_attn_out,
        grad_gain_two,
        grad_w_query,
        grad_w_gate,
        grad_w_proj,
        grad_subkeys,
        grad_values,
    )


def solution(mesh):
    placed = (
        P(("dp", "row"), "col"),
        P("dp"),
        P(("dp", "col"), None, None),
        P(),
        P(None, "col", "row"),
        P("row", "col"),
        P(),
        P("col", "row"),
        P("col", "row"),
        P("row", "col"),
        P(),
        P(("dp", "row", "col"), None),
        P(("dp", "row"), "col"),
    )
    return jax.shard_map(
        per_device,
        mesh=mesh,
        in_specs=placed,
        out_specs=(
            P(("dp", "row"), "col"),
            P(("dp", "row"), "col"),
            P(),
            P(None, "col", "row"),
            P("row", "col"),
            P(),
            P("col", "row"),
            P("col", "row"),
            P("row", "col"),
            P(),
            P(("dp", "row", "col"), None),
        ),
        check_vma=False,
    )
```

```python
import functools

import jax
import jax.numpy as jnp
from jax import lax
from jax.experimental import pallas as pl
from jax.experimental.pallas import tpu as pltpu
from jax.sharding import PartitionSpec as P

D = 1024
HDIM = 64
HALF = 512
SUBKEYS = 256
TOPK = 32
FBLK = 128


EPSILON = 1e-06


MESH = pl.DeviceIdType.MESH
VMEM = pl.BlockSpec(memory_space=pltpu.VMEM)
ANY = pl.BlockSpec(memory_space=pl.ANY)
DMA = pltpu.SemaphoreType.DMA


def here():
    return lax.axis_index("dp"), lax.axis_index("row"), lax.axis_index("col")


def grid_sizes():
    return lax.axis_size("dp"), lax.axis_size("row"), lax.axis_size("col")


def remote(src, dst, send_sem, recv_sem, device):
    return pltpu.make_async_remote_copy(
        src_ref=src,
        dst_ref=dst,
        send_sem=send_sem,
        recv_sem=recv_sem,
        device_id=device,
        device_id_type=MESH,
    )


def arrived(dst, sem):
    pltpu.make_async_copy(dst, dst, sem).wait()


def greet_plane(spot, sizes):
    barrier = pltpu.get_barrier_semaphore()
    dp, row, col = spot
    _, rows, cols = sizes
    for j in range(rows):
        for k in range(cols):
            if j + k > 0:
                pl.semaphore_signal(
                    barrier,
                    inc=1,
                    device_id=(dp, lax.rem(row + j, rows), lax.rem(col + k, cols)),
                    device_id_type=MESH,
                )
    pl.semaphore_wait(barrier, rows * cols - 1)


def greet_partner(spot, sizes):
    barrier = pltpu.get_barrier_semaphore()
    dp, row, col = spot
    pl.semaphore_signal(barrier, inc=1, device_id=(dp, row, 1 - col), device_id_type=MESH)
    pl.semaphore_wait(barrier, 1)


def device_of(index, sizes):
    _, rows, cols = sizes
    return (
        lax.div(index, rows * cols),
        lax.rem(lax.div(index, cols), rows),
        lax.rem(index, cols),
    )


def index_of(spot, sizes):
    return (spot[0] * sizes[1] + spot[1]) * sizes[2] + spot[2]


def greet_all(spot, sizes):
    barrier = pltpu.get_barrier_semaphore()
    count = sizes[0] * sizes[1] * sizes[2]
    me = index_of(spot, sizes)

    def greet(step, carry):
        pl.semaphore_signal(
            barrier,
            inc=1,
            device_id=device_of(lax.rem(me + step, count), sizes),
            device_id_type=MESH,
        )
        return carry

    lax.fori_loop(1, count, greet, 0)
    pl.semaphore_wait(barrier, count - 1)


class Gather:
    def __init__(self, spot, sizes, src, dst, send, recv):
        self.spot, self.sizes, self.src, self.dst = spot, sizes, src, dst
        self.send, self.recv = send, recv
        self.tokens, self.width = src.shape
        dp, row, col = spot
        _, rows, cols = sizes
        self.half = rows // cols
        self.target = lax.div(row, self.half)
        self.slot = lax.rem(row, self.half) * cols + col
        first = pl.multiple_of(lax.rem(row, self.half) * self.tokens, self.tokens)
        left = pl.multiple_of(col * self.width, self.width)
        self.there = dst.at[pl.ds(first, self.tokens), pl.ds(left, self.width)]

    def copy(self, step):
        dp, row, _ = self.spot
        device = (dp, lax.rem(row + step, self.sizes[1]), self.target)
        return remote(self.src, self.there, self.send.at[step], self.recv.at[self.slot], device)

    def start(self):
        col = self.spot[2]

        for step in range(1, self.sizes[1]):
            self.copy(step).start()

        @pl.when(self.target == col)
        def _():
            pltpu.make_async_copy(self.src, self.there, self.recv.at[self.slot]).start()

        @pl.when(self.target != col)
        def _():
            self.copy(0).start()

    def wait(self):
        cols = self.sizes[2]
        for i in range(self.half):
            for k in range(cols):
                arrived(
                    self.dst.at[pl.ds(i * self.tokens, self.tokens), pl.ds(k * self.width, self.width)],
                    self.recv.at[i * cols + k],
                )
        for step in range(1, self.sizes[1]):
            self.copy(step).wait_send()

        @pl.when(self.target != self.spot[2])
        def _():
            self.copy(0).wait_send()


class Scatter:
    def __init__(self, spot, sizes, src, landing, send, recv):
        self.spot, self.sizes, self.src, self.landing = spot, sizes, src, landing
        self.send, self.recv = send, recv
        _, self.tokens, self.width = landing.shape
        self.half = sizes[1] // sizes[2]

    def parts(self):
        dp, row, col = self.spot
        cols = self.sizes[2]
        for i in range(self.half):
            for k in range(cols):
                piece = self.src.at[
                    pl.ds(i * self.tokens, self.tokens), pl.ds(k * self.width, self.width)
                ]
                target = col * self.half + i
                mine = jnp.logical_and(target == row, col == k)
                there = self.landing.at[row]
                copy = remote(
                    piece, there, self.send.at[i * cols + k], self.recv.at[row], (dp, target, k)
                )
                yield mine, copy, pltpu.make_async_copy(piece, there, self.recv.at[row])

    def start(self):
        for mine, copy, own in self.parts():
            pl.when(jnp.logical_not(mine))(copy.start)
            pl.when(mine)(own.start)

    def wait(self):
        for q in range(self.sizes[1]):
            arrived(self.landing.at[q], self.recv.at[q])

    def wait_send(self):
        for mine, copy, _ in self.parts():
            pl.when(jnp.logical_not(mine))(copy.wait_send)


def plane_sems(sizes):
    rows, cols = sizes[1], sizes[2]
    return [DMA((rows,)), DMA((rows,))]


def start_kernel(sizes, *refs):
    x, dy, wqkv, wquery, wgate, wproj, wattn = refs[:7]
    xs, dys, wqkv_all, wquery_all, wgate_all, wproj_all, wattn_all = refs[7:14]
    xsend, xrecv, ysend, yrecv, wsend, wrecv, wlocal = refs[14:]
    spot = here()
    dp, row, col = spot
    greet_plane(spot, sizes)
    gather_x = Gather(spot, sizes, x, xs, xsend, xrecv)
    gather_y = Gather(spot, sizes, dy, dys, ysend, yrecv)
    gather_x.start()
    gather_y.start()
    copies = []
    for n, (src, dst, dim) in enumerate(
        (
            (wqkv, wqkv_all, 1),
            (wquery, wquery_all, 0),
            (wgate, wgate_all, 0),
            (wproj, wproj_all, 1),
            (wattn, wattn_all, 1),
        )
    ):
        size = src.shape[dim]
        window = [slice(None)] * len(src.shape)
        window[dim] = pl.ds(pl.multiple_of(col * size, size), size)
        there = dst.at[tuple(window)]
        away = remote(src, there, wsend.at[n], wrecv.at[n], (dp, row, 1 - col))
        own = pltpu.make_async_copy(src, there, wlocal.at[n])
        away.start()
        own.start()
        copies += [away, own]
    for copy in copies:
        copy.wait()
    gather_x.wait()
    gather_y.wait()


def start_all(sizes, x, dy, wqkv, wquery, wgate, wproj, wattn):
    tokens, width = x.shape
    half = sizes[1] // sizes[2]
    cols = sizes[2]
    low = jnp.bfloat16

    def twice(operand, dim):
        shape = list(operand.shape)
        shape[dim] *= cols
        return jax.ShapeDtypeStruct(tuple(shape), low)

    whole = jax.ShapeDtypeStruct((half * tokens, cols * width), low)
    return pl.pallas_call(
        functools.partial(start_kernel, sizes),
        in_specs=[VMEM] * 7,
        out_specs=[ANY] * 7,
        out_shape=[
            whole,
            whole,
            twice(wqkv, 1),
            twice(wquery, 0),
            twice(wgate, 0),
            twice(wproj, 1),
            twice(wattn, 1),
        ],
        scratch_shapes=plane_sems(sizes) * 2 + [DMA((5,))] * 3,
        compiler_params=pltpu.CompilerParams(collective_id=0, has_side_effects=True),
        name="start_all",
    )(x, dy, wqkv, wquery, wgate, wproj, wattn)


def swap_kernel(sizes, src, dst, send, recv, own):
    spot = here()
    dp, row, col = spot
    greet_partner(spot, sizes)
    size = src.shape[1]
    there = dst.at[:, pl.ds(pl.multiple_of(col * size, size), size)]
    away = remote(src, there, send, recv, (dp, row, 1 - col))
    local = pltpu.make_async_copy(src, there, own)
    away.start()
    local.start()
    away.wait()
    local.wait()


def swap_tokens(sizes, src):
    shape = (src.shape[0], src.shape[1] * sizes[2], src.shape[2])
    return pl.pallas_call(
        functools.partial(swap_kernel, sizes),
        in_specs=[VMEM],
        out_specs=VMEM,
        out_shape=jax.ShapeDtypeStruct(shape, src.dtype),
        scratch_shapes=[DMA, DMA, DMA],
        compiler_params=pltpu.CompilerParams(collective_id=1, has_side_effects=True),
        name="swap_tokens",
    )(src)


def pair_sum_kernel(sizes, src, out, landing, send, recv):
    spot = here()
    dp, row, col = spot
    greet_partner(spot, sizes)
    size = landing.shape[1]
    other = pl.multiple_of((1 - col) * size, size)
    away = remote(src.at[:, pl.ds(other, size)], landing, send, recv, (dp, row, 1 - col))
    away.start()
    away.wait()
    own = src[:, pl.ds(pl.multiple_of(col * size, size), size)]
    out[...] = (own + landing[...]).astype(out.dtype)


def pair_sum(sizes, src):
    shape = (src.shape[0], src.shape[1] // sizes[2], src.shape[2])
    return pl.pallas_call(
        functools.partial(pair_sum_kernel, sizes),
        in_specs=[VMEM],
        out_specs=VMEM,
        out_shape=jax.ShapeDtypeStruct(shape, jnp.bfloat16),
        scratch_shapes=[pltpu.VMEM(shape, src.dtype), DMA, DMA],
        compiler_params=pltpu.CompilerParams(collective_id=2, has_side_effects=True),
        name="pair_sum",
    )(src)


def fold(column):
    return jnp.broadcast_to(column, (column.shape[0], 128))


def join_kernel(
    sizes, part, x, gain, hidden, normed_all, landing, mine, theirs, block,
    ssend, srecv, gsend, grecv, psend, precv,
):
    spot = here()
    dp, row, col = spot
    greet_plane(spot, sizes)
    scatter = Scatter(spot, sizes, part, landing, ssend, srecv)
    scatter.start()
    scatter.wait()
    total = x[...].astype(jnp.float32)
    for q in range(sizes[1]):
        total = total + landing[q].astype(jnp.float32)
    hidden[...] = total
    mine[...] = fold(jnp.sum(total * total, axis=1, keepdims=True))
    pair = remote(mine, theirs, psend, precv, (dp, row, 1 - col))
    pair.start()
    pair.wait()
    squares = mine[:, :1] + theirs[:, :1]
    scale = lax.rsqrt(squares / D + EPSILON)
    block[...] = (hidden[...] * scale * gain[...].astype(jnp.float32)).astype(jnp.bfloat16)
    gather = Gather(spot, sizes, block, normed_all, gsend, grecv)
    gather.start()
    scatter.wait_send()
    gather.wait()


def join(sizes, part, x, gain):
    tokens, width = x.shape
    rows = sizes[1]
    return pl.pallas_call(
        functools.partial(join_kernel, sizes),
        in_specs=[VMEM] * 3,
        out_specs=[VMEM, VMEM],
        out_shape=[
            jax.ShapeDtypeStruct((tokens, width), jnp.float32),
            jax.ShapeDtypeStruct(part.shape, jnp.bfloat16),
        ],
        scratch_shapes=[
            pltpu.VMEM((rows, tokens, width), jnp.bfloat16),
            pltpu.VMEM((tokens, 128), jnp.float32),
            pltpu.VMEM((tokens, 128), jnp.float32),
            pltpu.VMEM((tokens, width), jnp.bfloat16),
        ]
        + plane_sems(sizes) * 2
        + [DMA, DMA],
        compiler_params=pltpu.CompilerParams(collective_id=3, has_side_effects=True),
        name="join",
    )(part, x, gain[None])


def norm_back(sizes, spot, landing, base, above, gain, mine, theirs, psend, precv):
    dp, row, col = spot
    normed_grad = landing[0].astype(jnp.float32)
    for q in range(1, sizes[1]):
        normed_grad = normed_grad + landing[q].astype(jnp.float32)
    values = base[...].astype(jnp.float32)
    unit_grad = normed_grad * gain[...].astype(jnp.float32)
    mine[0] = fold(jnp.sum(values * values, axis=1, keepdims=True))
    mine[1] = fold(jnp.sum(unit_grad * values, axis=1, keepdims=True))
    pair = remote(mine, theirs, psend, precv, (dp, row, 1 - col))
    pair.start()
    pair.wait()
    scale = lax.rsqrt((mine[0, :, :1] + theirs[0, :, :1]) / D + EPSILON)
    inner = scale * (mine[1, :, :1] + theirs[1, :, :1]) / D
    unit = values * scale
    grad = above[...].astype(jnp.float32) + scale * (unit_grad - unit * inner)
    return grad, jnp.sum(normed_grad * unit, axis=0, keepdims=True)


def slab(ref, dim, index, count):
    size = ref.shape[dim] // count
    window = [slice(None)] * len(ref.shape)
    window[dim] = pl.ds(pl.multiple_of(index * size, size), size)
    return ref.at[tuple(window)]


def add_into(target, addend):
    target[...] = (target[...].astype(jnp.float32) + addend[...].astype(jnp.float32)).astype(
        target.dtype
    )


class PairSum:
    def __init__(self, spot, sizes, terms, dims, halves, landings, send, recv):
        self.col, self.cols = spot[2], sizes[2]
        self.terms, self.dims, self.halves, self.landings = terms, dims, halves, landings
        self.copies = [
            remote(
                slab(term, dim, 1 - spot[2], sizes[2]), landing, send.at[n], recv.at[n],
                (spot[0], spot[1], 1 - spot[2]),
            )
            for n, (term, dim, landing) in enumerate(zip(terms, dims, landings))
        ]

    def start(self):
        for copy in self.copies:
            copy.start()

    def finish(self):
        for copy, term, dim, half, landing in zip(
            self.copies, self.terms, self.dims, self.halves, self.landings
        ):
            copy.wait()
            own = slab(term, dim, self.col, self.cols)
            half[...] = (own[...].astype(jnp.float32) + landing[...].astype(jnp.float32)).astype(
                half.dtype
            )


class LineReduce:
    def __init__(self, spot, sizes, arrays, dims, below, above, sems):
        self.spot, self.count = spot, sizes[0]
        self.arrays, self.dims, self.below, self.above = arrays, dims, below, above
        self.up_send, self.up_recv, self.down_send, self.down_recv = sems

    def copy(self, n, k, up):
        dp, row, col = self.spot
        landing = self.below[n] if up else self.above[n]
        send, recv = (
            (self.up_send, self.up_recv) if up else (self.down_send, self.down_recv)
        )
        dim = self.dims[n]
        return remote(
            slab(self.arrays[n], dim, k, self.count),
            slab(landing, dim, k, self.count),
            send.at[n, k],
            recv.at[n, k],
            (jnp.clip(dp + (1 if up else -1), 0, self.count - 1), row, col),
        )

    def send(self, k, up):
        for n in range(len(self.arrays)):
            self.copy(n, k, up).start()

    def start(self):
        dp, last = self.spot[0], self.count - 1

        @pl.when(dp == 0)
        def _():
            lax.fori_loop(0, last, lambda i, c: (self.send(last - i, True), c)[1], 0)

        @pl.when(dp == last)
        def _():
            lax.fori_loop(0, last, lambda i, c: (self.send(i, False), c)[1], 0)

    def take(self, k, up):
        for n, (array, dim) in enumerate(zip(self.arrays, self.dims)):
            landing = slab((self.below if up else self.above)[n], dim, k, self.count)
            arrived(landing, (self.up_recv if up else self.down_recv).at[n, k])
            add_into(slab(array, dim, k, self.count), landing)

    def event(self, time):
        dp, last = self.spot[0], self.count - 1

        @pl.when(jnp.logical_and(dp > 0, time >= dp))
        def _():
            k = dp + last - time
            self.take(k, True)
            pl.when(k > dp)(lambda: self.send(k, True))

        @pl.when(jnp.logical_and(dp < last, time >= last - dp))
        def _():
            k = time - (last - dp)
            self.take(k, False)
            pl.when(k < dp)(lambda: self.send(k, False))

    def events(self):
        lax.fori_loop(1, self.count, lambda time, c: (self.event(time), c)[1], 0)

    def finish(self):
        dp = self.spot[0]

        def one(k, carry):
            @pl.when(dp < k)
            def _():
                for n in range(len(self.arrays)):
                    self.copy(n, k, True).wait_send()

            @pl.when(dp > k)
            def _():
                for n in range(len(self.arrays)):
                    self.copy(n, k, False).wait_send()

            return carry

        lax.fori_loop(0, self.count, one, 0)


class LineGather:
    def __init__(self, spot, sizes, arrays, dims, sems):
        self.spot, self.count = spot, sizes[0]
        self.arrays, self.dims = arrays, dims
        self.up_send, self.down_send, self.recv = sems

    def copy(self, n, k, up):
        dp, row, col = self.spot
        part = slab(self.arrays[n], self.dims[n], k, self.count)
        return remote(
            part,
            part,
            (self.up_send if up else self.down_send).at[n, k],
            self.recv.at[n, k],
            (jnp.clip(dp + (1 if up else -1), 0, self.count - 1), row, col),
        )

    def send(self, k, up):
        dp = self.spot[0]

        @pl.when(dp < self.count - 1 if up else dp > 0)
        def _():
            for n in range(len(self.arrays)):
                self.copy(n, k, up).start()

    def start(self):
        self.send(self.spot[0], True)
        self.send(self.spot[0], False)

    def take(self, k):
        for n, (array, dim) in enumerate(zip(self.arrays, self.dims)):
            arrived(slab(array, dim, k, self.count), self.recv.at[n, k])

    def event(self, time):
        dp = self.spot[0]

        @pl.when(dp - time >= 0)
        def _():
            self.take(dp - time)
            self.send(dp - time, True)

        @pl.when(dp + time < self.count)
        def _():
            self.take(dp + time)
            self.send(dp + time, False)

    def events(self):
        lax.fori_loop(1, self.count, lambda time, c: (self.event(time), c)[1], 0)

    def finish(self):
        dp, last = self.spot[0], self.count - 1

        def one(k, carry):
            @pl.when(jnp.logical_and(k <= dp, dp < last))
            def _():
                for n in range(len(self.arrays)):
                    self.copy(n, k, True).wait_send()

            @pl.when(jnp.logical_and(k >= dp, dp > 0))
            def _():
                for n in range(len(self.arrays)):
                    self.copy(n, k, False).wait_send()

            return carry

        lax.fori_loop(0, self.count, one, 0)


def line_sems(sizes, arrays, kinds):
    return [DMA((arrays, sizes[0])) for _ in range(kinds)]


def greet_cross(spot, sizes):
    barrier = pltpu.get_barrier_semaphore()
    dp, row, col = spot
    dps, rows, cols = sizes
    for j in range(rows):
        for k in range(cols):
            if j + k > 0:
                pl.semaphore_signal(
                    barrier,
                    inc=1,
                    device_id=(dp, lax.rem(row + j, rows), lax.rem(col + k, cols)),
                    device_id_type=MESH,
                )
    for j in (1, dps - 1):
        pl.semaphore_signal(
            barrier, inc=1, device_id=(lax.rem(dp + j, dps), row, col), device_id_type=MESH
        )
    pl.semaphore_wait(barrier, rows * cols + 1)


FIRST_DIMS = (0, 0, 0, 0)
FIRST_COLS = (0, 0, 1, 0)
LAST_DIMS = (1, 0)
LAST_COLS = (1, 1)


def halved(shape, dim, cols):
    shape = list(shape)
    shape[dim] //= cols
    return tuple(shape)


def middle_kernel(sizes, *refs):
    part, out_part, hidden, dy, gain = refs[:5]
    terms = refs[5:9]
    output, grad, grad_all, gain_grad = refs[9:13]
    shards = refs[13:17]
    landing, out_landing, mine, theirs, block = refs[17:22]
    halves, pair_land, below, above = refs[22:26], refs[26:30], refs[30:34], refs[34:38]
    (
        ssend, srecv, osend, orecv, gsend, grecv, psend, precv, hsend, hrecv, *line
    ) = refs[38:]
    spot = here()
    greet_cross(spot, sizes)
    scatter = Scatter(spot, sizes, part, landing, ssend, srecv)
    scatter.start()
    pair = PairSum(spot, sizes, terms, FIRST_COLS, halves, pair_land, hsend, hrecv)
    pair.start()
    out_scatter = Scatter(spot, sizes, out_part, out_landing, osend, orecv)
    out_scatter.start()
    pair.finish()
    reduce = LineReduce(spot, sizes, halves, FIRST_DIMS, below, above, line)
    reduce.start()
    scatter.wait()
    total, gains = norm_back(sizes, spot, landing, hidden, dy, gain, mine, theirs, psend, precv)
    gain_grad[...] = gains
    grad[...] = total
    block[...] = total.astype(jnp.bfloat16)
    gather = Gather(spot, sizes, block, grad_all, gsend, grecv)
    gather.start()
    reduce.event(1)
    out_scatter.wait()
    result = hidden[...]
    for q in range(sizes[1]):
        result = result + out_landing[q].astype(jnp.float32)
    output[...] = result.astype(jnp.bfloat16)
    lax.fori_loop(2, sizes[0], lambda time, c: (reduce.event(time), c)[1], 0)
    for half, dim, shard in zip(halves, FIRST_DIMS, shards):
        shard[...] = slab(half, dim, spot[0], sizes[0])[...]
    scatter.wait_send()
    out_scatter.wait_send()
    gather.wait()
    reduce.finish()


def middle(sizes, part, out_part, hidden, dy, gain, terms):
    tokens, width = hidden.shape
    dps, rows, cols = sizes
    low, wide = jnp.bfloat16, jnp.float32
    halves = [halved(t.shape, d, cols) for t, d in zip(terms, FIRST_COLS)]
    shards = [halved(h, d, dps) for h, d in zip(halves, FIRST_DIMS)]
    return pl.pallas_call(
        functools.partial(middle_kernel, sizes),
        in_specs=[VMEM] * 9,
        out_specs=[VMEM] * 8,
        out_shape=[
            jax.ShapeDtypeStruct((tokens, width), low),
            jax.ShapeDtypeStruct((tokens, width), wide),
            jax.ShapeDtypeStruct(part.shape, low),
            jax.ShapeDtypeStruct((1, width), wide),
        ]
        + [jax.ShapeDtypeStruct(s, low) for s in shards],
        scratch_shapes=[
            pltpu.VMEM((rows, tokens, width), low),
            pltpu.VMEM((rows, tokens, width), low),
            pltpu.VMEM((2, tokens, 128), wide),
            pltpu.VMEM((2, tokens, 128), wide),
            pltpu.VMEM((tokens, width), low),
        ]
        + [pltpu.VMEM(h, low) for h in halves] * 4
        + plane_sems(sizes) * 3
        + [DMA, DMA, DMA((4,)), DMA((4,))]
        + line_sems(sizes, 4, 4),
        compiler_params=pltpu.CompilerParams(collective_id=4, has_side_effects=True),
        name="middle",
    )(part, out_part, hidden, dy, gain[None], *terms)


def last_kernel(sizes, *refs):
    part, x, above_grad, gain, other_gain = refs[:5]
    shards, terms = refs[5:9], refs[9:11]
    table, grads_all = refs[11:13]
    grad, gain_sums, row_grads = refs[13:16]
    firsts, lasts, keys_all = refs[16:20], refs[20:22], refs[22]
    landing, mine, theirs, own_gain, gain_landing, tables, chunks = refs[23:30]
    halves, pair_land, below, above = refs[30:32], refs[32:34], refs[34:36], refs[36:38]
    (
        ssend, srecv, psend, precv, bsend, brecv, hsend, hrecv, tsem, csem,
        xsend, xrecv, kxsend, kxrecv, *line
    ) = refs[38:]
    spot = here()
    dp, row, col = spot
    dps, rows, cols = sizes
    count = dps * rows * cols
    me = index_of(spot, sizes)
    loads = dps * cols

    def load(index):
        slot = lax.rem(index, 2)
        where = (lax.div(index, cols), lax.rem(index, cols))
        return (
            pltpu.make_async_copy(table.at[where], tables.at[slot], tsem.at[slot]),
            pltpu.make_async_copy(grads_all.at[where], chunks.at[slot], csem.at[slot]),
        )

    for copy in load(0):
        copy.start()
    greet_all(spot, sizes)
    scatter = Scatter(spot, sizes, part, landing, ssend, srecv)
    scatter.start()
    pair = PairSum(spot, sizes, terms, LAST_COLS, halves, pair_land, hsend, hrecv)
    pair.start()
    for first, dim, shard in zip(firsts, FIRST_DIMS, shards):
        slab(first, dim, dp, dps)[...] = shard[...]
    gather = LineGather(spot, sizes, firsts, FIRST_DIMS, line[:3])
    gather.start()
    pair.finish()
    reduce = LineReduce(spot, sizes, halves, LAST_DIMS, below, above, line[3:7])
    reduce.start()

    def product(index):
        slot = lax.rem(index, 2)
        for copy in load(index):
            copy.wait()

        @pl.when(index + 1 < loads)
        def _():
            for copy in load(index + 1):
                copy.start()

        def strip(n, carry):
            columns = pl.ds(pl.multiple_of(n * 256, 256), 256)
            term = lax.dot_general(
                tables[slot, :, columns],
                chunks[slot],
                (((0,), (0,)), ((), ())),
                preferred_element_type=jnp.float32,
            )

            @pl.when(index == 0)
            def _():
                row_grads[columns] = term

            @pl.when(index > 0)
            def _():
                row_grads[columns] = row_grads[columns] + term

            return carry

        lax.fori_loop(0, tables.shape[2] // 256, strip, 0)

    def products(first, end):
        lax.fori_loop(first, end, lambda index, c: (product(index), c)[1], 0)

    products(0, loads // 4)
    scatter.wait()
    total, gains = norm_back(sizes, spot, landing, x, above_grad, gain, mine, theirs, psend, precv)
    lines = gains.shape[1] // 128
    for line_index in range(lines):
        columns = slice(line_index * 128, (line_index + 1) * 128)
        own_gain[line_index : line_index + 1] = gains[:, columns]
        own_gain[lines + line_index : lines + line_index + 1] = other_gain[:, columns]

    def tell(step, carry):
        device = device_of(lax.rem(me + step, count), sizes)
        remote(own_gain, gain_landing.at[me], bsend, brecv, device).start()
        return carry

    lax.fori_loop(1, count, tell, 0)
    gain_landing[me] = own_gain[...]
    grad[...] = total
    gather.event(1)
    reduce.event(1)
    products(loads // 4, loads // 2)
    lax.fori_loop(2, dps, lambda time, c: (gather.event(time), reduce.event(time), c)[2], 0)
    for first, half, dim in zip(lasts, halves, LAST_DIMS):
        slab(first, dim, dp, dps)[...] = slab(half, dim, dp, dps)[...]
    final = LineGather(spot, sizes, lasts, LAST_DIMS, line[7:10])
    final.start()
    keys = firsts[3]

    def sideways(k):
        return remote(
            keys, keys_all.at[row, col], xsend, xrecv.at[rows - k],
            (dp, lax.rem(row + k, rows), col),
        )

    def cross(src, k):
        there = keys_all.at[lax.rem(row + k, rows), col]
        return remote(src, there, kxsend, kxrecv, (dp, row, 1 - col))

    for k in range(1, rows):
        sideways(k).start()
    cross(keys, 0).start()
    keys_all[row, col] = keys[...]
    products(loads // 2, 3 * loads // 4)
    final.event(1)
    for k in range(1, rows):
        landed = keys_all.at[lax.rem(row + k, rows), col]
        arrived(landed, xrecv.at[k])
        cross(landed, k).start()
    products(3 * loads // 4, loads)
    lax.fori_loop(2, dps, lambda time, c: (final.event(time), c)[1], 0)
    arrived(keys_all.at[:, 1 - col], kxrecv)
    scatter.wait_send()
    arrived(gain_landing.at[pl.ds(0, count - 1)], brecv)
    for c in range(cols):

        def add(index, sums):
            return sums + gain_landing[index * cols + c]

        gain_sums[c] = lax.fori_loop(0, dps * rows, add, jnp.zeros(own_gain.shape, jnp.float32))
    arrived(gain_landing.at[pl.ds(0, count - 1)], bsend)
    arrived(keys_all.at[:, col], kxsend)
    arrived(keys_all.at[pl.ds(0, rows - 1), col], xsend)
    gather.finish()
    reduce.finish()
    final.finish()


def last(sizes, part, x, above, gain, other_gain, shards, terms, table, grads_all):
    tokens, width = x.shape
    dps, rows, cols = sizes
    lines = 2 * width // 128
    count = dps * rows * cols
    low, wide = jnp.bfloat16, jnp.float32
    shape = jax.ShapeDtypeStruct

    def grown(shard, dim):
        full = list(shard.shape)
        full[dim] *= dps
        return tuple(full)

    firsts = [grown(s, d) for s, d in zip(shards, FIRST_DIMS)]
    halves = [halved(t.shape, d, cols) for t, d in zip(terms, LAST_COLS)]
    rows_dev = table.shape[-1]
    features = grads_all.shape[-1]
    chunk = table.shape[2]
    return pl.pallas_call(
        functools.partial(last_kernel, sizes),
        in_specs=[VMEM] * 11 + [ANY] * 2,
        out_specs=[VMEM] * 10,
        out_shape=[
            shape((tokens, width), wide),
            shape((cols, lines, 128), wide),
            shape((rows_dev, features), wide),
        ]
        + [shape(s, low) for s in firsts + halves]
        + [shape((rows, cols) + firsts[3], low)],
        scratch_shapes=[
            pltpu.VMEM((rows, tokens, width), low),
            pltpu.VMEM((2, tokens, 128), wide),
            pltpu.VMEM((2, tokens, 128), wide),
            pltpu.VMEM((lines, 128), wide),
            pltpu.VMEM((count, lines, 128), wide),
            pltpu.VMEM((2, chunk, rows_dev), low),
            pltpu.VMEM((2, chunk, features), low),
        ]
        + [pltpu.VMEM(h, low) for h in halves] * 4
        + plane_sems(sizes)
        + [DMA, DMA, DMA, DMA, DMA((2,)), DMA((2,)), DMA((2,)), DMA((2,))]
        + [DMA, DMA((rows,)), DMA, DMA]
        + line_sems(sizes, 4, 3)
        + line_sems(sizes, 2, 7),
        compiler_params=pltpu.CompilerParams(collective_id=5, has_side_effects=True),
        name="last",
    )(part, x, above, gain[None], other_gain, *shards, *terms, table, grads_all)


def allowed_mask(query_count, key_count, first_pos, prefix_len):
    query_pos = first_pos + lax.iota(jnp.int32, query_count)
    key_pos = lax.iota(jnp.int32, key_count)
    return (key_pos[None, :] <= query_pos[:, None]) | (key_pos[None, :] < prefix_len)


def flat_picks(picks_head):
    blocks = picks_head.shape[0] // FBLK
    return jnp.swapaxes(picks_head.reshape(blocks, FBLK, TOPK), 1, 2).reshape(blocks, TOPK * FBLK)


def one_hot(row_values, size):
    hot = lax.broadcasted_iota(jnp.int32, (size, row_values.shape[1]), 0) == row_values
    return jnp.where(hot, 1.0, 0.0).astype(jnp.bfloat16)


def route_kernel(rows_dev, owners, cap, picks_ref, rank_ref, meta_ref):
    lane = lax.broadcasted_iota(jnp.int32, (FBLK, FBLK), 0)
    before = jnp.where(lane < lax.broadcasted_iota(jnp.int32, (FBLK, FBLK), 1), 1.0, 0.0).astype(
        jnp.bfloat16
    )
    picks = picks_ref[0]
    owner = picks // rows_dev
    local = picks % rows_dev
    hot = one_hot(owner, owners)
    running = jnp.zeros((owners, 1), jnp.float32)
    ranks = []
    for chunk in range(picks.shape[1] // FBLK):
        part = hot[:, chunk * FBLK : (chunk + 1) * FBLK]
        earlier = jnp.dot(part, before, preferred_element_type=jnp.float32)
        wide = part.astype(jnp.float32)
        ranks.append(jnp.sum(wide * (earlier + running), axis=0, keepdims=True))
        running = running + jnp.sum(wide, axis=1, keepdims=True)
    rank = jnp.concatenate(ranks, axis=1).astype(jnp.int32)
    rank_ref[0] = rank
    slot_hot = one_hot(rank, cap)
    token = lax.broadcasted_iota(jnp.int32, picks.shape, 1) % FBLK
    outs = []
    for payload in (local % SUBKEYS, local // SUBKEYS, token):
        scaled = hot * payload.astype(jnp.float32).astype(jnp.bfloat16)
        outs.append(
            lax.dot_general(
                scaled, slot_hot, (((1,), (1,)), ((), ())), preferred_element_type=jnp.float32
            ).astype(jnp.int32)
        )
    meta_ref[0] = (outs[1] * FBLK + outs[2]) * SUBKEYS + outs[0]


def route(flat, rows_dev, owners, cap):
    blocks, count = flat.shape
    rank, meta = pl.pallas_call(
        functools.partial(route_kernel, rows_dev, owners, cap),
        grid=(blocks,),
        in_specs=[pl.BlockSpec((1, 1, count), lambda i: (i, 0, 0))],
        out_specs=[
            pl.BlockSpec((1, 1, count), lambda i: (i, 0, 0)),
            pl.BlockSpec((1, owners, cap), lambda i: (i, 0, 0)),
        ],
        out_shape=[
            jax.ShapeDtypeStruct((blocks, 1, count), jnp.int32),
            jax.ShapeDtypeStruct((blocks, owners, cap), jnp.int32),
        ],
        name="route",
    )(flat[:, None, :])
    return rank, meta


def weigh_kernel(rows_dev, owners, cap, query_ref, keys_ref, picks_ref, rank_ref, weights_ref, slots_ref):
    picks = picks_ref[0]
    first = lax.dot_general(
        keys_ref[0], query_ref[:, :HALF], (((1,), (1,)), ((), ())), preferred_element_type=jnp.float32
    )
    second = lax.dot_general(
        keys_ref[1], query_ref[:, HALF:], (((1,), (1,)), ((), ())), preferred_element_type=jnp.float32
    )
    upper = picks // SUBKEYS
    lower = picks % SUBKEYS
    key_id = lax.broadcasted_iota(jnp.int32, (SUBKEYS, FBLK), 0)
    rows = []
    for pick in range(TOPK):
        columns = slice(pick * FBLK, (pick + 1) * FBLK)
        chosen = jnp.where(key_id == upper[:, columns], first, 0.0) + jnp.where(
            key_id == lower[:, columns], second, 0.0
        )
        rows.append(jnp.sum(chosen, axis=0, keepdims=True))
    scores = jnp.concatenate(rows, axis=0)
    powers = jnp.exp(scores - jnp.max(scores, axis=0, keepdims=True))
    weights = powers / jnp.sum(powers, axis=0, keepdims=True)
    weights_ref[0] = weights
    flat = jnp.concatenate([weights[pick : pick + 1] for pick in range(TOPK)], axis=1)
    scaled = one_hot(picks // rows_dev, owners) * flat.astype(jnp.bfloat16)
    slots_ref[0] = lax.dot_general(
        scaled,
        one_hot(rank_ref[0], cap),
        (((1,), (1,)), ((), ())),
        preferred_element_type=jnp.float32,
    ).astype(jnp.bfloat16)


def weigh(query_rows, keys_head, flat, rank, rows_dev, owners, cap):
    blocks, count = flat.shape
    return pl.pallas_call(
        functools.partial(weigh_kernel, rows_dev, owners, cap),
        grid=(blocks,),
        in_specs=[
            pl.BlockSpec((FBLK, 2 * HALF), lambda i: (i, 0)),
            pl.BlockSpec((2, SUBKEYS, HALF), lambda i: (0, 0, 0)),
            pl.BlockSpec((1, 1, count), lambda i: (i, 0, 0)),
            pl.BlockSpec((1, 1, count), lambda i: (i, 0, 0)),
        ],
        out_specs=[
            pl.BlockSpec((1, TOPK, FBLK), lambda i: (i, 0, 0)),
            pl.BlockSpec((1, owners, cap), lambda i: (i, 0, 0)),
        ],
        out_shape=[
            jax.ShapeDtypeStruct((blocks, TOPK, FBLK), jnp.float32),
            jax.ShapeDtypeStruct((blocks, owners, cap), jnp.bfloat16),
        ],
        name="weigh",
    )(query_rows, keys_head, flat[:, None, :], rank)


def own_block(tokens_ref, dp, col, row, width):
    left = pl.multiple_of(row * width, width)
    return tokens_ref.at[dp, col, :, pl.ds(left, width)]


def send_rows(spot, sizes, src, landing, send, recv):
    count = sizes[0] * sizes[1] * sizes[2]
    me = index_of(spot, sizes)

    def one(step, carry):
        other = lax.rem(me + step, count)
        remote(src.at[other], landing.at[me], send, recv, device_of(other, sizes)).start()
        return carry

    lax.fori_loop(1, count, one, 0)
    landing[me] = src[me]


def all_rows(landing, sem):
    return arrived(landing.at[pl.ds(0, landing.shape[0] - 1)], sem)


def slot_row(sizes, table, dp, col, block):
    pieces = []
    for row in range(sizes[1]):
        index = (dp * sizes[1] + row) * sizes[2] + col
        pieces.append(table[index, block : block + 1, :])
    return jnp.concatenate(pieces, axis=1)


def read_kernel(
    sizes, blocks, grads, meta, slots, values,
    grads_all, table, own_part, other_part, meta_in,
    slots_in, tables, parts, msend, mrecv, ssend, srecv, zsend, zrecv, xsend, xrecv, csend, crecv,
    local, tsem, psem, qsend, qrecv,
):
    spot = here()
    dp, row, col = spot
    dps, rows, cols = sizes
    tokens, width = grads.shape
    areas = values.shape[0] // SUBKEYS
    greet_all(spot, sizes)
    send_rows(spot, sizes, meta, meta_in, msend, mrecv)
    send_rows(spot, sizes, slots, slots_in, ssend, srecv)

    def block_at(j, k, c):
        return own_block(grads_all, lax.rem(dp + j, dps), c, lax.rem(row + k, rows), width)

    def cross(src, j, k):
        remote(src, block_at(j, k, col), csend, crecv, (dp, row, 1 - col)).start()

    def sideways(src, j):
        for k in range(1, rows):
            remote(
                src, block_at(j, 0, col), xsend, xrecv.at[j, rows - k],
                (dp, lax.rem(row + k, rows), col),
            ).start()

    for k in range(1, dps):
        remote(
            grads, block_at(0, 0, col), zsend, zrecv.at[dps - k], (lax.rem(dp + k, dps), row, col)
        ).start()
    sideways(grads, 0)
    cross(grads, 0, 0)
    keep = pltpu.make_async_copy(grads, block_at(0, 0, col), local)
    keep.start()

    def from_above(j):
        src = block_at(j, 0, col)
        arrived(src, zrecv.at[j])
        sideways(src, j)
        cross(src, j, 0)

    def from_side(j):
        for k in range(1, rows):
            src = block_at(j, k, col)
            arrived(src, xrecv.at[j, k])
            cross(src, j, k)

    all_rows(meta_in, mrecv)
    all_rows(slots_in, srecv)

    def chunk(turn, kk):
        source_dp = lax.rem(dp + 1 + turn, dps)
        source_col = 1 - col if kk == 0 else col
        table_out = pltpu.make_async_copy(
            tables.at[kk], table.at[source_dp, source_col], tsem.at[kk]
        )

        @pl.when(turn > 0)
        def _():
            table_out.wait()

        for block in range(blocks):
            row_meta = slot_row(sizes, meta_in, source_dp, source_col, block)
            key = row_meta // SUBKEYS
            low = row_meta % SUBKEYS
            weight = slot_row(sizes, slots_in, source_dp, source_col, block)
            at_key = lax.broadcasted_iota(jnp.int32, (areas * FBLK, key.shape[1]), 0) == key
            left = jnp.where(at_key, weight, 0.0).astype(jnp.bfloat16)
            stacked = lax.dot_general(
                left,
                one_hot(low, SUBKEYS),
                (((1,), (1,)), ((), ())),
                preferred_element_type=jnp.float32,
            ).astype(jnp.bfloat16)
            for area in range(areas):
                tables[
                    kk,
                    block * FBLK : (block + 1) * FBLK,
                    area * SUBKEYS : (area + 1) * SUBKEYS,
                ] = stacked[area * FBLK : (area + 1) * FBLK]
        table_out.start()
        if kk == 0:
            part_out = remote(
                parts.at[0], other_part.at[source_dp], qsend, qrecv, (dp, row, 1 - col)
            )
        else:
            part_out = pltpu.make_async_copy(parts.at[1], own_part.at[source_dp], psem)

        @pl.when(turn > 0)
        def _():
            if kk == 0:
                part_out.wait_send()
            else:
                part_out.wait()

        def strip(n, carry):
            columns = pl.ds(pl.multiple_of(n * 256, 256), 256)
            parts[kk, :, columns] = jnp.dot(
                tables[kk], values[:, columns], preferred_element_type=jnp.float32
            ).astype(jnp.bfloat16)
            return carry

        lax.fori_loop(0, values.shape[1] // 256, strip, 0)
        part_out.start()

    def step(turn, carry):
        chunk(turn, 0)

        @pl.when(jnp.logical_and(turn > 0, 2 * turn < dps))
        def _():
            from_above(2 * turn)

        @pl.when(turn > 0)
        def _():
            from_side(turn - 1)

        chunk(turn, 1)

        @pl.when(2 * turn + 1 < dps)
        def _():
            from_above(2 * turn + 1)

        return carry

    lax.fori_loop(0, dps, step, 0)
    from_side(dps - 1)
    keep.wait()
    for kk in range(2):
        pltpu.make_async_copy(tables.at[kk], table.at[0, 0], tsem.at[kk]).wait()
    pltpu.make_async_copy(parts.at[1], own_part.at[0], psem).wait()
    remote(parts.at[0], other_part.at[0], qsend, qrecv, (dp, row, 1 - col)).wait_send()
    arrived(other_part, qrecv)
    arrived(grads_all.at[:, 0], crecv)
    arrived(grads_all.at[:, 0], csend)
    arrived(grads_all.at[pl.ds(0, dps - 1), 0, :, pl.ds(0, width)], zsend)
    arrived(grads_all.at[:, 0, :, pl.ds(0, (rows - 1) * width)], xsend)
    all_rows(meta_in, msend)
    all_rows(slots_in, ssend)


def read_memory(sizes, grads, meta, slots, values):
    dps, rows, cols = sizes
    tokens, width = grads.shape
    rows_dev, features = values.shape
    blocks = tokens // FBLK
    low = jnp.bfloat16
    shape = jax.ShapeDtypeStruct
    return pl.pallas_call(
        functools.partial(read_kernel, sizes, blocks),
        in_specs=[VMEM] * 4,
        out_specs=[ANY, ANY, ANY, ANY, VMEM],
        out_shape=[
            shape((dps, cols, tokens, rows * width), low),
            shape((dps, cols, tokens, rows_dev), low),
            shape((dps, tokens, features), low),
            shape((dps, tokens, features), low),
            shape(meta.shape, meta.dtype),
        ],
        scratch_shapes=[
            pltpu.VMEM(slots.shape, slots.dtype),
            pltpu.VMEM((2, tokens, rows_dev), low),
            pltpu.VMEM((2, tokens, features), low),
            DMA, DMA, DMA, DMA,
            DMA, DMA((dps,)),
            DMA, DMA((dps, rows)),
            DMA, DMA,
            DMA, DMA((2,)), DMA, DMA, DMA,
        ],
        compiler_params=pltpu.CompilerParams(collective_id=6, has_side_effects=True),
        name="read_memory",
    )(grads, meta, slots, values)


def back_kernel(
    sizes, blocks, grads_all, own_part, other_part, meta_in, values_t,
    memory, back, side_land, deep_land,
    chunks, found, hots, mine, theirs, acc, side, total, deep,
    gsem, osem, tsem, xsend, xrecv, zsend, zrecv, fsend, frecv, flocal, ssem, dsem,
):
    spot = here()
    dp, row, col = spot
    dps, rows, cols = sizes
    tokens, width = memory.shape
    areas = values_t.shape[1] // SUBKEYS
    count = dps * rows * cols
    me = index_of(spot, sizes)
    greet_all(spot, sizes)

    def source(turn):
        return lax.rem(dp + 1 + turn, dps)

    def load_parts(turn):
        return (
            pltpu.make_async_copy(own_part.at[source(turn)], mine, osem),
            pltpu.make_async_copy(other_part.at[source(turn)], theirs, tsem),
        )

    def load_chunk(turn, kk):
        return pltpu.make_async_copy(
            grads_all.at[source(turn), 1 - col if kk == 0 else col], chunks.at[kk], gsem.at[kk]
        )

    def piece(turn, k):
        left = pl.multiple_of(lax.rem(row + k, rows) * width, width)
        return acc.at[turn, :, pl.ds(left, width)]

    def combine(turn):
        for copy in load_parts(turn):
            copy.wait()
        acc[turn] = (mine[...].astype(jnp.float32) + theirs[...].astype(jnp.float32)).astype(
            jnp.bfloat16
        )

        @pl.when(turn + 1 < dps)
        def _():
            for copy in load_parts(turn + 1):
                copy.start()

        for k in range(1, rows):
            remote(
                piece(turn, k), side_land.at[turn, rows - k], xsend, xrecv.at[turn, rows - k],
                (dp, lax.rem(row + k, rows), col),
            ).start()

    def row_total(turn):
        copies = []
        for k in range(1, rows):
            arrived(side_land.at[turn, k], xrecv.at[turn, k])
            copies.append(pltpu.make_async_copy(side_land.at[turn, k], side.at[k], ssem.at[k]))
            copies[-1].start()
        result = acc[turn, :, pl.ds(pl.multiple_of(row * width, width), width)].astype(jnp.float32)
        for k in range(1, rows):
            copies[k - 1].wait()
            result = result + side[k].astype(jnp.float32)
        return result

    def deeper(turn):
        total[turn] = row_total(turn).astype(jnp.bfloat16)
        remote(
            total.at[turn], deep_land.at[dps - 2 - turn], zsend, zrecv.at[dps - 2 - turn],
            (source(turn), row, col),
        ).start()

    for copy in load_parts(0):
        copy.start()
    for kk in range(2):
        load_chunk(0, kk).start()

    def chunk(turn, kk):
        source_dp = source(turn)
        source_col = 1 - col if kk == 0 else col
        keys = []
        for block in range(blocks):
            row_meta = slot_row(sizes, meta_in, source_dp, source_col, block)
            keys.append(row_meta // SUBKEYS)
            hots[block] = one_hot(row_meta % SUBKEYS, SUBKEYS)
        load_chunk(turn, kk).wait()

        def area_step(area, sums):
            columns = pl.ds(pl.multiple_of(area * SUBKEYS, SUBKEYS), SUBKEYS)
            grid = jnp.dot(
                chunks[kk], values_t[:, columns], preferred_element_type=jnp.float32
            ).astype(jnp.bfloat16)
            new = []
            for block in range(blocks):
                product = jnp.dot(
                    grid[block * FBLK : (block + 1) * FBLK],
                    hots[block],
                    preferred_element_type=jnp.float32,
                )
                spot_id = lax.broadcasted_iota(jnp.int32, product.shape, 0) + area * FBLK
                new.append(
                    sums[block]
                    + jnp.sum(
                        jnp.where(spot_id == keys[block], product, 0.0), axis=0, keepdims=True
                    )
                )
            return tuple(new)

        sums = lax.fori_loop(
            0, areas, area_step, tuple(jnp.zeros(keys[0].shape, jnp.float32) for _ in range(blocks))
        )

        @pl.when(turn + 1 < dps)
        def _():
            load_chunk(turn + 1, kk).start()

        for r in range(rows):
            index = (source_dp * rows + r) * cols + source_col
            for block in range(blocks):
                found[index, block : block + 1, :] = sums[block][:, r * 128 : (r + 1) * 128]
            away = remote(found.at[index], back.at[me], fsend, frecv, (source_dp, r, source_col))
            own = jnp.logical_and(jnp.logical_and(source_dp == dp, row == r), source_col == col)
            if kk == 0:
                away.start()
            else:
                pl.when(jnp.logical_not(own))(away.start)
                pl.when(own)(pltpu.make_async_copy(found.at[index], back.at[me], flocal).start)

    def step(turn, carry):
        @pl.when(2 * turn < dps)
        def _():
            combine(2 * turn)

        @pl.when(turn > 0)
        def _():
            deeper(turn - 1)

        chunk(turn, 0)

        @pl.when(2 * turn + 1 < dps)
        def _():
            combine(2 * turn + 1)

        chunk(turn, 1)
        return carry

    lax.fori_loop(0, dps, step, 0)
    result = row_total(dps - 1)
    for k in range(dps - 1):
        arrived(deep_land.at[k], zrecv.at[k])
        copy = pltpu.make_async_copy(deep_land.at[k], deep.at[k % 2], dsem.at[k % 2])
        copy.start()
        copy.wait()
        result = result + deep[k % 2].astype(jnp.float32)
    memory[...] = result
    arrived(back.at[pl.ds(0, count - 1)], frecv)
    arrived(back.at[0], flocal)
    arrived(back.at[pl.ds(0, count - 1)], fsend)
    arrived(side_land.at[:, pl.ds(0, rows - 1)], xsend)
    arrived(deep_land.at[pl.ds(0, dps - 1)], zsend)


def back_memory(sizes, grads_all, own_part, other_part, meta_in, values_t):
    dps, rows, cols = sizes
    _, _, tokens, features = grads_all.shape
    width = features // rows
    blocks = tokens // FBLK
    count = dps * rows * cols
    low, wide = jnp.bfloat16, jnp.float32
    shape = jax.ShapeDtypeStruct
    memory, back, _, _ = pl.pallas_call(
        functools.partial(back_kernel, sizes, blocks),
        in_specs=[ANY, ANY, ANY, VMEM, VMEM],
        out_specs=[VMEM, VMEM, ANY, ANY],
        out_shape=[
            shape((tokens, width), wide),
            shape((count, blocks, 128), wide),
            shape((dps, rows, tokens, width), low),
            shape((dps, tokens, width), low),
        ],
        scratch_shapes=[
            pltpu.VMEM((2, tokens, features), low),
            pltpu.VMEM((count, blocks, 128), wide),
            pltpu.VMEM((blocks, SUBKEYS, rows * 128), low),
            pltpu.VMEM((tokens, features), low),
            pltpu.VMEM((tokens, features), low),
            pltpu.VMEM((dps, tokens, features), low),
            pltpu.VMEM((rows, tokens, width), low),
            pltpu.VMEM((dps, tokens, width), low),
            pltpu.VMEM((2, tokens, width), low),
            DMA((2,)), DMA, DMA,
            DMA, DMA((dps, rows)),
            DMA, DMA((dps,)),
            DMA, DMA, DMA, DMA((rows,)), DMA((2,)),
        ],
        compiler_params=pltpu.CompilerParams(collective_id=7, has_side_effects=True),
        name="back_memory",
    )(grads_all, own_part, other_part, meta_in, values_t)
    return memory, back


def unweigh_kernel(rows_dev, owners, back_ref, picks_ref, rank_ref, weights_ref, first_ref, second_ref):
    picks = picks_ref[0]
    hot = one_hot(picks // rows_dev, owners)
    back = back_ref[0]
    high = back.astype(jnp.bfloat16)
    rest = back - high.astype(jnp.float32)
    middle = rest.astype(jnp.bfloat16)
    lowest = (rest - middle.astype(jnp.float32)).astype(jnp.bfloat16)
    spread_back = (
        jnp.dot(high, hot, preferred_element_type=jnp.float32)
        + jnp.dot(middle, hot, preferred_element_type=jnp.float32)
        + jnp.dot(lowest, hot, preferred_element_type=jnp.float32)
    )
    slot = lax.broadcasted_iota(jnp.int32, spread_back.shape, 0)
    flat = jnp.sum(jnp.where(slot == rank_ref[0], spread_back, 0.0), axis=0, keepdims=True)
    grads = jnp.concatenate(
        [flat[:, pick * FBLK : (pick + 1) * FBLK] for pick in range(TOPK)], axis=0
    )
    weights = weights_ref[0]
    grads = weights * (grads - jnp.sum(weights * grads, axis=0, keepdims=True))
    upper = picks // SUBKEYS
    lower = picks % SUBKEYS
    key_id = lax.broadcasted_iota(jnp.int32, (SUBKEYS, FBLK), 0)
    first = jnp.zeros((SUBKEYS, FBLK), jnp.float32)
    second = jnp.zeros((SUBKEYS, FBLK), jnp.float32)
    for pick in range(TOPK):
        columns = slice(pick * FBLK, (pick + 1) * FBLK)
        value = grads[pick : pick + 1]
        first = first + jnp.where(key_id == upper[:, columns], value, 0.0)
        second = second + jnp.where(key_id == lower[:, columns], value, 0.0)
    first_ref[...] = first.astype(jnp.bfloat16)
    second_ref[...] = second.astype(jnp.bfloat16)


def unweigh(back, flat, rank, weights, rows_dev, owners):
    blocks, count = flat.shape
    cap = back.shape[1]
    return pl.pallas_call(
        functools.partial(unweigh_kernel, rows_dev, owners),
        grid=(blocks,),
        in_specs=[
            pl.BlockSpec((1, cap, owners), lambda i: (i, 0, 0)),
            pl.BlockSpec((1, 1, count), lambda i: (i, 0, 0)),
            pl.BlockSpec((1, 1, count), lambda i: (i, 0, 0)),
            pl.BlockSpec((1, TOPK, FBLK), lambda i: (i, 0, 0)),
        ],
        out_specs=[
            pl.BlockSpec((SUBKEYS, FBLK), lambda i: (0, i)),
            pl.BlockSpec((SUBKEYS, FBLK), lambda i: (0, i)),
        ],
        out_shape=[jax.ShapeDtypeStruct((SUBKEYS, blocks * FBLK), jnp.bfloat16)] * 2,
        name="unweigh",
    )(back, flat[:, None, :], rank, weights)


def memory_all(query_rows, grad_memory, picks, subkeys, values):
    sizes = grid_sizes()
    owners = sizes[0] * sizes[1] * sizes[2]
    rows_dev = values.shape[0]
    cap = FBLK * TOPK // owners
    head_id = lax.axis_index("row")
    keys_head = lax.dynamic_index_in_dim(subkeys, head_id, 0, keepdims=False)
    picks_head = lax.dynamic_index_in_dim(picks, head_id, 1, keepdims=False)
    flat = flat_picks(picks_head)
    rank, meta = route(flat, rows_dev, owners, cap)
    weights, slots = weigh(query_rows, keys_head, flat, rank, rows_dev, owners, cap)
    spare = ((0, 0), (0, 0), (0, 128 - cap))
    meta = jnp.pad(jnp.swapaxes(meta, 0, 1), spare, constant_values=-1)
    slots = jnp.pad(jnp.swapaxes(slots, 0, 1).astype(jnp.float32), spare)
    grads_all, table, own_part, other_part, meta_in = read_memory(
        sizes, grad_memory, meta, slots, values
    )
    memory, back = back_memory(sizes, grads_all, own_part, other_part, meta_in, values.T)
    first_t, second_t = unweigh(
        jnp.transpose(back, (1, 2, 0))[:, :cap], flat, rank, weights, rows_dev, owners
    )
    grad_query = jnp.concatenate(
        [
            lax.dot_general(
                part, keys_head[i], (((0,), (0,)), ((), ())), preferred_element_type=jnp.float32
            )
            for i, part in enumerate((first_t, second_t))
        ],
        axis=1,
    ).astype(jnp.bfloat16)
    grad_keys = jnp.stack(
        [
            jnp.dot(first_t, query_rows[:, :HALF], preferred_element_type=jnp.float32),
            jnp.dot(second_t, query_rows[:, HALF:], preferred_element_type=jnp.float32),
        ]
    )
    return memory, grad_query, grad_keys, table, grads_all


def head_scores(query_head, key_head, allowed):
    raw_scores = jnp.einsum(
        "qd,kd->qk", query_head, key_head, preferred_element_type=jnp.float32
    ) * HDIM ** (-0.5)
    return jnp.where(allowed, raw_scores, -jnp.inf)


def attend_forward(queries, keys, values, allowed):
    outputs = []
    log_sums = []
    for head_index in range(queries.shape[1] // HDIM):
        columns = slice(head_index * HDIM, (head_index + 1) * HDIM)
        scores = head_scores(queries[:, columns], keys[:, columns], allowed)
        peak_score = jnp.max(scores, axis=1, keepdims=True)
        exp_scores = jnp.exp(scores - peak_score)
        row_sum = jnp.sum(exp_scores, axis=1, keepdims=True)
        probabilities = (exp_scores / row_sum).astype(jnp.bfloat16)
        outputs.append(
            jnp.dot(probabilities, values[:, columns], preferred_element_type=jnp.float32)
        )
        log_sums.append(peak_score[:, 0] + jnp.log(row_sum[:, 0]))
    return (jnp.concatenate(outputs, axis=1), jnp.stack(log_sums))


def attend_backward(queries, keys, values, allowed, log_sums, grad_out):
    grad_queries = []
    grad_keys = []
    grad_values = []
    for head_index in range(queries.shape[1] // HDIM):
        columns = slice(head_index * HDIM, (head_index + 1) * HDIM)
        query_head = queries[:, columns]
        key_head = keys[:, columns]
        value_head = values[:, columns]
        grad_head = grad_out[:, columns]
        scores = head_scores(query_head, key_head, allowed)
        probabilities = jnp.exp(scores - log_sums[head_index][:, None])
        grad_probs = jnp.einsum(
            "qd,kd->qk", grad_head, value_head, preferred_element_type=jnp.float32
        )
        inner_sum = jnp.sum(probabilities * grad_probs, axis=1, keepdims=True)
        grad_scores = (probabilities * (grad_probs - inner_sum)).astype(jnp.bfloat16)
        grad_queries.append(
            jnp.dot(grad_scores, key_head, preferred_element_type=jnp.float32) * HDIM ** (-0.5)
        )
        grad_keys.append(
            jnp.einsum("qk,qd->kd", grad_scores, query_head, preferred_element_type=jnp.float32)
            * HDIM ** (-0.5)
        )
        grad_values.append(
            jnp.einsum(
                "qk,qd->kd",
                probabilities.astype(jnp.bfloat16),
                grad_head,
                preferred_element_type=jnp.float32,
            )
        )
    stacked = jnp.stack([jnp.concatenate(grad_keys, axis=1), jnp.concatenate(grad_values, axis=1)])
    return (jnp.concatenate(grad_queries, axis=1), stacked)


def dense(left, right):
    return jnp.dot(left, right, preferred_element_type=jnp.float32)


def dense_nt(left, right):
    return lax.dot_general(left, right, (((1,), (1,)), ((), ())), preferred_element_type=jnp.float32)


def dense_tn(left, right):
    return lax.dot_general(left, right, (((0,), (0,)), ((), ())), preferred_element_type=jnp.float32)


def per_device(
    inputs,
    prefix,
    picks,
    gain_attn,
    w_qkv,
    w_attn_out,
    gain_mem,
    w_query,
    w_gate,
    w_proj,
    subkeys,
    values,
    cotangent,
):
    low = jnp.bfloat16
    sizes = grid_sizes()
    width_part = inputs.shape[1]
    own_tokens = picks.shape[0]
    seq_tokens = own_tokens * sizes[2]
    col = lax.axis_index("col")
    col_first = col * width_part
    gain_one = lax.dynamic_slice_in_dim(gain_attn, col_first, width_part)
    gain_two = lax.dynamic_slice_in_dim(gain_mem, col_first, width_part)

    x_own, dy_own, qkv_w, query_w, gate_w, proj_w, attn_w = start_all(
        sizes, inputs, cotangent, w_qkv, w_query, w_gate, w_proj, w_attn_out
    )
    residual = x_own.astype(jnp.float32)
    scale_one = lax.rsqrt(jnp.sum(residual * residual, axis=1, keepdims=True) / D + EPSILON)
    normed_one = (residual * scale_one * gain_attn.astype(jnp.float32)).astype(low)
    qkv = jnp.einsum("tc,jcf->jtf", normed_one, qkv_w, preferred_element_type=jnp.float32).astype(low)
    kv_all = swap_tokens(sizes, qkv[1:])
    allowed = allowed_mask(own_tokens, seq_tokens, col * own_tokens, prefix[0])
    attended_sum, log_sums = attend_forward(qkv[0], kv_all[0], kv_all[1], allowed)
    attended = attended_sum.astype(low)
    hidden, normed_two = join(sizes, dense(attended, attn_w).astype(low), inputs, gain_two)
    query_rows = dense(normed_two, query_w).astype(low)
    gate_value = dense(normed_two, gate_w)
    sigmoid_gate = jax.nn.sigmoid(gate_value)
    silu_gate = gate_value * sigmoid_gate
    grad_gated = dense_nt(dy_own, proj_w)
    grad_memory = (grad_gated * silu_gate).astype(low)
    memory, grad_query, grad_keys, table, grads_all = memory_all(
        query_rows, grad_memory, picks, subkeys, values
    )
    gated_value = (memory * silu_gate).astype(low)
    out_part = dense(gated_value, proj_w).astype(low)
    grad_gate = (
        grad_gated * memory * sigmoid_gate * (1.0 + gate_value * (1.0 - sigmoid_gate))
    ).astype(low)
    grad_part = (dense_nt(grad_query, query_w) + dense_nt(grad_gate, gate_w)).astype(low)
    first_terms = [
        dense_tn(normed_two, grad_query).astype(low),
        dense_tn(normed_two, grad_gate).astype(low),
        dense_tn(gated_value, dy_own).astype(low),
        grad_keys.reshape(-1, HALF).astype(low),
    ]
    output, grad_hidden, grad_hidden_all, gain_two_grad, *shards = middle(
        sizes, grad_part, out_part, hidden, cotangent, gain_two, first_terms
    )
    grad_attended = dense_nt(grad_hidden_all, attn_w).astype(low)
    grad_query_own, grad_kv_part = attend_backward(
        qkv[0], kv_all[0], kv_all[1], allowed, log_sums, grad_attended
    )
    grad_kv = pair_sum(sizes, grad_kv_part)
    grad_q = grad_query_own.astype(low)
    x_part = (
        dense_nt(grad_q, qkv_w[0]) + dense_nt(grad_kv[0], qkv_w[1]) + dense_nt(grad_kv[1], qkv_w[2])
    ).astype(low)
    last_terms = [
        jnp.stack([dense_tn(normed_one, part) for part in (grad_q, grad_kv[0], grad_kv[1])]).astype(low),
        dense_tn(attended, grad_hidden_all).astype(low),
    ]
    (
        grad_inputs, gain_sums, grad_values,
        grad_w_query, grad_w_gate, grad_w_proj, _, grad_w_qkv, grad_w_attn_out, grad_subkeys,
    ) = last(
        sizes, x_part, inputs, grad_hidden, gain_one, gain_two_grad, shards, last_terms, table, grads_all
    )
    gain_rows = gain_sums.reshape(sizes[2], 2, width_part)
    grad_gain_one = gain_rows[:, 0].reshape(-1)
    grad_gain_two = gain_rows[:, 1].reshape(-1)

    return (
        output,
        grad_inputs,
        grad_gain_one,
        grad_w_qkv.astype(jnp.float32),
        grad_w_attn_out.astype(jnp.float32),
        grad_gain_two,
        grad_w_query.astype(jnp.float32),
        grad_w_gate.astype(jnp.float32),
        grad_w_proj.astype(jnp.float32),
        grad_subkeys.astype(jnp.float32),
        grad_values,
    )


def solution(mesh):
    placed = (
        P(("dp", "row"), "col"),
        P("dp"),
        P(("dp", "col"), None, None),
        P(),
        P(None, "col", "row"),
        P("row", "col"),
        P(),
        P("col", "row"),
        P("col", "row"),
        P("row", "col"),
        P(),
        P(("dp", "row", "col"), None),
        P(("dp", "row"), "col"),
    )
    return jax.shard_map(
        per_device,
        mesh=mesh,
        in_specs=placed,
        out_specs=(
            P(("dp", "row"), "col"),
            P(("dp", "row"), "col"),
            P(),
            P(None, "col", "row"),
            P("row", "col"),
            P(),
            P("col", "row"),
            P("col", "row"),
            P("row", "col"),
            P(),
            P(("dp", "row", "col"), None),
        ),
        check_vma=False,
    )
```

```python
import functools

import jax
import jax.numpy as jnp
from jax import lax
from jax.experimental import pallas as pl
from jax.experimental.pallas import tpu as pltpu
from jax.sharding import PartitionSpec as P

D = 1024
HDIM = 64
HALF = 512
SUBKEYS = 256
TOPK = 32
FBLK = 128


EPSILON = 1e-06


MESH = pl.DeviceIdType.MESH
VMEM = pl.BlockSpec(memory_space=pltpu.VMEM)
ANY = pl.BlockSpec(memory_space=pl.ANY)
DMA = pltpu.SemaphoreType.DMA


def here():
    return lax.axis_index("dp"), lax.axis_index("row"), lax.axis_index("col")


def grid_sizes():
    return lax.axis_size("dp"), lax.axis_size("row"), lax.axis_size("col")


def remote(src, dst, send_sem, recv_sem, device):
    return pltpu.make_async_remote_copy(
        src_ref=src,
        dst_ref=dst,
        send_sem=send_sem,
        recv_sem=recv_sem,
        device_id=device,
        device_id_type=MESH,
    )


def arrived(dst, sem):
    pltpu.make_async_copy(dst, dst, sem).wait()


def greet_plane(spot, sizes):
    barrier = pltpu.get_barrier_semaphore()
    dp, row, col = spot
    _, rows, cols = sizes
    for j in range(rows):
        for k in range(cols):
            if j + k > 0:
                pl.semaphore_signal(
                    barrier,
                    inc=1,
                    device_id=(dp, lax.rem(row + j, rows), lax.rem(col + k, cols)),
                    device_id_type=MESH,
                )
    pl.semaphore_wait(barrier, rows * cols - 1)


def greet_partner(spot, sizes):
    barrier = pltpu.get_barrier_semaphore()
    dp, row, col = spot
    pl.semaphore_signal(barrier, inc=1, device_id=(dp, row, 1 - col), device_id_type=MESH)
    pl.semaphore_wait(barrier, 1)


def device_of(index, sizes):
    _, rows, cols = sizes
    return (
        lax.div(index, rows * cols),
        lax.rem(lax.div(index, cols), rows),
        lax.rem(index, cols),
    )


def index_of(spot, sizes):
    return (spot[0] * sizes[1] + spot[1]) * sizes[2] + spot[2]


def greet_all(spot, sizes):
    barrier = pltpu.get_barrier_semaphore()
    count = sizes[0] * sizes[1] * sizes[2]
    me = index_of(spot, sizes)

    def greet(step, carry):
        pl.semaphore_signal(
            barrier,
            inc=1,
            device_id=device_of(lax.rem(me + step, count), sizes),
            device_id_type=MESH,
        )
        return carry

    lax.fori_loop(1, count, greet, 0)
    pl.semaphore_wait(barrier, count - 1)


class Gather:
    def __init__(self, spot, sizes, src, dst, send, recv):
        self.spot, self.sizes, self.src, self.dst = spot, sizes, src, dst
        self.send, self.recv = send, recv
        self.tokens, self.width = src.shape
        dp, row, col = spot
        _, rows, cols = sizes
        self.half = rows // cols
        self.target = lax.div(row, self.half)
        self.slot = lax.rem(row, self.half) * cols + col
        first = pl.multiple_of(lax.rem(row, self.half) * self.tokens, self.tokens)
        left = pl.multiple_of(col * self.width, self.width)
        self.there = dst.at[pl.ds(first, self.tokens), pl.ds(left, self.width)]

    def copy(self, step):
        dp, row, _ = self.spot
        device = (dp, lax.rem(row + step, self.sizes[1]), self.target)
        return remote(self.src, self.there, self.send.at[step], self.recv.at[self.slot], device)

    def start(self):
        col = self.spot[2]

        for step in range(1, self.sizes[1]):
            self.copy(step).start()

        @pl.when(self.target == col)
        def _():
            pltpu.make_async_copy(self.src, self.there, self.recv.at[self.slot]).start()

        @pl.when(self.target != col)
        def _():
            self.copy(0).start()

    def wait(self):
        cols = self.sizes[2]
        for i in range(self.half):
            for k in range(cols):
                arrived(
                    self.dst.at[pl.ds(i * self.tokens, self.tokens), pl.ds(k * self.width, self.width)],
                    self.recv.at[i * cols + k],
                )
        for step in range(1, self.sizes[1]):
            self.copy(step).wait_send()

        @pl.when(self.target != self.spot[2])
        def _():
            self.copy(0).wait_send()


class Scatter:
    def __init__(self, spot, sizes, src, landing, send, recv):
        self.spot, self.sizes, self.src, self.landing = spot, sizes, src, landing
        self.send, self.recv = send, recv
        _, self.tokens, self.width = landing.shape
        self.half = sizes[1] // sizes[2]

    def parts(self):
        dp, row, col = self.spot
        cols = self.sizes[2]
        for i in range(self.half):
            for k in range(cols):
                piece = self.src.at[
                    pl.ds(i * self.tokens, self.tokens), pl.ds(k * self.width, self.width)
                ]
                target = col * self.half + i
                mine = jnp.logical_and(target == row, col == k)
                there = self.landing.at[row]
                copy = remote(
                    piece, there, self.send.at[i * cols + k], self.recv.at[row], (dp, target, k)
                )
                yield mine, copy, pltpu.make_async_copy(piece, there, self.recv.at[row])

    def start(self):
        for mine, copy, own in self.parts():
            pl.when(jnp.logical_not(mine))(copy.start)
            pl.when(mine)(own.start)

    def wait(self):
        for q in range(self.sizes[1]):
            arrived(self.landing.at[q], self.recv.at[q])

    def wait_send(self):
        for mine, copy, _ in self.parts():
            pl.when(jnp.logical_not(mine))(copy.wait_send)


def plane_sems(sizes):
    rows, cols = sizes[1], sizes[2]
    return [DMA((rows,)), DMA((rows,))]


def start_kernel(sizes, *refs):
    x, dy, wqkv, wquery, wgate, wproj, wattn = refs[:7]
    xs, dys, wqkv_all, wquery_all, wgate_all, wproj_all, wattn_all = refs[7:14]
    xsend, xrecv, ysend, yrecv, wsend, wrecv, wlocal = refs[14:]
    spot = here()
    dp, row, col = spot
    greet_plane(spot, sizes)
    gather_x = Gather(spot, sizes, x, xs, xsend, xrecv)
    gather_y = Gather(spot, sizes, dy, dys, ysend, yrecv)
    gather_x.start()
    gather_y.start()
    copies = []
    for n, (src, dst, dim) in enumerate(
        (
            (wqkv, wqkv_all, 1),
            (wquery, wquery_all, 0),
            (wgate, wgate_all, 0),
            (wproj, wproj_all, 1),
            (wattn, wattn_all, 1),
        )
    ):
        size = src.shape[dim]
        window = [slice(None)] * len(src.shape)
        window[dim] = pl.ds(pl.multiple_of(col * size, size), size)
        there = dst.at[tuple(window)]
        away = remote(src, there, wsend.at[n], wrecv.at[n], (dp, row, 1 - col))
        own = pltpu.make_async_copy(src, there, wlocal.at[n])
        away.start()
        own.start()
        copies += [away, own]
    for copy in copies:
        copy.wait()
    gather_x.wait()
    gather_y.wait()


def start_all(sizes, x, dy, wqkv, wquery, wgate, wproj, wattn):
    tokens, width = x.shape
    half = sizes[1] // sizes[2]
    cols = sizes[2]
    low = jnp.bfloat16

    def twice(operand, dim):
        shape = list(operand.shape)
        shape[dim] *= cols
        return jax.ShapeDtypeStruct(tuple(shape), low)

    whole = jax.ShapeDtypeStruct((half * tokens, cols * width), low)
    return pl.pallas_call(
        functools.partial(start_kernel, sizes),
        in_specs=[VMEM] * 7,
        out_specs=[ANY] * 7,
        out_shape=[
            whole,
            whole,
            twice(wqkv, 1),
            twice(wquery, 0),
            twice(wgate, 0),
            twice(wproj, 1),
            twice(wattn, 1),
        ],
        scratch_shapes=plane_sems(sizes) * 2 + [DMA((5,))] * 3,
        compiler_params=pltpu.CompilerParams(collective_id=0, has_side_effects=True),
        name="start_all",
    )(x, dy, wqkv, wquery, wgate, wproj, wattn)


def swap_kernel(sizes, src, dst, send, recv, own):
    spot = here()
    dp, row, col = spot
    greet_partner(spot, sizes)
    size = src.shape[1]
    there = dst.at[:, pl.ds(pl.multiple_of(col * size, size), size)]
    away = remote(src, there, send, recv, (dp, row, 1 - col))
    local = pltpu.make_async_copy(src, there, own)
    away.start()
    local.start()
    away.wait()
    local.wait()


def swap_tokens(sizes, src):
    shape = (src.shape[0], src.shape[1] * sizes[2], src.shape[2])
    return pl.pallas_call(
        functools.partial(swap_kernel, sizes),
        in_specs=[VMEM],
        out_specs=VMEM,
        out_shape=jax.ShapeDtypeStruct(shape, src.dtype),
        scratch_shapes=[DMA, DMA, DMA],
        compiler_params=pltpu.CompilerParams(collective_id=1, has_side_effects=True),
        name="swap_tokens",
    )(src)


def fold(column):
    return jnp.broadcast_to(column, (column.shape[0], 128))


def join_kernel(
    sizes, part, x, gain, hidden, normed_all, landing, mine, theirs, block,
    ssend, srecv, gsend, grecv, psend, precv,
):
    spot = here()
    dp, row, col = spot
    greet_plane(spot, sizes)
    scatter = Scatter(spot, sizes, part, landing, ssend, srecv)
    scatter.start()
    scatter.wait()
    total = x[...].astype(jnp.float32)
    for q in range(sizes[1]):
        total = total + landing[q].astype(jnp.float32)
    hidden[...] = total
    mine[...] = fold(jnp.sum(total * total, axis=1, keepdims=True))
    pair = remote(mine, theirs, psend, precv, (dp, row, 1 - col))
    pair.start()
    pair.wait()
    squares = mine[:, :1] + theirs[:, :1]
    scale = lax.rsqrt(squares / D + EPSILON)
    block[...] = (hidden[...] * scale * gain[...].astype(jnp.float32)).astype(jnp.bfloat16)
    gather = Gather(spot, sizes, block, normed_all, gsend, grecv)
    gather.start()
    scatter.wait_send()
    gather.wait()


def join(sizes, part, x, gain):
    tokens, width = x.shape
    rows = sizes[1]
    return pl.pallas_call(
        functools.partial(join_kernel, sizes),
        in_specs=[VMEM] * 3,
        out_specs=[VMEM, VMEM],
        out_shape=[
            jax.ShapeDtypeStruct((tokens, width), jnp.float32),
            jax.ShapeDtypeStruct(part.shape, jnp.bfloat16),
        ],
        scratch_shapes=[
            pltpu.VMEM((rows, tokens, width), jnp.bfloat16),
            pltpu.VMEM((tokens, 128), jnp.float32),
            pltpu.VMEM((tokens, 128), jnp.float32),
            pltpu.VMEM((tokens, width), jnp.bfloat16),
        ]
        + plane_sems(sizes) * 2
        + [DMA, DMA],
        compiler_params=pltpu.CompilerParams(collective_id=3, has_side_effects=True),
        name="join",
    )(part, x, gain[None])


def norm_back(sizes, spot, landing, base, above, gain, mine, theirs, psend, precv):
    dp, row, col = spot
    normed_grad = landing[0].astype(jnp.float32)
    for q in range(1, sizes[1]):
        normed_grad = normed_grad + landing[q].astype(jnp.float32)
    values = base[...].astype(jnp.float32)
    unit_grad = normed_grad * gain[...].astype(jnp.float32)
    mine[0] = fold(jnp.sum(values * values, axis=1, keepdims=True))
    mine[1] = fold(jnp.sum(unit_grad * values, axis=1, keepdims=True))
    pair = remote(mine, theirs, psend, precv, (dp, row, 1 - col))
    pair.start()
    pair.wait()
    scale = lax.rsqrt((mine[0, :, :1] + theirs[0, :, :1]) / D + EPSILON)
    inner = scale * (mine[1, :, :1] + theirs[1, :, :1]) / D
    unit = values * scale
    grad = above[...].astype(jnp.float32) + scale * (unit_grad - unit * inner)
    return grad, jnp.sum(normed_grad * unit, axis=0, keepdims=True)


def slab(ref, dim, index, count):
    size = ref.shape[dim] // count
    window = [slice(None)] * len(ref.shape)
    window[dim] = pl.ds(pl.multiple_of(index * size, size), size)
    return ref.at[tuple(window)]


def add_into(target, addend):
    target[...] = (target[...].astype(jnp.float32) + addend[...].astype(jnp.float32)).astype(
        target.dtype
    )


class PairSum:
    def __init__(self, spot, sizes, terms, dims, halves, landings, send, recv):
        self.col, self.cols = spot[2], sizes[2]
        self.terms, self.dims, self.halves, self.landings = terms, dims, halves, landings
        self.copies = [
            remote(
                slab(term, dim, 1 - spot[2], sizes[2]), landing, send.at[n], recv.at[n],
                (spot[0], spot[1], 1 - spot[2]),
            )
            for n, (term, dim, landing) in enumerate(zip(terms, dims, landings))
        ]

    def start(self):
        for copy in self.copies:
            copy.start()

    def finish(self):
        for copy, term, dim, half, landing in zip(
            self.copies, self.terms, self.dims, self.halves, self.landings
        ):
            copy.wait()
            own = slab(term, dim, self.col, self.cols)
            half[...] = (own[...].astype(jnp.float32) + landing[...].astype(jnp.float32)).astype(
                half.dtype
            )


class LineReduce:
    def __init__(self, spot, sizes, arrays, dims, below, above, sems):
        self.spot, self.count = spot, sizes[0]
        self.arrays, self.dims, self.below, self.above = arrays, dims, below, above
        self.up_send, self.up_recv, self.down_send, self.down_recv = sems

    def copy(self, n, k, up):
        dp, row, col = self.spot
        landing = self.below[n] if up else self.above[n]
        send, recv = (
            (self.up_send, self.up_recv) if up else (self.down_send, self.down_recv)
        )
        dim = self.dims[n]
        return remote(
            slab(self.arrays[n], dim, k, self.count),
            slab(landing, dim, k, self.count),
            send.at[n, k],
            recv.at[n, k],
            (jnp.clip(dp + (1 if up else -1), 0, self.count - 1), row, col),
        )

    def send(self, k, up):
        for n in range(len(self.arrays)):
            self.copy(n, k, up).start()

    def start(self):
        dp, last = self.spot[0], self.count - 1

        @pl.when(dp == 0)
        def _():
            lax.fori_loop(0, last, lambda i, c: (self.send(last - i, True), c)[1], 0)

        @pl.when(dp == last)
        def _():
            lax.fori_loop(0, last, lambda i, c: (self.send(i, False), c)[1], 0)

    def take(self, k, up):
        for n, (array, dim) in enumerate(zip(self.arrays, self.dims)):
            landing = slab((self.below if up else self.above)[n], dim, k, self.count)
            arrived(landing, (self.up_recv if up else self.down_recv).at[n, k])
            add_into(slab(array, dim, k, self.count), landing)

    def event(self, time):
        dp, last = self.spot[0], self.count - 1

        @pl.when(jnp.logical_and(dp > 0, time >= dp))
        def _():
            k = dp + last - time
            self.take(k, True)
            pl.when(k > dp)(lambda: self.send(k, True))

        @pl.when(jnp.logical_and(dp < last, time >= last - dp))
        def _():
            k = time - (last - dp)
            self.take(k, False)
            pl.when(k < dp)(lambda: self.send(k, False))

    def events(self):
        lax.fori_loop(1, self.count, lambda time, c: (self.event(time), c)[1], 0)

    def finish(self):
        dp = self.spot[0]

        def one(k, carry):
            @pl.when(dp < k)
            def _():
                for n in range(len(self.arrays)):
                    self.copy(n, k, True).wait_send()

            @pl.when(dp > k)
            def _():
                for n in range(len(self.arrays)):
                    self.copy(n, k, False).wait_send()

            return carry

        lax.fori_loop(0, self.count, one, 0)


class LineGather:
    def __init__(self, spot, sizes, arrays, dims, sems):
        self.spot, self.count = spot, sizes[0]
        self.arrays, self.dims = arrays, dims
        self.up_send, self.down_send, self.recv = sems

    def copy(self, n, k, up):
        dp, row, col = self.spot
        part = slab(self.arrays[n], self.dims[n], k, self.count)
        return remote(
            part,
            part,
            (self.up_send if up else self.down_send).at[n, k],
            self.recv.at[n, k],
            (jnp.clip(dp + (1 if up else -1), 0, self.count - 1), row, col),
        )

    def send(self, k, up):
        dp = self.spot[0]

        @pl.when(dp < self.count - 1 if up else dp > 0)
        def _():
            for n in range(len(self.arrays)):
                self.copy(n, k, up).start()

    def start(self):
        self.send(self.spot[0], True)
        self.send(self.spot[0], False)

    def take(self, k):
        for n, (array, dim) in enumerate(zip(self.arrays, self.dims)):
            arrived(slab(array, dim, k, self.count), self.recv.at[n, k])

    def event(self, time):
        dp = self.spot[0]

        @pl.when(dp - time >= 0)
        def _():
            self.take(dp - time)
            self.send(dp - time, True)

        @pl.when(dp + time < self.count)
        def _():
            self.take(dp + time)
            self.send(dp + time, False)

    def events(self):
        lax.fori_loop(1, self.count, lambda time, c: (self.event(time), c)[1], 0)

    def finish(self):
        dp, last = self.spot[0], self.count - 1

        def one(k, carry):
            @pl.when(jnp.logical_and(k <= dp, dp < last))
            def _():
                for n in range(len(self.arrays)):
                    self.copy(n, k, True).wait_send()

            @pl.when(jnp.logical_and(k >= dp, dp > 0))
            def _():
                for n in range(len(self.arrays)):
                    self.copy(n, k, False).wait_send()

            return carry

        lax.fori_loop(0, self.count, one, 0)


def line_sems(sizes, arrays, kinds):
    return [DMA((arrays, sizes[0])) for _ in range(kinds)]


def greet_cross(spot, sizes):
    barrier = pltpu.get_barrier_semaphore()
    dp, row, col = spot
    dps, rows, cols = sizes
    for j in range(rows):
        for k in range(cols):
            if j + k > 0:
                pl.semaphore_signal(
                    barrier,
                    inc=1,
                    device_id=(dp, lax.rem(row + j, rows), lax.rem(col + k, cols)),
                    device_id_type=MESH,
                )
    for j in (1, dps - 1):
        pl.semaphore_signal(
            barrier, inc=1, device_id=(lax.rem(dp + j, dps), row, col), device_id_type=MESH
        )
    pl.semaphore_wait(barrier, rows * cols + 1)


FIRST_DIMS = (0, 0, 0, 0)
FIRST_COLS = (0, 0, 1, 0)
LAST_DIMS = (1, 0)
LAST_COLS = (1, 1)


def halved(shape, dim, cols):
    shape = list(shape)
    shape[dim] //= cols
    return tuple(shape)


def middle_kernel(sizes, *refs):
    part, hidden, dy, gain = refs[:4]
    terms = refs[4:8]
    grad, grad_all, gain_grad = refs[8:11]
    shards = refs[11:15]
    landing, mine, theirs, block = refs[15:19]
    halves, pair_land, below, above = refs[19:23], refs[23:27], refs[27:31], refs[31:35]
    ssend, srecv, gsend, grecv, psend, precv, hsend, hrecv, *line = refs[35:]
    spot = here()
    greet_cross(spot, sizes)
    scatter = Scatter(spot, sizes, part, landing, ssend, srecv)
    scatter.start()
    pair = PairSum(spot, sizes, terms, FIRST_COLS, halves, pair_land, hsend, hrecv)
    pair.start()
    pair.finish()
    reduce = LineReduce(spot, sizes, halves, FIRST_DIMS, below, above, line)
    reduce.start()
    scatter.wait()
    total, gains = norm_back(sizes, spot, landing, hidden, dy, gain, mine, theirs, psend, precv)
    gain_grad[...] = gains
    grad[...] = total
    block[...] = total.astype(jnp.bfloat16)
    gather = Gather(spot, sizes, block, grad_all, gsend, grecv)
    gather.start()
    lax.fori_loop(1, sizes[0], lambda time, c: (reduce.event(time), c)[1], 0)
    for half, dim, shard in zip(halves, FIRST_DIMS, shards):
        shard[...] = slab(half, dim, spot[0], sizes[0])[...]
    scatter.wait_send()
    gather.wait()
    reduce.finish()


def middle(sizes, part, hidden, dy, gain, terms):
    tokens, width = hidden.shape
    dps, rows, cols = sizes
    low, wide = jnp.bfloat16, jnp.float32
    halves = [halved(t.shape, d, cols) for t, d in zip(terms, FIRST_COLS)]
    shards = [halved(h, d, dps) for h, d in zip(halves, FIRST_DIMS)]
    return pl.pallas_call(
        functools.partial(middle_kernel, sizes),
        in_specs=[VMEM] * 8,
        out_specs=[VMEM] * 7,
        out_shape=[
            jax.ShapeDtypeStruct((tokens, width), wide),
            jax.ShapeDtypeStruct(part.shape, low),
            jax.ShapeDtypeStruct((1, width), wide),
        ]
        + [jax.ShapeDtypeStruct(s, low) for s in shards],
        scratch_shapes=[
            pltpu.VMEM((rows, tokens, width), low),
            pltpu.VMEM((2, tokens, 128), wide),
            pltpu.VMEM((2, tokens, 128), wide),
            pltpu.VMEM((tokens, width), low),
        ]
        + [pltpu.VMEM(h, low) for h in halves] * 4
        + plane_sems(sizes) * 2
        + [DMA, DMA, DMA((4,)), DMA((4,))]
        + line_sems(sizes, 4, 4),
        compiler_params=pltpu.CompilerParams(collective_id=4, has_side_effects=True),
        name="middle",
    )(part, hidden, dy, gain[None], *terms)


def last_kernel(sizes, *refs):
    part, x, above_grad, gain, other_gain = refs[:5]
    keys, terms = refs[5], refs[6:8]
    table, grads_all = refs[8:10]
    grad, gain_sums, row_grads = refs[10:13]
    lasts, keys_all = refs[13:15], refs[15]
    landing, mine, theirs, own_gain, gain_landing, tables, chunks = refs[16:23]
    halves, pair_land, below, above = refs[23:25], refs[25:27], refs[27:29], refs[29:31]
    (
        ssend, srecv, psend, precv, bsend, brecv, hsend, hrecv, tsem, csem,
        xsend, xrecv, kxsend, kxrecv, *line
    ) = refs[31:]
    spot = here()
    dp, row, col = spot
    dps, rows, cols = sizes
    count = dps * rows * cols
    me = index_of(spot, sizes)
    loads = dps * cols
    block = grads_all.shape[-1]

    def load(index):
        slot = lax.rem(index, 2)
        where = (lax.div(index, cols), lax.rem(index, cols))
        return (
            pltpu.make_async_copy(table.at[where], tables.at[slot], tsem.at[slot]),
        ) + tuple(
            pltpu.make_async_copy(
                grads_all.at[where + (r,)],
                chunks.at[slot, :, pl.ds(r * block, block)],
                csem.at[slot, r],
            )
            for r in range(rows)
        )

    for copy in load(0):
        copy.start()
    greet_all(spot, sizes)
    scatter = Scatter(spot, sizes, part, landing, ssend, srecv)
    scatter.start()
    pair = PairSum(spot, sizes, terms, LAST_COLS, halves, pair_land, hsend, hrecv)
    pair.start()
    pair.finish()
    reduce = LineReduce(spot, sizes, halves, LAST_DIMS, below, above, line[:4])
    reduce.start()

    wide_strip = min(512, tables.shape[2])

    def product(index):
        slot = lax.rem(index, 2)
        for copy in load(index):
            copy.wait()

        @pl.when(index + 1 < loads)
        def _():
            for copy in load(index + 1):
                copy.start()

        def strip(n, carry):
            columns = pl.ds(pl.multiple_of(n * wide_strip, wide_strip), wide_strip)
            term = lax.dot_general(
                tables[slot, :, columns],
                chunks[slot],
                (((0,), (0,)), ((), ())),
                preferred_element_type=jnp.float32,
            )

            @pl.when(index == 0)
            def _():
                row_grads[columns] = term

            @pl.when(index > 0)
            def _():
                row_grads[columns] = row_grads[columns] + term

            return carry

        lax.fori_loop(0, tables.shape[2] // wide_strip, strip, 0)

    def products(first, end):
        lax.fori_loop(first, end, lambda index, c: (product(index), c)[1], 0)

    def sideways(k):
        return remote(
            keys, keys_all.at[row, col], xsend, xrecv.at[rows - k],
            (dp, lax.rem(row + k, rows), col),
        )

    def cross(src, k):
        there = keys_all.at[lax.rem(row + k, rows), col]
        return remote(src, there, kxsend, kxrecv, (dp, row, 1 - col))

    products(0, loads // 4)
    scatter.wait()
    total, gains = norm_back(sizes, spot, landing, x, above_grad, gain, mine, theirs, psend, precv)
    lines = gains.shape[1] // 128
    for line_index in range(lines):
        columns = slice(line_index * 128, (line_index + 1) * 128)
        own_gain[line_index : line_index + 1] = gains[:, columns]
        own_gain[lines + line_index : lines + line_index + 1] = other_gain[:, columns]

    def tell(step, carry):
        device = device_of(lax.rem(me + step, count), sizes)
        remote(own_gain, gain_landing.at[me], bsend, brecv, device).start()
        return carry

    lax.fori_loop(1, count, tell, 0)
    gain_landing[me] = own_gain[...]
    grad[...] = total
    for k in range(1, rows):
        sideways(k).start()
    cross(keys, 0).start()
    keys_all[row, col] = keys[...]
    reduce.event(1)
    products(loads // 4, loads // 2)
    lax.fori_loop(2, dps, lambda time, c: (reduce.event(time), c)[1], 0)
    for first, half, dim in zip(lasts, halves, LAST_DIMS):
        slab(first, dim, dp, dps)[...] = slab(half, dim, dp, dps)[...]
    final = LineGather(spot, sizes, lasts, LAST_DIMS, line[4:7])
    final.start()
    products(loads // 2, 3 * loads // 4)
    final.event(1)
    for k in range(1, rows):
        landed = keys_all.at[lax.rem(row + k, rows), col]
        arrived(landed, xrecv.at[k])
        cross(landed, k).start()
    products(3 * loads // 4, loads)
    lax.fori_loop(2, dps, lambda time, c: (final.event(time), c)[1], 0)
    arrived(keys_all.at[:, 1 - col], kxrecv)
    scatter.wait_send()
    arrived(gain_landing.at[pl.ds(0, count - 1)], brecv)
    for c in range(cols):

        def add(index, sums):
            return sums + gain_landing[index * cols + c]

        gain_sums[c] = lax.fori_loop(0, dps * rows, add, jnp.zeros(own_gain.shape, jnp.float32))
    arrived(gain_landing.at[pl.ds(0, count - 1)], bsend)
    arrived(keys_all.at[:, col], kxsend)
    arrived(keys_all.at[pl.ds(0, rows - 1), col], xsend)
    reduce.finish()
    final.finish()


def last(sizes, part, x, above, gain, other_gain, keys, terms, table, grads_all):
    tokens, width = x.shape
    dps, rows, cols = sizes
    lines = 2 * width // 128
    count = dps * rows * cols
    low, wide = jnp.bfloat16, jnp.float32
    shape = jax.ShapeDtypeStruct

    halves = [halved(t.shape, d, cols) for t, d in zip(terms, LAST_COLS)]
    rows_dev = table.shape[-1]
    features = grads_all.shape[-1] * rows
    chunk = table.shape[2]
    return pl.pallas_call(
        functools.partial(last_kernel, sizes),
        in_specs=[VMEM] * 8 + [ANY] * 2,
        out_specs=[VMEM] * 6,
        out_shape=[
            shape((tokens, width), wide),
            shape((cols, lines, 128), wide),
            shape((rows_dev, features), wide),
        ]
        + [shape(s, low) for s in halves]
        + [shape((rows, cols) + keys.shape, low)],
        scratch_shapes=[
            pltpu.VMEM((rows, tokens, width), low),
            pltpu.VMEM((2, tokens, 128), wide),
            pltpu.VMEM((2, tokens, 128), wide),
            pltpu.VMEM((lines, 128), wide),
            pltpu.VMEM((count, lines, 128), wide),
            pltpu.VMEM((2, chunk, rows_dev), low),
            pltpu.VMEM((2, chunk, features), low),
        ]
        + [pltpu.VMEM(h, low) for h in halves] * 4
        + plane_sems(sizes)
        + [DMA, DMA, DMA, DMA, DMA((2,)), DMA((2,)), DMA((2,)), DMA((2, rows))]
        + [DMA, DMA((rows,)), DMA, DMA]
        + line_sems(sizes, 2, 7),
        compiler_params=pltpu.CompilerParams(collective_id=5, has_side_effects=True),
        name="last",
    )(part, x, above, gain[None], other_gain, keys, *terms, table, grads_all)


def turn_kernel(sizes, *refs):
    prefix, queries, kv, grad_out, log_sums, out_part, hidden = refs[:7]
    shards = refs[7:11]
    grad_q, grad_kv, output = refs[11:14]
    firsts = refs[14:18]
    totals, kv_landing, out_landing = refs[18:21]
    osend, orecv, ksend, krecv, *line = refs[21:]
    spot = here()
    dp, row, col = spot
    dps = sizes[0]
    tokens, width = queries.shape
    keys = kv.shape[1]
    tile = tokens // 2
    greet_cross(spot, sizes)
    for first, dim, shard in zip(firsts, FIRST_DIMS, shards):
        slab(first, dim, dp, dps)[...] = shard[...]
    gather = LineGather(spot, sizes, firsts, FIRST_DIMS, line)
    gather.start()
    out_scatter = Scatter(spot, sizes, out_part, out_landing, osend, orecv)
    out_scatter.start()
    limit = prefix[0]
    key_pos = lax.broadcasted_iota(jnp.int32, (keys, tile), 0)
    lane = lax.broadcasted_iota(jnp.int32, (1, 2 * HDIM), 1)
    sides = [
        jnp.where(jnp.logical_and(lane >= a * HDIM, lane < (a + 1) * HDIM), 1.0, 0.0).astype(
            jnp.bfloat16
        )
        for a in range(2)
    ]

    def unit(index, carry):
        pair, part = lax.div(index, 2), lax.rem(index, 2)
        lanes = pl.ds(pl.multiple_of(pair * 2 * HDIM, 2 * HDIM), 2 * HDIM)
        lines = pl.ds(pl.multiple_of(part * tile, tile), tile)
        query_pos = col * tokens + part * tile + lax.broadcasted_iota(jnp.int32, (1, tile), 1)
        allowed = jnp.logical_or(key_pos <= query_pos, key_pos < limit)
        q2, g2 = queries[lines, lanes], grad_out[lines, lanes]
        k2, v2 = kv[0, :, lanes], kv[1, :, lanes]
        dq = jnp.zeros((tile, 2 * HDIM), jnp.float32)
        dk = jnp.zeros((keys, 2 * HDIM), jnp.float32)
        dv = jnp.zeros((keys, 2 * HDIM), jnp.float32)
        for a in range(2):
            ka = k2 * sides[a]
            scores = jnp.where(allowed, dense_nt(ka, q2) * HDIM ** (-0.5), -jnp.inf)
            probs = jnp.exp(scores - log_sums[pl.ds(2 * pair + a, 1), lines])
            grad_probs = dense_nt(v2 * sides[a], g2)
            inner = jnp.sum(probs * grad_probs, axis=0, keepdims=True)
            grad_scores = (probs * (grad_probs - inner)).astype(jnp.bfloat16)
            dq = dq + dense_tn(grad_scores, ka)
            dk = dk + dense(grad_scores, q2 * sides[a])
            dv = dv + dense(probs.astype(jnp.bfloat16), g2 * sides[a])
        grad_q[lines, lanes] = (dq * HDIM ** (-0.5)).astype(jnp.bfloat16)
        dk = dk * HDIM ** (-0.5)

        @pl.when(part == 0)
        def _():
            totals[0, :, lanes] = dk
            totals[1, :, lanes] = dv

        @pl.when(part > 0)
        def _():
            totals[0, :, lanes] = totals[0, :, lanes] + dk
            totals[1, :, lanes] = totals[1, :, lanes] + dv

        pl.when(index == 1)(lambda: gather.event(1))
        pl.when(index == 3)(lambda: gather.event(2))
        return carry

    lax.fori_loop(0, 2 * width // (2 * HDIM), unit, 0)
    size = kv_landing.shape[1]
    other = pl.multiple_of((1 - col) * size, size)
    away = remote(totals.at[:, pl.ds(other, size)], kv_landing, ksend, krecv, (dp, row, 1 - col))
    away.start()
    out_scatter.wait()
    result = hidden[...]
    for q in range(sizes[1]):
        result = result + out_landing[q].astype(jnp.float32)
    output[...] = result.astype(jnp.bfloat16)
    away.wait()
    own = totals[:, pl.ds(pl.multiple_of(col * size, size), size)]
    grad_kv[...] = (own + kv_landing[...]).astype(jnp.bfloat16)
    lax.fori_loop(3, dps, lambda time, c: (gather.event(time), c)[1], 0)
    out_scatter.wait_send()
    gather.finish()


def turn(sizes, prefix, queries, kv, grad_out, log_sums, out_part, hidden, shards):
    tokens, width = queries.shape
    dps, rows, cols = sizes
    low, wide = jnp.bfloat16, jnp.float32
    shape = jax.ShapeDtypeStruct

    def grown(shard, dim):
        full = list(shard.shape)
        full[dim] *= dps
        return tuple(full)

    firsts = [grown(s, d) for s, d in zip(shards, FIRST_DIMS)]
    return pl.pallas_call(
        functools.partial(turn_kernel, sizes),
        in_specs=[pl.BlockSpec(memory_space=pltpu.SMEM)] + [VMEM] * 10,
        out_specs=[VMEM] * 7,
        out_shape=[
            shape((tokens, width), low),
            shape((2, tokens, width), low),
            shape(hidden.shape, low),
        ]
        + [shape(s, low) for s in firsts],
        scratch_shapes=[
            pltpu.VMEM(kv.shape, wide),
            pltpu.VMEM((2, tokens, width), wide),
            pltpu.VMEM((rows,) + hidden.shape, low),
        ]
        + plane_sems(sizes)
        + [DMA, DMA]
        + line_sems(sizes, 4, 3),
        compiler_params=pltpu.CompilerParams(collective_id=2, has_side_effects=True),
        name="turn",
    )(prefix, queries, kv, grad_out, log_sums, out_part, hidden, *shards)


def allowed_mask(query_count, key_count, first_pos, prefix_len):
    query_pos = first_pos + lax.iota(jnp.int32, query_count)
    key_pos = lax.iota(jnp.int32, key_count)
    return (key_pos[None, :] <= query_pos[:, None]) | (key_pos[None, :] < prefix_len)


def flat_picks(picks_head):
    blocks = picks_head.shape[0] // FBLK
    return jnp.swapaxes(picks_head.reshape(blocks, FBLK, TOPK), 1, 2).reshape(blocks, TOPK * FBLK)


def one_hot(row_values, size):
    hot = lax.broadcasted_iota(jnp.int32, (size, row_values.shape[1]), 0) == row_values
    return jnp.where(hot, 1.0, 0.0).astype(jnp.bfloat16)


def route_kernel(rows_dev, owners, cap, picks_ref, rank_ref, meta_ref):
    lane = lax.broadcasted_iota(jnp.int32, (FBLK, FBLK), 0)
    before = jnp.where(lane < lax.broadcasted_iota(jnp.int32, (FBLK, FBLK), 1), 1.0, 0.0).astype(
        jnp.bfloat16
    )
    picks = picks_ref[0]
    owner = picks // rows_dev
    local = picks % rows_dev
    hot = one_hot(owner, owners)
    running = jnp.zeros((owners, 1), jnp.float32)
    ranks = []
    for chunk in range(picks.shape[1] // FBLK):
        part = hot[:, chunk * FBLK : (chunk + 1) * FBLK]
        earlier = jnp.dot(part, before, preferred_element_type=jnp.float32)
        wide = part.astype(jnp.float32)
        ranks.append(jnp.sum(wide * (earlier + running), axis=0, keepdims=True))
        running = running + jnp.sum(wide, axis=1, keepdims=True)
    rank = jnp.concatenate(ranks, axis=1).astype(jnp.int32)
    rank_ref[0] = rank
    slot_hot = one_hot(rank, cap)
    token = lax.broadcasted_iota(jnp.int32, picks.shape, 1) % FBLK
    outs = []
    for payload in (local % SUBKEYS, local // SUBKEYS, token):
        scaled = hot * payload.astype(jnp.float32).astype(jnp.bfloat16)
        outs.append(
            lax.dot_general(
                scaled, slot_hot, (((1,), (1,)), ((), ())), preferred_element_type=jnp.float32
            ).astype(jnp.int32)
        )
    meta_ref[0] = (outs[1] * FBLK + outs[2]) * SUBKEYS + outs[0]


def route(flat, rows_dev, owners, cap):
    blocks, count = flat.shape
    rank, meta = pl.pallas_call(
        functools.partial(route_kernel, rows_dev, owners, cap),
        grid=(blocks,),
        in_specs=[pl.BlockSpec((1, 1, count), lambda i: (i, 0, 0))],
        out_specs=[
            pl.BlockSpec((1, 1, count), lambda i: (i, 0, 0)),
            pl.BlockSpec((1, owners, cap), lambda i: (i, 0, 0)),
        ],
        out_shape=[
            jax.ShapeDtypeStruct((blocks, 1, count), jnp.int32),
            jax.ShapeDtypeStruct((blocks, owners, cap), jnp.int32),
        ],
        name="route",
    )(flat[:, None, :])
    return rank, meta


def weigh_kernel(rows_dev, owners, cap, query_ref, keys_ref, picks_ref, rank_ref, weights_ref, slots_ref):
    picks = picks_ref[0]
    first = lax.dot_general(
        keys_ref[0], query_ref[:, :HALF], (((1,), (1,)), ((), ())), preferred_element_type=jnp.float32
    )
    second = lax.dot_general(
        keys_ref[1], query_ref[:, HALF:], (((1,), (1,)), ((), ())), preferred_element_type=jnp.float32
    )
    upper = picks // SUBKEYS
    lower = picks % SUBKEYS
    key_id = lax.broadcasted_iota(jnp.int32, (SUBKEYS, FBLK), 0)
    rows = []
    for pick in range(TOPK):
        columns = slice(pick * FBLK, (pick + 1) * FBLK)
        chosen = jnp.where(key_id == upper[:, columns], first, 0.0) + jnp.where(
            key_id == lower[:, columns], second, 0.0
        )
        rows.append(jnp.sum(chosen, axis=0, keepdims=True))
    scores = jnp.concatenate(rows, axis=0)
    powers = jnp.exp(scores - jnp.max(scores, axis=0, keepdims=True))
    weights = powers / jnp.sum(powers, axis=0, keepdims=True)
    weights_ref[0] = weights
    flat = jnp.concatenate([weights[pick : pick + 1] for pick in range(TOPK)], axis=1)
    scaled = one_hot(picks // rows_dev, owners) * flat.astype(jnp.bfloat16)
    slots_ref[0] = lax.dot_general(
        scaled,
        one_hot(rank_ref[0], cap),
        (((1,), (1,)), ((), ())),
        preferred_element_type=jnp.float32,
    ).astype(jnp.bfloat16)


def weigh(query_rows, keys_head, flat, rank, rows_dev, owners, cap):
    blocks, count = flat.shape
    return pl.pallas_call(
        functools.partial(weigh_kernel, rows_dev, owners, cap),
        grid=(blocks,),
        in_specs=[
            pl.BlockSpec((FBLK, 2 * HALF), lambda i: (i, 0)),
            pl.BlockSpec((2, SUBKEYS, HALF), lambda i: (0, 0, 0)),
            pl.BlockSpec((1, 1, count), lambda i: (i, 0, 0)),
            pl.BlockSpec((1, 1, count), lambda i: (i, 0, 0)),
        ],
        out_specs=[
            pl.BlockSpec((1, TOPK, FBLK), lambda i: (i, 0, 0)),
            pl.BlockSpec((1, owners, cap), lambda i: (i, 0, 0)),
        ],
        out_shape=[
            jax.ShapeDtypeStruct((blocks, TOPK, FBLK), jnp.float32),
            jax.ShapeDtypeStruct((blocks, owners, cap), jnp.bfloat16),
        ],
        name="weigh",
    )(query_rows, keys_head, flat[:, None, :], rank)


def send_rows(spot, sizes, src, landing, send, recv):
    count = sizes[0] * sizes[1] * sizes[2]
    me = index_of(spot, sizes)

    def one(step, carry):
        other = lax.rem(me + step, count)
        remote(src.at[other], landing.at[me], send, recv, device_of(other, sizes)).start()
        return carry

    lax.fori_loop(1, count, one, 0)
    landing[me] = src[me]


def all_rows(landing, sem):
    return arrived(landing.at[pl.ds(0, landing.shape[0] - 1)], sem)


def slot_row(sizes, table, dp, col, block):
    pieces = []
    for row in range(sizes[1]):
        index = (dp * sizes[1] + row) * sizes[2] + col
        pieces.append(table[index, pl.ds(block, 1), :])
    return jnp.concatenate(pieces, axis=1)


def nth_place(dp, q, dps):
    twice = 2 * jnp.minimum(dp, dps - 1 - dp)
    inside = q <= twice
    distance = jnp.where(inside, lax.div(q + 1, 2), q - lax.div(twice, 2))
    below = jnp.logical_or(
        jnp.logical_and(inside, lax.rem(q, 2) == 1),
        jnp.logical_and(jnp.logical_not(inside), dp > dps - 1 - dp),
    )
    return dp + jnp.where(below, -distance, distance), below


def plane_neighbours(row, rows):
    across = row + 1 - 2 * lax.rem(row, 2)
    along = lax.rem(row + rows // 2, rows)
    return across, along, lax.rem(across + rows // 2, rows)


RING = 3


def memory_kernel(
    sizes, blocks, grads, meta, slots, values, values_t,
    grads_all, table, other_part, memory, back,
    meta_in, slots_in, tables, parts,
    chunks, found, sums, grids, theirs, acc, first_land, side_land, deep_land, total,
    msend, mrecv, ssend, srecv, zup, zdown, zrecv, wsend, wrecv, csend, crecv,
    local, tsem, qsend, qrecv,
    gsem, esem, hsend, hrecv, xsend, xrecv, dsend, drecv, fsend, frecv, flocal,
):
    spot = here()
    dp, row, col = spot
    dps, rows, cols = sizes
    tokens, width = grads.shape
    half = tokens // 2
    areas = values.shape[0] // SUBKEYS
    count = dps * rows * cols
    me = index_of(spot, sizes)
    across, along, opposite = plane_neighbours(row, rows)
    first_half, second_half = pl.ds(0, half), pl.ds(half, half)
    greet_all(spot, sizes)
    send_rows(spot, sizes, meta, meta_in, msend, mrecv)
    send_rows(spot, sizes, slots, slots_in, ssend, srecv)

    def place_of(u):
        return nth_place(dp, dps - 1 - u, dps)[0]

    def block_at(place, r, lines=slice(None)):
        return grads_all.at[place, col, r, lines]

    def cross(q, place, r, src=None):
        there = block_at(place, r)
        remote(there if src is None else src, there, csend, crecv.at[q], (dp, row, 1 - col)).start()

    def line_copy(place, up, src=None):
        there = block_at(place, row)
        return remote(
            there if src is None else src,
            there,
            (zup if up else zdown).at[place],
            zrecv.at[place],
            (jnp.clip(dp + (1 if up else -1), 0, dps - 1), row, col),
        )

    def sideways(q, place, src=None):
        there = block_at(place, row)
        for n, r in enumerate((across, along)):
            remote(
                there if src is None else src, there, wsend, wrecv.at[q, n], (dp, r, col)
            ).start()

    pl.when(dp < dps - 1)(lambda: line_copy(dp, True, grads).start())
    pl.when(dp > 0)(lambda: line_copy(dp, False, grads).start())
    sideways(0, dp, grads)
    cross(0, dp, row, grads)
    keep = pltpu.make_async_copy(grads, block_at(dp, row), local)
    keep.start()

    def from_line(q):
        place, below = nth_place(dp, q, dps)
        arrived(block_at(place, row), zrecv.at[place])
        pl.when(jnp.logical_and(below, dp < dps - 1))(lambda: line_copy(place, True).start())
        pl.when(jnp.logical_and(jnp.logical_not(below), dp > 0))(
            lambda: line_copy(place, False).start()
        )
        sideways(q, place)
        cross(q, place, row)

    def from_sides(q):
        place, _ = nth_place(dp, q, dps)
        for n, (r, other, lines) in enumerate(
            ((across, along, first_half), (along, across, second_half))
        ):
            arrived(block_at(place, r), wrecv.at[q, n])
            half = block_at(place, r, lines)
            remote(half, half, wsend, wrecv.at[q, 2 + n], (dp, other, col)).start()
            cross(q, place, r)

    def from_opposite(q):
        place, _ = nth_place(dp, q, dps)
        for n, lines in enumerate((first_half, second_half)):
            arrived(block_at(place, opposite, lines), wrecv.at[q, 2 + n])
        cross(q, place, opposite)

    all_rows(meta_in, mrecv)
    all_rows(slots_in, srecv)

    def write_places(chunk):
        turn = lax.div(chunk, 2)
        slot = lax.rem(chunk, 2)
        return turn, slot, place_of(turn), jnp.where(slot == 0, 1 - col, col)

    def table_copy(chunk):
        _, slot, source_dp, source_col = write_places(chunk)
        return pltpu.make_async_copy(
            tables.at[slot], table.at[source_dp, source_col], tsem.at[slot]
        )

    def build(chunk):
        turn, slot, source_dp, source_col = write_places(chunk)
        pl.when(turn > 0)(lambda: table_copy(chunk).wait())
        def one(block, carry):
            row_meta = slot_row(sizes, meta_in, source_dp, source_col, block)
            key = row_meta // SUBKEYS
            low = row_meta % SUBKEYS
            weight = slot_row(sizes, slots_in, source_dp, source_col, block)
            at_key = lax.broadcasted_iota(jnp.int32, (areas * FBLK, key.shape[1]), 0) == key
            left = jnp.where(at_key, weight, 0.0).astype(jnp.bfloat16)
            stacked = lax.dot_general(
                left,
                one_hot(low, SUBKEYS),
                (((1,), (1,)), ((), ())),
                preferred_element_type=jnp.float32,
            ).astype(jnp.bfloat16)
            for area in range(areas):
                tables[
                    slot,
                    pl.ds(pl.multiple_of(block * FBLK, FBLK), FBLK),
                    area * SUBKEYS : (area + 1) * SUBKEYS,
                ] = stacked[area * FBLK : (area + 1) * FBLK]
            return carry

        lax.fori_loop(0, blocks, one, 0)
        table_copy(chunk).start()

    def away(turn, source_dp):
        return remote(parts.at[0], other_part.at[source_dp], qsend, qrecv.at[turn], (dp, row, 1 - col))

    def multiply(chunk):
        turn, slot, source_dp, _ = write_places(chunk)
        later = turn > 0
        pl.when(jnp.logical_and(later, slot == 0))(lambda: away(turn, source_dp).wait_send())

        def strip(n, carry):
            columns = pl.ds(pl.multiple_of(n * 512, 512), 512)
            parts[slot, :, columns] = jnp.dot(
                tables[slot], values[:, columns], preferred_element_type=jnp.float32
            ).astype(jnp.bfloat16)
            return carry

        lax.fori_loop(0, values.shape[1] // 512, strip, 0)
        pl.when(slot == 0)(lambda: away(turn, source_dp).start())

    def load_part(u):
        return pltpu.make_async_copy(other_part.at[place_of(u)], theirs, esem)

    def strip(u, r, lines=slice(None)):
        return acc.at[lax.rem(u, RING), lines, pl.ds(pl.multiple_of(r * width, width), width)]

    lines_of = (pl.ds(0, half), pl.ds(half, half))

    def halves(u):
        return [
            remote(
                strip(u, opposite, lines_of[n]), first_land.at[u, n],
                hsend.at[lax.rem(u, RING), n], hrecv.at[u, n], (dp, r, col),
            )
            for n, r in enumerate((across, along))
        ]

    def wholes(u):
        return [
            remote(
                strip(u, r), side_land.at[u, n],
                xsend.at[lax.rem(u, RING), n], xrecv.at[u, n], (dp, r, col),
            )
            for n, r in enumerate((across, along))
        ]

    def sent(u):
        for copy in halves(u) + wholes(u):
            copy.wait_send()

    def combine(u):
        arrived(other_part.at[place_of(u)], qrecv.at[u])
        pl.when(u >= RING)(lambda: sent(u - RING))
        load_part(u).start()
        load_part(u).wait()
        acc[lax.rem(u, RING)] = (
            parts[1].astype(jnp.float32) + theirs[...].astype(jnp.float32)
        ).astype(jnp.bfloat16)
        for copy in halves(u):
            copy.start()

    def relay(u):
        for n, r in enumerate((along, across)):
            arrived(first_land.at[u, n], hrecv.at[u, n])
            add_into(strip(u, r, lines_of[n]), first_land.at[u, n])
        for copy in wholes(u):
            copy.start()

    def deep_copy(u):
        place = place_of(u)
        up = place > dp
        target = jnp.where(up, dp + 1, dp - 1)
        there = jnp.where(jnp.logical_and(jnp.logical_not(up), target == place), dps, place)
        return remote(
            total.at[u], deep_land.at[there], dsend.at[u], drecv.at[there],
            (jnp.clip(target, 0, dps - 1), row, col),
        )

    def finish(u):
        for n in range(2):
            arrived(side_land.at[u, n], xrecv.at[u, n])
        place = place_of(u)
        result = (
            strip(u, row)[...].astype(jnp.float32)
            + side_land[u, 0].astype(jnp.float32)
            + side_land[u, 1].astype(jnp.float32)
        )
        memory[...] = result

        def more(index):
            arrived(deep_land.at[index], drecv.at[index])
            memory[...] = memory[...] + deep_land[index].astype(jnp.float32)

        below = jnp.logical_and(place >= dp, dp > 0)
        above = jnp.logical_and(place <= dp, dp < dps - 1)
        pl.when(jnp.logical_or(below, jnp.logical_and(above, place < dp)))(lambda: more(place))
        pl.when(jnp.logical_and(above, place == dp))(lambda: more(dps))

        @pl.when(u < dps - 1)
        def _():
            total[u] = memory[...].astype(jnp.bfloat16)
            deep_copy(u).start()

    def read_places(chunk):
        slot = lax.rem(chunk, 2)
        place = nth_place(dp, lax.div(chunk, 2), dps)[0]
        return slot, place, jnp.where(slot == 0, col, 1 - col)

    def load_chunk(chunk):
        slot, source_dp, source_col = read_places(chunk)
        return [
            pltpu.make_async_copy(
                grads_all.at[source_dp, source_col, r],
                chunks.at[slot, :, pl.ds(r * width, width)],
                gsem.at[slot, r],
            )
            for r in range(rows)
        ]

    def start_chunk(chunk):
        slot, source_dp, source_col = read_places(chunk)

        @pl.when(slot == 1)
        def _():
            arrived(grads_all.at[source_dp, source_col], crecv.at[lax.div(chunk, 2)])

        for copy in load_chunk(chunk):
            copy.start()

    wide_strip = min(512, areas * SUBKEYS)
    per_strip = wide_strip // SUBKEYS

    def search(chunk, part):
        slot, source_dp, source_col = read_places(chunk)

        @pl.when(part == 0)
        def _():
            for copy in load_chunk(chunk):
                copy.wait()

            def strip(n, carry):
                columns = pl.ds(pl.multiple_of(n * wide_strip, wide_strip), wide_strip)
                grid = jnp.dot(
                    chunks[slot], values_t[:, columns], preferred_element_type=jnp.float32
                ).astype(jnp.bfloat16)
                for area in range(per_strip):
                    grids[n * per_strip + area] = grid[:, area * SUBKEYS : (area + 1) * SUBKEYS]
                return carry

            lax.fori_loop(0, areas // per_strip, strip, 0)

            @pl.when(chunk + 2 < dps * cols)
            def _():
                start_chunk(chunk + 2)

        @pl.when(part == 1)
        def _():
            def one(block, carry):
                row_meta = slot_row(sizes, meta_in, source_dp, source_col, block)
                lines = pl.ds(pl.multiple_of(block * FBLK, FBLK), FBLK)
                stacked = grids[:, lines, :].reshape(areas * FBLK, SUBKEYS)
                product = jnp.dot(
                    stacked, one_hot(row_meta % SUBKEYS, SUBKEYS), preferred_element_type=jnp.float32
                )
                spot_id = lax.broadcasted_iota(jnp.int32, product.shape, 0)
                sums[block] = jnp.sum(
                    jnp.where(spot_id == row_meta // SUBKEYS, product, 0.0), axis=0, keepdims=True
                )
                return carry

            lax.fori_loop(0, blocks, one, 0)

            for r in range(rows):
                index = (source_dp * rows + r) * cols + source_col
                for block in range(blocks):
                    found[index, block : block + 1, :] = sums[block, :, r * 128 : (r + 1) * 128]
                away = remote(found.at[index], back.at[me], fsend, frecv, (source_dp, r, source_col))
                own = jnp.logical_and(
                    jnp.logical_and(source_dp == dp, row == r), source_col == col
                )
                pl.when(jnp.logical_not(own))(away.start)
                pl.when(own)(pltpu.make_async_copy(found.at[index], back.at[me], flocal).start)

    writes = 4 * dps

    def poll(p, carry):
        phase = lax.rem(p, 2)
        writing = p < writes
        pl.when(jnp.logical_and(writing, phase == 0))(lambda: build(lax.div(p, 2)))
        pl.when(jnp.logical_and(writing, phase == 1))(lambda: multiply(lax.div(p, 2)))

        @pl.when(p == writes)
        def _():
            keep.wait()
            start_chunk(0)
            start_chunk(1)

        pl.when(p >= writes)(lambda: search(lax.div(p - writes, 2), phase))
        turn, third = lax.div(p, 3), lax.rem(p, 3)
        early = jnp.logical_and(third == 0, jnp.logical_and(turn > 0, turn + 1 < dps))
        pl.when(p == 1)(lambda: from_line(1))
        pl.when(early)(lambda: from_line(turn + 1))
        pl.when(jnp.logical_and(third == 2, turn < dps))(lambda: from_sides(turn))
        ready = jnp.logical_and(turn > 0, turn <= dps)
        pl.when(jnp.logical_and(third == 1, ready))(lambda: from_opposite(turn - 1))
        for event, delay in ((finish, FINISH_AT), (relay, RELAY_AT), (combine, COMBINE_AT)):
            late = p - delay
            now = jnp.logical_and(
                jnp.logical_and(late >= 0, lax.rem(late, 4) == 0), late < 4 * dps
            )
            pl.when(now)(functools.partial(event, lax.div(late, 4)))
        return carry

    lax.fori_loop(0, 8 * dps, poll, 0)
    for slot in range(2):
        pltpu.make_async_copy(tables.at[slot], table.at[0, 0], tsem.at[slot]).wait()
    away(0, 0).wait_send()
    arrived(grads_all.at[:, 0], csend)
    arrived(grads_all.at[:, 0, pl.ds(0, rows - 1)], wsend)
    all_rows(meta_in, msend)
    all_rows(slots_in, ssend)

    def line_sent(k, carry):
        pl.when(jnp.logical_and(k <= dp, dp < dps - 1))(lambda: line_copy(k, True).wait_send())
        pl.when(jnp.logical_and(k >= dp, dp > 0))(lambda: line_copy(k, False).wait_send())
        return carry

    lax.fori_loop(0, dps, line_sent, 0)
    arrived(back.at[pl.ds(0, count - 1)], frecv)
    arrived(back.at[0], flocal)
    arrived(back.at[pl.ds(0, count - 1)], fsend)
    for u in range(max(0, dps - RING), dps):
        sent(u)
    lax.fori_loop(0, dps - 1, lambda u, c: (deep_copy(u).wait_send(), c)[1], 0)


COMBINE_AT, RELAY_AT, FINISH_AT = 6, 9, 14


def use_memory(sizes, grads, meta, slots, values, values_t):
    dps, rows, cols = sizes
    tokens, width = grads.shape
    rows_dev, features = values.shape
    blocks = tokens // FBLK
    count = dps * rows * cols
    low, wide = jnp.bfloat16, jnp.float32
    shape = jax.ShapeDtypeStruct
    grads_all, table, _, memory, back = pl.pallas_call(
        functools.partial(memory_kernel, sizes, blocks),
        in_specs=[VMEM] * 5,
        out_specs=[ANY] * 3 + [VMEM] * 2,
        out_shape=[
            shape((dps, cols, rows, tokens, width), low),
            shape((dps, cols, tokens, rows_dev), low),
            shape((dps, tokens, features), low),
            shape((tokens, width), wide),
            shape((count, blocks, 128), wide),
        ],
        scratch_shapes=[
            pltpu.VMEM(meta.shape, meta.dtype),
            pltpu.VMEM(slots.shape, slots.dtype),
            pltpu.VMEM((2, tokens, rows_dev), low),
            pltpu.VMEM((2, tokens, features), low),
            pltpu.VMEM((2, tokens, features), low),
            pltpu.VMEM((count, blocks, 128), wide),
            pltpu.VMEM((blocks, 1, rows * 128), wide),
            pltpu.VMEM((rows_dev // SUBKEYS, tokens, SUBKEYS), low),
            pltpu.VMEM((tokens, features), low),
            pltpu.VMEM((RING, tokens, features), low),
            pltpu.VMEM((dps, 2, tokens // 2, width), low),
            pltpu.VMEM((dps, 2, tokens, width), low),
            pltpu.VMEM((dps + 1, tokens, width), low),
            pltpu.VMEM((dps, tokens, width), low),
            DMA, DMA, DMA, DMA,
            DMA((dps,)), DMA((dps,)), DMA((dps,)),
            DMA, DMA((dps, 4)),
            DMA, DMA((dps,)),
            DMA, DMA((2,)), DMA, DMA((dps,)),
            DMA((2, rows)), DMA,
            DMA((RING, 2)), DMA((dps, 2)),
            DMA((RING, 2)), DMA((dps, 2)),
            DMA((dps,)), DMA((dps + 1,)),
            DMA, DMA, DMA,
        ],
        compiler_params=pltpu.CompilerParams(collective_id=6, has_side_effects=True),
        name="use_memory",
    )(grads, meta, slots, values, values_t)
    return grads_all, table, memory, back


def unweigh_kernel(rows_dev, owners, back_ref, picks_ref, rank_ref, weights_ref, first_ref, second_ref):
    picks = picks_ref[0]
    hot = one_hot(picks // rows_dev, owners)
    back = back_ref[0]
    high = back.astype(jnp.bfloat16)
    rest = back - high.astype(jnp.float32)
    middle = rest.astype(jnp.bfloat16)
    lowest = (rest - middle.astype(jnp.float32)).astype(jnp.bfloat16)
    spread_back = (
        jnp.dot(high, hot, preferred_element_type=jnp.float32)
        + jnp.dot(middle, hot, preferred_element_type=jnp.float32)
        + jnp.dot(lowest, hot, preferred_element_type=jnp.float32)
    )
    slot = lax.broadcasted_iota(jnp.int32, spread_back.shape, 0)
    flat = jnp.sum(jnp.where(slot == rank_ref[0], spread_back, 0.0), axis=0, keepdims=True)
    grads = jnp.concatenate(
        [flat[:, pick * FBLK : (pick + 1) * FBLK] for pick in range(TOPK)], axis=0
    )
    weights = weights_ref[0]
    grads = weights * (grads - jnp.sum(weights * grads, axis=0, keepdims=True))
    upper = picks // SUBKEYS
    lower = picks % SUBKEYS
    key_id = lax.broadcasted_iota(jnp.int32, (SUBKEYS, FBLK), 0)
    first = jnp.zeros((SUBKEYS, FBLK), jnp.float32)
    second = jnp.zeros((SUBKEYS, FBLK), jnp.float32)
    for pick in range(TOPK):
        columns = slice(pick * FBLK, (pick + 1) * FBLK)
        value = grads[pick : pick + 1]
        first = first + jnp.where(key_id == upper[:, columns], value, 0.0)
        second = second + jnp.where(key_id == lower[:, columns], value, 0.0)
    first_ref[...] = first.astype(jnp.bfloat16)
    second_ref[...] = second.astype(jnp.bfloat16)


def unweigh(back, flat, rank, weights, rows_dev, owners):
    blocks, count = flat.shape
    cap = back.shape[1]
    return pl.pallas_call(
        functools.partial(unweigh_kernel, rows_dev, owners),
        grid=(blocks,),
        in_specs=[
            pl.BlockSpec((1, cap, owners), lambda i: (i, 0, 0)),
            pl.BlockSpec((1, 1, count), lambda i: (i, 0, 0)),
            pl.BlockSpec((1, 1, count), lambda i: (i, 0, 0)),
            pl.BlockSpec((1, TOPK, FBLK), lambda i: (i, 0, 0)),
        ],
        out_specs=[
            pl.BlockSpec((SUBKEYS, FBLK), lambda i: (0, i)),
            pl.BlockSpec((SUBKEYS, FBLK), lambda i: (0, i)),
        ],
        out_shape=[jax.ShapeDtypeStruct((SUBKEYS, blocks * FBLK), jnp.bfloat16)] * 2,
        name="unweigh",
    )(back, flat[:, None, :], rank, weights)


def memory_all(query_rows, grad_memory, picks, subkeys, values):
    sizes = grid_sizes()
    owners = sizes[0] * sizes[1] * sizes[2]
    rows_dev = values.shape[0]
    cap = FBLK * TOPK // owners
    head_id = lax.axis_index("row")
    keys_head = lax.dynamic_index_in_dim(subkeys, head_id, 0, keepdims=False)
    picks_head = lax.dynamic_index_in_dim(picks, head_id, 1, keepdims=False)
    flat = flat_picks(picks_head)
    rank, meta = route(flat, rows_dev, owners, cap)
    weights, slots = weigh(query_rows, keys_head, flat, rank, rows_dev, owners, cap)
    spare = ((0, 0), (0, 0), (0, 128 - cap))
    meta = jnp.pad(jnp.swapaxes(meta, 0, 1), spare, constant_values=-1)
    slots = jnp.pad(jnp.swapaxes(slots, 0, 1).astype(jnp.float32), spare)
    grads_all, table, memory, back = use_memory(
        sizes, grad_memory, meta, slots, values, values.T
    )
    first_t, second_t = unweigh(
        jnp.transpose(back, (1, 2, 0))[:, :cap], flat, rank, weights, rows_dev, owners
    )
    grad_query = jnp.concatenate(
        [
            lax.dot_general(
                part, keys_head[i], (((0,), (0,)), ((), ())), preferred_element_type=jnp.float32
            )
            for i, part in enumerate((first_t, second_t))
        ],
        axis=1,
    ).astype(jnp.bfloat16)
    grad_keys = jnp.stack(
        [
            jnp.dot(first_t, query_rows[:, :HALF], preferred_element_type=jnp.float32),
            jnp.dot(second_t, query_rows[:, HALF:], preferred_element_type=jnp.float32),
        ]
    )
    return memory, grad_query, grad_keys, table, grads_all


def head_scores(query_head, key_head, allowed):
    raw_scores = jnp.einsum(
        "qd,kd->qk", query_head, key_head, preferred_element_type=jnp.float32
    ) * HDIM ** (-0.5)
    return jnp.where(allowed, raw_scores, -jnp.inf)


def attend_forward(queries, keys, values, allowed):
    outputs = []
    log_sums = []
    for head_index in range(queries.shape[1] // HDIM):
        columns = slice(head_index * HDIM, (head_index + 1) * HDIM)
        scores = head_scores(queries[:, columns], keys[:, columns], allowed)
        peak_score = jnp.max(scores, axis=1, keepdims=True)
        exp_scores = jnp.exp(scores - peak_score)
        row_sum = jnp.sum(exp_scores, axis=1, keepdims=True)
        probabilities = (exp_scores / row_sum).astype(jnp.bfloat16)
        outputs.append(
            jnp.dot(probabilities, values[:, columns], preferred_element_type=jnp.float32)
        )
        log_sums.append(peak_score[:, 0] + jnp.log(row_sum[:, 0]))
    return (jnp.concatenate(outputs, axis=1), jnp.stack(log_sums))


def dense(left, right):
    return jnp.dot(left, right, preferred_element_type=jnp.float32)


def dense_nt(left, right):
    return lax.dot_general(left, right, (((1,), (1,)), ((), ())), preferred_element_type=jnp.float32)


def dense_tn(left, right):
    return lax.dot_general(left, right, (((0,), (0,)), ((), ())), preferred_element_type=jnp.float32)


def per_device(
    inputs,
    prefix,
    picks,
    gain_attn,
    w_qkv,
    w_attn_out,
    gain_mem,
    w_query,
    w_gate,
    w_proj,
    subkeys,
    values,
    cotangent,
):
    low = jnp.bfloat16
    sizes = grid_sizes()
    width_part = inputs.shape[1]
    own_tokens = picks.shape[0]
    seq_tokens = own_tokens * sizes[2]
    col = lax.axis_index("col")
    col_first = col * width_part
    gain_one = lax.dynamic_slice_in_dim(gain_attn, col_first, width_part)
    gain_two = lax.dynamic_slice_in_dim(gain_mem, col_first, width_part)

    x_own, dy_own, qkv_w, query_w, gate_w, proj_w, attn_w = start_all(
        sizes, inputs, cotangent, w_qkv, w_query, w_gate, w_proj, w_attn_out
    )
    residual = x_own.astype(jnp.float32)
    scale_one = lax.rsqrt(jnp.sum(residual * residual, axis=1, keepdims=True) / D + EPSILON)
    normed_one = (residual * scale_one * gain_attn.astype(jnp.float32)).astype(low)
    qkv = jnp.einsum("tc,jcf->jtf", normed_one, qkv_w, preferred_element_type=jnp.float32).astype(low)
    kv_all = swap_tokens(sizes, qkv[1:])
    allowed = allowed_mask(own_tokens, seq_tokens, col * own_tokens, prefix[0])
    attended_sum, log_sums = attend_forward(qkv[0], kv_all[0], kv_all[1], allowed)
    attended = attended_sum.astype(low)
    hidden, normed_two = join(sizes, dense(attended, attn_w).astype(low), inputs, gain_two)
    query_rows = dense(normed_two, query_w).astype(low)
    gate_value = dense(normed_two, gate_w)
    sigmoid_gate = jax.nn.sigmoid(gate_value)
    silu_gate = gate_value * sigmoid_gate
    grad_gated = dense_nt(dy_own, proj_w)
    grad_memory = (grad_gated * silu_gate).astype(low)
    memory, grad_query, grad_keys, table, grads_all = memory_all(
        query_rows, grad_memory, picks, subkeys, values
    )
    gated_value = (memory * silu_gate).astype(low)
    out_part = dense(gated_value, proj_w).astype(low)
    grad_gate = (
        grad_gated * memory * sigmoid_gate * (1.0 + gate_value * (1.0 - sigmoid_gate))
    ).astype(low)
    grad_part = (dense_nt(grad_query, query_w) + dense_nt(grad_gate, gate_w)).astype(low)
    first_terms = [
        dense_tn(normed_two, grad_query).astype(low),
        dense_tn(normed_two, grad_gate).astype(low),
        dense_tn(gated_value, dy_own).astype(low),
        grad_keys.reshape(-1, HALF).astype(low),
    ]
    grad_hidden, grad_hidden_all, gain_two_grad, *shards = middle(
        sizes, grad_part, hidden, cotangent, gain_two, first_terms
    )
    grad_attended = dense_nt(grad_hidden_all, attn_w).astype(low)
    grad_q, grad_kv, output, grad_w_query, grad_w_gate, grad_w_proj, grad_keys_half = turn(
        sizes, prefix, qkv[0], kv_all, grad_attended, log_sums, out_part, hidden, shards
    )
    x_part = (
        dense_nt(grad_q, qkv_w[0]) + dense_nt(grad_kv[0], qkv_w[1]) + dense_nt(grad_kv[1], qkv_w[2])
    ).astype(low)
    last_terms = [
        jnp.stack([dense_tn(normed_one, part) for part in (grad_q, grad_kv[0], grad_kv[1])]).astype(low),
        dense_tn(attended, grad_hidden_all).astype(low),
    ]
    grad_inputs, gain_sums, grad_values, grad_w_qkv, grad_w_attn_out, grad_subkeys = last(
        sizes, x_part, inputs, grad_hidden, gain_one, gain_two_grad, grad_keys_half, last_terms,
        table, grads_all,
    )
    gain_rows = gain_sums.reshape(sizes[2], 2, width_part)
    grad_gain_one = gain_rows[:, 0].reshape(-1)
    grad_gain_two = gain_rows[:, 1].reshape(-1)

    return (
        output,
        grad_inputs,
        grad_gain_one,
        grad_w_qkv.astype(jnp.float32),
        grad_w_attn_out.astype(jnp.float32),
        grad_gain_two,
        grad_w_query.astype(jnp.float32),
        grad_w_gate.astype(jnp.float32),
        grad_w_proj.astype(jnp.float32),
        grad_subkeys.astype(jnp.float32),
        grad_values,
    )


def solution(mesh):
    placed = (
        P(("dp", "row"), "col"),
        P("dp"),
        P(("dp", "col"), None, None),
        P(),
        P(None, "col", "row"),
        P("row", "col"),
        P(),
        P("col", "row"),
        P("col", "row"),
        P("row", "col"),
        P(),
        P(("dp", "row", "col"), None),
        P(("dp", "row"), "col"),
    )
    return jax.shard_map(
        per_device,
        mesh=mesh,
        in_specs=placed,
        out_specs=(
            P(("dp", "row"), "col"),
            P(("dp", "row"), "col"),
            P(),
            P(None, "col", "row"),
            P("row", "col"),
            P(),
            P("col", "row"),
            P("col", "row"),
            P("row", "col"),
            P(),
            P(("dp", "row", "col"), None),
        ),
        check_vma=False,
    )
```

```python
import functools

import jax
import jax.numpy as jnp
from jax import lax
from jax.experimental import pallas as pl
from jax.experimental.pallas import tpu as pltpu
from jax.sharding import PartitionSpec as P

D = 1024
HDIM = 64
HALF = 512
SUBKEYS = 256
TOPK = 32
FBLK = 128


EPSILON = 1e-06


MESH = pl.DeviceIdType.MESH
VMEM = pl.BlockSpec(memory_space=pltpu.VMEM)
ANY = pl.BlockSpec(memory_space=pl.ANY)
DMA = pltpu.SemaphoreType.DMA


def here():
    return lax.axis_index("dp"), lax.axis_index("row"), lax.axis_index("col")


def grid_sizes():
    return lax.axis_size("dp"), lax.axis_size("row"), lax.axis_size("col")


def remote(src, dst, send_sem, recv_sem, device):
    return pltpu.make_async_remote_copy(
        src_ref=src,
        dst_ref=dst,
        send_sem=send_sem,
        recv_sem=recv_sem,
        device_id=device,
        device_id_type=MESH,
    )


def arrived(dst, sem):
    pltpu.make_async_copy(dst, dst, sem).wait()


def greet_plane(spot, sizes):
    barrier = pltpu.get_barrier_semaphore()
    dp, row, col = spot
    _, rows, cols = sizes
    for j in range(rows):
        for k in range(cols):
            if j + k > 0:
                pl.semaphore_signal(
                    barrier,
                    inc=1,
                    device_id=(dp, lax.rem(row + j, rows), lax.rem(col + k, cols)),
                    device_id_type=MESH,
                )
    pl.semaphore_wait(barrier, rows * cols - 1)


def greet_partner(spot, sizes):
    barrier = pltpu.get_barrier_semaphore()
    dp, row, col = spot
    pl.semaphore_signal(barrier, inc=1, device_id=(dp, row, 1 - col), device_id_type=MESH)
    pl.semaphore_wait(barrier, 1)


def index_of(spot, sizes):
    return (spot[0] * sizes[1] + spot[1]) * sizes[2] + spot[2]


def each_other(spot, sizes, action):
    dp, row, col = spot
    dps, rows, cols = sizes

    def level(step, carry):
        there = lax.rem(dp + step, dps)
        for j in range(rows):
            for k in range(cols):
                device = (there, lax.rem(row + j, rows), lax.rem(col + k, cols))
                if j + k > 0:
                    action(device)
                else:
                    pl.when(step > 0)(functools.partial(action, device))
        return carry

    lax.fori_loop(0, dps, level, 0)


def greet_all(spot, sizes):
    barrier = pltpu.get_barrier_semaphore()

    def greet(device):
        pl.semaphore_signal(barrier, inc=1, device_id=device, device_id_type=MESH)

    each_other(spot, sizes, greet)
    pl.semaphore_wait(barrier, sizes[0] * sizes[1] * sizes[2] - 1)


class Gather:
    def __init__(self, spot, sizes, src, dst, send, recv):
        self.spot, self.sizes, self.src, self.dst = spot, sizes, src, dst
        self.send, self.recv = send, recv
        self.tokens, self.width = src.shape
        dp, row, col = spot
        _, rows, cols = sizes
        self.half = rows // cols
        self.target = lax.div(row, self.half)
        self.slot = lax.rem(row, self.half) * cols + col
        first = pl.multiple_of(lax.rem(row, self.half) * self.tokens, self.tokens)
        left = pl.multiple_of(col * self.width, self.width)
        self.there = dst.at[pl.ds(first, self.tokens), pl.ds(left, self.width)]

    def copy(self, step):
        dp, row, _ = self.spot
        device = (dp, lax.rem(row + step, self.sizes[1]), self.target)
        return remote(self.src, self.there, self.send.at[step], self.recv.at[self.slot], device)

    def start(self):
        col = self.spot[2]

        for step in range(1, self.sizes[1]):
            self.copy(step).start()

        @pl.when(self.target == col)
        def _():
            pltpu.make_async_copy(self.src, self.there, self.recv.at[self.slot]).start()

        @pl.when(self.target != col)
        def _():
            self.copy(0).start()

    def wait(self):
        cols = self.sizes[2]
        for i in range(self.half):
            for k in range(cols):
                arrived(
                    self.dst.at[pl.ds(i * self.tokens, self.tokens), pl.ds(k * self.width, self.width)],
                    self.recv.at[i * cols + k],
                )
        for step in range(1, self.sizes[1]):
            self.copy(step).wait_send()

        @pl.when(self.target != self.spot[2])
        def _():
            self.copy(0).wait_send()


class Scatter:
    def __init__(self, spot, sizes, src, landing, send, recv):
        self.spot, self.sizes, self.src, self.landing = spot, sizes, src, landing
        self.send, self.recv = send, recv
        _, self.tokens, self.width = landing.shape
        self.half = sizes[1] // sizes[2]

    def parts(self):
        dp, row, col = self.spot
        cols = self.sizes[2]
        for i in range(self.half):
            for k in range(cols):
                piece = self.src.at[
                    pl.ds(i * self.tokens, self.tokens), pl.ds(k * self.width, self.width)
                ]
                target = col * self.half + i
                mine = jnp.logical_and(target == row, col == k)
                there = self.landing.at[row]
                copy = remote(
                    piece, there, self.send.at[i * cols + k], self.recv.at[row], (dp, target, k)
                )
                yield mine, copy, pltpu.make_async_copy(piece, there, self.recv.at[row])

    def start(self):
        for mine, copy, own in self.parts():
            pl.when(jnp.logical_not(mine))(copy.start)
            pl.when(mine)(own.start)

    def wait(self):
        for q in range(self.sizes[1]):
            arrived(self.landing.at[q], self.recv.at[q])

    def wait_send(self):
        for mine, copy, _ in self.parts():
            pl.when(jnp.logical_not(mine))(copy.wait_send)


def plane_sems(sizes):
    rows, cols = sizes[1], sizes[2]
    return [DMA((rows,)), DMA((rows,))]


def start_kernel(sizes, rows_dev, *refs):
    x, dy, wqkv, wquery, wgate, wproj, wattn, picks = refs[:8]
    xs, dys, wqkv_all, wquery_all, wgate_all, wproj_all, wattn_all, rank, meta = refs[8:17]
    xsend, xrecv, ysend, yrecv, wsend, wrecv, wlocal = refs[17:]
    spot = here()
    dp, row, col = spot
    greet_plane(spot, sizes)
    gather_x = Gather(spot, sizes, x, xs, xsend, xrecv)
    gather_y = Gather(spot, sizes, dy, dys, ysend, yrecv)
    gather_x.start()
    gather_y.start()
    copies = []
    for n, (src, dst, dim) in enumerate(
        (
            (wqkv, wqkv_all, 1),
            (wquery, wquery_all, 0),
            (wgate, wgate_all, 0),
            (wproj, wproj_all, 1),
            (wattn, wattn_all, 1),
        )
    ):
        size = src.shape[dim]
        window = [slice(None)] * len(src.shape)
        window[dim] = pl.ds(pl.multiple_of(col * size, size), size)
        there = dst.at[tuple(window)]
        away = remote(src, there, wsend.at[n], wrecv.at[n], (dp, row, 1 - col))
        own = pltpu.make_async_copy(src, there, wlocal.at[n])
        away.start()
        own.start()
        copies += [away, own]

    def one(block, carry):
        rank[block], meta[block] = route_block(
            picks[block], rows_dev, meta.shape[1], meta.shape[2]
        )
        return carry

    lax.fori_loop(0, picks.shape[0], one, 0)
    for copy in copies:
        copy.wait()
    gather_x.wait()
    gather_y.wait()


def start_all(sizes, rows_dev, x, dy, wqkv, wquery, wgate, wproj, wattn, flat):
    tokens, width = x.shape
    half = sizes[1] // sizes[2]
    cols = sizes[2]
    low = jnp.bfloat16

    def twice(operand, dim):
        shape = list(operand.shape)
        shape[dim] *= cols
        return jax.ShapeDtypeStruct(tuple(shape), low)

    whole = jax.ShapeDtypeStruct((half * tokens, cols * width), low)
    blocks, count = flat.shape
    owners = sizes[0] * sizes[1] * sizes[2]
    return pl.pallas_call(
        functools.partial(start_kernel, sizes, rows_dev),
        in_specs=[VMEM] * 8,
        out_specs=[ANY] * 7 + [VMEM] * 2,
        out_shape=[
            whole,
            whole,
            twice(wqkv, 1),
            twice(wquery, 0),
            twice(wgate, 0),
            twice(wproj, 1),
            twice(wattn, 1),
            jax.ShapeDtypeStruct((blocks, 1, count), jnp.int32),
            jax.ShapeDtypeStruct((blocks, owners, count // owners), jnp.int32),
        ],
        scratch_shapes=plane_sems(sizes) * 2 + [DMA((5,))] * 3,
        compiler_params=pltpu.CompilerParams(collective_id=0, has_side_effects=True),
        name="start_all",
    )(x, dy, wqkv, wquery, wgate, wproj, wattn, flat[:, None])


def swap_kernel(sizes, src, dst, send, recv, own):
    spot = here()
    dp, row, col = spot
    greet_partner(spot, sizes)
    size = src.shape[1]
    there = dst.at[:, pl.ds(pl.multiple_of(col * size, size), size)]
    away = remote(src, there, send, recv, (dp, row, 1 - col))
    local = pltpu.make_async_copy(src, there, own)
    away.start()
    local.start()
    away.wait()
    local.wait()


def swap_tokens(sizes, src):
    shape = (src.shape[0], src.shape[1] * sizes[2], src.shape[2])
    return pl.pallas_call(
        functools.partial(swap_kernel, sizes),
        in_specs=[VMEM],
        out_specs=VMEM,
        out_shape=jax.ShapeDtypeStruct(shape, src.dtype),
        scratch_shapes=[DMA, DMA, DMA],
        compiler_params=pltpu.CompilerParams(collective_id=1, has_side_effects=True),
        name="swap_tokens",
    )(src)


def fold(column):
    return jnp.broadcast_to(column, (column.shape[0], 128))


def join_kernel(
    sizes, part, x, gain, hidden, normed_all, landing, mine, theirs, block,
    ssend, srecv, gsend, grecv, psend, precv,
):
    spot = here()
    dp, row, col = spot
    greet_plane(spot, sizes)
    scatter = Scatter(spot, sizes, part, landing, ssend, srecv)
    scatter.start()
    scatter.wait()
    total = x[...].astype(jnp.float32)
    for q in range(sizes[1]):
        total = total + landing[q].astype(jnp.float32)
    hidden[...] = total
    mine[...] = fold(jnp.sum(total * total, axis=1, keepdims=True))
    pair = remote(mine, theirs, psend, precv, (dp, row, 1 - col))
    pair.start()
    pair.wait()
    squares = mine[:, :1] + theirs[:, :1]
    scale = lax.rsqrt(squares / D + EPSILON)
    block[...] = (hidden[...] * scale * gain[...].astype(jnp.float32)).astype(jnp.bfloat16)
    gather = Gather(spot, sizes, block, normed_all, gsend, grecv)
    gather.start()
    scatter.wait_send()
    gather.wait()


def join(sizes, part, x, gain):
    tokens, width = x.shape
    rows = sizes[1]
    return pl.pallas_call(
        functools.partial(join_kernel, sizes),
        in_specs=[VMEM] * 3,
        out_specs=[VMEM, VMEM],
        out_shape=[
            jax.ShapeDtypeStruct((tokens, width), jnp.float32),
            jax.ShapeDtypeStruct(part.shape, jnp.bfloat16),
        ],
        scratch_shapes=[
            pltpu.VMEM((rows, tokens, width), jnp.bfloat16),
            pltpu.VMEM((tokens, 128), jnp.float32),
            pltpu.VMEM((tokens, 128), jnp.float32),
            pltpu.VMEM((tokens, width), jnp.bfloat16),
        ]
        + plane_sems(sizes) * 2
        + [DMA, DMA],
        compiler_params=pltpu.CompilerParams(collective_id=3, has_side_effects=True),
        name="join",
    )(part, x, gain[None])


def norm_back(sizes, spot, landing, base, above, gain, mine, theirs, psend, precv):
    dp, row, col = spot
    normed_grad = landing[0].astype(jnp.float32)
    for q in range(1, sizes[1]):
        normed_grad = normed_grad + landing[q].astype(jnp.float32)
    values = base[...].astype(jnp.float32)
    unit_grad = normed_grad * gain[...].astype(jnp.float32)
    mine[0] = fold(jnp.sum(values * values, axis=1, keepdims=True))
    mine[1] = fold(jnp.sum(unit_grad * values, axis=1, keepdims=True))
    pair = remote(mine, theirs, psend, precv, (dp, row, 1 - col))
    pair.start()
    pair.wait()
    scale = lax.rsqrt((mine[0, :, :1] + theirs[0, :, :1]) / D + EPSILON)
    inner = scale * (mine[1, :, :1] + theirs[1, :, :1]) / D
    unit = values * scale
    grad = above[...].astype(jnp.float32) + scale * (unit_grad - unit * inner)
    return grad, jnp.sum(normed_grad * unit, axis=0, keepdims=True)


def slab(ref, dim, index, count):
    size = ref.shape[dim] // count
    window = [slice(None)] * len(ref.shape)
    window[dim] = pl.ds(pl.multiple_of(index * size, size), size)
    return ref.at[tuple(window)]


def add_into(target, addend):
    target[...] = (target[...].astype(jnp.float32) + addend[...].astype(jnp.float32)).astype(
        target.dtype
    )


class PairSum:
    def __init__(self, spot, sizes, terms, dims, halves, landings, send, recv):
        self.col, self.cols = spot[2], sizes[2]
        self.terms, self.dims, self.halves, self.landings = terms, dims, halves, landings
        self.copies = [
            remote(
                slab(term, dim, 1 - spot[2], sizes[2]), landing, send.at[n], recv.at[n],
                (spot[0], spot[1], 1 - spot[2]),
            )
            for n, (term, dim, landing) in enumerate(zip(terms, dims, landings))
        ]

    def start(self):
        for copy in self.copies:
            copy.start()

    def finish(self):
        for copy, term, dim, half, landing in zip(
            self.copies, self.terms, self.dims, self.halves, self.landings
        ):
            copy.wait()
            own = slab(term, dim, self.col, self.cols)
            half[...] = (own[...].astype(jnp.float32) + landing[...].astype(jnp.float32)).astype(
                half.dtype
            )


class LineReduce:
    def __init__(self, spot, sizes, arrays, dims, below, above, sems):
        self.spot, self.count = spot, sizes[0]
        self.arrays, self.dims, self.below, self.above = arrays, dims, below, above
        self.up_send, self.up_recv, self.down_send, self.down_recv = sems

    def copy(self, n, k, up):
        dp, row, col = self.spot
        landing = self.below[n] if up else self.above[n]
        send, recv = (
            (self.up_send, self.up_recv) if up else (self.down_send, self.down_recv)
        )
        dim = self.dims[n]
        return remote(
            slab(self.arrays[n], dim, k, self.count),
            slab(landing, dim, k, self.count),
            send.at[n, k],
            recv.at[n, k],
            (jnp.clip(dp + (1 if up else -1), 0, self.count - 1), row, col),
        )

    def send(self, k, up):
        for n in range(len(self.arrays)):
            self.copy(n, k, up).start()

    def start(self):
        dp, last = self.spot[0], self.count - 1

        @pl.when(dp == 0)
        def _():
            lax.fori_loop(0, last, lambda i, c: (self.send(last - i, True), c)[1], 0)

        @pl.when(dp == last)
        def _():
            lax.fori_loop(0, last, lambda i, c: (self.send(i, False), c)[1], 0)

    def take(self, k, up):
        for n, (array, dim) in enumerate(zip(self.arrays, self.dims)):
            landing = slab((self.below if up else self.above)[n], dim, k, self.count)
            arrived(landing, (self.up_recv if up else self.down_recv).at[n, k])
            add_into(slab(array, dim, k, self.count), landing)

    def event(self, time):
        dp, last = self.spot[0], self.count - 1

        @pl.when(jnp.logical_and(dp > 0, time >= dp))
        def _():
            k = dp + last - time
            self.take(k, True)
            pl.when(k > dp)(lambda: self.send(k, True))

        @pl.when(jnp.logical_and(dp < last, time >= last - dp))
        def _():
            k = time - (last - dp)
            self.take(k, False)
            pl.when(k < dp)(lambda: self.send(k, False))

    def events(self):
        lax.fori_loop(1, self.count, lambda time, c: (self.event(time), c)[1], 0)

    def finish(self):
        dp = self.spot[0]

        def one(k, carry):
            @pl.when(dp < k)
            def _():
                for n in range(len(self.arrays)):
                    self.copy(n, k, True).wait_send()

            @pl.when(dp > k)
            def _():
                for n in range(len(self.arrays)):
                    self.copy(n, k, False).wait_send()

            return carry

        lax.fori_loop(0, self.count, one, 0)


class LineGather:
    def __init__(self, spot, sizes, arrays, dims, sems):
        self.spot, self.count = spot, sizes[0]
        self.arrays, self.dims = arrays, dims
        self.up_send, self.down_send, self.recv = sems

    def copy(self, n, k, up):
        dp, row, col = self.spot
        part = slab(self.arrays[n], self.dims[n], k, self.count)
        return remote(
            part,
            part,
            (self.up_send if up else self.down_send).at[n, k],
            self.recv.at[n, k],
            (jnp.clip(dp + (1 if up else -1), 0, self.count - 1), row, col),
        )

    def send(self, k, up):
        dp = self.spot[0]

        @pl.when(dp < self.count - 1 if up else dp > 0)
        def _():
            for n in range(len(self.arrays)):
                self.copy(n, k, up).start()

    def start(self):
        self.send(self.spot[0], True)
        self.send(self.spot[0], False)

    def take(self, k):
        for n, (array, dim) in enumerate(zip(self.arrays, self.dims)):
            arrived(slab(array, dim, k, self.count), self.recv.at[n, k])

    def event(self, time):
        dp = self.spot[0]

        @pl.when(dp - time >= 0)
        def _():
            self.take(dp - time)
            self.send(dp - time, True)

        @pl.when(dp + time < self.count)
        def _():
            self.take(dp + time)
            self.send(dp + time, False)

    def events(self):
        lax.fori_loop(1, self.count, lambda time, c: (self.event(time), c)[1], 0)

    def finish(self):
        dp, last = self.spot[0], self.count - 1

        def one(k, carry):
            @pl.when(jnp.logical_and(k <= dp, dp < last))
            def _():
                for n in range(len(self.arrays)):
                    self.copy(n, k, True).wait_send()

            @pl.when(jnp.logical_and(k >= dp, dp > 0))
            def _():
                for n in range(len(self.arrays)):
                    self.copy(n, k, False).wait_send()

            return carry

        lax.fori_loop(0, self.count, one, 0)


def line_sems(sizes, arrays, kinds):
    return [DMA((arrays, sizes[0])) for _ in range(kinds)]


def greet_cross(spot, sizes):
    barrier = pltpu.get_barrier_semaphore()
    dp, row, col = spot
    dps, rows, cols = sizes
    for j in range(rows):
        for k in range(cols):
            if j + k > 0:
                pl.semaphore_signal(
                    barrier,
                    inc=1,
                    device_id=(dp, lax.rem(row + j, rows), lax.rem(col + k, cols)),
                    device_id_type=MESH,
                )
    for j in (1, dps - 1):
        pl.semaphore_signal(
            barrier, inc=1, device_id=(lax.rem(dp + j, dps), row, col), device_id_type=MESH
        )
    pl.semaphore_wait(barrier, rows * cols + 1)


FIRST_DIMS = (0, 0, 0)
FIRST_COLS = (0, 1, 0)
LAST_DIMS = (1, 0)
LAST_COLS = (1, 1)


def halved(shape, dim, cols):
    shape = list(shape)
    shape[dim] //= cols
    return tuple(shape)


def middle_kernel(sizes, *refs):
    part, hidden, dy, gain = refs[:4]
    terms = refs[4:7]
    grad, grad_all, gain_grad = refs[7:10]
    shards = refs[10:13]
    landing, mine, theirs, block = refs[13:17]
    halves, pair_land, below, above = refs[17:20], refs[20:23], refs[23:26], refs[26:29]
    ssend, srecv, gsend, grecv, psend, precv, hsend, hrecv, *line = refs[29:]
    spot = here()
    greet_cross(spot, sizes)
    scatter = Scatter(spot, sizes, part, landing, ssend, srecv)
    scatter.start()
    pair = PairSum(spot, sizes, terms, FIRST_COLS, halves, pair_land, hsend, hrecv)
    pair.start()
    pair.finish()
    reduce = LineReduce(spot, sizes, halves, FIRST_DIMS, below, above, line)
    reduce.start()
    scatter.wait()
    total, gains = norm_back(sizes, spot, landing, hidden, dy, gain, mine, theirs, psend, precv)
    gain_grad[...] = gains
    grad[...] = total
    block[...] = total.astype(jnp.bfloat16)
    gather = Gather(spot, sizes, block, grad_all, gsend, grecv)
    gather.start()
    lax.fori_loop(1, sizes[0], lambda time, c: (reduce.event(time), c)[1], 0)
    for half, dim, shard in zip(halves, FIRST_DIMS, shards):
        shard[...] = slab(half, dim, spot[0], sizes[0])[...]
    scatter.wait_send()
    gather.wait()
    reduce.finish()


def middle(sizes, part, hidden, dy, gain, terms):
    tokens, width = hidden.shape
    dps, rows, cols = sizes
    low, wide = jnp.bfloat16, jnp.float32
    halves = [halved(t.shape, d, cols) for t, d in zip(terms, FIRST_COLS)]
    shards = [halved(h, d, dps) for h, d in zip(halves, FIRST_DIMS)]
    return pl.pallas_call(
        functools.partial(middle_kernel, sizes),
        in_specs=[VMEM] * 7,
        out_specs=[VMEM] * 6,
        out_shape=[
            jax.ShapeDtypeStruct((tokens, width), wide),
            jax.ShapeDtypeStruct(part.shape, low),
            jax.ShapeDtypeStruct((1, width), wide),
        ]
        + [jax.ShapeDtypeStruct(s, low) for s in shards],
        scratch_shapes=[
            pltpu.VMEM((rows, tokens, width), low),
            pltpu.VMEM((2, tokens, 128), wide),
            pltpu.VMEM((2, tokens, 128), wide),
            pltpu.VMEM((tokens, width), low),
        ]
        + [pltpu.VMEM(h, low) for h in halves] * 4
        + plane_sems(sizes) * 2
        + [DMA, DMA, DMA((3,)), DMA((3,))]
        + line_sems(sizes, 3, 4),
        compiler_params=pltpu.CompilerParams(collective_id=4, has_side_effects=True),
        name="middle",
    )(part, hidden, dy, gain[None], *terms)


def last_kernel(sizes, *refs):
    part, x, above_grad, gain, other_gain = refs[:5]
    keys, shard, terms = refs[5], refs[6], refs[7:9]
    table, grads_all = refs[9:11]
    grad, gain_sums, row_grads, first = refs[11:15]
    lasts, keys_all = refs[15:17], refs[17]
    landing, mine, theirs, own_gain, gain_landing, tables, chunks = refs[18:25]
    halves, pair_land, below, above = refs[25:27], refs[27:29], refs[29:31], refs[31:33]
    (
        ssend, srecv, psend, precv, bsend, brecv, hsend, hrecv, tsem, csem,
        xsend, xrecv, kxsend, kxrecv, *line
    ) = refs[33:]
    spot = here()
    dp, row, col = spot
    dps, rows, cols = sizes
    count = dps * rows * cols
    me = index_of(spot, sizes)
    loads = dps * cols
    block = grads_all.shape[-1]

    def load(index):
        slot = lax.rem(index, 2)
        where = (lax.div(index, cols), lax.rem(index, cols))
        return (
            pltpu.make_async_copy(table.at[where], tables.at[slot], tsem.at[slot]),
        ) + tuple(
            pltpu.make_async_copy(
                grads_all.at[where + (r,)],
                chunks.at[slot, :, pl.ds(r * block, block)],
                csem.at[slot, r],
            )
            for r in range(rows)
        )

    for copy in load(0):
        copy.start()
    greet_all(spot, sizes)
    scatter = Scatter(spot, sizes, part, landing, ssend, srecv)
    scatter.start()
    pair = PairSum(spot, sizes, terms, LAST_COLS, halves, pair_land, hsend, hrecv)
    pair.start()
    slab(first, 0, dp, dps)[...] = shard[...]
    gather = LineGather(spot, sizes, [first], [0], line[7:])
    gather.start()
    pair.finish()
    reduce = LineReduce(spot, sizes, halves, LAST_DIMS, below, above, line[:4])
    reduce.start()

    wide_strip = min(512, tables.shape[2])

    def product(index):
        slot = lax.rem(index, 2)
        for copy in load(index):
            copy.wait()

        @pl.when(index + 1 < loads)
        def _():
            for copy in load(index + 1):
                copy.start()

        def strip(n, carry):
            columns = pl.ds(pl.multiple_of(n * wide_strip, wide_strip), wide_strip)
            term = lax.dot_general(
                tables[slot, :, columns],
                chunks[slot],
                (((0,), (0,)), ((), ())),
                preferred_element_type=jnp.float32,
            )

            @pl.when(index == 0)
            def _():
                row_grads[columns] = term

            @pl.when(index > 0)
            def _():
                row_grads[columns] = row_grads[columns] + term

            return carry

        lax.fori_loop(0, tables.shape[2] // wide_strip, strip, 0)

    def products(first, end):
        lax.fori_loop(first, end, lambda index, c: (product(index), c)[1], 0)

    def sideways(k):
        return remote(
            keys, keys_all.at[row, col], xsend, xrecv.at[rows - k],
            (dp, lax.rem(row + k, rows), col),
        )

    def cross(src, k):
        there = keys_all.at[lax.rem(row + k, rows), col]
        return remote(src, there, kxsend, kxrecv, (dp, row, 1 - col))

    products(0, loads // 4)
    scatter.wait()
    total, gains = norm_back(sizes, spot, landing, x, above_grad, gain, mine, theirs, psend, precv)
    lines = gains.shape[1] // 128
    for line_index in range(lines):
        columns = slice(line_index * 128, (line_index + 1) * 128)
        own_gain[line_index : line_index + 1] = gains[:, columns]
        own_gain[lines + line_index : lines + line_index + 1] = other_gain[:, columns]

    def tell(device):
        remote(own_gain, gain_landing.at[me], bsend, brecv, device).start()

    each_other(spot, sizes, tell)
    gain_landing[me] = own_gain[...]
    grad[...] = total
    for k in range(1, rows):
        sideways(k).start()
    cross(keys, 0).start()
    keys_all[row, col] = keys[...]
    gather.event(1)
    reduce.event(1)
    products(loads // 4, loads // 2)
    lax.fori_loop(2, dps, lambda time, c: (gather.event(time), reduce.event(time), c)[2], 0)
    for first, half, dim in zip(lasts, halves, LAST_DIMS):
        slab(first, dim, dp, dps)[...] = slab(half, dim, dp, dps)[...]
    final = LineGather(spot, sizes, lasts, LAST_DIMS, line[4:7])
    final.start()
    products(loads // 2, 3 * loads // 4)
    final.event(1)
    for k in range(1, rows):
        landed = keys_all.at[lax.rem(row + k, rows), col]
        arrived(landed, xrecv.at[k])
        cross(landed, k).start()
    products(3 * loads // 4, loads)
    lax.fori_loop(2, dps, lambda time, c: (final.event(time), c)[1], 0)
    arrived(keys_all.at[:, 1 - col], kxrecv)
    scatter.wait_send()
    arrived(gain_landing.at[pl.ds(0, count - 1)], brecv)
    for c in range(cols):

        def add(index, sums):
            return sums + gain_landing[index * cols + c]

        gain_sums[c] = lax.fori_loop(0, dps * rows, add, jnp.zeros(own_gain.shape, jnp.float32))
    arrived(gain_landing.at[pl.ds(0, count - 1)], bsend)
    arrived(keys_all.at[:, col], kxsend)
    arrived(keys_all.at[pl.ds(0, rows - 1), col], xsend)
    gather.finish()
    reduce.finish()
    final.finish()


def last(sizes, part, x, above, gain, other_gain, keys, shard, terms, table, grads_all):
    tokens, width = x.shape
    dps, rows, cols = sizes
    lines = 2 * width // 128
    count = dps * rows * cols
    low, wide = jnp.bfloat16, jnp.float32
    shape = jax.ShapeDtypeStruct

    halves = [halved(t.shape, d, cols) for t, d in zip(terms, LAST_COLS)]
    rows_dev = table.shape[-1]
    features = grads_all.shape[-1] * rows
    chunk = table.shape[2]
    return pl.pallas_call(
        functools.partial(last_kernel, sizes),
        in_specs=[VMEM] * 9 + [ANY] * 2,
        out_specs=[VMEM] * 7,
        out_shape=[
            shape((tokens, width), wide),
            shape((cols, lines, 128), wide),
            shape((rows_dev, features), wide),
            shape((shard.shape[0] * dps, shard.shape[1]), low),
        ]
        + [shape(s, low) for s in halves]
        + [shape((rows, cols) + keys.shape, low)],
        scratch_shapes=[
            pltpu.VMEM((rows, tokens, width), low),
            pltpu.VMEM((2, tokens, 128), wide),
            pltpu.VMEM((2, tokens, 128), wide),
            pltpu.VMEM((lines, 128), wide),
            pltpu.VMEM((count, lines, 128), wide),
            pltpu.VMEM((2, chunk, rows_dev), low),
            pltpu.VMEM((2, chunk, features), low),
        ]
        + [pltpu.VMEM(h, low) for h in halves] * 4
        + plane_sems(sizes)
        + [DMA, DMA, DMA, DMA, DMA((2,)), DMA((2,)), DMA((2,)), DMA((2, rows))]
        + [DMA, DMA((rows,)), DMA, DMA]
        + line_sems(sizes, 2, 7)
        + line_sems(sizes, 1, 3),
        compiler_params=pltpu.CompilerParams(collective_id=5, has_side_effects=True),
        name="last",
    )(part, x, above, gain[None], other_gain, keys, shard, *terms, table, grads_all)


def turn_kernel(sizes, *refs):
    prefix, queries, kv, grad_out, log_sums, out_part, hidden = refs[:7]
    shards, term = refs[7:10], refs[10]
    grad_q, grad_kv, output = refs[11:14]
    firsts, term_shard = refs[14:17], refs[17]
    totals, kv_landing, out_landing, half, pair_land, below, above = refs[18:25]
    osend, orecv, ksend, krecv, hsend, hrecv, *line = refs[25:]
    spot = here()
    dp, row, col = spot
    dps = sizes[0]
    tokens, width = queries.shape
    keys = kv.shape[1]
    tile = tokens // 2
    greet_cross(spot, sizes)
    for first, dim, shard in zip(firsts, FIRST_DIMS, shards):
        slab(first, dim, dp, dps)[...] = shard[...]
    pair = PairSum(spot, sizes, [term], [0], [half], [pair_land], hsend, hrecv)
    pair.start()
    gather = LineGather(spot, sizes, firsts, FIRST_DIMS, line[:3])
    gather.start()
    out_scatter = Scatter(spot, sizes, out_part, out_landing, osend, orecv)
    out_scatter.start()
    pair.finish()
    reduce = LineReduce(spot, sizes, [half], [0], [below], [above], line[3:])
    reduce.start()

    def events(time):
        gather.event(time)
        reduce.event(time)

    limit = prefix[0]
    key_pos = lax.broadcasted_iota(jnp.int32, (keys, tile), 0)
    lane = lax.broadcasted_iota(jnp.int32, (1, 2 * HDIM), 1)
    sides = [
        jnp.where(jnp.logical_and(lane >= a * HDIM, lane < (a + 1) * HDIM), 1.0, 0.0).astype(
            jnp.bfloat16
        )
        for a in range(2)
    ]

    def unit(index, carry):
        pair, part = lax.div(index, 2), lax.rem(index, 2)
        lanes = pl.ds(pl.multiple_of(pair * 2 * HDIM, 2 * HDIM), 2 * HDIM)
        lines = pl.ds(pl.multiple_of(part * tile, tile), tile)
        query_pos = col * tokens + part * tile + lax.broadcasted_iota(jnp.int32, (1, tile), 1)
        allowed = jnp.logical_or(key_pos <= query_pos, key_pos < limit)
        q2, g2 = queries[lines, lanes], grad_out[lines, lanes]
        k2, v2 = kv[0, :, lanes], kv[1, :, lanes]
        dq = jnp.zeros((tile, 2 * HDIM), jnp.float32)
        dk = jnp.zeros((keys, 2 * HDIM), jnp.float32)
        dv = jnp.zeros((keys, 2 * HDIM), jnp.float32)
        for a in range(2):
            ka = k2 * sides[a]
            scores = jnp.where(allowed, dense_nt(ka, q2) * HDIM ** (-0.5), -jnp.inf)
            probs = jnp.exp(scores - log_sums[pl.ds(2 * pair + a, 1), lines])
            grad_probs = dense_nt(v2 * sides[a], g2)
            inner = jnp.sum(probs * grad_probs, axis=0, keepdims=True)
            grad_scores = (probs * (grad_probs - inner)).astype(jnp.bfloat16)
            dq = dq + dense_tn(grad_scores, ka)
            dk = dk + dense(grad_scores, q2 * sides[a])
            dv = dv + dense(probs.astype(jnp.bfloat16), g2 * sides[a])
        grad_q[lines, lanes] = (dq * HDIM ** (-0.5)).astype(jnp.bfloat16)
        dk = dk * HDIM ** (-0.5)

        @pl.when(part == 0)
        def _():
            totals[0, :, lanes] = dk
            totals[1, :, lanes] = dv

        @pl.when(part > 0)
        def _():
            totals[0, :, lanes] = totals[0, :, lanes] + dk
            totals[1, :, lanes] = totals[1, :, lanes] + dv

        pl.when(index == 1)(lambda: events(1))
        pl.when(index == 3)(lambda: events(2))
        return carry

    lax.fori_loop(0, 2 * width // (2 * HDIM), unit, 0)
    size = kv_landing.shape[1]
    other = pl.multiple_of((1 - col) * size, size)
    away = remote(totals.at[:, pl.ds(other, size)], kv_landing, ksend, krecv, (dp, row, 1 - col))
    away.start()
    out_scatter.wait()
    result = hidden[...]
    for q in range(sizes[1]):
        result = result + out_landing[q].astype(jnp.float32)
    output[...] = result.astype(jnp.bfloat16)
    away.wait()
    own = totals[:, pl.ds(pl.multiple_of(col * size, size), size)]
    grad_kv[...] = (own + kv_landing[...]).astype(jnp.bfloat16)
    lax.fori_loop(3, dps, lambda time, c: (events(time), c)[1], 0)
    term_shard[...] = slab(half, 0, dp, dps)[...]
    out_scatter.wait_send()
    gather.finish()
    reduce.finish()


def turn(sizes, prefix, queries, kv, grad_out, log_sums, out_part, hidden, shards, term):
    tokens, width = queries.shape
    dps, rows, cols = sizes
    low, wide = jnp.bfloat16, jnp.float32
    shape = jax.ShapeDtypeStruct

    def grown(shard, dim):
        full = list(shard.shape)
        full[dim] *= dps
        return tuple(full)

    firsts = [grown(s, d) for s, d in zip(shards, FIRST_DIMS)]
    half = halved(term.shape, 0, cols)
    return pl.pallas_call(
        functools.partial(turn_kernel, sizes),
        in_specs=[pl.BlockSpec(memory_space=pltpu.SMEM)] + [VMEM] * 10,
        out_specs=[VMEM] * 7,
        out_shape=[
            shape((tokens, width), low),
            shape((2, tokens, width), low),
            shape(hidden.shape, low),
        ]
        + [shape(s, low) for s in firsts]
        + [shape(halved(half, 0, dps), low)],
        scratch_shapes=[
            pltpu.VMEM(kv.shape, wide),
            pltpu.VMEM((2, tokens, width), wide),
            pltpu.VMEM((rows,) + hidden.shape, low),
        ]
        + [pltpu.VMEM(half, low)] * 4
        + plane_sems(sizes)
        + [DMA, DMA, DMA((1,)), DMA((1,))]
        + line_sems(sizes, 3, 3)
        + line_sems(sizes, 1, 4),
        compiler_params=pltpu.CompilerParams(collective_id=2, has_side_effects=True),
        name="turn",
    )(prefix, queries, kv, grad_out, log_sums, out_part, hidden, *shards, term)


def allowed_mask(query_count, key_count, first_pos, prefix_len):
    query_pos = first_pos + lax.iota(jnp.int32, query_count)
    key_pos = lax.iota(jnp.int32, key_count)
    return (key_pos[None, :] <= query_pos[:, None]) | (key_pos[None, :] < prefix_len)


def flat_picks(picks_head):
    blocks = picks_head.shape[0] // FBLK
    return jnp.swapaxes(picks_head.reshape(blocks, FBLK, TOPK), 1, 2).reshape(blocks, TOPK * FBLK)


def one_hot(row_values, size):
    hot = lax.broadcasted_iota(jnp.int32, (size, row_values.shape[1]), 0) == row_values
    return jnp.where(hot, 1.0, 0.0).astype(jnp.bfloat16)


def route_block(picks, rows_dev, owners, cap):
    lane = lax.broadcasted_iota(jnp.int32, (FBLK, FBLK), 0)
    before = jnp.where(lane < lax.broadcasted_iota(jnp.int32, (FBLK, FBLK), 1), 1.0, 0.0).astype(
        jnp.bfloat16
    )
    owner = picks // rows_dev
    local = picks % rows_dev
    hot = one_hot(owner, owners)
    running = jnp.zeros((owners, 1), jnp.float32)
    ranks = []
    for chunk in range(picks.shape[1] // FBLK):
        part = hot[:, chunk * FBLK : (chunk + 1) * FBLK]
        earlier = jnp.dot(part, before, preferred_element_type=jnp.float32)
        wide = part.astype(jnp.float32)
        ranks.append(jnp.sum(wide * (earlier + running), axis=0, keepdims=True))
        running = running + jnp.sum(wide, axis=1, keepdims=True)
    rank = jnp.concatenate(ranks, axis=1).astype(jnp.int32)
    slot_hot = one_hot(rank, cap)
    token = lax.broadcasted_iota(jnp.int32, picks.shape, 1) % FBLK
    outs = []
    for payload in (local % SUBKEYS, local // SUBKEYS, token):
        scaled = hot * payload.astype(jnp.float32).astype(jnp.bfloat16)
        outs.append(
            lax.dot_general(
                scaled, slot_hot, (((1,), (1,)), ((), ())), preferred_element_type=jnp.float32
            ).astype(jnp.int32)
        )
    return rank, (outs[1] * FBLK + outs[2]) * SUBKEYS + outs[0]


def weigh_kernel(rows_dev, owners, cap, query_ref, keys_ref, picks_ref, rank_ref, weights_ref, slots_ref):
    picks = picks_ref[0]
    first = lax.dot_general(
        keys_ref[0], query_ref[:, :HALF], (((1,), (1,)), ((), ())), preferred_element_type=jnp.float32
    )
    second = lax.dot_general(
        keys_ref[1], query_ref[:, HALF:], (((1,), (1,)), ((), ())), preferred_element_type=jnp.float32
    )
    upper = picks // SUBKEYS
    lower = picks % SUBKEYS
    key_id = lax.broadcasted_iota(jnp.int32, (SUBKEYS, FBLK), 0)
    rows = []
    for pick in range(TOPK):
        columns = slice(pick * FBLK, (pick + 1) * FBLK)
        chosen = jnp.where(key_id == upper[:, columns], first, 0.0) + jnp.where(
            key_id == lower[:, columns], second, 0.0
        )
        rows.append(jnp.sum(chosen, axis=0, keepdims=True))
    scores = jnp.concatenate(rows, axis=0)
    powers = jnp.exp(scores - jnp.max(scores, axis=0, keepdims=True))
    weights = powers / jnp.sum(powers, axis=0, keepdims=True)
    weights_ref[0] = weights
    flat = jnp.concatenate([weights[pick : pick + 1] for pick in range(TOPK)], axis=1)
    scaled = one_hot(picks // rows_dev, owners) * flat.astype(jnp.bfloat16)
    slots_ref[0] = lax.dot_general(
        scaled,
        one_hot(rank_ref[0], cap),
        (((1,), (1,)), ((), ())),
        preferred_element_type=jnp.float32,
    ).astype(jnp.bfloat16)


def weigh(query_rows, keys_head, flat, rank, rows_dev, owners, cap):
    blocks, count = flat.shape
    return pl.pallas_call(
        functools.partial(weigh_kernel, rows_dev, owners, cap),
        grid=(blocks,),
        in_specs=[
            pl.BlockSpec((FBLK, 2 * HALF), lambda i: (i, 0)),
            pl.BlockSpec((2, SUBKEYS, HALF), lambda i: (0, 0, 0)),
            pl.BlockSpec((1, 1, count), lambda i: (i, 0, 0)),
            pl.BlockSpec((1, 1, count), lambda i: (i, 0, 0)),
        ],
        out_specs=[
            pl.BlockSpec((1, TOPK, FBLK), lambda i: (i, 0, 0)),
            pl.BlockSpec((1, owners, cap), lambda i: (i, 0, 0)),
        ],
        out_shape=[
            jax.ShapeDtypeStruct((blocks, TOPK, FBLK), jnp.float32),
            jax.ShapeDtypeStruct((blocks, owners, cap), jnp.bfloat16),
        ],
        name="weigh",
    )(query_rows, keys_head, flat[:, None, :], rank)


def send_rows(spot, sizes, src, landing, send, recv):
    me = index_of(spot, sizes)

    def one(device):
        remote(src.at[index_of(device, sizes)], landing.at[me], send, recv, device).start()

    each_other(spot, sizes, one)
    landing[me] = src[me]


def all_rows(landing, sem):
    return arrived(landing.at[pl.ds(0, landing.shape[0] - 1)], sem)


def slot_row(sizes, table, dp, col, block):
    pieces = []
    for row in range(sizes[1]):
        index = (dp * sizes[1] + row) * sizes[2] + col
        pieces.append(table[index, pl.ds(block, 1), :])
    return jnp.concatenate(pieces, axis=1)


def nth_place(dp, q, dps):
    twice = 2 * jnp.minimum(dp, dps - 1 - dp)
    inside = q <= twice
    distance = jnp.where(inside, lax.div(q + 1, 2), q - lax.div(twice, 2))
    below = jnp.logical_or(
        jnp.logical_and(inside, lax.rem(q, 2) == 1),
        jnp.logical_and(jnp.logical_not(inside), dp > dps - 1 - dp),
    )
    return dp + jnp.where(below, -distance, distance), below


def plane_neighbours(row, rows):
    across = row + 1 - 2 * lax.rem(row, 2)
    along = lax.rem(row + rows // 2, rows)
    return across, along, lax.rem(across + rows // 2, rows)


RING = 3


def memory_kernel(
    sizes, blocks, grads, meta, slots, values,
    grads_all, table, other_part, memory, back,
    meta_in, slots_in, values_t, tables, parts,
    chunks, found, sums, grids, theirs, acc, first_land, side_land, deep_land, total,
    msend, mrecv, ssend, srecv, zup, zdown, zrecv, wsend, wrecv, csend, crecv,
    local, tsem, qsend, qrecv,
    gsem, esem, hsend, hrecv, xsend, xrecv, dsend, drecv, fsend, frecv, flocal,
):
    spot = here()
    dp, row, col = spot
    dps, rows, cols = sizes
    tokens, width = grads.shape
    half = tokens // 2
    areas = values.shape[0] // SUBKEYS
    count = dps * rows * cols
    me = index_of(spot, sizes)
    across, along, opposite = plane_neighbours(row, rows)
    first_half, second_half = pl.ds(0, half), pl.ds(half, half)
    greet_all(spot, sizes)
    send_rows(spot, sizes, meta, meta_in, msend, mrecv)
    send_rows(spot, sizes, slots, slots_in, ssend, srecv)

    def place_of(u):
        return nth_place(dp, dps - 1 - u, dps)[0]

    def block_at(place, r, lines=slice(None)):
        return grads_all.at[place, col, r, lines]

    def cross(q, place, r, src=None):
        there = block_at(place, r)
        remote(there if src is None else src, there, csend, crecv.at[q], (dp, row, 1 - col)).start()

    def line_copy(place, up, src=None):
        there = block_at(place, row)
        return remote(
            there if src is None else src,
            there,
            (zup if up else zdown).at[place],
            zrecv.at[place],
            (jnp.clip(dp + (1 if up else -1), 0, dps - 1), row, col),
        )

    def sideways(q, place, src=None):
        there = block_at(place, row)
        for n, r in enumerate((across, along)):
            remote(
                there if src is None else src, there, wsend, wrecv.at[q, n], (dp, r, col)
            ).start()

    pl.when(dp < dps - 1)(lambda: line_copy(dp, True, grads).start())
    pl.when(dp > 0)(lambda: line_copy(dp, False, grads).start())
    sideways(0, dp, grads)
    cross(0, dp, row, grads)
    keep = pltpu.make_async_copy(grads, block_at(dp, row), local)
    keep.start()

    def from_line(q):
        place, below = nth_place(dp, q, dps)
        arrived(block_at(place, row), zrecv.at[place])
        pl.when(jnp.logical_and(below, dp < dps - 1))(lambda: line_copy(place, True).start())
        pl.when(jnp.logical_and(jnp.logical_not(below), dp > 0))(
            lambda: line_copy(place, False).start()
        )
        sideways(q, place)
        cross(q, place, row)

    def from_sides(q):
        place, _ = nth_place(dp, q, dps)
        for n, (r, other, lines) in enumerate(
            ((across, along, first_half), (along, across, second_half))
        ):
            arrived(block_at(place, r), wrecv.at[q, n])
            half = block_at(place, r, lines)
            remote(half, half, wsend, wrecv.at[q, 2 + n], (dp, other, col)).start()
            cross(q, place, r)

    def from_opposite(q):
        place, _ = nth_place(dp, q, dps)
        for n, lines in enumerate((first_half, second_half)):
            arrived(block_at(place, opposite, lines), wrecv.at[q, 2 + n])
        cross(q, place, opposite)

    def turn_rows(n, carry):
        lines = pl.ds(pl.multiple_of(n * 256, 256), 256)
        values_t[:, lines] = values[lines].T
        return carry

    lax.fori_loop(0, values.shape[0] // 256, turn_rows, 0)
    all_rows(meta_in, mrecv)
    all_rows(slots_in, srecv)

    def write_places(chunk):
        turn = lax.div(chunk, 2)
        slot = lax.rem(chunk, 2)
        return turn, slot, place_of(turn), jnp.where(slot == 0, 1 - col, col)

    def table_copy(chunk):
        _, slot, source_dp, source_col = write_places(chunk)
        return pltpu.make_async_copy(
            tables.at[slot], table.at[source_dp, source_col], tsem.at[slot]
        )

    def build(chunk):
        turn, slot, source_dp, source_col = write_places(chunk)
        pl.when(turn > 0)(lambda: table_copy(chunk).wait())
        def one(block, carry):
            row_meta = slot_row(sizes, meta_in, source_dp, source_col, block)
            key = row_meta // SUBKEYS
            low = row_meta % SUBKEYS
            weight = slot_row(sizes, slots_in, source_dp, source_col, block)
            at_key = lax.broadcasted_iota(jnp.int32, (areas * FBLK, key.shape[1]), 0) == key
            left = jnp.where(at_key, weight, 0.0).astype(jnp.bfloat16)
            stacked = lax.dot_general(
                left,
                one_hot(low, SUBKEYS),
                (((1,), (1,)), ((), ())),
                preferred_element_type=jnp.float32,
            ).astype(jnp.bfloat16)
            for area in range(areas):
                tables[
                    slot,
                    pl.ds(pl.multiple_of(block * FBLK, FBLK), FBLK),
                    area * SUBKEYS : (area + 1) * SUBKEYS,
                ] = stacked[area * FBLK : (area + 1) * FBLK]
            return carry

        lax.fori_loop(0, blocks, one, 0)
        table_copy(chunk).start()

    def away(turn, source_dp):
        return remote(parts.at[0], other_part.at[source_dp], qsend, qrecv.at[turn], (dp, row, 1 - col))

    def multiply(chunk):
        turn, slot, source_dp, _ = write_places(chunk)
        later = turn > 0
        pl.when(jnp.logical_and(later, slot == 0))(lambda: away(turn, source_dp).wait_send())

        def strip(n, carry):
            columns = pl.ds(pl.multiple_of(n * 512, 512), 512)
            parts[slot, :, columns] = jnp.dot(
                tables[slot], values[:, columns], preferred_element_type=jnp.float32
            ).astype(jnp.bfloat16)
            return carry

        lax.fori_loop(0, values.shape[1] // 512, strip, 0)
        pl.when(slot == 0)(lambda: away(turn, source_dp).start())

    def load_part(u):
        return pltpu.make_async_copy(other_part.at[place_of(u)], theirs, esem)

    def strip(u, r, lines=slice(None)):
        return acc.at[lax.rem(u, RING), lines, pl.ds(pl.multiple_of(r * width, width), width)]

    lines_of = (pl.ds(0, half), pl.ds(half, half))

    def halves(u):
        return [
            remote(
                strip(u, opposite, lines_of[n]), first_land.at[u, n],
                hsend.at[lax.rem(u, RING), n], hrecv.at[u, n], (dp, r, col),
            )
            for n, r in enumerate((across, along))
        ]

    def wholes(u):
        return [
            remote(
                strip(u, r), side_land.at[u, n],
                xsend.at[lax.rem(u, RING), n], xrecv.at[u, n], (dp, r, col),
            )
            for n, r in enumerate((across, along))
        ]

    def sent(u):
        for copy in halves(u) + wholes(u):
            copy.wait_send()

    def fetch(u):
        arrived(other_part.at[place_of(u)], qrecv.at[u])
        load_part(u).start()

    def combine(u):
        pl.when(u >= RING)(lambda: sent(u - RING))
        load_part(u).wait()
        acc[lax.rem(u, RING)] = (
            parts[1].astype(jnp.float32) + theirs[...].astype(jnp.float32)
        ).astype(jnp.bfloat16)
        for copy in halves(u):
            copy.start()

    def relay(u):
        for n, r in enumerate((along, across)):
            arrived(first_land.at[u, n], hrecv.at[u, n])
            add_into(strip(u, r, lines_of[n]), first_land.at[u, n])
        for copy in wholes(u):
            copy.start()

    def deep_copy(u):
        place = place_of(u)
        up = place > dp
        target = jnp.where(up, dp + 1, dp - 1)
        there = jnp.where(jnp.logical_and(jnp.logical_not(up), target == place), dps, place)
        return remote(
            total.at[u], deep_land.at[there], dsend.at[u], drecv.at[there],
            (jnp.clip(target, 0, dps - 1), row, col),
        )

    def finish(u):
        for n in range(2):
            arrived(side_land.at[u, n], xrecv.at[u, n])
        place = place_of(u)
        result = (
            strip(u, row)[...].astype(jnp.float32)
            + side_land[u, 0].astype(jnp.float32)
            + side_land[u, 1].astype(jnp.float32)
        )
        memory[...] = result

        def more(index):
            arrived(deep_land.at[index], drecv.at[index])
            memory[...] = memory[...] + deep_land[index].astype(jnp.float32)

        below = jnp.logical_and(place >= dp, dp > 0)
        above = jnp.logical_and(place <= dp, dp < dps - 1)
        pl.when(jnp.logical_or(below, jnp.logical_and(above, place < dp)))(lambda: more(place))
        pl.when(jnp.logical_and(above, place == dp))(lambda: more(dps))

        @pl.when(u < dps - 1)
        def _():
            total[u] = memory[...].astype(jnp.bfloat16)
            deep_copy(u).start()

    def read_places(chunk):
        slot = lax.rem(chunk, 2)
        place = nth_place(dp, lax.div(chunk, 2), dps)[0]
        return slot, place, jnp.where(slot == 0, col, 1 - col)

    def load_chunk(chunk):
        slot, source_dp, source_col = read_places(chunk)
        return [
            pltpu.make_async_copy(
                grads_all.at[source_dp, source_col, r],
                chunks.at[slot, :, pl.ds(r * width, width)],
                gsem.at[slot, r],
            )
            for r in range(rows)
        ]

    def start_chunk(chunk):
        slot, source_dp, source_col = read_places(chunk)

        @pl.when(slot == 1)
        def _():
            arrived(grads_all.at[source_dp, source_col], crecv.at[lax.div(chunk, 2)])

        for copy in load_chunk(chunk):
            copy.start()

    wide_strip = min(2048, areas * SUBKEYS)
    per_strip = wide_strip // SUBKEYS

    def search(chunk, part):
        slot, source_dp, source_col = read_places(chunk)

        @pl.when(part == 0)
        def _():
            for copy in load_chunk(chunk):
                copy.wait()

            def strip(n, carry):
                columns = pl.ds(pl.multiple_of(n * wide_strip, wide_strip), wide_strip)
                grid = jnp.dot(
                    chunks[slot], values_t[:, columns], preferred_element_type=jnp.float32
                ).astype(jnp.bfloat16)
                for area in range(per_strip):
                    grids[n * per_strip + area] = grid[:, area * SUBKEYS : (area + 1) * SUBKEYS]
                return carry

            lax.fori_loop(0, areas // per_strip, strip, 0)

            @pl.when(chunk + 2 < dps * cols)
            def _():
                start_chunk(chunk + 2)

        @pl.when(part == 1)
        def _():
            def one(block, carry):
                row_meta = slot_row(sizes, meta_in, source_dp, source_col, block)
                lines = pl.ds(pl.multiple_of(block * FBLK, FBLK), FBLK)
                stacked = grids[:, lines, :].reshape(areas * FBLK, SUBKEYS)
                product = jnp.dot(
                    stacked, one_hot(row_meta % SUBKEYS, SUBKEYS), preferred_element_type=jnp.float32
                )
                spot_id = lax.broadcasted_iota(jnp.int32, product.shape, 0)
                sums[block] = jnp.sum(
                    jnp.where(spot_id == row_meta // SUBKEYS, product, 0.0), axis=0, keepdims=True
                )
                return carry

            lax.fori_loop(0, blocks, one, 0)

            for r in range(rows):
                index = (source_dp * rows + r) * cols + source_col
                for block in range(blocks):
                    found[index, block : block + 1, :] = sums[block, :, r * 128 : (r + 1) * 128]
                away = remote(found.at[index], back.at[me], fsend, frecv, (source_dp, r, source_col))
                own = jnp.logical_and(
                    jnp.logical_and(source_dp == dp, row == r), source_col == col
                )
                pl.when(jnp.logical_not(own))(away.start)
                pl.when(own)(pltpu.make_async_copy(found.at[index], back.at[me], flocal).start)

    writes = 4 * dps

    def poll(p, carry):
        phase = lax.rem(p, 2)
        writing = p < writes
        pl.when(jnp.logical_and(writing, phase == 0))(lambda: build(lax.div(p, 2)))
        pl.when(jnp.logical_and(writing, phase == 1))(lambda: multiply(lax.div(p, 2)))

        @pl.when(p == writes)
        def _():
            keep.wait()
            start_chunk(0)
            start_chunk(1)

        pl.when(p >= writes)(lambda: search(lax.div(p - writes, 2), phase))
        turn, third = lax.div(p, 3), lax.rem(p, 3)
        pl.when(jnp.logical_and(third == 2, turn + 1 < dps))(lambda: from_line(turn + 1))
        for event, delay in ((from_sides, 1), (from_opposite, 2)):
            now = jnp.logical_and(turn >= delay, turn < dps + delay)
            pl.when(jnp.logical_and(third == 0, now))(functools.partial(event, turn - delay))
        for event, delay in ((finish, FINISH_AT), (relay, RELAY_AT), (combine, COMBINE_AT), (fetch, FETCH_AT)):
            late = p - delay
            now = jnp.logical_and(
                jnp.logical_and(late >= 0, lax.rem(late, 4) == 0), late < 4 * dps
            )
            pl.when(now)(functools.partial(event, lax.div(late, 4)))
        return carry

    lax.fori_loop(0, 8 * dps, poll, 0)
    for slot in range(2):
        pltpu.make_async_copy(tables.at[slot], table.at[0, 0], tsem.at[slot]).wait()
    away(0, 0).wait_send()
    arrived(grads_all.at[:, 0], csend)
    arrived(grads_all.at[:, 0, pl.ds(0, rows - 1)], wsend)
    all_rows(meta_in, msend)
    all_rows(slots_in, ssend)

    def line_sent(k, carry):
        pl.when(jnp.logical_and(k <= dp, dp < dps - 1))(lambda: line_copy(k, True).wait_send())
        pl.when(jnp.logical_and(k >= dp, dp > 0))(lambda: line_copy(k, False).wait_send())
        return carry

    lax.fori_loop(0, dps, line_sent, 0)
    arrived(back.at[pl.ds(0, count - 1)], frecv)
    arrived(back.at[0], flocal)
    arrived(back.at[pl.ds(0, count - 1)], fsend)
    for u in range(max(0, dps - RING), dps):
        sent(u)
    lax.fori_loop(0, dps - 1, lambda u, c: (deep_copy(u).wait_send(), c)[1], 0)


FETCH_AT, COMBINE_AT, RELAY_AT, FINISH_AT = 5, 6, 10, 16


def use_memory(sizes, grads, meta, slots, values):
    dps, rows, cols = sizes
    tokens, width = grads.shape
    rows_dev, features = values.shape
    blocks = tokens // FBLK
    count = dps * rows * cols
    low, wide = jnp.bfloat16, jnp.float32
    shape = jax.ShapeDtypeStruct
    grads_all, table, _, memory, back = pl.pallas_call(
        functools.partial(memory_kernel, sizes, blocks),
        in_specs=[VMEM] * 4,
        out_specs=[ANY] * 3 + [VMEM] * 2,
        out_shape=[
            shape((dps, cols, rows, tokens, width), low),
            shape((dps, cols, tokens, rows_dev), low),
            shape((dps, tokens, features), low),
            shape((tokens, width), wide),
            shape((count, blocks, 128), wide),
        ],
        scratch_shapes=[
            pltpu.VMEM(meta.shape, meta.dtype),
            pltpu.VMEM(slots.shape, slots.dtype),
            pltpu.VMEM((features, rows_dev), low),
            pltpu.VMEM((2, tokens, rows_dev), low),
            pltpu.VMEM((2, tokens, features), low),
            pltpu.VMEM((2, tokens, features), low),
            pltpu.VMEM((count, blocks, 128), wide),
            pltpu.VMEM((blocks, 1, rows * 128), wide),
            pltpu.VMEM((rows_dev // SUBKEYS, tokens, SUBKEYS), low),
            pltpu.VMEM((tokens, features), low),
            pltpu.VMEM((RING, tokens, features), low),
            pltpu.VMEM((dps, 2, tokens // 2, width), low),
            pltpu.VMEM((dps, 2, tokens, width), low),
            pltpu.VMEM((dps + 1, tokens, width), low),
            pltpu.VMEM((dps, tokens, width), low),
            DMA, DMA, DMA, DMA,
            DMA((dps,)), DMA((dps,)), DMA((dps,)),
            DMA, DMA((dps, 4)),
            DMA, DMA((dps,)),
            DMA, DMA((2,)), DMA, DMA((dps,)),
            DMA((2, rows)), DMA,
            DMA((RING, 2)), DMA((dps, 2)),
            DMA((RING, 2)), DMA((dps, 2)),
            DMA((dps,)), DMA((dps + 1,)),
            DMA, DMA, DMA,
        ],
        compiler_params=pltpu.CompilerParams(collective_id=6, has_side_effects=True),
        name="use_memory",
    )(grads, meta, slots, values)
    return grads_all, table, memory, back


def unweigh_kernel(rows_dev, owners, back_ref, picks_ref, rank_ref, weights_ref, first_ref, second_ref):
    picks = picks_ref[0]
    hot = one_hot(picks // rows_dev, owners)
    back = back_ref[0]
    high = back.astype(jnp.bfloat16)
    rest = back - high.astype(jnp.float32)
    middle = rest.astype(jnp.bfloat16)
    lowest = (rest - middle.astype(jnp.float32)).astype(jnp.bfloat16)
    spread_back = (
        jnp.dot(high, hot, preferred_element_type=jnp.float32)
        + jnp.dot(middle, hot, preferred_element_type=jnp.float32)
        + jnp.dot(lowest, hot, preferred_element_type=jnp.float32)
    )
    slot = lax.broadcasted_iota(jnp.int32, spread_back.shape, 0)
    flat = jnp.sum(jnp.where(slot == rank_ref[0], spread_back, 0.0), axis=0, keepdims=True)
    grads = jnp.concatenate(
        [flat[:, pick * FBLK : (pick + 1) * FBLK] for pick in range(TOPK)], axis=0
    )
    weights = weights_ref[0]
    grads = weights * (grads - jnp.sum(weights * grads, axis=0, keepdims=True))
    upper = picks // SUBKEYS
    lower = picks % SUBKEYS
    key_id = lax.broadcasted_iota(jnp.int32, (SUBKEYS, FBLK), 0)
    first = jnp.zeros((SUBKEYS, FBLK), jnp.float32)
    second = jnp.zeros((SUBKEYS, FBLK), jnp.float32)
    for pick in range(TOPK):
        columns = slice(pick * FBLK, (pick + 1) * FBLK)
        value = grads[pick : pick + 1]
        first = first + jnp.where(key_id == upper[:, columns], value, 0.0)
        second = second + jnp.where(key_id == lower[:, columns], value, 0.0)
    first_ref[...] = first.astype(jnp.bfloat16)
    second_ref[...] = second.astype(jnp.bfloat16)


def unweigh(back, flat, rank, weights, rows_dev, owners):
    blocks, count = flat.shape
    cap = back.shape[1]
    return pl.pallas_call(
        functools.partial(unweigh_kernel, rows_dev, owners),
        grid=(blocks,),
        in_specs=[
            pl.BlockSpec((1, cap, owners), lambda i: (i, 0, 0)),
            pl.BlockSpec((1, 1, count), lambda i: (i, 0, 0)),
            pl.BlockSpec((1, 1, count), lambda i: (i, 0, 0)),
            pl.BlockSpec((1, TOPK, FBLK), lambda i: (i, 0, 0)),
        ],
        out_specs=[
            pl.BlockSpec((SUBKEYS, FBLK), lambda i: (0, i)),
            pl.BlockSpec((SUBKEYS, FBLK), lambda i: (0, i)),
        ],
        out_shape=[jax.ShapeDtypeStruct((SUBKEYS, blocks * FBLK), jnp.bfloat16)] * 2,
        name="unweigh",
    )(back, flat[:, None, :], rank, weights)


def memory_all(query_rows, grad_memory, flat, rank, meta, subkeys, values):
    sizes = grid_sizes()
    owners = sizes[0] * sizes[1] * sizes[2]
    rows_dev = values.shape[0]
    cap = FBLK * TOPK // owners
    head_id = lax.axis_index("row")
    keys_head = lax.dynamic_index_in_dim(subkeys, head_id, 0, keepdims=False)
    weights, slots = weigh(query_rows, keys_head, flat, rank, rows_dev, owners, cap)
    spare = ((0, 0), (0, 0), (0, 128 - cap))
    meta = jnp.pad(jnp.swapaxes(meta, 0, 1), spare, constant_values=-1)
    slots = jnp.pad(jnp.swapaxes(slots, 0, 1).astype(jnp.float32), spare)
    grads_all, table, memory, back = use_memory(
        sizes, grad_memory, meta, slots, values
    )
    first_t, second_t = unweigh(
        jnp.transpose(back, (1, 2, 0))[:, :cap], flat, rank, weights, rows_dev, owners
    )
    grad_query = jnp.concatenate(
        [
            lax.dot_general(
                part, keys_head[i], (((0,), (0,)), ((), ())), preferred_element_type=jnp.float32
            )
            for i, part in enumerate((first_t, second_t))
        ],
        axis=1,
    ).astype(jnp.bfloat16)
    grad_keys = jnp.stack(
        [
            jnp.dot(first_t, query_rows[:, :HALF], preferred_element_type=jnp.float32),
            jnp.dot(second_t, query_rows[:, HALF:], preferred_element_type=jnp.float32),
        ]
    )
    return memory, grad_query, grad_keys, table, grads_all


def head_scores(query_head, key_head, allowed):
    raw_scores = jnp.einsum(
        "qd,kd->qk", query_head, key_head, preferred_element_type=jnp.float32
    ) * HDIM ** (-0.5)
    return jnp.where(allowed, raw_scores, -jnp.inf)


def attend_forward(queries, keys, values, allowed):
    outputs = []
    log_sums = []
    for head_index in range(queries.shape[1] // HDIM):
        columns = slice(head_index * HDIM, (head_index + 1) * HDIM)
        scores = head_scores(queries[:, columns], keys[:, columns], allowed)
        peak_score = jnp.max(scores, axis=1, keepdims=True)
        exp_scores = jnp.exp(scores - peak_score)
        row_sum = jnp.sum(exp_scores, axis=1, keepdims=True)
        probabilities = (exp_scores / row_sum).astype(jnp.bfloat16)
        outputs.append(
            jnp.dot(probabilities, values[:, columns], preferred_element_type=jnp.float32)
        )
        log_sums.append(peak_score[:, 0] + jnp.log(row_sum[:, 0]))
    return (jnp.concatenate(outputs, axis=1), jnp.stack(log_sums))


def dense(left, right):
    return jnp.dot(left, right, preferred_element_type=jnp.float32)


def dense_nt(left, right):
    return lax.dot_general(left, right, (((1,), (1,)), ((), ())), preferred_element_type=jnp.float32)


def dense_tn(left, right):
    return lax.dot_general(left, right, (((0,), (0,)), ((), ())), preferred_element_type=jnp.float32)


def per_device(
    inputs,
    prefix,
    picks,
    gain_attn,
    w_qkv,
    w_attn_out,
    gain_mem,
    w_query,
    w_gate,
    w_proj,
    subkeys,
    values,
    cotangent,
):
    low = jnp.bfloat16
    sizes = grid_sizes()
    width_part = inputs.shape[1]
    own_tokens = picks.shape[0]
    seq_tokens = own_tokens * sizes[2]
    col = lax.axis_index("col")
    col_first = col * width_part
    gain_one = lax.dynamic_slice_in_dim(gain_attn, col_first, width_part)
    gain_two = lax.dynamic_slice_in_dim(gain_mem, col_first, width_part)

    flat = flat_picks(lax.dynamic_index_in_dim(picks, lax.axis_index("row"), 1, keepdims=False))
    x_own, dy_own, qkv_w, query_w, gate_w, proj_w, attn_w, rank, meta = start_all(
        sizes, values.shape[0], inputs, cotangent, w_qkv, w_query, w_gate, w_proj, w_attn_out, flat
    )
    residual = x_own.astype(jnp.float32)
    scale_one = lax.rsqrt(jnp.sum(residual * residual, axis=1, keepdims=True) / D + EPSILON)
    normed_one = (residual * scale_one * gain_attn.astype(jnp.float32)).astype(low)
    qkv = jnp.einsum("tc,jcf->jtf", normed_one, qkv_w, preferred_element_type=jnp.float32).astype(low)
    kv_all = swap_tokens(sizes, qkv[1:])
    allowed = allowed_mask(own_tokens, seq_tokens, col * own_tokens, prefix[0])
    attended_sum, log_sums = attend_forward(qkv[0], kv_all[0], kv_all[1], allowed)
    attended = attended_sum.astype(low)
    hidden, normed_two = join(sizes, dense(attended, attn_w).astype(low), inputs, gain_two)
    query_rows = dense(normed_two, query_w).astype(low)
    gate_value = dense(normed_two, gate_w)
    sigmoid_gate = jax.nn.sigmoid(gate_value)
    silu_gate = gate_value * sigmoid_gate
    grad_gated = dense_nt(dy_own, proj_w)
    grad_memory = (grad_gated * silu_gate).astype(low)
    memory, grad_query, grad_keys, table, grads_all = memory_all(
        query_rows, grad_memory, flat, rank, meta, subkeys, values
    )
    gated_value = (memory * silu_gate).astype(low)
    out_part = dense(gated_value, proj_w).astype(low)
    grad_gate = (
        grad_gated * memory * sigmoid_gate * (1.0 + gate_value * (1.0 - sigmoid_gate))
    ).astype(low)
    grad_part = (dense_nt(grad_query, query_w) + dense_nt(grad_gate, gate_w)).astype(low)
    query_term = dense_tn(normed_two, grad_query).astype(low)
    first_terms = [
        dense_tn(normed_two, grad_gate).astype(low),
        dense_tn(gated_value, dy_own).astype(low),
        grad_keys.reshape(-1, HALF).astype(low),
    ]
    grad_hidden, grad_hidden_all, gain_two_grad, *shards = middle(
        sizes, grad_part, hidden, cotangent, gain_two, first_terms
    )
    grad_attended = dense_nt(grad_hidden_all, attn_w).astype(low)
    grad_q, grad_kv, output, grad_w_gate, grad_w_proj, grad_keys_half, query_shard = turn(
        sizes, prefix, qkv[0], kv_all, grad_attended, log_sums, out_part, hidden, shards, query_term
    )
    x_part = (
        dense_nt(grad_q, qkv_w[0]) + dense_nt(grad_kv[0], qkv_w[1]) + dense_nt(grad_kv[1], qkv_w[2])
    ).astype(low)
    last_terms = [
        jnp.stack([dense_tn(normed_one, part) for part in (grad_q, grad_kv[0], grad_kv[1])]).astype(low),
        dense_tn(attended, grad_hidden_all).astype(low),
    ]
    (
        grad_inputs, gain_sums, grad_values, grad_w_query, grad_w_qkv, grad_w_attn_out, grad_subkeys,
    ) = last(
        sizes, x_part, inputs, grad_hidden, gain_one, gain_two_grad, grad_keys_half, query_shard,
        last_terms, table, grads_all,
    )
    gain_rows = gain_sums.reshape(sizes[2], 2, width_part)
    grad_gain_one = gain_rows[:, 0].reshape(-1)
    grad_gain_two = gain_rows[:, 1].reshape(-1)

    return (
        output,
        grad_inputs,
        grad_gain_one,
        grad_w_qkv.astype(jnp.float32),
        grad_w_attn_out.astype(jnp.float32),
        grad_gain_two,
        grad_w_query.astype(jnp.float32),
        grad_w_gate.astype(jnp.float32),
        grad_w_proj.astype(jnp.float32),
        grad_subkeys.astype(jnp.float32),
        grad_values,
    )


def solution(mesh):
    placed = (
        P(("dp", "row"), "col"),
        P("dp"),
        P(("dp", "col"), None, None),
        P(),
        P(None, "col", "row"),
        P("row", "col"),
        P(),
        P("col", "row"),
        P("col", "row"),
        P("row", "col"),
        P(),
        P(("dp", "row", "col"), None),
        P(("dp", "row"), "col"),
    )
    return jax.shard_map(
        per_device,
        mesh=mesh,
        in_specs=placed,
        out_specs=(
            P(("dp", "row"), "col"),
            P(("dp", "row"), "col"),
            P(),
            P(None, "col", "row"),
            P("row", "col"),
            P(),
            P("col", "row"),
            P("col", "row"),
            P("row", "col"),
            P(),
            P(("dp", "row", "col"), None),
        ),
        check_vma=False,
    )
```

```python
import functools

import jax
import jax.numpy as jnp
from jax import lax
from jax.experimental import pallas as pl
from jax.experimental.pallas import tpu as pltpu
from jax.sharding import PartitionSpec as P

D = 1024
HDIM = 64
HALF = 512
SUBKEYS = 256
TOPK = 32
FBLK = 128


EPSILON = 1e-06


MESH = pl.DeviceIdType.MESH
VMEM = pl.BlockSpec(memory_space=pltpu.VMEM)
ANY = pl.BlockSpec(memory_space=pl.ANY)
DMA = pltpu.SemaphoreType.DMA


def here():
    return lax.axis_index("dp"), lax.axis_index("row"), lax.axis_index("col")


def grid_sizes():
    return lax.axis_size("dp"), lax.axis_size("row"), lax.axis_size("col")


def remote(src, dst, send_sem, recv_sem, device):
    return pltpu.make_async_remote_copy(
        src_ref=src,
        dst_ref=dst,
        send_sem=send_sem,
        recv_sem=recv_sem,
        device_id=device,
        device_id_type=MESH,
    )


def arrived(dst, sem):
    pltpu.make_async_copy(dst, dst, sem).wait()


def greet_plane(spot, sizes):
    barrier = pltpu.get_barrier_semaphore()
    dp, row, col = spot
    _, rows, cols = sizes
    for j in range(rows):
        for k in range(cols):
            if j + k > 0:
                pl.semaphore_signal(
                    barrier,
                    inc=1,
                    device_id=(dp, lax.rem(row + j, rows), lax.rem(col + k, cols)),
                    device_id_type=MESH,
                )
    pl.semaphore_wait(barrier, rows * cols - 1)


def greet_partner(spot, sizes):
    barrier = pltpu.get_barrier_semaphore()
    dp, row, col = spot
    pl.semaphore_signal(barrier, inc=1, device_id=(dp, row, 1 - col), device_id_type=MESH)
    pl.semaphore_wait(barrier, 1)


def index_of(spot, sizes):
    return (spot[0] * sizes[1] + spot[1]) * sizes[2] + spot[2]


def each_other(spot, sizes, action):
    dp, row, col = spot
    dps, rows, cols = sizes

    def level(step, carry):
        there = lax.rem(dp + step, dps)
        for j in range(rows):
            for k in range(cols):
                device = (there, lax.rem(row + j, rows), lax.rem(col + k, cols))
                if j + k > 0:
                    action(device)
                else:
                    pl.when(step > 0)(functools.partial(action, device))
        return carry

    lax.fori_loop(0, dps, level, 0)


def greet_all(spot, sizes):
    barrier = pltpu.get_barrier_semaphore()

    def greet(device):
        pl.semaphore_signal(barrier, inc=1, device_id=device, device_id_type=MESH)

    each_other(spot, sizes, greet)
    pl.semaphore_wait(barrier, sizes[0] * sizes[1] * sizes[2] - 1)


class Gather:
    def __init__(self, spot, sizes, src, dst, send, recv):
        self.spot, self.sizes, self.src, self.dst = spot, sizes, src, dst
        self.send, self.recv = send, recv
        self.tokens, self.width = src.shape
        dp, row, col = spot
        _, rows, cols = sizes
        self.half = rows // cols
        self.target = lax.div(row, self.half)
        self.slot = lax.rem(row, self.half) * cols + col
        first = pl.multiple_of(lax.rem(row, self.half) * self.tokens, self.tokens)
        left = pl.multiple_of(col * self.width, self.width)
        self.there = dst.at[pl.ds(first, self.tokens), pl.ds(left, self.width)]

    def copy(self, step):
        dp, row, _ = self.spot
        device = (dp, lax.rem(row + step, self.sizes[1]), self.target)
        return remote(self.src, self.there, self.send.at[step], self.recv.at[self.slot], device)

    def start(self):
        col = self.spot[2]

        for step in range(1, self.sizes[1]):
            self.copy(step).start()

        @pl.when(self.target == col)
        def _():
            pltpu.make_async_copy(self.src, self.there, self.recv.at[self.slot]).start()

        @pl.when(self.target != col)
        def _():
            self.copy(0).start()

    def wait(self):
        cols = self.sizes[2]
        for i in range(self.half):
            for k in range(cols):
                arrived(
                    self.dst.at[pl.ds(i * self.tokens, self.tokens), pl.ds(k * self.width, self.width)],
                    self.recv.at[i * cols + k],
                )
        for step in range(1, self.sizes[1]):
            self.copy(step).wait_send()

        @pl.when(self.target != self.spot[2])
        def _():
            self.copy(0).wait_send()


class Scatter:
    def __init__(self, spot, sizes, src, landing, send, recv):
        self.spot, self.sizes, self.src, self.landing = spot, sizes, src, landing
        self.send, self.recv = send, recv
        _, self.tokens, self.width = landing.shape
        self.half = sizes[1] // sizes[2]

    def parts(self):
        dp, row, col = self.spot
        cols = self.sizes[2]
        for i in range(self.half):
            for k in range(cols):
                piece = self.src.at[
                    pl.ds(i * self.tokens, self.tokens), pl.ds(k * self.width, self.width)
                ]
                target = col * self.half + i
                mine = jnp.logical_and(target == row, col == k)
                there = self.landing.at[row]
                copy = remote(
                    piece, there, self.send.at[i * cols + k], self.recv.at[row], (dp, target, k)
                )
                yield mine, copy, pltpu.make_async_copy(piece, there, self.recv.at[row])

    def start(self):
        for mine, copy, own in self.parts():
            pl.when(jnp.logical_not(mine))(copy.start)
            pl.when(mine)(own.start)

    def wait(self):
        for q in range(self.sizes[1]):
            arrived(self.landing.at[q], self.recv.at[q])

    def wait_send(self):
        for mine, copy, _ in self.parts():
            pl.when(jnp.logical_not(mine))(copy.wait_send)


def plane_sems(sizes):
    rows, cols = sizes[1], sizes[2]
    return [DMA((rows,)), DMA((rows,))]


def start_kernel(sizes, rows_dev, *refs):
    x, wqkv, wquery, wgate, wproj, wattn, picks = refs[:7]
    xs, wqkv_all, wquery_all, wgate_all, wproj_all, wattn_all, rank, meta = refs[7:15]
    xsend, xrecv, wsend, wrecv, wlocal = refs[15:]
    spot = here()
    dp, row, col = spot
    greet_plane(spot, sizes)
    gather_x = Gather(spot, sizes, x, xs, xsend, xrecv)
    gather_x.start()
    copies = []
    for n, (src, dst, dim) in enumerate(
        (
            (wqkv, wqkv_all, 1),
            (wquery, wquery_all, 0),
            (wgate, wgate_all, 0),
            (wproj, wproj_all, 1),
            (wattn, wattn_all, 1),
        )
    ):
        size = src.shape[dim]
        window = [slice(None)] * len(src.shape)
        window[dim] = pl.ds(pl.multiple_of(col * size, size), size)
        there = dst.at[tuple(window)]
        away = remote(src, there, wsend.at[n], wrecv.at[n], (dp, row, 1 - col))
        own = pltpu.make_async_copy(src, there, wlocal.at[n])
        away.start()
        own.start()
        copies += [away, own]

    def one(block, carry):
        rank[block], meta[block] = route_block(
            picks[block], rows_dev, meta.shape[1], meta.shape[2]
        )
        return carry

    lax.fori_loop(0, picks.shape[0], one, 0)
    for copy in copies:
        copy.wait()
    gather_x.wait()


def start_all(sizes, rows_dev, x, wqkv, wquery, wgate, wproj, wattn, flat):
    tokens, width = x.shape
    half = sizes[1] // sizes[2]
    cols = sizes[2]
    low = jnp.bfloat16

    def twice(operand, dim):
        shape = list(operand.shape)
        shape[dim] *= cols
        return jax.ShapeDtypeStruct(tuple(shape), low)

    whole = jax.ShapeDtypeStruct((half * tokens, cols * width), low)
    blocks, count = flat.shape
    owners = sizes[0] * sizes[1] * sizes[2]
    return pl.pallas_call(
        functools.partial(start_kernel, sizes, rows_dev),
        in_specs=[VMEM] * 7,
        out_specs=[ANY] * 6 + [VMEM] * 2,
        out_shape=[
            whole,
            twice(wqkv, 1),
            twice(wquery, 0),
            twice(wgate, 0),
            twice(wproj, 1),
            twice(wattn, 1),
            jax.ShapeDtypeStruct((blocks, 1, count), jnp.int32),
            jax.ShapeDtypeStruct((blocks, owners, count // owners), jnp.int32),
        ],
        scratch_shapes=plane_sems(sizes) + [DMA((5,))] * 3,
        compiler_params=pltpu.CompilerParams(collective_id=0, has_side_effects=True),
        name="start_all",
    )(x, wqkv, wquery, wgate, wproj, wattn, flat[:, None])


def lane_sides():
    lane = lax.broadcasted_iota(jnp.int32, (1, 2 * HDIM), 1)
    return [
        jnp.where(jnp.logical_and(lane >= a * HDIM, lane < (a + 1) * HDIM), 1.0, 0.0).astype(
            jnp.bfloat16
        )
        for a in range(2)
    ]


def attend_kernel(
    sizes, prefix, qkv, dy, attended, log_sums, kv, dys, ysend, yrecv, send, recv, local
):
    spot = here()
    dp, row, col = spot
    greet_plane(spot, sizes)
    _, tokens, width = qkv.shape
    keys = kv.shape[1]
    tile = tokens // 2
    there = kv.at[:, pl.ds(pl.multiple_of(col * tokens, tokens), tokens)]
    away = remote(qkv.at[pl.ds(1, 2)], there, send, recv, (dp, row, 1 - col))
    home = pltpu.make_async_copy(qkv.at[pl.ds(1, 2)], there, local)
    away.start()
    home.start()
    gather = Gather(spot, sizes, dy, dys, ysend, yrecv)
    gather.start()
    limit = prefix[0]
    key_pos = lax.broadcasted_iota(jnp.int32, (keys, tile), 0)
    sides = lane_sides()
    away.wait()
    home.wait()

    def unit(index, carry):
        pair, part = lax.div(index, 2), lax.rem(index, 2)
        lanes = pl.ds(pl.multiple_of(pair * 2 * HDIM, 2 * HDIM), 2 * HDIM)
        lines = pl.ds(pl.multiple_of(part * tile, tile), tile)
        query_pos = col * tokens + part * tile + lax.broadcasted_iota(jnp.int32, (1, tile), 1)
        allowed = jnp.logical_or(key_pos <= query_pos, key_pos < limit)
        q2, k2, v2 = qkv[0, lines, lanes], kv[0, :, lanes], kv[1, :, lanes]
        total = jnp.zeros((tile, 2 * HDIM), jnp.float32)
        for a in range(2):
            scores = jnp.where(allowed, dense_nt(k2 * sides[a], q2) * HDIM ** (-0.5), -jnp.inf)
            peak = jnp.max(scores, axis=0, keepdims=True)
            powers = jnp.exp(scores - peak)
            power_sum = jnp.sum(powers, axis=0, keepdims=True)
            probs = (powers / power_sum).astype(jnp.bfloat16)
            total = total + dense_tn(probs, v2 * sides[a])
            log_sums[pl.ds(2 * pair + a, 1), lines] = peak + jnp.log(power_sum)
        attended[lines, lanes] = total.astype(jnp.bfloat16)
        return carry

    lax.fori_loop(0, 2 * width // (2 * HDIM), unit, 0)
    gather.wait()


def attend(sizes, prefix, qkv, dy):
    _, tokens, width = qkv.shape
    low, wide = jnp.bfloat16, jnp.float32
    shape = jax.ShapeDtypeStruct
    half = sizes[1] // sizes[2]
    return pl.pallas_call(
        functools.partial(attend_kernel, sizes),
        in_specs=[pl.BlockSpec(memory_space=pltpu.SMEM), VMEM, VMEM],
        out_specs=[VMEM, VMEM, VMEM, ANY],
        out_shape=[
            shape((tokens, width), low),
            shape((width // HDIM, tokens), wide),
            shape((2, tokens * sizes[2], width), low),
            shape((half * dy.shape[0], sizes[2] * dy.shape[1]), low),
        ],
        scratch_shapes=plane_sems(sizes) + [DMA, DMA, DMA],
        compiler_params=pltpu.CompilerParams(collective_id=1, has_side_effects=True),
        name="attend",
    )(prefix, qkv, dy)


def fold(column):
    return jnp.broadcast_to(column, (column.shape[0], 128))


def join_kernel(
    sizes, part, x, gain, hidden, normed_all, landing, mine, theirs, block,
    ssend, srecv, gsend, grecv, psend, precv,
):
    spot = here()
    dp, row, col = spot
    greet_plane(spot, sizes)
    scatter = Scatter(spot, sizes, part, landing, ssend, srecv)
    scatter.start()
    scatter.wait()
    total = x[...].astype(jnp.float32)
    for q in range(sizes[1]):
        total = total + landing[q].astype(jnp.float32)
    hidden[...] = total
    mine[...] = fold(jnp.sum(total * total, axis=1, keepdims=True))
    pair = remote(mine, theirs, psend, precv, (dp, row, 1 - col))
    pair.start()
    pair.wait()
    squares = mine[:, :1] + theirs[:, :1]
    scale = lax.rsqrt(squares / D + EPSILON)
    block[...] = (hidden[...] * scale * gain[...].astype(jnp.float32)).astype(jnp.bfloat16)
    gather = Gather(spot, sizes, block, normed_all, gsend, grecv)
    gather.start()
    scatter.wait_send()
    gather.wait()


def join(sizes, part, x, gain):
    tokens, width = x.shape
    rows = sizes[1]
    return pl.pallas_call(
        functools.partial(join_kernel, sizes),
        in_specs=[VMEM] * 3,
        out_specs=[VMEM, VMEM],
        out_shape=[
            jax.ShapeDtypeStruct((tokens, width), jnp.float32),
            jax.ShapeDtypeStruct(part.shape, jnp.bfloat16),
        ],
        scratch_shapes=[
            pltpu.VMEM((rows, tokens, width), jnp.bfloat16),
            pltpu.VMEM((tokens, 128), jnp.float32),
            pltpu.VMEM((tokens, 128), jnp.float32),
            pltpu.VMEM((tokens, width), jnp.bfloat16),
        ]
        + plane_sems(sizes) * 2
        + [DMA, DMA],
        compiler_params=pltpu.CompilerParams(collective_id=3, has_side_effects=True),
        name="join",
    )(part, x, gain[None])


def norm_back(sizes, spot, landing, base, above, gain, mine, theirs, psend, precv):
    dp, row, col = spot
    normed_grad = landing[0].astype(jnp.float32)
    for q in range(1, sizes[1]):
        normed_grad = normed_grad + landing[q].astype(jnp.float32)
    values = base[...].astype(jnp.float32)
    unit_grad = normed_grad * gain[...].astype(jnp.float32)
    mine[0] = fold(jnp.sum(values * values, axis=1, keepdims=True))
    mine[1] = fold(jnp.sum(unit_grad * values, axis=1, keepdims=True))
    pair = remote(mine, theirs, psend, precv, (dp, row, 1 - col))
    pair.start()
    pair.wait()
    scale = lax.rsqrt((mine[0, :, :1] + theirs[0, :, :1]) / D + EPSILON)
    inner = scale * (mine[1, :, :1] + theirs[1, :, :1]) / D
    unit = values * scale
    grad = above[...].astype(jnp.float32) + scale * (unit_grad - unit * inner)
    return grad, jnp.sum(normed_grad * unit, axis=0, keepdims=True)


def slab(ref, dim, index, count):
    size = ref.shape[dim] // count
    window = [slice(None)] * len(ref.shape)
    window[dim] = pl.ds(pl.multiple_of(index * size, size), size)
    return ref.at[tuple(window)]


def add_into(target, addend):
    target[...] = (target[...].astype(jnp.float32) + addend[...].astype(jnp.float32)).astype(
        target.dtype
    )


class PairSum:
    def __init__(self, spot, sizes, terms, dims, halves, landings, send, recv):
        self.col, self.cols = spot[2], sizes[2]
        self.terms, self.dims, self.halves, self.landings = terms, dims, halves, landings
        self.copies = [
            remote(
                slab(term, dim, 1 - spot[2], sizes[2]), landing, send.at[n], recv.at[n],
                (spot[0], spot[1], 1 - spot[2]),
            )
            for n, (term, dim, landing) in enumerate(zip(terms, dims, landings))
        ]

    def start(self):
        for copy in self.copies:
            copy.start()

    def finish(self):
        for copy, term, dim, half, landing in zip(
            self.copies, self.terms, self.dims, self.halves, self.landings
        ):
            copy.wait()
            own = slab(term, dim, self.col, self.cols)
            half[...] = (own[...].astype(jnp.float32) + landing[...].astype(jnp.float32)).astype(
                half.dtype
            )


class LineReduce:
    def __init__(self, spot, sizes, arrays, dims, below, above, sems):
        self.spot, self.count = spot, sizes[0]
        self.arrays, self.dims, self.below, self.above = arrays, dims, below, above
        self.up_send, self.up_recv, self.down_send, self.down_recv = sems

    def copy(self, n, k, up):
        dp, row, col = self.spot
        landing = self.below[n] if up else self.above[n]
        send, recv = (
            (self.up_send, self.up_recv) if up else (self.down_send, self.down_recv)
        )
        dim = self.dims[n]
        return remote(
            slab(self.arrays[n], dim, k, self.count),
            slab(landing, dim, k, self.count),
            send.at[n, k],
            recv.at[n, k],
            (jnp.clip(dp + (1 if up else -1), 0, self.count - 1), row, col),
        )

    def send(self, k, up):
        for n in range(len(self.arrays)):
            self.copy(n, k, up).start()

    def start(self):
        dp, last = self.spot[0], self.count - 1

        @pl.when(dp == 0)
        def _():
            lax.fori_loop(0, last, lambda i, c: (self.send(last - i, True), c)[1], 0)

        @pl.when(dp == last)
        def _():
            lax.fori_loop(0, last, lambda i, c: (self.send(i, False), c)[1], 0)

    def take(self, k, up):
        for n, (array, dim) in enumerate(zip(self.arrays, self.dims)):
            landing = slab((self.below if up else self.above)[n], dim, k, self.count)
            arrived(landing, (self.up_recv if up else self.down_recv).at[n, k])
            add_into(slab(array, dim, k, self.count), landing)

    def event(self, time):
        dp, last = self.spot[0], self.count - 1

        @pl.when(jnp.logical_and(dp > 0, time >= dp))
        def _():
            k = dp + last - time
            self.take(k, True)
            pl.when(k > dp)(lambda: self.send(k, True))

        @pl.when(jnp.logical_and(dp < last, time >= last - dp))
        def _():
            k = time - (last - dp)
            self.take(k, False)
            pl.when(k < dp)(lambda: self.send(k, False))

    def events(self):
        lax.fori_loop(1, self.count, lambda time, c: (self.event(time), c)[1], 0)

    def finish(self):
        dp = self.spot[0]

        def one(k, carry):
            @pl.when(dp < k)
            def _():
                for n in range(len(self.arrays)):
                    self.copy(n, k, True).wait_send()

            @pl.when(dp > k)
            def _():
                for n in range(len(self.arrays)):
                    self.copy(n, k, False).wait_send()

            return carry

        lax.fori_loop(0, self.count, one, 0)


class LineGather:
    def __init__(self, spot, sizes, arrays, dims, sems):
        self.spot, self.count = spot, sizes[0]
        self.arrays, self.dims = arrays, dims
        self.up_send, self.down_send, self.recv = sems

    def copy(self, n, k, up):
        dp, row, col = self.spot
        part = slab(self.arrays[n], self.dims[n], k, self.count)
        return remote(
            part,
            part,
            (self.up_send if up else self.down_send).at[n, k],
            self.recv.at[n, k],
            (jnp.clip(dp + (1 if up else -1), 0, self.count - 1), row, col),
        )

    def send(self, k, up):
        dp = self.spot[0]

        @pl.when(dp < self.count - 1 if up else dp > 0)
        def _():
            for n in range(len(self.arrays)):
                self.copy(n, k, up).start()

    def start(self):
        self.send(self.spot[0], True)
        self.send(self.spot[0], False)

    def take(self, k):
        for n, (array, dim) in enumerate(zip(self.arrays, self.dims)):
            arrived(slab(array, dim, k, self.count), self.recv.at[n, k])

    def event(self, time):
        dp = self.spot[0]

        @pl.when(dp - time >= 0)
        def _():
            self.take(dp - time)
            self.send(dp - time, True)

        @pl.when(dp + time < self.count)
        def _():
            self.take(dp + time)
            self.send(dp + time, False)

    def events(self):
        lax.fori_loop(1, self.count, lambda time, c: (self.event(time), c)[1], 0)

    def finish(self):
        dp, last = self.spot[0], self.count - 1

        def one(k, carry):
            @pl.when(jnp.logical_and(k <= dp, dp < last))
            def _():
                for n in range(len(self.arrays)):
                    self.copy(n, k, True).wait_send()

            @pl.when(jnp.logical_and(k >= dp, dp > 0))
            def _():
                for n in range(len(self.arrays)):
                    self.copy(n, k, False).wait_send()

            return carry

        lax.fori_loop(0, self.count, one, 0)


def line_sems(sizes, arrays, kinds):
    return [DMA((arrays, sizes[0])) for _ in range(kinds)]


def greet_cross(spot, sizes):
    barrier = pltpu.get_barrier_semaphore()
    dp, row, col = spot
    dps, rows, cols = sizes
    for j in range(rows):
        for k in range(cols):
            if j + k > 0:
                pl.semaphore_signal(
                    barrier,
                    inc=1,
                    device_id=(dp, lax.rem(row + j, rows), lax.rem(col + k, cols)),
                    device_id_type=MESH,
                )
    for j in (1, dps - 1):
        pl.semaphore_signal(
            barrier, inc=1, device_id=(lax.rem(dp + j, dps), row, col), device_id_type=MESH
        )
    pl.semaphore_wait(barrier, rows * cols + 1)


FIRST_DIMS = (0, 0, 0)
FIRST_COLS = (0, 1, 0)
LAST_DIMS = (1, 0)
LAST_COLS = (1, 1)


def halved(shape, dim, cols):
    shape = list(shape)
    shape[dim] //= cols
    return tuple(shape)


def middle_kernel(sizes, *refs):
    part, hidden, dy, gain = refs[:4]
    terms = refs[4:7]
    grad, grad_all, gain_grad = refs[7:10]
    shards = refs[10:13]
    landing, mine, theirs, block = refs[13:17]
    halves, pair_land, below, above = refs[17:20], refs[20:23], refs[23:26], refs[26:29]
    ssend, srecv, gsend, grecv, psend, precv, hsend, hrecv, *line = refs[29:]
    spot = here()
    greet_cross(spot, sizes)
    scatter = Scatter(spot, sizes, part, landing, ssend, srecv)
    scatter.start()
    pair = PairSum(spot, sizes, terms, FIRST_COLS, halves, pair_land, hsend, hrecv)
    pair.start()
    pair.finish()
    reduce = LineReduce(spot, sizes, halves, FIRST_DIMS, below, above, line)
    reduce.start()
    scatter.wait()
    total, gains = norm_back(sizes, spot, landing, hidden, dy, gain, mine, theirs, psend, precv)
    gain_grad[...] = gains
    grad[...] = total
    block[...] = total.astype(jnp.bfloat16)
    gather = Gather(spot, sizes, block, grad_all, gsend, grecv)
    gather.start()
    lax.fori_loop(1, sizes[0], lambda time, c: (reduce.event(time), c)[1], 0)
    for half, dim, shard in zip(halves, FIRST_DIMS, shards):
        shard[...] = slab(half, dim, spot[0], sizes[0])[...]
    scatter.wait_send()
    gather.wait()
    reduce.finish()


def middle(sizes, part, hidden, dy, gain, terms):
    tokens, width = hidden.shape
    dps, rows, cols = sizes
    low, wide = jnp.bfloat16, jnp.float32
    halves = [halved(t.shape, d, cols) for t, d in zip(terms, FIRST_COLS)]
    shards = [halved(h, d, dps) for h, d in zip(halves, FIRST_DIMS)]
    return pl.pallas_call(
        functools.partial(middle_kernel, sizes),
        in_specs=[VMEM] * 7,
        out_specs=[VMEM] * 6,
        out_shape=[
            jax.ShapeDtypeStruct((tokens, width), wide),
            jax.ShapeDtypeStruct(part.shape, low),
            jax.ShapeDtypeStruct((1, width), wide),
        ]
        + [jax.ShapeDtypeStruct(s, low) for s in shards],
        scratch_shapes=[
            pltpu.VMEM((rows, tokens, width), low),
            pltpu.VMEM((2, tokens, 128), wide),
            pltpu.VMEM((2, tokens, 128), wide),
            pltpu.VMEM((tokens, width), low),
        ]
        + [pltpu.VMEM(h, low) for h in halves] * 4
        + plane_sems(sizes) * 2
        + [DMA, DMA, DMA((3,)), DMA((3,))]
        + line_sems(sizes, 3, 4),
        compiler_params=pltpu.CompilerParams(collective_id=4, has_side_effects=True),
        name="middle",
    )(part, hidden, dy, gain[None], *terms)


def last_kernel(sizes, *refs):
    part, x, above_grad, gain, other_gain = refs[:5]
    keys, shard, terms = refs[5], refs[6], refs[7:9]
    table, grads_all = refs[9:11]
    grad, gain_sums, row_grads, first = refs[11:15]
    lasts, keys_all = refs[15:17], refs[17]
    landing, mine, theirs, own_gain, gain_landing, tables, chunks, row_sums = refs[18:26]
    halves, pair_land, below, above = refs[26:28], refs[28:30], refs[30:32], refs[32:34]
    (
        ssend, srecv, psend, precv, bsend, brecv, hsend, hrecv, tsem, csem,
        xsend, xrecv, kxsend, kxrecv, *line
    ) = refs[34:]
    spot = here()
    dp, row, col = spot
    dps, rows, cols = sizes
    count = dps * rows * cols
    me = index_of(spot, sizes)
    loads = dps * cols
    block = grads_all.shape[-1]

    def load(index):
        slot = lax.rem(index, 2)
        where = (lax.div(index, cols), lax.rem(index, cols))
        return (
            pltpu.make_async_copy(table.at[where], tables.at[slot], tsem.at[slot]),
        ) + tuple(
            pltpu.make_async_copy(
                grads_all.at[where + (r,)],
                chunks.at[slot, :, pl.ds(r * block, block)],
                csem.at[slot, r],
            )
            for r in range(rows)
        )

    for copy in load(0):
        copy.start()
    greet_all(spot, sizes)
    scatter = Scatter(spot, sizes, part, landing, ssend, srecv)
    scatter.start()
    pair = PairSum(spot, sizes, terms, LAST_COLS, halves, pair_land, hsend, hrecv)
    pair.start()
    slab(first, 0, dp, dps)[...] = shard[...]
    gather = LineGather(spot, sizes, [first], [0], line[7:])
    gather.start()
    pair.finish()
    reduce = LineReduce(spot, sizes, halves, LAST_DIMS, below, above, line[:4])
    reduce.start()

    wide_strip = min(512, tables.shape[2])

    def product(index):
        slot = lax.rem(index, 2)
        for copy in load(index):
            copy.wait()

        @pl.when(index + 1 < loads)
        def _():
            for copy in load(index + 1):
                copy.start()

        def strip(n, carry):
            columns = pl.ds(pl.multiple_of(n * wide_strip, wide_strip), wide_strip)
            term = lax.dot_general(
                tables[slot, :, columns],
                chunks[slot],
                (((0,), (0,)), ((), ())),
                preferred_element_type=jnp.float32,
            )

            @pl.when(index == 0)
            def _():
                row_sums[columns] = term

            @pl.when(jnp.logical_and(index > 0, index < loads - 1))
            def _():
                row_sums[columns] = row_sums[columns] + term

            @pl.when(index == loads - 1)
            def _():
                row_grads[columns] = (row_sums[columns] + term).astype(jnp.bfloat16)

            return carry

        lax.fori_loop(0, tables.shape[2] // wide_strip, strip, 0)

    def products(first, end):
        lax.fori_loop(first, end, lambda index, c: (product(index), c)[1], 0)

    def sideways(k):
        return remote(
            keys, keys_all.at[row, col], xsend, xrecv.at[rows - k],
            (dp, lax.rem(row + k, rows), col),
        )

    def cross(src, k):
        there = keys_all.at[lax.rem(row + k, rows), col]
        return remote(src, there, kxsend, kxrecv, (dp, row, 1 - col))

    products(0, loads // 4)
    gather.event(1)
    reduce.event(1)
    scatter.wait()
    total, gains = norm_back(sizes, spot, landing, x, above_grad, gain, mine, theirs, psend, precv)
    lines = gains.shape[1] // 128
    for line_index in range(lines):
        columns = slice(line_index * 128, (line_index + 1) * 128)
        own_gain[line_index : line_index + 1] = gains[:, columns]
        own_gain[lines + line_index : lines + line_index + 1] = other_gain[:, columns]

    def tell(device):
        remote(own_gain, gain_landing.at[me], bsend, brecv, device).start()

    each_other(spot, sizes, tell)
    gain_landing[me] = own_gain[...]
    grad[...] = total
    for k in range(1, rows):
        sideways(k).start()
    cross(keys, 0).start()
    keys_all[row, col] = keys[...]
    products(loads // 4, loads // 2)

    def both(time):
        gather.event(time)
        reduce.event(time)

    both(2)
    products(loads // 2, 3 * loads // 4)
    lax.fori_loop(3, dps, lambda time, c: (both(time), c)[1], 0)
    for first, half, dim in zip(lasts, halves, LAST_DIMS):
        slab(first, dim, dp, dps)[...] = slab(half, dim, dp, dps)[...]
    final = LineGather(spot, sizes, lasts, LAST_DIMS, line[4:7])
    final.start()
    products(3 * loads // 4, 7 * loads // 8)
    final.event(1)
    for k in range(1, rows):
        landed = keys_all.at[lax.rem(row + k, rows), col]
        arrived(landed, xrecv.at[k])
        cross(landed, k).start()
    products(7 * loads // 8, loads)
    lax.fori_loop(2, dps, lambda time, c: (final.event(time), c)[1], 0)
    arrived(keys_all.at[:, 1 - col], kxrecv)
    scatter.wait_send()
    arrived(gain_landing.at[pl.ds(0, count - 1)], brecv)
    for c in range(cols):

        def add(index, sums):
            return sums + gain_landing[index * cols + c]

        gain_sums[c] = lax.fori_loop(0, dps * rows, add, jnp.zeros(own_gain.shape, jnp.float32))
    arrived(gain_landing.at[pl.ds(0, count - 1)], bsend)
    arrived(keys_all.at[:, col], kxsend)
    arrived(keys_all.at[pl.ds(0, rows - 1), col], xsend)
    gather.finish()
    reduce.finish()
    final.finish()


def last(sizes, part, x, above, gain, other_gain, keys, shard, terms, table, grads_all):
    tokens, width = x.shape
    dps, rows, cols = sizes
    lines = 2 * width // 128
    count = dps * rows * cols
    low, wide = jnp.bfloat16, jnp.float32
    shape = jax.ShapeDtypeStruct

    halves = [halved(t.shape, d, cols) for t, d in zip(terms, LAST_COLS)]
    rows_dev = table.shape[-1]
    features = grads_all.shape[-1] * rows
    chunk = table.shape[2]
    return pl.pallas_call(
        functools.partial(last_kernel, sizes),
        in_specs=[VMEM] * 9 + [ANY] * 2,
        out_specs=[VMEM] * 7,
        out_shape=[
            shape((tokens, width), wide),
            shape((cols, lines, 128), wide),
            shape((rows_dev, features), low),
            shape((shard.shape[0] * dps, shard.shape[1]), low),
        ]
        + [shape(s, low) for s in halves]
        + [shape((rows, cols) + keys.shape, low)],
        scratch_shapes=[
            pltpu.VMEM((rows, tokens, width), low),
            pltpu.VMEM((2, tokens, 128), wide),
            pltpu.VMEM((2, tokens, 128), wide),
            pltpu.VMEM((lines, 128), wide),
            pltpu.VMEM((count, lines, 128), wide),
            pltpu.VMEM((2, chunk, rows_dev), low),
            pltpu.VMEM((2, chunk, features), low),
            pltpu.VMEM((rows_dev, features), wide),
        ]
        + [pltpu.VMEM(h, low) for h in halves] * 4
        + plane_sems(sizes)
        + [DMA, DMA, DMA, DMA, DMA((2,)), DMA((2,)), DMA((2,)), DMA((2, rows))]
        + [DMA, DMA((rows,)), DMA, DMA]
        + line_sems(sizes, 2, 7)
        + line_sems(sizes, 1, 3),
        compiler_params=pltpu.CompilerParams(collective_id=5, has_side_effects=True),
        name="last",
    )(part, x, above, gain[None], other_gain, keys, shard, *terms, table, grads_all)


def turn_kernel(sizes, *refs):
    prefix, queries, kv, grad_out, log_sums, out_part, hidden = refs[:7]
    shards, term = refs[7:10], refs[10]
    grad_q, grad_kv, output = refs[11:14]
    firsts, term_shard = refs[14:17], refs[17]
    totals, kv_landing, out_landing, half, pair_land, below, above = refs[18:25]
    osend, orecv, ksend, krecv, hsend, hrecv, *line = refs[25:]
    spot = here()
    dp, row, col = spot
    dps = sizes[0]
    tokens, width = queries.shape
    keys = kv.shape[1]
    tile = tokens // 2
    greet_cross(spot, sizes)
    for first, dim, shard in zip(firsts, FIRST_DIMS, shards):
        slab(first, dim, dp, dps)[...] = shard[...]
    pair = PairSum(spot, sizes, [term], [0], [half], [pair_land], hsend, hrecv)
    pair.start()
    gather = LineGather(spot, sizes, firsts, FIRST_DIMS, line[:3])
    gather.start()
    out_scatter = Scatter(spot, sizes, out_part, out_landing, osend, orecv)
    out_scatter.start()
    pair.finish()
    reduce = LineReduce(spot, sizes, [half], [0], [below], [above], line[3:])
    reduce.start()

    def events(time):
        gather.event(time)
        reduce.event(time)

    limit = prefix[0]
    key_pos = lax.broadcasted_iota(jnp.int32, (keys, tile), 0)
    sides = lane_sides()

    def unit(index, carry):
        pair, part = lax.div(index, 2), lax.rem(index, 2)
        lanes = pl.ds(pl.multiple_of(pair * 2 * HDIM, 2 * HDIM), 2 * HDIM)
        lines = pl.ds(pl.multiple_of(part * tile, tile), tile)
        query_pos = col * tokens + part * tile + lax.broadcasted_iota(jnp.int32, (1, tile), 1)
        allowed = jnp.logical_or(key_pos <= query_pos, key_pos < limit)
        q2, g2 = queries[lines, lanes], grad_out[lines, lanes]
        k2, v2 = kv[0, :, lanes], kv[1, :, lanes]
        dq = jnp.zeros((tile, 2 * HDIM), jnp.float32)
        dk = jnp.zeros((keys, 2 * HDIM), jnp.float32)
        dv = jnp.zeros((keys, 2 * HDIM), jnp.float32)
        for a in range(2):
            ka = k2 * sides[a]
            scores = jnp.where(allowed, dense_nt(ka, q2) * HDIM ** (-0.5), -jnp.inf)
            probs = jnp.exp(scores - log_sums[pl.ds(2 * pair + a, 1), lines])
            grad_probs = dense_nt(v2 * sides[a], g2)
            inner = jnp.sum(probs * grad_probs, axis=0, keepdims=True)
            grad_scores = (probs * (grad_probs - inner)).astype(jnp.bfloat16)
            dq = dq + dense_tn(grad_scores, ka)
            dk = dk + dense(grad_scores, q2 * sides[a])
            dv = dv + dense(probs.astype(jnp.bfloat16), g2 * sides[a])
        grad_q[lines, lanes] = (dq * HDIM ** (-0.5)).astype(jnp.bfloat16)
        dk = dk * HDIM ** (-0.5)

        @pl.when(part == 0)
        def _():
            totals[0, :, lanes] = dk
            totals[1, :, lanes] = dv

        @pl.when(part > 0)
        def _():
            totals[0, :, lanes] = totals[0, :, lanes] + dk
            totals[1, :, lanes] = totals[1, :, lanes] + dv

        pl.when(index == 1)(lambda: events(1))
        pl.when(index == 3)(lambda: events(2))
        return carry

    lax.fori_loop(0, 2 * width // (2 * HDIM), unit, 0)
    size = kv_landing.shape[1]
    other = pl.multiple_of((1 - col) * size, size)
    away = remote(totals.at[:, pl.ds(other, size)], kv_landing, ksend, krecv, (dp, row, 1 - col))
    away.start()
    out_scatter.wait()
    result = hidden[...]
    for q in range(sizes[1]):
        result = result + out_landing[q].astype(jnp.float32)
    output[...] = result.astype(jnp.bfloat16)
    away.wait()
    own = totals[:, pl.ds(pl.multiple_of(col * size, size), size)]
    grad_kv[...] = (own + kv_landing[...]).astype(jnp.bfloat16)
    lax.fori_loop(3, dps, lambda time, c: (events(time), c)[1], 0)
    term_shard[...] = slab(half, 0, dp, dps)[...]
    out_scatter.wait_send()
    gather.finish()
    reduce.finish()


def turn(sizes, prefix, queries, kv, grad_out, log_sums, out_part, hidden, shards, term):
    tokens, width = queries.shape
    dps, rows, cols = sizes
    low, wide = jnp.bfloat16, jnp.float32
    shape = jax.ShapeDtypeStruct

    def grown(shard, dim):
        full = list(shard.shape)
        full[dim] *= dps
        return tuple(full)

    firsts = [grown(s, d) for s, d in zip(shards, FIRST_DIMS)]
    half = halved(term.shape, 0, cols)
    return pl.pallas_call(
        functools.partial(turn_kernel, sizes),
        in_specs=[pl.BlockSpec(memory_space=pltpu.SMEM)] + [VMEM] * 10,
        out_specs=[VMEM] * 7,
        out_shape=[
            shape((tokens, width), low),
            shape((2, tokens, width), low),
            shape(hidden.shape, low),
        ]
        + [shape(s, low) for s in firsts]
        + [shape(halved(half, 0, dps), low)],
        scratch_shapes=[
            pltpu.VMEM(kv.shape, wide),
            pltpu.VMEM((2, tokens, width), wide),
            pltpu.VMEM((rows,) + hidden.shape, low),
        ]
        + [pltpu.VMEM(half, low)] * 4
        + plane_sems(sizes)
        + [DMA, DMA, DMA((1,)), DMA((1,))]
        + line_sems(sizes, 3, 3)
        + line_sems(sizes, 1, 4),
        compiler_params=pltpu.CompilerParams(collective_id=2, has_side_effects=True),
        name="turn",
    )(prefix, queries, kv, grad_out, log_sums, out_part, hidden, *shards, term)


def flat_picks(picks_head):
    blocks = picks_head.shape[0] // FBLK
    return jnp.swapaxes(picks_head.reshape(blocks, FBLK, TOPK), 1, 2).reshape(blocks, TOPK * FBLK)


def one_hot(row_values, size):
    hot = lax.broadcasted_iota(jnp.int32, (size, row_values.shape[1]), 0) == row_values
    return jnp.where(hot, 1.0, 0.0).astype(jnp.bfloat16)


def route_block(picks, rows_dev, owners, cap):
    lane = lax.broadcasted_iota(jnp.int32, (FBLK, FBLK), 0)
    before = jnp.where(lane < lax.broadcasted_iota(jnp.int32, (FBLK, FBLK), 1), 1.0, 0.0).astype(
        jnp.bfloat16
    )
    owner = picks // rows_dev
    local = picks % rows_dev
    hot = one_hot(owner, owners)
    running = jnp.zeros((owners, 1), jnp.float32)
    ranks = []
    for chunk in range(picks.shape[1] // FBLK):
        part = hot[:, chunk * FBLK : (chunk + 1) * FBLK]
        earlier = jnp.dot(part, before, preferred_element_type=jnp.float32)
        wide = part.astype(jnp.float32)
        ranks.append(jnp.sum(wide * (earlier + running), axis=0, keepdims=True))
        running = running + jnp.sum(wide, axis=1, keepdims=True)
    rank = jnp.concatenate(ranks, axis=1).astype(jnp.int32)
    slot_hot = one_hot(rank, cap)
    token = lax.broadcasted_iota(jnp.int32, picks.shape, 1) % FBLK
    outs = []
    for payload in (local % SUBKEYS, local // SUBKEYS, token):
        scaled = hot * payload.astype(jnp.float32).astype(jnp.bfloat16)
        outs.append(
            lax.dot_general(
                scaled, slot_hot, (((1,), (1,)), ((), ())), preferred_element_type=jnp.float32
            ).astype(jnp.int32)
        )
    return rank, (outs[1] * FBLK + outs[2]) * SUBKEYS + outs[0]


def weigh_kernel(rows_dev, owners, cap, query_ref, keys_ref, picks_ref, rank_ref, weights_ref, slots_ref):
    picks = picks_ref[0]
    first = lax.dot_general(
        keys_ref[0], query_ref[:, :HALF], (((1,), (1,)), ((), ())), preferred_element_type=jnp.float32
    )
    second = lax.dot_general(
        keys_ref[1], query_ref[:, HALF:], (((1,), (1,)), ((), ())), preferred_element_type=jnp.float32
    )
    upper = picks // SUBKEYS
    lower = picks % SUBKEYS
    key_id = lax.broadcasted_iota(jnp.int32, (SUBKEYS, FBLK), 0)
    rows = []
    for pick in range(TOPK):
        columns = slice(pick * FBLK, (pick + 1) * FBLK)
        chosen = jnp.where(key_id == upper[:, columns], first, 0.0) + jnp.where(
            key_id == lower[:, columns], second, 0.0
        )
        rows.append(jnp.sum(chosen, axis=0, keepdims=True))
    scores = jnp.concatenate(rows, axis=0)
    powers = jnp.exp(scores - jnp.max(scores, axis=0, keepdims=True))
    weights = powers / jnp.sum(powers, axis=0, keepdims=True)
    weights_ref[0] = weights
    flat = jnp.concatenate([weights[pick : pick + 1] for pick in range(TOPK)], axis=1)
    scaled = one_hot(picks // rows_dev, owners) * flat.astype(jnp.bfloat16)
    slots_ref[0] = lax.dot_general(
        scaled,
        one_hot(rank_ref[0], cap),
        (((1,), (1,)), ((), ())),
        preferred_element_type=jnp.float32,
    ).astype(jnp.bfloat16)


def weigh(query_rows, keys_head, flat, rank, rows_dev, owners, cap):
    blocks, count = flat.shape
    return pl.pallas_call(
        functools.partial(weigh_kernel, rows_dev, owners, cap),
        grid=(blocks,),
        in_specs=[
            pl.BlockSpec((FBLK, 2 * HALF), lambda i: (i, 0)),
            pl.BlockSpec((2, SUBKEYS, HALF), lambda i: (0, 0, 0)),
            pl.BlockSpec((1, 1, count), lambda i: (i, 0, 0)),
            pl.BlockSpec((1, 1, count), lambda i: (i, 0, 0)),
        ],
        out_specs=[
            pl.BlockSpec((1, TOPK, FBLK), lambda i: (i, 0, 0)),
            pl.BlockSpec((1, owners, cap), lambda i: (i, 0, 0)),
        ],
        out_shape=[
            jax.ShapeDtypeStruct((blocks, TOPK, FBLK), jnp.float32),
            jax.ShapeDtypeStruct((blocks, owners, cap), jnp.bfloat16),
        ],
        name="weigh",
    )(query_rows, keys_head, flat[:, None, :], rank)


def send_rows(spot, sizes, src, landing, send, recv):
    me = index_of(spot, sizes)

    def one(device):
        remote(src.at[index_of(device, sizes)], landing.at[me], send, recv, device).start()

    each_other(spot, sizes, one)
    landing[me] = src[me]


def all_rows(landing, sem):
    return arrived(landing.at[pl.ds(0, landing.shape[0] - 1)], sem)


def slot_row(sizes, table, dp, col, block):
    pieces = []
    for row in range(sizes[1]):
        index = (dp * sizes[1] + row) * sizes[2] + col
        pieces.append(table[index, pl.ds(block, 1), :])
    return jnp.concatenate(pieces, axis=1)


def nth_place(dp, q, dps):
    twice = 2 * jnp.minimum(dp, dps - 1 - dp)
    inside = q <= twice
    distance = jnp.where(inside, lax.div(q + 1, 2), q - lax.div(twice, 2))
    below = jnp.logical_or(
        jnp.logical_and(inside, lax.rem(q, 2) == 1),
        jnp.logical_and(jnp.logical_not(inside), dp > dps - 1 - dp),
    )
    return dp + jnp.where(below, -distance, distance), below


def plane_neighbours(row, rows):
    across = row + 1 - 2 * lax.rem(row, 2)
    along = lax.rem(row + rows // 2, rows)
    return across, along, lax.rem(across + rows // 2, rows)


RING = 3


def memory_kernel(
    sizes, blocks, grads, meta, slots, values,
    grads_all, table, other_part, memory, back,
    meta_in, slots_in, values_t, tables, parts,
    chunks, found, sums, grids, theirs, acc, first_land, side_land, deep_land, total,
    msend, mrecv, ssend, srecv, zup, zdown, zrecv, wsend, wrecv, csend, crecv,
    local, tsem, qsend, qrecv,
    gsem, esem, hsend, hrecv, xsend, xrecv, dsend, drecv, fsend, frecv, flocal,
):
    spot = here()
    dp, row, col = spot
    dps, rows, cols = sizes
    tokens, width = grads.shape
    half = tokens // 2
    areas = values.shape[0] // SUBKEYS
    count = dps * rows * cols
    me = index_of(spot, sizes)
    across, along, opposite = plane_neighbours(row, rows)
    first_half, second_half = pl.ds(0, half), pl.ds(half, half)
    greet_all(spot, sizes)
    send_rows(spot, sizes, meta, meta_in, msend, mrecv)
    send_rows(spot, sizes, slots, slots_in, ssend, srecv)

    def place_of(u):
        return nth_place(dp, dps - 1 - u, dps)[0]

    def block_at(place, r, lines=slice(None)):
        return grads_all.at[place, col, r, lines]

    def cross(q, place, r, src=None):
        there = block_at(place, r)
        remote(there if src is None else src, there, csend, crecv.at[q], (dp, row, 1 - col)).start()

    def line_copy(place, up, src=None):
        there = block_at(place, row)
        return remote(
            there if src is None else src,
            there,
            (zup if up else zdown).at[place],
            zrecv.at[place],
            (jnp.clip(dp + (1 if up else -1), 0, dps - 1), row, col),
        )

    def sideways(q, place, src=None):
        there = block_at(place, row)
        for n, r in enumerate((across, along)):
            remote(
                there if src is None else src, there, wsend, wrecv.at[q, n], (dp, r, col)
            ).start()

    pl.when(dp < dps - 1)(lambda: line_copy(dp, True, grads).start())
    pl.when(dp > 0)(lambda: line_copy(dp, False, grads).start())
    sideways(0, dp, grads)
    cross(0, dp, row, grads)
    keep = pltpu.make_async_copy(grads, block_at(dp, row), local)
    keep.start()

    def from_line(q):
        place, below = nth_place(dp, q, dps)
        arrived(block_at(place, row), zrecv.at[place])
        pl.when(jnp.logical_and(below, dp < dps - 1))(lambda: line_copy(place, True).start())
        pl.when(jnp.logical_and(jnp.logical_not(below), dp > 0))(
            lambda: line_copy(place, False).start()
        )
        sideways(q, place)
        cross(q, place, row)

    def from_sides(q):
        place, _ = nth_place(dp, q, dps)
        for n, (r, other, lines) in enumerate(
            ((across, along, first_half), (along, across, second_half))
        ):
            arrived(block_at(place, r), wrecv.at[q, n])
            half = block_at(place, r, lines)
            remote(half, half, wsend, wrecv.at[q, 2 + n], (dp, other, col)).start()
            cross(q, place, r)

    def from_opposite(q):
        place, _ = nth_place(dp, q, dps)
        for n, lines in enumerate((first_half, second_half)):
            arrived(block_at(place, opposite, lines), wrecv.at[q, 2 + n])
        cross(q, place, opposite)

    def turn_rows(n, carry):
        lines = pl.ds(pl.multiple_of(n * 256, 256), 256)
        values_t[:, lines] = values[lines].T
        return carry

    lax.fori_loop(0, values.shape[0] // 256, turn_rows, 0)
    all_rows(meta_in, mrecv)
    all_rows(slots_in, srecv)

    def write_places(chunk):
        turn = lax.div(chunk, 2)
        slot = lax.rem(chunk, 2)
        return turn, slot, place_of(turn), jnp.where(slot == 0, 1 - col, col)

    def table_copy(chunk):
        _, slot, source_dp, source_col = write_places(chunk)
        return pltpu.make_async_copy(
            tables.at[slot], table.at[source_dp, source_col], tsem.at[slot]
        )

    def build(chunk):
        turn, slot, source_dp, source_col = write_places(chunk)
        pl.when(turn > 0)(lambda: table_copy(chunk).wait())
        def one(block, carry):
            row_meta = slot_row(sizes, meta_in, source_dp, source_col, block)
            key = row_meta // SUBKEYS
            low = row_meta % SUBKEYS
            weight = slot_row(sizes, slots_in, source_dp, source_col, block)
            at_key = lax.broadcasted_iota(jnp.int32, (areas * FBLK, key.shape[1]), 0) == key
            left = jnp.where(at_key, weight, 0.0).astype(jnp.bfloat16)
            stacked = lax.dot_general(
                left,
                one_hot(low, SUBKEYS),
                (((1,), (1,)), ((), ())),
                preferred_element_type=jnp.float32,
            ).astype(jnp.bfloat16)
            for area in range(areas):
                tables[
                    slot,
                    pl.ds(pl.multiple_of(block * FBLK, FBLK), FBLK),
                    area * SUBKEYS : (area + 1) * SUBKEYS,
                ] = stacked[area * FBLK : (area + 1) * FBLK]
            return carry

        lax.fori_loop(0, blocks, one, 0)
        table_copy(chunk).start()

    def away(turn, source_dp):
        return remote(parts.at[0], other_part.at[source_dp], qsend, qrecv.at[turn], (dp, row, 1 - col))

    def multiply(chunk):
        turn, slot, source_dp, _ = write_places(chunk)
        later = turn > 0
        pl.when(jnp.logical_and(later, slot == 0))(lambda: away(turn, source_dp).wait_send())

        def strip(n, carry):
            columns = pl.ds(pl.multiple_of(n * 512, 512), 512)
            parts[slot, :, columns] = jnp.dot(
                tables[slot], values[:, columns], preferred_element_type=jnp.float32
            ).astype(jnp.bfloat16)
            return carry

        lax.fori_loop(0, values.shape[1] // 512, strip, 0)
        pl.when(slot == 0)(lambda: away(turn, source_dp).start())

    def load_part(u):
        return pltpu.make_async_copy(other_part.at[place_of(u)], theirs, esem)

    def strip(u, r, lines=slice(None)):
        return acc.at[lax.rem(u, RING), lines, pl.ds(pl.multiple_of(r * width, width), width)]

    lines_of = (pl.ds(0, half), pl.ds(half, half))

    def halves(u):
        return [
            remote(
                strip(u, opposite, lines_of[n]), first_land.at[u, n],
                hsend.at[lax.rem(u, RING), n], hrecv.at[u, n], (dp, r, col),
            )
            for n, r in enumerate((across, along))
        ]

    def wholes(u):
        return [
            remote(
                strip(u, r), side_land.at[u, n],
                xsend.at[lax.rem(u, RING), n], xrecv.at[u, n], (dp, r, col),
            )
            for n, r in enumerate((across, along))
        ]

    def sent(u):
        for copy in halves(u) + wholes(u):
            copy.wait_send()

    def fetch(u):
        arrived(other_part.at[place_of(u)], qrecv.at[u])
        load_part(u).start()

    def combine(u):
        pl.when(u >= RING)(lambda: sent(u - RING))
        load_part(u).wait()
        acc[lax.rem(u, RING)] = (
            parts[1].astype(jnp.float32) + theirs[...].astype(jnp.float32)
        ).astype(jnp.bfloat16)
        for copy in halves(u):
            copy.start()

    def relay(u):
        for n, r in enumerate((along, across)):
            arrived(first_land.at[u, n], hrecv.at[u, n])
            add_into(strip(u, r, lines_of[n]), first_land.at[u, n])
        for copy in wholes(u):
            copy.start()

    def deep_copy(u):
        place = place_of(u)
        up = place > dp
        target = jnp.where(up, dp + 1, dp - 1)
        there = jnp.where(jnp.logical_and(jnp.logical_not(up), target == place), dps, place)
        return remote(
            total.at[u], deep_land.at[there], dsend.at[u], drecv.at[there],
            (jnp.clip(target, 0, dps - 1), row, col),
        )

    def finish(u):
        for n in range(2):
            arrived(side_land.at[u, n], xrecv.at[u, n])
        place = place_of(u)
        result = (
            strip(u, row)[...].astype(jnp.float32)
            + side_land[u, 0].astype(jnp.float32)
            + side_land[u, 1].astype(jnp.float32)
        )
        memory[...] = result

        def more(index):
            arrived(deep_land.at[index], drecv.at[index])
            memory[...] = memory[...] + deep_land[index].astype(jnp.float32)

        below = jnp.logical_and(place >= dp, dp > 0)
        above = jnp.logical_and(place <= dp, dp < dps - 1)
        pl.when(jnp.logical_or(below, jnp.logical_and(above, place < dp)))(lambda: more(place))
        pl.when(jnp.logical_and(above, place == dp))(lambda: more(dps))

        @pl.when(u < dps - 1)
        def _():
            total[u] = memory[...].astype(jnp.bfloat16)
            deep_copy(u).start()

    def read_places(chunk):
        slot = lax.rem(chunk, 2)
        place = nth_place(dp, lax.div(chunk, 2), dps)[0]
        return slot, place, jnp.where(slot == 0, col, 1 - col)

    def load_chunk(chunk):
        slot, source_dp, source_col = read_places(chunk)
        return [
            pltpu.make_async_copy(
                grads_all.at[source_dp, source_col, r],
                chunks.at[slot, :, pl.ds(r * width, width)],
                gsem.at[slot, r],
            )
            for r in range(rows)
        ]

    def start_chunk(chunk):
        slot, source_dp, source_col = read_places(chunk)

        @pl.when(slot == 1)
        def _():
            arrived(grads_all.at[source_dp, source_col], crecv.at[lax.div(chunk, 2)])

        for copy in load_chunk(chunk):
            copy.start()

    wide_strip = min(2048, areas * SUBKEYS)
    per_strip = wide_strip // SUBKEYS

    def search(chunk, part):
        slot, source_dp, source_col = read_places(chunk)

        @pl.when(part == 0)
        def _():
            for copy in load_chunk(chunk):
                copy.wait()

            def strip(n, carry):
                columns = pl.ds(pl.multiple_of(n * wide_strip, wide_strip), wide_strip)
                grid = jnp.dot(
                    chunks[slot], values_t[:, columns], preferred_element_type=jnp.float32
                ).astype(jnp.bfloat16)
                for area in range(per_strip):
                    grids[n * per_strip + area] = grid[:, area * SUBKEYS : (area + 1) * SUBKEYS]
                return carry

            lax.fori_loop(0, areas // per_strip, strip, 0)

            @pl.when(chunk + 2 < dps * cols)
            def _():
                start_chunk(chunk + 2)

        @pl.when(part == 1)
        def _():
            def one(block, carry):
                row_meta = slot_row(sizes, meta_in, source_dp, source_col, block)
                lines = pl.ds(pl.multiple_of(block * FBLK, FBLK), FBLK)
                stacked = grids[:, lines, :].reshape(areas * FBLK, SUBKEYS)
                product = jnp.dot(
                    stacked, one_hot(row_meta % SUBKEYS, SUBKEYS), preferred_element_type=jnp.float32
                )
                spot_id = lax.broadcasted_iota(jnp.int32, product.shape, 0)
                sums[block] = jnp.sum(
                    jnp.where(spot_id == row_meta // SUBKEYS, product, 0.0), axis=0, keepdims=True
                )
                return carry

            lax.fori_loop(0, blocks, one, 0)

            for r in range(rows):
                index = (source_dp * rows + r) * cols + source_col
                for block in range(blocks):
                    found[index, block : block + 1, :] = sums[block, :, r * 128 : (r + 1) * 128]
                away = remote(found.at[index], back.at[me], fsend, frecv, (source_dp, r, source_col))
                own = jnp.logical_and(
                    jnp.logical_and(source_dp == dp, row == r), source_col == col
                )
                pl.when(jnp.logical_not(own))(away.start)
                pl.when(own)(pltpu.make_async_copy(found.at[index], back.at[me], flocal).start)

    writes = 4 * dps

    def poll(p, carry):
        phase = lax.rem(p, 2)
        writing = p < writes
        pl.when(jnp.logical_and(writing, phase == 0))(lambda: build(lax.div(p, 2)))
        pl.when(jnp.logical_and(writing, phase == 1))(lambda: multiply(lax.div(p, 2)))

        @pl.when(p == writes)
        def _():
            keep.wait()
            start_chunk(0)
            start_chunk(1)

        pl.when(p >= writes)(lambda: search(lax.div(p - writes, 2), phase))
        turn, third = lax.div(p, 3), lax.rem(p, 3)
        pl.when(jnp.logical_and(third == 2, turn + 1 < dps))(lambda: from_line(turn + 1))
        for event, delay in ((from_sides, 1), (from_opposite, 2)):
            now = jnp.logical_and(turn >= delay, turn < dps + delay)
            pl.when(jnp.logical_and(third == 0, now))(functools.partial(event, turn - delay))
        for event, delay in ((finish, FINISH_AT), (relay, RELAY_AT), (combine, COMBINE_AT), (fetch, FETCH_AT)):
            late = p - delay
            now = jnp.logical_and(
                jnp.logical_and(late >= 0, lax.rem(late, 4) == 0), late < 4 * dps
            )
            pl.when(now)(functools.partial(event, lax.div(late, 4)))
        return carry

    lax.fori_loop(0, 8 * dps, poll, 0)
    for slot in range(2):
        pltpu.make_async_copy(tables.at[slot], table.at[0, 0], tsem.at[slot]).wait()
    away(0, 0).wait_send()
    arrived(grads_all.at[:, 0], csend)
    arrived(grads_all.at[:, 0, pl.ds(0, rows - 1)], wsend)
    all_rows(meta_in, msend)
    all_rows(slots_in, ssend)

    def line_sent(k, carry):
        pl.when(jnp.logical_and(k <= dp, dp < dps - 1))(lambda: line_copy(k, True).wait_send())
        pl.when(jnp.logical_and(k >= dp, dp > 0))(lambda: line_copy(k, False).wait_send())
        return carry

    lax.fori_loop(0, dps, line_sent, 0)
    arrived(back.at[pl.ds(0, count - 1)], frecv)
    arrived(back.at[0], flocal)
    arrived(back.at[pl.ds(0, count - 1)], fsend)
    for u in range(max(0, dps - RING), dps):
        sent(u)
    lax.fori_loop(0, dps - 1, lambda u, c: (deep_copy(u).wait_send(), c)[1], 0)


FETCH_AT, COMBINE_AT, RELAY_AT, FINISH_AT = 5, 6, 10, 16


def use_memory(sizes, grads, meta, slots, values):
    dps, rows, cols = sizes
    tokens, width = grads.shape
    rows_dev, features = values.shape
    blocks = tokens // FBLK
    count = dps * rows * cols
    low, wide = jnp.bfloat16, jnp.float32
    shape = jax.ShapeDtypeStruct
    grads_all, table, _, memory, back = pl.pallas_call(
        functools.partial(memory_kernel, sizes, blocks),
        in_specs=[VMEM] * 4,
        out_specs=[ANY] * 3 + [VMEM] * 2,
        out_shape=[
            shape((dps, cols, rows, tokens, width), low),
            shape((dps, cols, tokens, rows_dev), low),
            shape((dps, tokens, features), low),
            shape((tokens, width), wide),
            shape((count, blocks, 128), wide),
        ],
        scratch_shapes=[
            pltpu.VMEM(meta.shape, meta.dtype),
            pltpu.VMEM(slots.shape, slots.dtype),
            pltpu.VMEM((features, rows_dev), low),
            pltpu.VMEM((2, tokens, rows_dev), low),
            pltpu.VMEM((2, tokens, features), low),
            pltpu.VMEM((2, tokens, features), low),
            pltpu.VMEM((count, blocks, 128), wide),
            pltpu.VMEM((blocks, 1, rows * 128), wide),
            pltpu.VMEM((rows_dev // SUBKEYS, tokens, SUBKEYS), low),
            pltpu.VMEM((tokens, features), low),
            pltpu.VMEM((RING, tokens, features), low),
            pltpu.VMEM((dps, 2, tokens // 2, width), low),
            pltpu.VMEM((dps, 2, tokens, width), low),
            pltpu.VMEM((dps + 1, tokens, width), low),
            pltpu.VMEM((dps, tokens, width), low),
            DMA, DMA, DMA, DMA,
            DMA((dps,)), DMA((dps,)), DMA((dps,)),
            DMA, DMA((dps, 4)),
            DMA, DMA((dps,)),
            DMA, DMA((2,)), DMA, DMA((dps,)),
            DMA((2, rows)), DMA,
            DMA((RING, 2)), DMA((dps, 2)),
            DMA((RING, 2)), DMA((dps, 2)),
            DMA((dps,)), DMA((dps + 1,)),
            DMA, DMA, DMA,
        ],
        compiler_params=pltpu.CompilerParams(collective_id=6, has_side_effects=True),
        name="use_memory",
    )(grads, meta, slots, values)
    return grads_all, table, memory, back


def unweigh_kernel(rows_dev, owners, back_ref, picks_ref, rank_ref, weights_ref, first_ref, second_ref):
    picks = picks_ref[0]
    hot = one_hot(picks // rows_dev, owners)
    back = back_ref[0]
    high = back.astype(jnp.bfloat16)
    rest = back - high.astype(jnp.float32)
    middle = rest.astype(jnp.bfloat16)
    lowest = (rest - middle.astype(jnp.float32)).astype(jnp.bfloat16)
    spread_back = (
        jnp.dot(high, hot, preferred_element_type=jnp.float32)
        + jnp.dot(middle, hot, preferred_element_type=jnp.float32)
        + jnp.dot(lowest, hot, preferred_element_type=jnp.float32)
    )
    slot = lax.broadcasted_iota(jnp.int32, spread_back.shape, 0)
    flat = jnp.sum(jnp.where(slot == rank_ref[0], spread_back, 0.0), axis=0, keepdims=True)
    grads = jnp.concatenate(
        [flat[:, pick * FBLK : (pick + 1) * FBLK] for pick in range(TOPK)], axis=0
    )
    weights = weights_ref[0]
    grads = weights * (grads - jnp.sum(weights * grads, axis=0, keepdims=True))
    upper = picks // SUBKEYS
    lower = picks % SUBKEYS
    key_id = lax.broadcasted_iota(jnp.int32, (SUBKEYS, FBLK), 0)
    first = jnp.zeros((SUBKEYS, FBLK), jnp.float32)
    second = jnp.zeros((SUBKEYS, FBLK), jnp.float32)
    for pick in range(TOPK):
        columns = slice(pick * FBLK, (pick + 1) * FBLK)
        value = grads[pick : pick + 1]
        first = first + jnp.where(key_id == upper[:, columns], value, 0.0)
        second = second + jnp.where(key_id == lower[:, columns], value, 0.0)
    first_ref[...] = first.astype(jnp.bfloat16)
    second_ref[...] = second.astype(jnp.bfloat16)


def unweigh(back, flat, rank, weights, rows_dev, owners):
    blocks, count = flat.shape
    cap = back.shape[1]
    return pl.pallas_call(
        functools.partial(unweigh_kernel, rows_dev, owners),
        grid=(blocks,),
        in_specs=[
            pl.BlockSpec((1, cap, owners), lambda i: (i, 0, 0)),
            pl.BlockSpec((1, 1, count), lambda i: (i, 0, 0)),
            pl.BlockSpec((1, 1, count), lambda i: (i, 0, 0)),
            pl.BlockSpec((1, TOPK, FBLK), lambda i: (i, 0, 0)),
        ],
        out_specs=[
            pl.BlockSpec((SUBKEYS, FBLK), lambda i: (0, i)),
            pl.BlockSpec((SUBKEYS, FBLK), lambda i: (0, i)),
        ],
        out_shape=[jax.ShapeDtypeStruct((SUBKEYS, blocks * FBLK), jnp.bfloat16)] * 2,
        name="unweigh",
    )(back, flat[:, None, :], rank, weights)


def memory_all(query_rows, grad_memory, flat, rank, meta, subkeys, values):
    sizes = grid_sizes()
    owners = sizes[0] * sizes[1] * sizes[2]
    rows_dev = values.shape[0]
    cap = FBLK * TOPK // owners
    head_id = lax.axis_index("row")
    keys_head = lax.dynamic_index_in_dim(subkeys, head_id, 0, keepdims=False)
    weights, slots = weigh(query_rows, keys_head, flat, rank, rows_dev, owners, cap)
    spare = ((0, 0), (0, 0), (0, 128 - cap))
    meta = jnp.pad(jnp.swapaxes(meta, 0, 1), spare, constant_values=-1)
    slots = jnp.pad(jnp.swapaxes(slots, 0, 1).astype(jnp.float32), spare)
    grads_all, table, memory, back = use_memory(
        sizes, grad_memory, meta, slots, values
    )
    first_t, second_t = unweigh(
        jnp.transpose(back, (1, 2, 0))[:, :cap], flat, rank, weights, rows_dev, owners
    )
    grad_query = jnp.concatenate(
        [
            lax.dot_general(
                part, keys_head[i], (((0,), (0,)), ((), ())), preferred_element_type=jnp.float32
            )
            for i, part in enumerate((first_t, second_t))
        ],
        axis=1,
    ).astype(jnp.bfloat16)
    grad_keys = jnp.stack(
        [
            jnp.dot(first_t, query_rows[:, :HALF], preferred_element_type=jnp.float32),
            jnp.dot(second_t, query_rows[:, HALF:], preferred_element_type=jnp.float32),
        ]
    )
    return memory, grad_query, grad_keys, table, grads_all


def dense(left, right):
    return jnp.dot(left, right, preferred_element_type=jnp.float32)


def dense_nt(left, right):
    return lax.dot_general(left, right, (((1,), (1,)), ((), ())), preferred_element_type=jnp.float32)


def dense_tn(left, right):
    return lax.dot_general(left, right, (((0,), (0,)), ((), ())), preferred_element_type=jnp.float32)


def per_device(
    inputs,
    prefix,
    picks,
    gain_attn,
    w_qkv,
    w_attn_out,
    gain_mem,
    w_query,
    w_gate,
    w_proj,
    subkeys,
    values,
    cotangent,
):
    low = jnp.bfloat16
    sizes = grid_sizes()
    width_part = inputs.shape[1]
    col = lax.axis_index("col")
    col_first = col * width_part
    gain_one = lax.dynamic_slice_in_dim(gain_attn, col_first, width_part)
    gain_two = lax.dynamic_slice_in_dim(gain_mem, col_first, width_part)

    flat = flat_picks(lax.dynamic_index_in_dim(picks, lax.axis_index("row"), 1, keepdims=False))
    x_own, qkv_w, query_w, gate_w, proj_w, attn_w, rank, meta = start_all(
        sizes, values.shape[0], inputs, w_qkv, w_query, w_gate, w_proj, w_attn_out, flat
    )
    residual = x_own.astype(jnp.float32)
    scale_one = lax.rsqrt(jnp.sum(residual * residual, axis=1, keepdims=True) / D + EPSILON)
    normed_one = (residual * scale_one * gain_attn.astype(jnp.float32)).astype(low)
    qkv = jnp.einsum("tc,jcf->jtf", normed_one, qkv_w, preferred_element_type=jnp.float32).astype(low)
    attended, log_sums, kv_all, dy_own = attend(sizes, prefix, qkv, cotangent)
    hidden, normed_two = join(sizes, dense(attended, attn_w).astype(low), inputs, gain_two)
    query_rows = dense(normed_two, query_w).astype(low)
    gate_value = dense(normed_two, gate_w)
    sigmoid_gate = jax.nn.sigmoid(gate_value)
    silu_gate = gate_value * sigmoid_gate
    grad_gated = dense_nt(dy_own, proj_w)
    grad_memory = (grad_gated * silu_gate).astype(low)
    memory, grad_query, grad_keys, table, grads_all = memory_all(
        query_rows, grad_memory, flat, rank, meta, subkeys, values
    )
    gated_value = (memory * silu_gate).astype(low)
    out_part = dense(gated_value, proj_w).astype(low)
    grad_gate = (
        grad_gated * memory * sigmoid_gate * (1.0 + gate_value * (1.0 - sigmoid_gate))
    ).astype(low)
    grad_part = (dense_nt(grad_query, query_w) + dense_nt(grad_gate, gate_w)).astype(low)
    query_term = dense_tn(normed_two, grad_query).astype(low)
    first_terms = [
        dense_tn(normed_two, grad_gate).astype(low),
        dense_tn(gated_value, dy_own).astype(low),
        grad_keys.reshape(-1, HALF).astype(low),
    ]
    grad_hidden, grad_hidden_all, gain_two_grad, *shards = middle(
        sizes, grad_part, hidden, cotangent, gain_two, first_terms
    )
    grad_attended = dense_nt(grad_hidden_all, attn_w).astype(low)
    grad_q, grad_kv, output, grad_w_gate, grad_w_proj, grad_keys_half, query_shard = turn(
        sizes, prefix, qkv[0], kv_all, grad_attended, log_sums, out_part, hidden, shards, query_term
    )
    x_part = (
        dense_nt(grad_q, qkv_w[0]) + dense_nt(grad_kv[0], qkv_w[1]) + dense_nt(grad_kv[1], qkv_w[2])
    ).astype(low)
    last_terms = [
        jnp.stack([dense_tn(normed_one, part) for part in (grad_q, grad_kv[0], grad_kv[1])]).astype(low),
        dense_tn(attended, grad_hidden_all).astype(low),
    ]
    (
        grad_inputs, gain_sums, grad_values, grad_w_query, grad_w_qkv, grad_w_attn_out, grad_subkeys,
    ) = last(
        sizes, x_part, inputs, grad_hidden, gain_one, gain_two_grad, grad_keys_half, query_shard,
        last_terms, table, grads_all,
    )
    gain_rows = gain_sums.reshape(sizes[2], 2, width_part)
    grad_gain_one = gain_rows[:, 0].reshape(-1)
    grad_gain_two = gain_rows[:, 1].reshape(-1)

    return (
        output,
        grad_inputs,
        grad_gain_one,
        grad_w_qkv.astype(jnp.float32),
        grad_w_attn_out.astype(jnp.float32),
        grad_gain_two,
        grad_w_query.astype(jnp.float32),
        grad_w_gate.astype(jnp.float32),
        grad_w_proj.astype(jnp.float32),
        grad_subkeys.astype(jnp.float32),
        grad_values.astype(jnp.float32),
    )


def solution(mesh):
    placed = (
        P(("dp", "row"), "col"),
        P("dp"),
        P(("dp", "col"), None, None),
        P(),
        P(None, "col", "row"),
        P("row", "col"),
        P(),
        P("col", "row"),
        P("col", "row"),
        P("row", "col"),
        P(),
        P(("dp", "row", "col"), None),
        P(("dp", "row"), "col"),
    )
    return jax.shard_map(
        per_device,
        mesh=mesh,
        in_specs=placed,
        out_specs=(
            P(("dp", "row"), "col"),
            P(("dp", "row"), "col"),
            P(),
            P(None, "col", "row"),
            P("row", "col"),
            P(),
            P("col", "row"),
            P("col", "row"),
            P("row", "col"),
            P(),
            P(("dp", "row", "col"), None),
        ),
        check_vma=False,
    )
```

```python
import functools

import jax
import jax.numpy as jnp
from jax import lax
from jax.experimental import pallas as pl
from jax.experimental.pallas import tpu as pltpu
from jax.sharding import PartitionSpec as P

D = 1024
HDIM = 64
HALF = 512
SUBKEYS = 256
TOPK = 32
FBLK = 128


EPSILON = 1e-06


MESH = pl.DeviceIdType.MESH
VMEM = pl.BlockSpec(memory_space=pltpu.VMEM)
ANY = pl.BlockSpec(memory_space=pl.ANY)
DMA = pltpu.SemaphoreType.DMA


def here():
    return lax.axis_index("dp"), lax.axis_index("row"), lax.axis_index("col")


def grid_sizes():
    return lax.axis_size("dp"), lax.axis_size("row"), lax.axis_size("col")


def remote(src, dst, send_sem, recv_sem, device):
    return pltpu.make_async_remote_copy(
        src_ref=src,
        dst_ref=dst,
        send_sem=send_sem,
        recv_sem=recv_sem,
        device_id=device,
        device_id_type=MESH,
    )


def arrived(dst, sem):
    pltpu.make_async_copy(dst, dst, sem).wait()


def greet_plane(spot, sizes):
    barrier = pltpu.get_barrier_semaphore()
    dp, row, col = spot
    _, rows, cols = sizes
    for j in range(rows):
        for k in range(cols):
            if j + k > 0:
                pl.semaphore_signal(
                    barrier,
                    inc=1,
                    device_id=(dp, lax.rem(row + j, rows), lax.rem(col + k, cols)),
                    device_id_type=MESH,
                )
    pl.semaphore_wait(barrier, rows * cols - 1)


def greet_partner(spot, sizes):
    barrier = pltpu.get_barrier_semaphore()
    dp, row, col = spot
    pl.semaphore_signal(barrier, inc=1, device_id=(dp, row, 1 - col), device_id_type=MESH)
    pl.semaphore_wait(barrier, 1)


def index_of(spot, sizes):
    return (spot[0] * sizes[1] + spot[1]) * sizes[2] + spot[2]


def each_other(spot, sizes, action):
    dp, row, col = spot
    dps, rows, cols = sizes

    def level(step, carry):
        there = lax.rem(dp + step, dps)
        for j in range(rows):
            for k in range(cols):
                device = (there, lax.rem(row + j, rows), lax.rem(col + k, cols))
                if j + k > 0:
                    action(device)
                else:
                    pl.when(step > 0)(functools.partial(action, device))
        return carry

    lax.fori_loop(0, dps, level, 0)


def greet_all(spot, sizes):
    barrier = pltpu.get_barrier_semaphore()

    def greet(device):
        pl.semaphore_signal(barrier, inc=1, device_id=device, device_id_type=MESH)

    each_other(spot, sizes, greet)
    pl.semaphore_wait(barrier, sizes[0] * sizes[1] * sizes[2] - 1)


class Gather:
    def __init__(self, spot, sizes, src, dst, send, recv):
        self.spot, self.sizes, self.src, self.dst = spot, sizes, src, dst
        self.send, self.recv = send, recv
        self.tokens, self.width = src.shape
        dp, row, col = spot
        _, rows, cols = sizes
        self.half = rows // cols
        self.target = lax.div(row, self.half)
        self.slot = lax.rem(row, self.half) * cols + col
        first = pl.multiple_of(lax.rem(row, self.half) * self.tokens, self.tokens)
        left = pl.multiple_of(col * self.width, self.width)
        self.there = dst.at[pl.ds(first, self.tokens), pl.ds(left, self.width)]

    def copy(self, step):
        dp, row, _ = self.spot
        device = (dp, lax.rem(row + step, self.sizes[1]), self.target)
        return remote(self.src, self.there, self.send.at[step], self.recv.at[self.slot], device)

    def start(self):
        col = self.spot[2]

        for step in range(1, self.sizes[1]):
            self.copy(step).start()

        @pl.when(self.target == col)
        def _():
            pltpu.make_async_copy(self.src, self.there, self.recv.at[self.slot]).start()

        @pl.when(self.target != col)
        def _():
            self.copy(0).start()

    def wait(self):
        cols = self.sizes[2]
        for i in range(self.half):
            for k in range(cols):
                arrived(
                    self.dst.at[pl.ds(i * self.tokens, self.tokens), pl.ds(k * self.width, self.width)],
                    self.recv.at[i * cols + k],
                )
        for step in range(1, self.sizes[1]):
            self.copy(step).wait_send()

        @pl.when(self.target != self.spot[2])
        def _():
            self.copy(0).wait_send()


class Scatter:
    def __init__(self, spot, sizes, src, landing, send, recv):
        self.spot, self.sizes, self.src, self.landing = spot, sizes, src, landing
        self.send, self.recv = send, recv
        _, self.tokens, self.width = landing.shape
        self.half = sizes[1] // sizes[2]

    def parts(self):
        dp, row, col = self.spot
        cols = self.sizes[2]
        for i in range(self.half):
            for k in range(cols):
                piece = self.src.at[
                    pl.ds(i * self.tokens, self.tokens), pl.ds(k * self.width, self.width)
                ]
                target = col * self.half + i
                mine = jnp.logical_and(target == row, col == k)
                there = self.landing.at[row]
                copy = remote(
                    piece, there, self.send.at[i * cols + k], self.recv.at[row], (dp, target, k)
                )
                yield mine, copy, pltpu.make_async_copy(piece, there, self.recv.at[row])

    def start(self):
        for mine, copy, own in self.parts():
            pl.when(jnp.logical_not(mine))(copy.start)
            pl.when(mine)(own.start)

    def wait(self):
        for q in range(self.sizes[1]):
            arrived(self.landing.at[q], self.recv.at[q])

    def wait_send(self):
        for mine, copy, _ in self.parts():
            pl.when(jnp.logical_not(mine))(copy.wait_send)


def plane_sems(sizes):
    rows, cols = sizes[1], sizes[2]
    return [DMA((rows,)), DMA((rows,))]


def start_kernel(sizes, rows_dev, *refs):
    x, wqkv, wquery, wgate, wproj, wattn, picks = refs[:7]
    xs, wqkv_all, wquery_all, wgate_all, wproj_all, wattn_all, rank, meta = refs[7:15]
    xsend, xrecv, wsend, wrecv, wlocal = refs[15:]
    spot = here()
    dp, row, col = spot
    greet_plane(spot, sizes)
    gather_x = Gather(spot, sizes, x, xs, xsend, xrecv)
    gather_x.start()
    copies = []
    for n, (src, dst, dim) in enumerate(
        (
            (wqkv, wqkv_all, 1),
            (wquery, wquery_all, 0),
            (wgate, wgate_all, 0),
            (wproj, wproj_all, 1),
            (wattn, wattn_all, 1),
        )
    ):
        size = src.shape[dim]
        window = [slice(None)] * len(src.shape)
        window[dim] = pl.ds(pl.multiple_of(col * size, size), size)
        there = dst.at[tuple(window)]
        away = remote(src, there, wsend.at[n], wrecv.at[n], (dp, row, 1 - col))
        own = pltpu.make_async_copy(src, there, wlocal.at[n])
        away.start()
        own.start()
        copies += [away, own]

    def one(block, carry):
        rank[block], meta[block] = route_block(
            picks[block], rows_dev, meta.shape[1], meta.shape[2]
        )
        return carry

    lax.fori_loop(0, picks.shape[0], one, 0)
    for copy in copies:
        copy.wait()
    gather_x.wait()


def start_all(sizes, rows_dev, x, wqkv, wquery, wgate, wproj, wattn, flat):
    tokens, width = x.shape
    half = sizes[1] // sizes[2]
    cols = sizes[2]
    low = jnp.bfloat16

    def twice(operand, dim):
        shape = list(operand.shape)
        shape[dim] *= cols
        return jax.ShapeDtypeStruct(tuple(shape), low)

    whole = jax.ShapeDtypeStruct((half * tokens, cols * width), low)
    blocks, count = flat.shape
    owners = sizes[0] * sizes[1] * sizes[2]
    return pl.pallas_call(
        functools.partial(start_kernel, sizes, rows_dev),
        in_specs=[VMEM] * 7,
        out_specs=[ANY] * 6 + [VMEM] * 2,
        out_shape=[
            whole,
            twice(wqkv, 1),
            twice(wquery, 0),
            twice(wgate, 0),
            twice(wproj, 1),
            twice(wattn, 1),
            jax.ShapeDtypeStruct((blocks, 1, count), jnp.int32),
            jax.ShapeDtypeStruct((blocks, owners, count // owners), jnp.int32),
        ],
        scratch_shapes=plane_sems(sizes) + [DMA((5,))] * 3,
        compiler_params=pltpu.CompilerParams(collective_id=0, has_side_effects=True),
        name="start_all",
    )(x, wqkv, wquery, wgate, wproj, wattn, flat[:, None])


def lane_sides():
    lane = lax.broadcasted_iota(jnp.int32, (1, 2 * HDIM), 1)
    return [
        jnp.where(jnp.logical_and(lane >= a * HDIM, lane < (a + 1) * HDIM), 1.0, 0.0).astype(
            jnp.bfloat16
        )
        for a in range(2)
    ]


def attend_kernel(
    sizes, prefix, qkv, dy, attended, log_sums, kv, dys, ysend, yrecv, send, recv, local
):
    spot = here()
    dp, row, col = spot
    greet_plane(spot, sizes)
    _, tokens, width = qkv.shape
    keys = kv.shape[1]
    tile = tokens // 2
    there = kv.at[:, pl.ds(pl.multiple_of(col * tokens, tokens), tokens)]
    away = remote(qkv.at[pl.ds(1, 2)], there, send, recv, (dp, row, 1 - col))
    home = pltpu.make_async_copy(qkv.at[pl.ds(1, 2)], there, local)
    away.start()
    home.start()
    gather = Gather(spot, sizes, dy, dys, ysend, yrecv)
    gather.start()
    limit = prefix[0]
    key_pos = lax.broadcasted_iota(jnp.int32, (keys, tile), 0)
    sides = lane_sides()
    away.wait()
    home.wait()

    def unit(index, carry):
        pair, part = lax.div(index, 2), lax.rem(index, 2)
        lanes = pl.ds(pl.multiple_of(pair * 2 * HDIM, 2 * HDIM), 2 * HDIM)
        lines = pl.ds(pl.multiple_of(part * tile, tile), tile)
        query_pos = col * tokens + part * tile + lax.broadcasted_iota(jnp.int32, (1, tile), 1)
        allowed = jnp.logical_or(key_pos <= query_pos, key_pos < limit)
        q2, k2, v2 = qkv[0, lines, lanes], kv[0, :, lanes], kv[1, :, lanes]
        total = jnp.zeros((tile, 2 * HDIM), jnp.float32)
        for a in range(2):
            scores = jnp.where(allowed, dense_nt(k2 * sides[a], q2) * HDIM ** (-0.5), -jnp.inf)
            peak = jnp.max(scores, axis=0, keepdims=True)
            powers = jnp.exp(scores - peak)
            power_sum = jnp.sum(powers, axis=0, keepdims=True)
            probs = (powers / power_sum).astype(jnp.bfloat16)
            total = total + dense_tn(probs, v2 * sides[a])
            log_sums[pl.ds(2 * pair + a, 1), lines] = peak + jnp.log(power_sum)
        attended[lines, lanes] = total.astype(jnp.bfloat16)
        return carry

    lax.fori_loop(0, 2 * width // (2 * HDIM), unit, 0)
    gather.wait()


def attend(sizes, prefix, qkv, dy):
    _, tokens, width = qkv.shape
    low, wide = jnp.bfloat16, jnp.float32
    shape = jax.ShapeDtypeStruct
    half = sizes[1] // sizes[2]
    return pl.pallas_call(
        functools.partial(attend_kernel, sizes),
        in_specs=[pl.BlockSpec(memory_space=pltpu.SMEM), VMEM, VMEM],
        out_specs=[VMEM, VMEM, VMEM, ANY],
        out_shape=[
            shape((tokens, width), low),
            shape((width // HDIM, tokens), wide),
            shape((2, tokens * sizes[2], width), low),
            shape((half * dy.shape[0], sizes[2] * dy.shape[1]), low),
        ],
        scratch_shapes=plane_sems(sizes) + [DMA, DMA, DMA],
        compiler_params=pltpu.CompilerParams(collective_id=1, has_side_effects=True),
        name="attend",
    )(prefix, qkv, dy)


def fold(column):
    return jnp.broadcast_to(column, (column.shape[0], 128))


def join_kernel(
    sizes, part, x, gain, hidden, normed_all, landing, mine, theirs, block,
    ssend, srecv, gsend, grecv, psend, precv,
):
    spot = here()
    dp, row, col = spot
    greet_plane(spot, sizes)
    scatter = Scatter(spot, sizes, part, landing, ssend, srecv)
    scatter.start()
    scatter.wait()
    total = x[...].astype(jnp.float32)
    for q in range(sizes[1]):
        total = total + landing[q].astype(jnp.float32)
    hidden[...] = total
    mine[...] = fold(jnp.sum(total * total, axis=1, keepdims=True))
    pair = remote(mine, theirs, psend, precv, (dp, row, 1 - col))
    pair.start()
    pair.wait()
    squares = mine[:, :1] + theirs[:, :1]
    scale = lax.rsqrt(squares / D + EPSILON)
    block[...] = (hidden[...] * scale * gain[...].astype(jnp.float32)).astype(jnp.bfloat16)
    gather = Gather(spot, sizes, block, normed_all, gsend, grecv)
    gather.start()
    scatter.wait_send()
    gather.wait()


def join(sizes, part, x, gain):
    tokens, width = x.shape
    rows = sizes[1]
    return pl.pallas_call(
        functools.partial(join_kernel, sizes),
        in_specs=[VMEM] * 3,
        out_specs=[VMEM, VMEM],
        out_shape=[
            jax.ShapeDtypeStruct((tokens, width), jnp.float32),
            jax.ShapeDtypeStruct(part.shape, jnp.bfloat16),
        ],
        scratch_shapes=[
            pltpu.VMEM((rows, tokens, width), jnp.bfloat16),
            pltpu.VMEM((tokens, 128), jnp.float32),
            pltpu.VMEM((tokens, 128), jnp.float32),
            pltpu.VMEM((tokens, width), jnp.bfloat16),
        ]
        + plane_sems(sizes) * 2
        + [DMA, DMA],
        compiler_params=pltpu.CompilerParams(collective_id=3, has_side_effects=True),
        name="join",
    )(part, x, gain[None])


def norm_back(sizes, spot, landing, base, above, gain, mine, theirs, psend, precv):
    dp, row, col = spot
    normed_grad = landing[0].astype(jnp.float32)
    for q in range(1, sizes[1]):
        normed_grad = normed_grad + landing[q].astype(jnp.float32)
    values = base[...].astype(jnp.float32)
    unit_grad = normed_grad * gain[...].astype(jnp.float32)
    mine[0] = fold(jnp.sum(values * values, axis=1, keepdims=True))
    mine[1] = fold(jnp.sum(unit_grad * values, axis=1, keepdims=True))
    pair = remote(mine, theirs, psend, precv, (dp, row, 1 - col))
    pair.start()
    pair.wait()
    scale = lax.rsqrt((mine[0, :, :1] + theirs[0, :, :1]) / D + EPSILON)
    inner = scale * (mine[1, :, :1] + theirs[1, :, :1]) / D
    unit = values * scale
    grad = above[...].astype(jnp.float32) + scale * (unit_grad - unit * inner)
    return grad, jnp.sum(normed_grad * unit, axis=0, keepdims=True)


def slab(ref, dim, index, count):
    size = ref.shape[dim] // count
    window = [slice(None)] * len(ref.shape)
    window[dim] = pl.ds(pl.multiple_of(index * size, size), size)
    return ref.at[tuple(window)]


def add_into(target, addend):
    target[...] = (target[...].astype(jnp.float32) + addend[...].astype(jnp.float32)).astype(
        target.dtype
    )


class PairSum:
    def __init__(self, spot, sizes, terms, dims, halves, landings, send, recv):
        self.col, self.cols = spot[2], sizes[2]
        self.terms, self.dims, self.halves, self.landings = terms, dims, halves, landings
        self.copies = [
            remote(
                slab(term, dim, 1 - spot[2], sizes[2]), landing, send.at[n], recv.at[n],
                (spot[0], spot[1], 1 - spot[2]),
            )
            for n, (term, dim, landing) in enumerate(zip(terms, dims, landings))
        ]

    def start(self):
        for copy in self.copies:
            copy.start()

    def finish(self):
        for copy, term, dim, half, landing in zip(
            self.copies, self.terms, self.dims, self.halves, self.landings
        ):
            copy.wait()
            own = slab(term, dim, self.col, self.cols)
            half[...] = (own[...].astype(jnp.float32) + landing[...].astype(jnp.float32)).astype(
                half.dtype
            )


class LineReduce:
    def __init__(self, spot, sizes, arrays, dims, below, above, sems):
        self.spot, self.count = spot, sizes[0]
        self.arrays, self.dims, self.below, self.above = arrays, dims, below, above
        self.up_send, self.up_recv, self.down_send, self.down_recv = sems

    def copy(self, n, k, up):
        dp, row, col = self.spot
        landing = self.below[n] if up else self.above[n]
        send, recv = (
            (self.up_send, self.up_recv) if up else (self.down_send, self.down_recv)
        )
        dim = self.dims[n]
        return remote(
            slab(self.arrays[n], dim, k, self.count),
            slab(landing, dim, k, self.count),
            send.at[n, k],
            recv.at[n, k],
            (jnp.clip(dp + (1 if up else -1), 0, self.count - 1), row, col),
        )

    def send(self, k, up):
        for n in range(len(self.arrays)):
            self.copy(n, k, up).start()

    def start(self):
        dp, last = self.spot[0], self.count - 1

        pl.when(dp == 0)(lambda: self.send(last, True))
        pl.when(dp == last)(lambda: self.send(0, False))

    def take(self, k, up):
        for n, (array, dim) in enumerate(zip(self.arrays, self.dims)):
            landing = slab((self.below if up else self.above)[n], dim, k, self.count)
            arrived(landing, (self.up_recv if up else self.down_recv).at[n, k])
            add_into(slab(array, dim, k, self.count), landing)

    def event(self, time):
        dp, last = self.spot[0], self.count - 1
        pl.when(jnp.logical_and(dp == 0, time < last))(lambda: self.send(last - time, True))
        pl.when(jnp.logical_and(dp == last, time < last))(lambda: self.send(time, False))

        @pl.when(jnp.logical_and(dp > 0, time >= dp))
        def _():
            k = dp + last - time
            self.take(k, True)
            pl.when(k > dp)(lambda: self.send(k, True))

        @pl.when(jnp.logical_and(dp < last, time >= last - dp))
        def _():
            k = time - (last - dp)
            self.take(k, False)
            pl.when(k < dp)(lambda: self.send(k, False))

    def events(self):
        lax.fori_loop(1, self.count, lambda time, c: (self.event(time), c)[1], 0)

    def finish(self):
        dp = self.spot[0]

        def one(k, carry):
            @pl.when(dp < k)
            def _():
                for n in range(len(self.arrays)):
                    self.copy(n, k, True).wait_send()

            @pl.when(dp > k)
            def _():
                for n in range(len(self.arrays)):
                    self.copy(n, k, False).wait_send()

            return carry

        lax.fori_loop(0, self.count, one, 0)


class LineGather:
    def __init__(self, spot, sizes, arrays, dims, sems):
        self.spot, self.count = spot, sizes[0]
        self.arrays, self.dims = arrays, dims
        self.up_send, self.down_send, self.recv = sems

    def copy(self, n, k, up):
        dp, row, col = self.spot
        part = slab(self.arrays[n], self.dims[n], k, self.count)
        return remote(
            part,
            part,
            (self.up_send if up else self.down_send).at[n, k],
            self.recv.at[n, k],
            (jnp.clip(dp + (1 if up else -1), 0, self.count - 1), row, col),
        )

    def send(self, k, up):
        dp = self.spot[0]

        @pl.when(dp < self.count - 1 if up else dp > 0)
        def _():
            for n in range(len(self.arrays)):
                self.copy(n, k, up).start()

    def start(self):
        self.send(self.spot[0], True)
        self.send(self.spot[0], False)

    def take(self, k):
        for n, (array, dim) in enumerate(zip(self.arrays, self.dims)):
            arrived(slab(array, dim, k, self.count), self.recv.at[n, k])

    def event(self, time):
        dp = self.spot[0]

        @pl.when(dp - time >= 0)
        def _():
            self.take(dp - time)
            self.send(dp - time, True)

        @pl.when(dp + time < self.count)
        def _():
            self.take(dp + time)
            self.send(dp + time, False)

    def events(self):
        lax.fori_loop(1, self.count, lambda time, c: (self.event(time), c)[1], 0)

    def finish(self):
        dp, last = self.spot[0], self.count - 1

        def one(k, carry):
            @pl.when(jnp.logical_and(k <= dp, dp < last))
            def _():
                for n in range(len(self.arrays)):
                    self.copy(n, k, True).wait_send()

            @pl.when(jnp.logical_and(k >= dp, dp > 0))
            def _():
                for n in range(len(self.arrays)):
                    self.copy(n, k, False).wait_send()

            return carry

        lax.fori_loop(0, self.count, one, 0)


def line_sems(sizes, arrays, kinds):
    return [DMA((arrays, sizes[0])) for _ in range(kinds)]


def greet_cross(spot, sizes):
    barrier = pltpu.get_barrier_semaphore()
    dp, row, col = spot
    dps, rows, cols = sizes
    for j in range(rows):
        for k in range(cols):
            if j + k > 0:
                pl.semaphore_signal(
                    barrier,
                    inc=1,
                    device_id=(dp, lax.rem(row + j, rows), lax.rem(col + k, cols)),
                    device_id_type=MESH,
                )
    for j in (1, dps - 1):
        pl.semaphore_signal(
            barrier, inc=1, device_id=(lax.rem(dp + j, dps), row, col), device_id_type=MESH
        )
    pl.semaphore_wait(barrier, rows * cols + 1)


FIRST_DIMS = (0, 0, 0)
FIRST_COLS = (0, 1, 0)
LAST_DIMS = (1, 0)
LAST_COLS = (1, 1)


def halved(shape, dim, cols):
    shape = list(shape)
    shape[dim] //= cols
    return tuple(shape)


def middle_kernel(sizes, *refs):
    part, hidden, dy, gain = refs[:4]
    terms = refs[4:7]
    grad, grad_all, gain_grad = refs[7:10]
    shards = refs[10:13]
    landing, mine, theirs, block = refs[13:17]
    halves, pair_land, below, above = refs[17:20], refs[20:23], refs[23:26], refs[26:29]
    ssend, srecv, gsend, grecv, psend, precv, hsend, hrecv, *line = refs[29:]
    spot = here()
    greet_cross(spot, sizes)
    scatter = Scatter(spot, sizes, part, landing, ssend, srecv)
    scatter.start()
    pair = PairSum(spot, sizes, terms, FIRST_COLS, halves, pair_land, hsend, hrecv)
    pair.start()
    pair.finish()
    reduce = LineReduce(spot, sizes, halves, FIRST_DIMS, below, above, line)
    reduce.start()
    reduce.event(1)
    scatter.wait()
    total, gains = norm_back(sizes, spot, landing, hidden, dy, gain, mine, theirs, psend, precv)
    gain_grad[...] = gains
    grad[...] = total
    block[...] = total.astype(jnp.bfloat16)
    gather = Gather(spot, sizes, block, grad_all, gsend, grecv)
    gather.start()
    lax.fori_loop(2, sizes[0], lambda time, c: (reduce.event(time), c)[1], 0)
    for half, dim, shard in zip(halves, FIRST_DIMS, shards):
        shard[...] = slab(half, dim, spot[0], sizes[0])[...]
    scatter.wait_send()
    gather.wait()
    reduce.finish()


def middle(sizes, part, hidden, dy, gain, terms):
    tokens, width = hidden.shape
    dps, rows, cols = sizes
    low, wide = jnp.bfloat16, jnp.float32
    halves = [halved(t.shape, d, cols) for t, d in zip(terms, FIRST_COLS)]
    shards = [halved(h, d, dps) for h, d in zip(halves, FIRST_DIMS)]
    return pl.pallas_call(
        functools.partial(middle_kernel, sizes),
        in_specs=[VMEM] * 7,
        out_specs=[VMEM] * 6,
        out_shape=[
            jax.ShapeDtypeStruct((tokens, width), wide),
            jax.ShapeDtypeStruct(part.shape, low),
            jax.ShapeDtypeStruct((1, width), wide),
        ]
        + [jax.ShapeDtypeStruct(s, low) for s in shards],
        scratch_shapes=[
            pltpu.VMEM((rows, tokens, width), low),
            pltpu.VMEM((2, tokens, 128), wide),
            pltpu.VMEM((2, tokens, 128), wide),
            pltpu.VMEM((tokens, width), low),
        ]
        + [pltpu.VMEM(h, low) for h in halves] * 4
        + plane_sems(sizes) * 2
        + [DMA, DMA, DMA((3,)), DMA((3,))]
        + line_sems(sizes, 3, 4),
        compiler_params=pltpu.CompilerParams(collective_id=4, has_side_effects=True),
        name="middle",
    )(part, hidden, dy, gain[None], *terms)


def last_kernel(sizes, *refs):
    part, x, above_grad, gain, other_gain = refs[:5]
    keys, shard, terms = refs[5], refs[6], refs[7:9]
    table, grads_all = refs[9:11]
    grad, gain_sums, row_grads, first = refs[11:15]
    lasts, keys_all = refs[15:17], refs[17]
    landing, mine, theirs, own_gain, gain_landing, tables, chunks, row_sums = refs[18:26]
    halves, pair_land, below, above = refs[26:28], refs[28:30], refs[30:32], refs[32:34]
    (
        ssend, srecv, psend, precv, bsend, brecv, hsend, hrecv, tsem, csem,
        xsend, xrecv, kxsend, kxrecv, *line
    ) = refs[34:]
    spot = here()
    dp, row, col = spot
    dps, rows, cols = sizes
    count = dps * rows * cols
    me = index_of(spot, sizes)
    loads = dps * cols
    block = grads_all.shape[-1]

    def load(index):
        slot = lax.rem(index, 2)
        where = (lax.div(index, cols), lax.rem(index, cols))
        return (
            pltpu.make_async_copy(table.at[where], tables.at[slot], tsem.at[slot]),
        ) + tuple(
            pltpu.make_async_copy(
                grads_all.at[where + (r,)],
                chunks.at[slot, :, pl.ds(r * block, block)],
                csem.at[slot, r],
            )
            for r in range(rows)
        )

    for copy in load(0):
        copy.start()
    greet_all(spot, sizes)
    scatter = Scatter(spot, sizes, part, landing, ssend, srecv)
    scatter.start()
    pair = PairSum(spot, sizes, terms, LAST_COLS, halves, pair_land, hsend, hrecv)
    pair.start()
    slab(first, 0, dp, dps)[...] = shard[...]
    gather = LineGather(spot, sizes, [first], [0], line[7:])
    gather.start()
    pair.finish()
    reduce = LineReduce(spot, sizes, halves, LAST_DIMS, below, above, line[:4])
    reduce.start()

    wide_strip = min(512, tables.shape[2])

    def product(index):
        slot = lax.rem(index, 2)
        for copy in load(index):
            copy.wait()

        @pl.when(index + 1 < loads)
        def _():
            for copy in load(index + 1):
                copy.start()

        def strip(n, carry):
            columns = pl.ds(pl.multiple_of(n * wide_strip, wide_strip), wide_strip)
            term = lax.dot_general(
                tables[slot, :, columns],
                chunks[slot],
                (((0,), (0,)), ((), ())),
                preferred_element_type=jnp.float32,
            )

            @pl.when(index == 0)
            def _():
                row_sums[columns] = term

            @pl.when(jnp.logical_and(index > 0, index < loads - 1))
            def _():
                row_sums[columns] = row_sums[columns] + term

            @pl.when(index == loads - 1)
            def _():
                row_grads[columns] = (row_sums[columns] + term).astype(jnp.bfloat16)

            return carry

        lax.fori_loop(0, tables.shape[2] // wide_strip, strip, 0)

    def products(first, end):
        lax.fori_loop(first, end, lambda index, c: (product(index), c)[1], 0)

    def sideways(k):
        return remote(
            keys, keys_all.at[row, col], xsend, xrecv.at[rows - k],
            (dp, lax.rem(row + k, rows), col),
        )

    def cross(src, k):
        there = keys_all.at[lax.rem(row + k, rows), col]
        return remote(src, there, kxsend, kxrecv, (dp, row, 1 - col))

    def both(time):
        reduce.event(time)
        gather.event(time)

    products(0, loads // 8)
    both(1)
    products(loads // 8, loads // 4)
    scatter.wait()
    total, gains = norm_back(sizes, spot, landing, x, above_grad, gain, mine, theirs, psend, precv)
    lines = gains.shape[1] // 128
    for line_index in range(lines):
        columns = slice(line_index * 128, (line_index + 1) * 128)
        own_gain[line_index : line_index + 1] = gains[:, columns]
        own_gain[lines + line_index : lines + line_index + 1] = other_gain[:, columns]

    def tell(device):
        remote(own_gain, gain_landing.at[me], bsend, brecv, device).start()

    each_other(spot, sizes, tell)
    gain_landing[me] = own_gain[...]
    grad[...] = total
    for k in range(1, rows):
        sideways(k).start()
    cross(keys, 0).start()
    keys_all[row, col] = keys[...]
    both(2)
    products(loads // 4, 3 * loads // 8)
    lax.fori_loop(3, dps, lambda time, c: (both(time), c)[1], 0)
    for first, half, dim in zip(lasts, halves, LAST_DIMS):
        slab(first, dim, dp, dps)[...] = slab(half, dim, dp, dps)[...]
    final = LineGather(spot, sizes, lasts, LAST_DIMS, line[4:7])
    final.start()
    products(3 * loads // 8, 5 * loads // 8)
    final.event(1)
    for k in range(1, rows):
        landed = keys_all.at[lax.rem(row + k, rows), col]
        arrived(landed, xrecv.at[k])
        cross(landed, k).start()
    products(5 * loads // 8, 7 * loads // 8)
    final.event(2)
    products(7 * loads // 8, loads)
    lax.fori_loop(3, dps, lambda time, c: (final.event(time), c)[1], 0)
    arrived(keys_all.at[:, 1 - col], kxrecv)
    scatter.wait_send()
    arrived(gain_landing.at[pl.ds(0, count - 1)], brecv)
    for c in range(cols):

        def add(index, sums):
            return sums + gain_landing[index * cols + c]

        gain_sums[c] = lax.fori_loop(0, dps * rows, add, jnp.zeros(own_gain.shape, jnp.float32))
    arrived(gain_landing.at[pl.ds(0, count - 1)], bsend)
    arrived(keys_all.at[:, col], kxsend)
    arrived(keys_all.at[pl.ds(0, rows - 1), col], xsend)
    gather.finish()
    reduce.finish()
    final.finish()


def last(sizes, part, x, above, gain, other_gain, keys, shard, terms, table, grads_all):
    tokens, width = x.shape
    dps, rows, cols = sizes
    lines = 2 * width // 128
    count = dps * rows * cols
    low, wide = jnp.bfloat16, jnp.float32
    shape = jax.ShapeDtypeStruct

    halves = [halved(t.shape, d, cols) for t, d in zip(terms, LAST_COLS)]
    rows_dev = table.shape[-1]
    features = grads_all.shape[-1] * rows
    chunk = table.shape[2]
    return pl.pallas_call(
        functools.partial(last_kernel, sizes),
        in_specs=[VMEM] * 9 + [ANY] * 2,
        out_specs=[VMEM] * 7,
        out_shape=[
            shape((tokens, width), wide),
            shape((cols, lines, 128), wide),
            shape((rows_dev, features), low),
            shape((shard.shape[0] * dps, shard.shape[1]), low),
        ]
        + [shape(s, low) for s in halves]
        + [shape((rows, cols) + keys.shape, low)],
        scratch_shapes=[
            pltpu.VMEM((rows, tokens, width), low),
            pltpu.VMEM((2, tokens, 128), wide),
            pltpu.VMEM((2, tokens, 128), wide),
            pltpu.VMEM((lines, 128), wide),
            pltpu.VMEM((count, lines, 128), wide),
            pltpu.VMEM((2, chunk, rows_dev), low),
            pltpu.VMEM((2, chunk, features), low),
            pltpu.VMEM((rows_dev, features), wide),
        ]
        + [pltpu.VMEM(h, low) for h in halves] * 4
        + plane_sems(sizes)
        + [DMA, DMA, DMA, DMA, DMA((2,)), DMA((2,)), DMA((2,)), DMA((2, rows))]
        + [DMA, DMA((rows,)), DMA, DMA]
        + line_sems(sizes, 2, 7)
        + line_sems(sizes, 1, 3),
        compiler_params=pltpu.CompilerParams(collective_id=5, has_side_effects=True),
        name="last",
    )(part, x, above, gain[None], other_gain, keys, shard, *terms, table, grads_all)


def turn_kernel(sizes, *refs):
    prefix, queries, kv, grad_out, log_sums, out_part, hidden = refs[:7]
    shards, term = refs[7:10], refs[10]
    grad_q, grad_kv, output = refs[11:14]
    firsts, term_shard = refs[14:17], refs[17]
    totals, kv_landing, out_landing, half, pair_land, below, above = refs[18:25]
    osend, orecv, ksend, krecv, hsend, hrecv, *line = refs[25:]
    spot = here()
    dp, row, col = spot
    dps = sizes[0]
    tokens, width = queries.shape
    keys = kv.shape[1]
    tile = tokens // 2
    greet_cross(spot, sizes)
    for first, dim, shard in zip(firsts, FIRST_DIMS, shards):
        slab(first, dim, dp, dps)[...] = shard[...]
    pair = PairSum(spot, sizes, [term], [0], [half], [pair_land], hsend, hrecv)
    pair.start()
    gather = LineGather(spot, sizes, firsts, FIRST_DIMS, line[:3])
    gather.start()
    out_scatter = Scatter(spot, sizes, out_part, out_landing, osend, orecv)
    out_scatter.start()
    pair.finish()
    reduce = LineReduce(spot, sizes, [half], [0], [below], [above], line[3:])
    reduce.start()

    def events(time):
        gather.event(time)
        reduce.event(time)

    limit = prefix[0]
    key_pos = lax.broadcasted_iota(jnp.int32, (keys, tile), 0)
    sides = lane_sides()

    def unit(index, carry):
        pair, part = lax.div(index, 2), lax.rem(index, 2)
        lanes = pl.ds(pl.multiple_of(pair * 2 * HDIM, 2 * HDIM), 2 * HDIM)
        lines = pl.ds(pl.multiple_of(part * tile, tile), tile)
        query_pos = col * tokens + part * tile + lax.broadcasted_iota(jnp.int32, (1, tile), 1)
        allowed = jnp.logical_or(key_pos <= query_pos, key_pos < limit)
        q2, g2 = queries[lines, lanes], grad_out[lines, lanes]
        k2, v2 = kv[0, :, lanes], kv[1, :, lanes]
        dq = jnp.zeros((tile, 2 * HDIM), jnp.float32)
        dk = jnp.zeros((keys, 2 * HDIM), jnp.float32)
        dv = jnp.zeros((keys, 2 * HDIM), jnp.float32)
        for a in range(2):
            ka = k2 * sides[a]
            scores = jnp.where(allowed, dense_nt(ka, q2) * HDIM ** (-0.5), -jnp.inf)
            probs = jnp.exp(scores - log_sums[pl.ds(2 * pair + a, 1), lines])
            grad_probs = dense_nt(v2 * sides[a], g2)
            inner = jnp.sum(probs * grad_probs, axis=0, keepdims=True)
            grad_scores = (probs * (grad_probs - inner)).astype(jnp.bfloat16)
            dq = dq + dense_tn(grad_scores, ka)
            dk = dk + dense(grad_scores, q2 * sides[a])
            dv = dv + dense(probs.astype(jnp.bfloat16), g2 * sides[a])
        grad_q[lines, lanes] = (dq * HDIM ** (-0.5)).astype(jnp.bfloat16)
        dk = dk * HDIM ** (-0.5)

        @pl.when(part == 0)
        def _():
            totals[0, :, lanes] = dk
            totals[1, :, lanes] = dv

        @pl.when(part > 0)
        def _():
            totals[0, :, lanes] = totals[0, :, lanes] + dk
            totals[1, :, lanes] = totals[1, :, lanes] + dv

        pl.when(index == 0)(lambda: events(1))
        pl.when(index == 2)(lambda: events(2))
        return carry

    lax.fori_loop(0, 2 * width // (2 * HDIM), unit, 0)
    size = kv_landing.shape[1]
    other = pl.multiple_of((1 - col) * size, size)
    away = remote(totals.at[:, pl.ds(other, size)], kv_landing, ksend, krecv, (dp, row, 1 - col))
    away.start()
    out_scatter.wait()
    result = hidden[...]
    for q in range(sizes[1]):
        result = result + out_landing[q].astype(jnp.float32)
    output[...] = result.astype(jnp.bfloat16)
    away.wait()
    own = totals[:, pl.ds(pl.multiple_of(col * size, size), size)]
    grad_kv[...] = (own + kv_landing[...]).astype(jnp.bfloat16)
    lax.fori_loop(3, dps, lambda time, c: (events(time), c)[1], 0)
    term_shard[...] = slab(half, 0, dp, dps)[...]
    out_scatter.wait_send()
    gather.finish()
    reduce.finish()


def turn(sizes, prefix, queries, kv, grad_out, log_sums, out_part, hidden, shards, term):
    tokens, width = queries.shape
    dps, rows, cols = sizes
    low, wide = jnp.bfloat16, jnp.float32
    shape = jax.ShapeDtypeStruct

    def grown(shard, dim):
        full = list(shard.shape)
        full[dim] *= dps
        return tuple(full)

    firsts = [grown(s, d) for s, d in zip(shards, FIRST_DIMS)]
    half = halved(term.shape, 0, cols)
    return pl.pallas_call(
        functools.partial(turn_kernel, sizes),
        in_specs=[pl.BlockSpec(memory_space=pltpu.SMEM)] + [VMEM] * 10,
        out_specs=[VMEM] * 7,
        out_shape=[
            shape((tokens, width), low),
            shape((2, tokens, width), low),
            shape(hidden.shape, low),
        ]
        + [shape(s, low) for s in firsts]
        + [shape(halved(half, 0, dps), low)],
        scratch_shapes=[
            pltpu.VMEM(kv.shape, wide),
            pltpu.VMEM((2, tokens, width), wide),
            pltpu.VMEM((rows,) + hidden.shape, low),
        ]
        + [pltpu.VMEM(half, low)] * 4
        + plane_sems(sizes)
        + [DMA, DMA, DMA((1,)), DMA((1,))]
        + line_sems(sizes, 3, 3)
        + line_sems(sizes, 1, 4),
        compiler_params=pltpu.CompilerParams(collective_id=2, has_side_effects=True),
        name="turn",
    )(prefix, queries, kv, grad_out, log_sums, out_part, hidden, *shards, term)


def flat_picks(picks_head):
    blocks = picks_head.shape[0] // FBLK
    return jnp.swapaxes(picks_head.reshape(blocks, FBLK, TOPK), 1, 2).reshape(blocks, TOPK * FBLK)


def one_hot(row_values, size):
    hot = lax.broadcasted_iota(jnp.int32, (size, row_values.shape[1]), 0) == row_values
    return jnp.where(hot, 1.0, 0.0).astype(jnp.bfloat16)


def route_block(picks, rows_dev, owners, cap):
    lane = lax.broadcasted_iota(jnp.int32, (FBLK, FBLK), 0)
    before = jnp.where(lane < lax.broadcasted_iota(jnp.int32, (FBLK, FBLK), 1), 1.0, 0.0).astype(
        jnp.bfloat16
    )
    owner = picks // rows_dev
    local = picks % rows_dev
    hot = one_hot(owner, owners)
    running = jnp.zeros((owners, 1), jnp.float32)
    ranks = []
    for chunk in range(picks.shape[1] // FBLK):
        part = hot[:, chunk * FBLK : (chunk + 1) * FBLK]
        earlier = jnp.dot(part, before, preferred_element_type=jnp.float32)
        wide = part.astype(jnp.float32)
        ranks.append(jnp.sum(wide * (earlier + running), axis=0, keepdims=True))
        running = running + jnp.sum(wide, axis=1, keepdims=True)
    rank = jnp.concatenate(ranks, axis=1).astype(jnp.int32)
    slot_hot = one_hot(rank, cap)
    token = lax.broadcasted_iota(jnp.int32, picks.shape, 1) % FBLK
    outs = []
    for payload in (local % SUBKEYS, local // SUBKEYS, token):
        scaled = hot * payload.astype(jnp.float32).astype(jnp.bfloat16)
        outs.append(
            lax.dot_general(
                scaled, slot_hot, (((1,), (1,)), ((), ())), preferred_element_type=jnp.float32
            ).astype(jnp.int32)
        )
    return rank, (outs[1] * FBLK + outs[2]) * SUBKEYS + outs[0]


def pick_rows(table, index):
    inner = index % 8
    outer = index // 8
    result = jnp.zeros(index.shape, jnp.float32)
    for group in range(SUBKEYS // 8):
        rows = table[group * 8 : (group + 1) * 8]
        found = [
            jnp.take_along_axis(rows, inner[n * 8 : (n + 1) * 8], axis=0)
            for n in range(index.shape[0] // 8)
        ]
        result = jnp.where(outer == group, jnp.concatenate(found, axis=0), result)
    return result


def weigh_kernel(
    rows_dev, owners, cap, query_ref, keys_ref, picks_ref, square_ref, rank_ref, weights_ref, slots_ref
):
    picks = picks_ref[0]
    square = square_ref[0]
    first = lax.dot_general(
        keys_ref[0], query_ref[:, :HALF], (((1,), (1,)), ((), ())), preferred_element_type=jnp.float32
    )
    second = lax.dot_general(
        keys_ref[1], query_ref[:, HALF:], (((1,), (1,)), ((), ())), preferred_element_type=jnp.float32
    )
    scores = pick_rows(first, square // SUBKEYS) + pick_rows(second, square % SUBKEYS)
    powers = jnp.exp(scores - jnp.max(scores, axis=0, keepdims=True))
    weights = powers / jnp.sum(powers, axis=0, keepdims=True)
    weights_ref[0] = weights
    flat = jnp.concatenate([weights[pick : pick + 1] for pick in range(TOPK)], axis=1)
    scaled = one_hot(picks // rows_dev, owners) * flat.astype(jnp.bfloat16)
    slots_ref[0] = lax.dot_general(
        one_hot(rank_ref[0], cap),
        scaled,
        (((1,), (1,)), ((), ())),
        preferred_element_type=jnp.float32,
    )


def weigh(query_rows, keys_head, flat, square, rank, rows_dev, owners, cap):
    blocks, count = flat.shape
    return pl.pallas_call(
        functools.partial(weigh_kernel, rows_dev, owners, cap),
        grid=(blocks,),
        in_specs=[
            pl.BlockSpec((FBLK, 2 * HALF), lambda i: (i, 0)),
            pl.BlockSpec((2, SUBKEYS, HALF), lambda i: (0, 0, 0)),
            pl.BlockSpec((1, 1, count), lambda i: (i, 0, 0)),
            pl.BlockSpec((1, TOPK, FBLK), lambda i: (i, 0, 0)),
            pl.BlockSpec((1, 1, count), lambda i: (i, 0, 0)),
        ],
        out_specs=[
            pl.BlockSpec((1, TOPK, FBLK), lambda i: (i, 0, 0)),
            pl.BlockSpec((1, cap, owners), lambda i: (i, 0, 0)),
        ],
        out_shape=[
            jax.ShapeDtypeStruct((blocks, TOPK, FBLK), jnp.float32),
            jax.ShapeDtypeStruct((blocks, cap, owners), jnp.float32),
        ],
        name="weigh",
    )(query_rows, keys_head, flat[:, None, :], square, rank)


def send_rows(spot, sizes, src, landing, send, recv):
    me = index_of(spot, sizes)

    def one(device):
        remote(src.at[index_of(device, sizes)], landing.at[me], send, recv, device).start()

    each_other(spot, sizes, one)
    landing[me] = src[me]


def all_rows(landing, sem):
    return arrived(landing.at[pl.ds(0, landing.shape[0] - 1)], sem)


def slot_row(sizes, table, dp, col, block):
    pieces = []
    for row in range(sizes[1]):
        index = (dp * sizes[1] + row) * sizes[2] + col
        pieces.append(table[index, pl.ds(block, 1), :])
    return jnp.concatenate(pieces, axis=1)


def nth_place(dp, q, dps):
    twice = 2 * jnp.minimum(dp, dps - 1 - dp)
    inside = q <= twice
    distance = jnp.where(inside, lax.div(q + 1, 2), q - lax.div(twice, 2))
    below = jnp.logical_or(
        jnp.logical_and(inside, lax.rem(q, 2) == 1),
        jnp.logical_and(jnp.logical_not(inside), dp > dps - 1 - dp),
    )
    return dp + jnp.where(below, -distance, distance), below


def plane_neighbours(row, rows):
    across = row + 1 - 2 * lax.rem(row, 2)
    along = lax.rem(row + rows // 2, rows)
    return across, along, lax.rem(across + rows // 2, rows)


RING = 3


def memory_kernel(
    sizes, blocks, grads, meta, slots, values,
    grads_all, table, other_part, memory, back,
    meta_in, slots_in, values_t, tables, parts,
    chunks, found, sums, grids, theirs, acc, first_land, side_land, deep_land, total,
    msend, mrecv, ssend, srecv, zup, zdown, zrecv, wsend, wrecv, csend, crecv,
    local, tsem, qsend, qrecv,
    gsem, esem, hsend, hrecv, xsend, xrecv, dsend, drecv, fsend, frecv, flocal,
):
    spot = here()
    dp, row, col = spot
    dps, rows, cols = sizes
    tokens, width = grads.shape
    half = tokens // 2
    areas = values.shape[0] // SUBKEYS
    count = dps * rows * cols
    me = index_of(spot, sizes)
    across, along, opposite = plane_neighbours(row, rows)
    first_half, second_half = pl.ds(0, half), pl.ds(half, half)
    greet_all(spot, sizes)
    send_rows(spot, sizes, meta, meta_in, msend, mrecv)
    send_rows(spot, sizes, slots, slots_in, ssend, srecv)

    def place_of(u):
        return nth_place(dp, dps - 1 - u, dps)[0]

    def block_at(place, r, lines=slice(None)):
        return grads_all.at[place, col, r, lines]

    def cross(q, place, r, src=None):
        there = block_at(place, r)
        remote(there if src is None else src, there, csend, crecv.at[q], (dp, row, 1 - col)).start()

    def line_copy(place, up, src=None):
        there = block_at(place, row)
        return remote(
            there if src is None else src,
            there,
            (zup if up else zdown).at[place],
            zrecv.at[place],
            (jnp.clip(dp + (1 if up else -1), 0, dps - 1), row, col),
        )

    def sideways(q, place, src=None):
        there = block_at(place, row)
        for n, r in enumerate((across, along)):
            remote(
                there if src is None else src, there, wsend, wrecv.at[q, n], (dp, r, col)
            ).start()

    pl.when(dp < dps - 1)(lambda: line_copy(dp, True, grads).start())
    pl.when(dp > 0)(lambda: line_copy(dp, False, grads).start())
    sideways(0, dp, grads)
    cross(0, dp, row, grads)
    keep = pltpu.make_async_copy(grads, block_at(dp, row), local)
    keep.start()

    def from_line(q):
        place, below = nth_place(dp, q, dps)
        arrived(block_at(place, row), zrecv.at[place])
        pl.when(jnp.logical_and(below, dp < dps - 1))(lambda: line_copy(place, True).start())
        pl.when(jnp.logical_and(jnp.logical_not(below), dp > 0))(
            lambda: line_copy(place, False).start()
        )
        sideways(q, place)
        cross(q, place, row)

    def from_sides(q):
        place, _ = nth_place(dp, q, dps)
        for n, (r, other, lines) in enumerate(
            ((across, along, first_half), (along, across, second_half))
        ):
            arrived(block_at(place, r), wrecv.at[q, n])
            half = block_at(place, r, lines)
            remote(half, half, wsend, wrecv.at[q, 2 + n], (dp, other, col)).start()
            cross(q, place, r)

    def from_opposite(q):
        place, _ = nth_place(dp, q, dps)
        for n, lines in enumerate((first_half, second_half)):
            arrived(block_at(place, opposite, lines), wrecv.at[q, 2 + n])
        cross(q, place, opposite)

    def turn_rows(n, carry):
        lines = pl.ds(pl.multiple_of(n * 256, 256), 256)
        values_t[:, lines] = values[lines].T
        return carry

    lax.fori_loop(0, values.shape[0] // 256, turn_rows, 0)
    all_rows(meta_in, mrecv)
    all_rows(slots_in, srecv)

    def write_places(chunk):
        turn = lax.div(chunk, 2)
        slot = lax.rem(chunk, 2)
        return turn, slot, place_of(turn), jnp.where(slot == 0, 1 - col, col)

    def table_copy(chunk):
        _, slot, source_dp, source_col = write_places(chunk)
        return pltpu.make_async_copy(
            tables.at[slot], table.at[source_dp, source_col], tsem.at[slot]
        )

    def build(chunk):
        turn, slot, source_dp, source_col = write_places(chunk)
        pl.when(turn > 0)(lambda: table_copy(chunk).wait())
        def one(block, carry):
            row_meta = slot_row(sizes, meta_in, source_dp, source_col, block)
            key = row_meta // SUBKEYS
            low = row_meta % SUBKEYS
            weight = slot_row(sizes, slots_in, source_dp, source_col, block)
            at_key = lax.broadcasted_iota(jnp.int32, (areas * FBLK, key.shape[1]), 0) == key
            left = jnp.where(at_key, weight, 0.0).astype(jnp.bfloat16)
            stacked = lax.dot_general(
                left,
                one_hot(low, SUBKEYS),
                (((1,), (1,)), ((), ())),
                preferred_element_type=jnp.float32,
            ).astype(jnp.bfloat16)
            for area in range(areas):
                tables[
                    slot,
                    pl.ds(pl.multiple_of(block * FBLK, FBLK), FBLK),
                    area * SUBKEYS : (area + 1) * SUBKEYS,
                ] = stacked[area * FBLK : (area + 1) * FBLK]
            return carry

        lax.fori_loop(0, blocks, one, 0)
        table_copy(chunk).start()

    def away(turn, source_dp):
        return remote(parts.at[0], other_part.at[source_dp], qsend, qrecv.at[turn], (dp, row, 1 - col))

    def multiply(chunk):
        turn, slot, source_dp, _ = write_places(chunk)
        later = turn > 0
        pl.when(jnp.logical_and(later, slot == 0))(lambda: away(turn, source_dp).wait_send())

        def strip(n, carry):
            columns = pl.ds(pl.multiple_of(n * 512, 512), 512)
            parts[slot, :, columns] = jnp.dot(
                tables[slot], values[:, columns], preferred_element_type=jnp.float32
            ).astype(jnp.bfloat16)
            return carry

        lax.fori_loop(0, values.shape[1] // 512, strip, 0)
        pl.when(slot == 0)(lambda: away(turn, source_dp).start())

    def load_part(u):
        return pltpu.make_async_copy(other_part.at[place_of(u)], theirs, esem)

    def strip(u, r, lines=slice(None)):
        return acc.at[lax.rem(u, RING), lines, pl.ds(pl.multiple_of(r * width, width), width)]

    lines_of = (pl.ds(0, half), pl.ds(half, half))

    def halves(u):
        return [
            remote(
                strip(u, opposite, lines_of[n]), first_land.at[u, n],
                hsend.at[lax.rem(u, RING), n], hrecv.at[u, n], (dp, r, col),
            )
            for n, r in enumerate((across, along))
        ]

    def wholes(u):
        return [
            remote(
                strip(u, r), side_land.at[u, n],
                xsend.at[lax.rem(u, RING), n], xrecv.at[u, n], (dp, r, col),
            )
            for n, r in enumerate((across, along))
        ]

    def sent(u):
        for copy in halves(u) + wholes(u):
            copy.wait_send()

    def fetch(u):
        arrived(other_part.at[place_of(u)], qrecv.at[u])
        load_part(u).start()

    def combine(u):
        pl.when(u >= RING)(lambda: sent(u - RING))
        load_part(u).wait()
        acc[lax.rem(u, RING)] = (
            parts[1].astype(jnp.float32) + theirs[...].astype(jnp.float32)
        ).astype(jnp.bfloat16)
        for copy in halves(u):
            copy.start()

    def relay(u):
        for n, r in enumerate((along, across)):
            arrived(first_land.at[u, n], hrecv.at[u, n])
            add_into(strip(u, r, lines_of[n]), first_land.at[u, n])
        for copy in wholes(u):
            copy.start()

    def deep_copy(u):
        place = place_of(u)
        up = place > dp
        target = jnp.where(up, dp + 1, dp - 1)
        there = jnp.where(jnp.logical_and(jnp.logical_not(up), target == place), dps, place)
        return remote(
            total.at[u], deep_land.at[there], dsend.at[u], drecv.at[there],
            (jnp.clip(target, 0, dps - 1), row, col),
        )

    def finish(u):
        for n in range(2):
            arrived(side_land.at[u, n], xrecv.at[u, n])
        place = place_of(u)
        result = (
            strip(u, row)[...].astype(jnp.float32)
            + side_land[u, 0].astype(jnp.float32)
            + side_land[u, 1].astype(jnp.float32)
        )
        memory[...] = result

        def more(index):
            arrived(deep_land.at[index], drecv.at[index])
            memory[...] = memory[...] + deep_land[index].astype(jnp.float32)

        below = jnp.logical_and(place >= dp, dp > 0)
        above = jnp.logical_and(place <= dp, dp < dps - 1)
        pl.when(jnp.logical_or(below, jnp.logical_and(above, place < dp)))(lambda: more(place))
        pl.when(jnp.logical_and(above, place == dp))(lambda: more(dps))

        @pl.when(u < dps - 1)
        def _():
            total[u] = memory[...].astype(jnp.bfloat16)
            deep_copy(u).start()

    def read_places(chunk):
        slot = lax.rem(chunk, 2)
        place = nth_place(dp, lax.div(chunk, 2), dps)[0]
        return slot, place, jnp.where(slot == 0, col, 1 - col)

    def load_chunk(chunk):
        slot, source_dp, source_col = read_places(chunk)
        return [
            pltpu.make_async_copy(
                grads_all.at[source_dp, source_col, r],
                chunks.at[slot, :, pl.ds(r * width, width)],
                gsem.at[slot, r],
            )
            for r in range(rows)
        ]

    def start_chunk(chunk):
        slot, source_dp, source_col = read_places(chunk)

        @pl.when(slot == 1)
        def _():
            arrived(grads_all.at[source_dp, source_col], crecv.at[lax.div(chunk, 2)])

        for copy in load_chunk(chunk):
            copy.start()

    wide_strip = min(2048, areas * SUBKEYS)
    per_strip = wide_strip // SUBKEYS

    def search(chunk, part):
        slot, source_dp, source_col = read_places(chunk)

        @pl.when(part == 0)
        def _():
            for copy in load_chunk(chunk):
                copy.wait()

            def strip(n, carry):
                columns = pl.ds(pl.multiple_of(n * wide_strip, wide_strip), wide_strip)
                grid = jnp.dot(
                    chunks[slot], values_t[:, columns], preferred_element_type=jnp.float32
                ).astype(jnp.bfloat16)
                for area in range(per_strip):
                    grids[n * per_strip + area] = grid[:, area * SUBKEYS : (area + 1) * SUBKEYS]
                return carry

            lax.fori_loop(0, areas // per_strip, strip, 0)

            @pl.when(chunk + 2 < dps * cols)
            def _():
                start_chunk(chunk + 2)

        @pl.when(part == 1)
        def _():
            def one(block, carry):
                row_meta = slot_row(sizes, meta_in, source_dp, source_col, block)
                lines = pl.ds(pl.multiple_of(block * FBLK, FBLK), FBLK)
                stacked = grids[:, lines, :].reshape(areas * FBLK, SUBKEYS)
                product = jnp.dot(
                    stacked, one_hot(row_meta % SUBKEYS, SUBKEYS), preferred_element_type=jnp.float32
                )
                spot_id = lax.broadcasted_iota(jnp.int32, product.shape, 0)
                sums[block] = jnp.sum(
                    jnp.where(spot_id == row_meta // SUBKEYS, product, 0.0), axis=0, keepdims=True
                )
                return carry

            lax.fori_loop(0, blocks, one, 0)

            for r in range(rows):
                index = (source_dp * rows + r) * cols + source_col
                for block in range(blocks):
                    found[index, block : block + 1, :] = sums[block, :, r * 128 : (r + 1) * 128]
                away = remote(found.at[index], back.at[me], fsend, frecv, (source_dp, r, source_col))
                own = jnp.logical_and(
                    jnp.logical_and(source_dp == dp, row == r), source_col == col
                )
                pl.when(jnp.logical_not(own))(away.start)
                pl.when(own)(pltpu.make_async_copy(found.at[index], back.at[me], flocal).start)

    writes = 4 * dps

    def poll(p, carry):
        phase = lax.rem(p, 2)
        writing = p < writes
        pl.when(jnp.logical_and(writing, phase == 0))(lambda: build(lax.div(p, 2)))
        pl.when(jnp.logical_and(writing, phase == 1))(lambda: multiply(lax.div(p, 2)))

        @pl.when(p == writes)
        def _():
            keep.wait()
            start_chunk(0)
            start_chunk(1)

        pl.when(p >= writes)(lambda: search(lax.div(p - writes, 2), phase))
        turn, third = lax.div(p, 3), lax.rem(p, 3)
        pl.when(jnp.logical_and(third == 2, turn + 1 < dps))(lambda: from_line(turn + 1))
        for event, delay in ((from_sides, 1), (from_opposite, 2)):
            now = jnp.logical_and(turn >= delay, turn < dps + delay)
            pl.when(jnp.logical_and(third == 0, now))(functools.partial(event, turn - delay))
        for event, delay in ((finish, FINISH_AT), (relay, RELAY_AT), (combine, COMBINE_AT), (fetch, FETCH_AT)):
            late = p - delay
            now = jnp.logical_and(
                jnp.logical_and(late >= 0, lax.rem(late, 4) == 0), late < 4 * dps
            )
            pl.when(now)(functools.partial(event, lax.div(late, 4)))
        return carry

    lax.fori_loop(0, 8 * dps, poll, 0)
    for slot in range(2):
        pltpu.make_async_copy(tables.at[slot], table.at[0, 0], tsem.at[slot]).wait()
    away(0, 0).wait_send()
    arrived(grads_all.at[:, 0], csend)
    arrived(grads_all.at[:, 0, pl.ds(0, rows - 1)], wsend)
    all_rows(meta_in, msend)
    all_rows(slots_in, ssend)

    def line_sent(k, carry):
        pl.when(jnp.logical_and(k <= dp, dp < dps - 1))(lambda: line_copy(k, True).wait_send())
        pl.when(jnp.logical_and(k >= dp, dp > 0))(lambda: line_copy(k, False).wait_send())
        return carry

    lax.fori_loop(0, dps, line_sent, 0)
    arrived(back.at[pl.ds(0, count - 1)], frecv)
    arrived(back.at[0], flocal)
    arrived(back.at[pl.ds(0, count - 1)], fsend)
    for u in range(max(0, dps - RING), dps):
        sent(u)
    lax.fori_loop(0, dps - 1, lambda u, c: (deep_copy(u).wait_send(), c)[1], 0)


FETCH_AT, COMBINE_AT, RELAY_AT, FINISH_AT = 5, 6, 10, 16


def use_memory(sizes, grads, meta, slots, values):
    dps, rows, cols = sizes
    tokens, width = grads.shape
    rows_dev, features = values.shape
    blocks = tokens // FBLK
    count = dps * rows * cols
    low, wide = jnp.bfloat16, jnp.float32
    shape = jax.ShapeDtypeStruct
    grads_all, table, _, memory, back = pl.pallas_call(
        functools.partial(memory_kernel, sizes, blocks),
        in_specs=[VMEM] * 4,
        out_specs=[ANY] * 3 + [VMEM] * 2,
        out_shape=[
            shape((dps, cols, rows, tokens, width), low),
            shape((dps, cols, tokens, rows_dev), low),
            shape((dps, tokens, features), low),
            shape((tokens, width), wide),
            shape((count, blocks, 128), wide),
        ],
        scratch_shapes=[
            pltpu.VMEM(meta.shape, meta.dtype),
            pltpu.VMEM(slots.shape, slots.dtype),
            pltpu.VMEM((features, rows_dev), low),
            pltpu.VMEM((2, tokens, rows_dev), low),
            pltpu.VMEM((2, tokens, features), low),
            pltpu.VMEM((2, tokens, features), low),
            pltpu.VMEM((count, blocks, 128), wide),
            pltpu.VMEM((blocks, 1, rows * 128), wide),
            pltpu.VMEM((rows_dev // SUBKEYS, tokens, SUBKEYS), low),
            pltpu.VMEM((tokens, features), low),
            pltpu.VMEM((RING, tokens, features), low),
            pltpu.VMEM((dps, 2, tokens // 2, width), low),
            pltpu.VMEM((dps, 2, tokens, width), low),
            pltpu.VMEM((dps + 1, tokens, width), low),
            pltpu.VMEM((dps, tokens, width), low),
            DMA, DMA, DMA, DMA,
            DMA((dps,)), DMA((dps,)), DMA((dps,)),
            DMA, DMA((dps, 4)),
            DMA, DMA((dps,)),
            DMA, DMA((2,)), DMA, DMA((dps,)),
            DMA((2, rows)), DMA,
            DMA((RING, 2)), DMA((dps, 2)),
            DMA((RING, 2)), DMA((dps, 2)),
            DMA((dps,)), DMA((dps + 1,)),
            DMA, DMA, DMA,
        ],
        compiler_params=pltpu.CompilerParams(collective_id=6, has_side_effects=True),
        name="use_memory",
    )(grads, meta, slots, values)
    return grads_all, table, memory, back


def unweigh_kernel(rows_dev, owners, back_ref, picks_ref, rank_ref, weights_ref, first_ref, second_ref):
    picks = picks_ref[0]
    hot = one_hot(picks // rows_dev, owners)
    back = back_ref[0]
    high = back.astype(jnp.bfloat16)
    rest = back - high.astype(jnp.float32)
    middle = rest.astype(jnp.bfloat16)
    lowest = (rest - middle.astype(jnp.float32)).astype(jnp.bfloat16)
    spread_back = (
        jnp.dot(high, hot, preferred_element_type=jnp.float32)
        + jnp.dot(middle, hot, preferred_element_type=jnp.float32)
        + jnp.dot(lowest, hot, preferred_element_type=jnp.float32)
    )
    slot = lax.broadcasted_iota(jnp.int32, spread_back.shape, 0)
    flat = jnp.sum(jnp.where(slot == rank_ref[0], spread_back, 0.0), axis=0, keepdims=True)
    grads = jnp.concatenate(
        [flat[:, pick * FBLK : (pick + 1) * FBLK] for pick in range(TOPK)], axis=0
    )
    weights = weights_ref[0]
    grads = weights * (grads - jnp.sum(weights * grads, axis=0, keepdims=True))
    upper = picks // SUBKEYS
    lower = picks % SUBKEYS
    tile = 64

    def some_keys(index, carry):
        lines = pl.ds(pl.multiple_of(index * tile, tile), tile)
        key_id = lax.broadcasted_iota(jnp.int32, (tile, FBLK), 0) + index * tile
        first = jnp.zeros((tile, FBLK), jnp.float32)
        second = jnp.zeros((tile, FBLK), jnp.float32)
        for pick in range(TOPK):
            columns = slice(pick * FBLK, (pick + 1) * FBLK)
            value = grads[pick : pick + 1]
            first = first + jnp.where(key_id == upper[:, columns], value, 0.0)
            second = second + jnp.where(key_id == lower[:, columns], value, 0.0)
        first_ref[lines] = first.astype(jnp.bfloat16)
        second_ref[lines] = second.astype(jnp.bfloat16)
        return carry

    lax.fori_loop(0, SUBKEYS // tile, some_keys, 0)


def unweigh(back, flat, rank, weights, rows_dev, owners):
    blocks, count = flat.shape
    cap = back.shape[1]
    return pl.pallas_call(
        functools.partial(unweigh_kernel, rows_dev, owners),
        grid=(blocks,),
        in_specs=[
            pl.BlockSpec((1, cap, owners), lambda i: (i, 0, 0)),
            pl.BlockSpec((1, 1, count), lambda i: (i, 0, 0)),
            pl.BlockSpec((1, 1, count), lambda i: (i, 0, 0)),
            pl.BlockSpec((1, TOPK, FBLK), lambda i: (i, 0, 0)),
        ],
        out_specs=[
            pl.BlockSpec((SUBKEYS, FBLK), lambda i: (0, i)),
            pl.BlockSpec((SUBKEYS, FBLK), lambda i: (0, i)),
        ],
        out_shape=[jax.ShapeDtypeStruct((SUBKEYS, blocks * FBLK), jnp.bfloat16)] * 2,
        name="unweigh",
    )(back, flat[:, None, :], rank, weights)


def memory_all(query_rows, grad_memory, flat, rank, meta, subkeys, values):
    sizes = grid_sizes()
    owners = sizes[0] * sizes[1] * sizes[2]
    rows_dev = values.shape[0]
    cap = FBLK * TOPK // owners
    head_id = lax.axis_index("row")
    keys_head = lax.dynamic_index_in_dim(subkeys, head_id, 0, keepdims=False)
    square = flat.reshape(-1, TOPK, FBLK)
    weights, slots = weigh(query_rows, keys_head, flat, square, rank, rows_dev, owners, cap)
    spare = ((0, 0), (0, 0), (0, 128 - cap))
    meta = jnp.pad(jnp.swapaxes(meta, 0, 1), spare, constant_values=-1)
    slots = jnp.pad(jnp.transpose(slots, (2, 0, 1)), spare)
    grads_all, table, memory, back = use_memory(
        sizes, grad_memory, meta, slots, values
    )
    first_t, second_t = unweigh(
        jnp.transpose(back, (1, 2, 0))[:, :cap], flat, rank, weights, rows_dev, owners
    )
    grad_query = jnp.concatenate(
        [
            lax.dot_general(
                part, keys_head[i], (((0,), (0,)), ((), ())), preferred_element_type=jnp.float32
            )
            for i, part in enumerate((first_t, second_t))
        ],
        axis=1,
    ).astype(jnp.bfloat16)
    grad_keys = jnp.stack(
        [
            jnp.dot(first_t, query_rows[:, :HALF], preferred_element_type=jnp.float32),
            jnp.dot(second_t, query_rows[:, HALF:], preferred_element_type=jnp.float32),
        ]
    )
    return memory, grad_query, grad_keys, table, grads_all


def dense(left, right):
    return jnp.dot(left, right, preferred_element_type=jnp.float32)


def dense_nt(left, right):
    return lax.dot_general(left, right, (((1,), (1,)), ((), ())), preferred_element_type=jnp.float32)


def dense_tn(left, right):
    return lax.dot_general(left, right, (((0,), (0,)), ((), ())), preferred_element_type=jnp.float32)


def per_device(
    inputs,
    prefix,
    picks,
    gain_attn,
    w_qkv,
    w_attn_out,
    gain_mem,
    w_query,
    w_gate,
    w_proj,
    subkeys,
    values,
    cotangent,
):
    low = jnp.bfloat16
    sizes = grid_sizes()
    width_part = inputs.shape[1]
    col = lax.axis_index("col")
    col_first = col * width_part
    gain_one = lax.dynamic_slice_in_dim(gain_attn, col_first, width_part)
    gain_two = lax.dynamic_slice_in_dim(gain_mem, col_first, width_part)

    flat = flat_picks(lax.dynamic_index_in_dim(picks, lax.axis_index("row"), 1, keepdims=False))
    x_own, qkv_w, query_w, gate_w, proj_w, attn_w, rank, meta = start_all(
        sizes, values.shape[0], inputs, w_qkv, w_query, w_gate, w_proj, w_attn_out, flat
    )
    residual = x_own.astype(jnp.float32)
    scale_one = lax.rsqrt(jnp.sum(residual * residual, axis=1, keepdims=True) / D + EPSILON)
    normed_one = (residual * scale_one * gain_attn.astype(jnp.float32)).astype(low)
    qkv = jnp.einsum("tc,jcf->jtf", normed_one, qkv_w, preferred_element_type=jnp.float32).astype(low)
    attended, log_sums, kv_all, dy_own = attend(sizes, prefix, qkv, cotangent)
    hidden, normed_two = join(sizes, dense(attended, attn_w).astype(low), inputs, gain_two)
    query_rows = dense(normed_two, query_w).astype(low)
    gate_value = dense(normed_two, gate_w)
    sigmoid_gate = jax.nn.sigmoid(gate_value)
    silu_gate = gate_value * sigmoid_gate
    grad_gated = dense_nt(dy_own, proj_w)
    grad_memory = (grad_gated * silu_gate).astype(low)
    memory, grad_query, grad_keys, table, grads_all = memory_all(
        query_rows, grad_memory, flat, rank, meta, subkeys, values
    )
    gated_value = (memory * silu_gate).astype(low)
    out_part = dense(gated_value, proj_w).astype(low)
    grad_gate = (
        grad_gated * memory * sigmoid_gate * (1.0 + gate_value * (1.0 - sigmoid_gate))
    ).astype(low)
    grad_part = (dense_nt(grad_query, query_w) + dense_nt(grad_gate, gate_w)).astype(low)
    query_term = dense_tn(normed_two, grad_query).astype(low)
    first_terms = [
        dense_tn(normed_two, grad_gate).astype(low),
        dense_tn(gated_value, dy_own).astype(low),
        grad_keys.reshape(-1, HALF).astype(low),
    ]
    grad_hidden, grad_hidden_all, gain_two_grad, *shards = middle(
        sizes, grad_part, hidden, cotangent, gain_two, first_terms
    )
    grad_attended = dense_nt(grad_hidden_all, attn_w).astype(low)
    grad_q, grad_kv, output, grad_w_gate, grad_w_proj, grad_keys_half, query_shard = turn(
        sizes, prefix, qkv[0], kv_all, grad_attended, log_sums, out_part, hidden, shards, query_term
    )
    x_part = (
        dense_nt(grad_q, qkv_w[0]) + dense_nt(grad_kv[0], qkv_w[1]) + dense_nt(grad_kv[1], qkv_w[2])
    ).astype(low)
    last_terms = [
        jnp.stack([dense_tn(normed_one, part) for part in (grad_q, grad_kv[0], grad_kv[1])]).astype(low),
        dense_tn(attended, grad_hidden_all).astype(low),
    ]
    (
        grad_inputs, gain_sums, grad_values, grad_w_query, grad_w_qkv, grad_w_attn_out, grad_subkeys,
    ) = last(
        sizes, x_part, inputs, grad_hidden, gain_one, gain_two_grad, grad_keys_half, query_shard,
        last_terms, table, grads_all,
    )
    gain_rows = gain_sums.reshape(sizes[2], 2, width_part)
    grad_gain_one = gain_rows[:, 0].reshape(-1)
    grad_gain_two = gain_rows[:, 1].reshape(-1)

    return (
        output,
        grad_inputs,
        grad_gain_one,
        grad_w_qkv.astype(jnp.float32),
        grad_w_attn_out.astype(jnp.float32),
        grad_gain_two,
        grad_w_query.astype(jnp.float32),
        grad_w_gate.astype(jnp.float32),
        grad_w_proj.astype(jnp.float32),
        grad_subkeys.astype(jnp.float32),
        grad_values.astype(jnp.float32),
    )


def solution(mesh):
    placed = (
        P(("dp", "row"), "col"),
        P("dp"),
        P(("dp", "col"), None, None),
        P(),
        P(None, "col", "row"),
        P("row", "col"),
        P(),
        P("col", "row"),
        P("col", "row"),
        P("row", "col"),
        P(),
        P(("dp", "row", "col"), None),
        P(("dp", "row"), "col"),
    )
    return jax.shard_map(
        per_device,
        mesh=mesh,
        in_specs=placed,
        out_specs=(
            P(("dp", "row"), "col"),
            P(("dp", "row"), "col"),
            P(),
            P(None, "col", "row"),
            P("row", "col"),
            P(),
            P("col", "row"),
            P("col", "row"),
            P("row", "col"),
            P(),
            P(("dp", "row", "col"), None),
        ),
        check_vma=False,
    )
```

```python
import functools

import jax
import jax.numpy as jnp
from jax import lax
from jax.experimental import pallas as pl
from jax.experimental.pallas import tpu as pltpu
from jax.sharding import PartitionSpec as P

D = 1024
HDIM = 64
HALF = 512
SUBKEYS = 256
TOPK = 32
FBLK = 128


EPSILON = 1e-06


MESH = pl.DeviceIdType.MESH
VMEM = pl.BlockSpec(memory_space=pltpu.VMEM)
ANY = pl.BlockSpec(memory_space=pl.ANY)
DMA = pltpu.SemaphoreType.DMA


def here():
    return lax.axis_index("dp"), lax.axis_index("row"), lax.axis_index("col")


def grid_sizes():
    return lax.axis_size("dp"), lax.axis_size("row"), lax.axis_size("col")


def remote(src, dst, send_sem, recv_sem, device):
    return pltpu.make_async_remote_copy(
        src_ref=src,
        dst_ref=dst,
        send_sem=send_sem,
        recv_sem=recv_sem,
        device_id=device,
        device_id_type=MESH,
    )


def arrived(dst, sem):
    pltpu.make_async_copy(dst, dst, sem).wait()


def greet_plane(spot, sizes):
    barrier = pltpu.get_barrier_semaphore()
    dp, row, col = spot
    _, rows, cols = sizes
    for j in range(rows):
        for k in range(cols):
            if j + k > 0:
                pl.semaphore_signal(
                    barrier,
                    inc=1,
                    device_id=(dp, lax.rem(row + j, rows), lax.rem(col + k, cols)),
                    device_id_type=MESH,
                )
    pl.semaphore_wait(barrier, rows * cols - 1)


def greet_partner(spot, sizes):
    barrier = pltpu.get_barrier_semaphore()
    dp, row, col = spot
    pl.semaphore_signal(barrier, inc=1, device_id=(dp, row, 1 - col), device_id_type=MESH)
    pl.semaphore_wait(barrier, 1)


def index_of(spot, sizes):
    return (spot[0] * sizes[1] + spot[1]) * sizes[2] + spot[2]


def each_other(spot, sizes, action):
    dp, row, col = spot
    dps, rows, cols = sizes

    def level(step, carry):
        there = lax.rem(dp + step, dps)
        for j in range(rows):
            for k in range(cols):
                device = (there, lax.rem(row + j, rows), lax.rem(col + k, cols))
                if j + k > 0:
                    action(device)
                else:
                    pl.when(step > 0)(functools.partial(action, device))
        return carry

    lax.fori_loop(0, dps, level, 0)


def greet_all(spot, sizes):
    barrier = pltpu.get_barrier_semaphore()

    def greet(device):
        pl.semaphore_signal(barrier, inc=1, device_id=device, device_id_type=MESH)

    each_other(spot, sizes, greet)
    pl.semaphore_wait(barrier, sizes[0] * sizes[1] * sizes[2] - 1)


class Gather:
    def __init__(self, spot, sizes, src, dst, send, recv):
        self.spot, self.sizes, self.src, self.dst = spot, sizes, src, dst
        self.send, self.recv = send, recv
        self.tokens, self.width = src.shape
        dp, row, col = spot
        _, rows, cols = sizes
        self.half = rows // cols
        self.target = lax.div(row, self.half)
        self.slot = lax.rem(row, self.half) * cols + col
        first = pl.multiple_of(lax.rem(row, self.half) * self.tokens, self.tokens)
        left = pl.multiple_of(col * self.width, self.width)
        self.there = dst.at[pl.ds(first, self.tokens), pl.ds(left, self.width)]

    def copy(self, step):
        dp, row, _ = self.spot
        device = (dp, lax.rem(row + step, self.sizes[1]), self.target)
        return remote(self.src, self.there, self.send.at[step], self.recv.at[self.slot], device)

    def start(self):
        col = self.spot[2]

        for step in range(1, self.sizes[1]):
            self.copy(step).start()

        @pl.when(self.target == col)
        def _():
            pltpu.make_async_copy(self.src, self.there, self.recv.at[self.slot]).start()

        @pl.when(self.target != col)
        def _():
            self.copy(0).start()

    def wait(self):
        cols = self.sizes[2]
        for i in range(self.half):
            for k in range(cols):
                arrived(
                    self.dst.at[pl.ds(i * self.tokens, self.tokens), pl.ds(k * self.width, self.width)],
                    self.recv.at[i * cols + k],
                )
        for step in range(1, self.sizes[1]):
            self.copy(step).wait_send()

        @pl.when(self.target != self.spot[2])
        def _():
            self.copy(0).wait_send()


class Scatter:
    def __init__(self, spot, sizes, src, landing, send, recv):
        self.spot, self.sizes, self.src, self.landing = spot, sizes, src, landing
        self.send, self.recv = send, recv
        _, self.tokens, self.width = landing.shape
        self.half = sizes[1] // sizes[2]

    def parts(self):
        dp, row, col = self.spot
        cols = self.sizes[2]
        for i in range(self.half):
            for k in range(cols):
                piece = self.src.at[
                    pl.ds(i * self.tokens, self.tokens), pl.ds(k * self.width, self.width)
                ]
                target = col * self.half + i
                mine = jnp.logical_and(target == row, col == k)
                there = self.landing.at[row]
                copy = remote(
                    piece, there, self.send.at[i * cols + k], self.recv.at[row], (dp, target, k)
                )
                yield mine, copy, pltpu.make_async_copy(piece, there, self.recv.at[row])

    def start(self):
        for mine, copy, own in self.parts():
            pl.when(jnp.logical_not(mine))(copy.start)
            pl.when(mine)(own.start)

    def wait(self):
        for q in range(self.sizes[1]):
            arrived(self.landing.at[q], self.recv.at[q])

    def wait_send(self):
        for mine, copy, _ in self.parts():
            pl.when(jnp.logical_not(mine))(copy.wait_send)


def plane_sems(sizes):
    rows, cols = sizes[1], sizes[2]
    return [DMA((rows,)), DMA((rows,))]


def start_kernel(sizes, rows_dev, *refs):
    x, wqkv, wquery, wgate, wproj, wattn, picks = refs[:7]
    xs, wqkv_all, wquery_all, wgate_all, wproj_all, wattn_all, rank, meta = refs[7:15]
    xsend, xrecv, wsend, wrecv, wlocal = refs[15:]
    spot = here()
    dp, row, col = spot
    greet_plane(spot, sizes)
    gather_x = Gather(spot, sizes, x, xs, xsend, xrecv)
    gather_x.start()
    copies = []
    for n, (src, dst, dim) in enumerate(
        (
            (wqkv, wqkv_all, 1),
            (wquery, wquery_all, 0),
            (wgate, wgate_all, 0),
            (wproj, wproj_all, 1),
            (wattn, wattn_all, 1),
        )
    ):
        size = src.shape[dim]
        window = [slice(None)] * len(src.shape)
        window[dim] = pl.ds(pl.multiple_of(col * size, size), size)
        there = dst.at[tuple(window)]
        away = remote(src, there, wsend.at[n], wrecv.at[n], (dp, row, 1 - col))
        own = pltpu.make_async_copy(src, there, wlocal.at[n])
        away.start()
        own.start()
        copies += [away, own]

    def one(block, carry):
        rank[block], meta[block] = route_block(
            picks[block], rows_dev, meta.shape[1], meta.shape[2]
        )
        return carry

    lax.fori_loop(0, picks.shape[0], one, 0)
    for copy in copies:
        copy.wait()
    gather_x.wait()


def start_all(sizes, rows_dev, x, wqkv, wquery, wgate, wproj, wattn, flat):
    tokens, width = x.shape
    half = sizes[1] // sizes[2]
    cols = sizes[2]
    low = jnp.bfloat16

    def twice(operand, dim):
        shape = list(operand.shape)
        shape[dim] *= cols
        return jax.ShapeDtypeStruct(tuple(shape), low)

    whole = jax.ShapeDtypeStruct((half * tokens, cols * width), low)
    blocks, count = flat.shape
    owners = sizes[0] * sizes[1] * sizes[2]
    return pl.pallas_call(
        functools.partial(start_kernel, sizes, rows_dev),
        in_specs=[VMEM] * 7,
        out_specs=[ANY] * 6 + [VMEM] * 2,
        out_shape=[
            whole,
            twice(wqkv, 1),
            twice(wquery, 0),
            twice(wgate, 0),
            twice(wproj, 1),
            twice(wattn, 1),
            jax.ShapeDtypeStruct((blocks, 1, count), jnp.int32),
            jax.ShapeDtypeStruct((blocks, owners, count // owners), jnp.int32),
        ],
        scratch_shapes=plane_sems(sizes) + [DMA((5,))] * 3,
        compiler_params=pltpu.CompilerParams(collective_id=0, has_side_effects=True),
        name="start_all",
    )(x, wqkv, wquery, wgate, wproj, wattn, flat[:, None])


def lane_sides():
    lane = lax.broadcasted_iota(jnp.int32, (1, 2 * HDIM), 1)
    return [
        jnp.where(jnp.logical_and(lane >= a * HDIM, lane < (a + 1) * HDIM), 1.0, 0.0).astype(
            jnp.bfloat16
        )
        for a in range(2)
    ]


def attend_kernel(
    sizes, prefix, qkv, dy, attended, log_sums, kv, dys, ysend, yrecv, send, recv, local
):
    spot = here()
    dp, row, col = spot
    greet_plane(spot, sizes)
    _, tokens, width = qkv.shape
    keys = kv.shape[1]
    tile = tokens // 2
    there = kv.at[:, pl.ds(pl.multiple_of(col * tokens, tokens), tokens)]
    away = remote(qkv.at[pl.ds(1, 2)], there, send, recv, (dp, row, 1 - col))
    home = pltpu.make_async_copy(qkv.at[pl.ds(1, 2)], there, local)
    away.start()
    home.start()
    gather = Gather(spot, sizes, dy, dys, ysend, yrecv)
    gather.start()
    limit = prefix[0]
    key_pos = lax.broadcasted_iota(jnp.int32, (keys, tile), 0)
    sides = lane_sides()
    away.wait()
    home.wait()

    def unit(index, carry):
        pair, part = lax.div(index, 2), lax.rem(index, 2)
        lanes = pl.ds(pl.multiple_of(pair * 2 * HDIM, 2 * HDIM), 2 * HDIM)
        lines = pl.ds(pl.multiple_of(part * tile, tile), tile)
        query_pos = col * tokens + part * tile + lax.broadcasted_iota(jnp.int32, (1, tile), 1)
        allowed = jnp.logical_or(key_pos <= query_pos, key_pos < limit)
        q2, k2, v2 = qkv[0, lines, lanes], kv[0, :, lanes], kv[1, :, lanes]
        total = jnp.zeros((tile, 2 * HDIM), jnp.float32)
        for a in range(2):
            scores = jnp.where(allowed, dense_nt(k2 * sides[a], q2) * HDIM ** (-0.5), -jnp.inf)
            peak = jnp.max(scores, axis=0, keepdims=True)
            powers = jnp.exp(scores - peak)
            power_sum = jnp.sum(powers, axis=0, keepdims=True)
            probs = (powers / power_sum).astype(jnp.bfloat16)
            total = total + dense_tn(probs, v2 * sides[a])
            log_sums[pl.ds(2 * pair + a, 1), lines] = peak + jnp.log(power_sum)
        attended[lines, lanes] = total.astype(jnp.bfloat16)
        return carry

    lax.fori_loop(0, 2 * width // (2 * HDIM), unit, 0)
    gather.wait()


def attend(sizes, prefix, qkv, dy):
    _, tokens, width = qkv.shape
    low, wide = jnp.bfloat16, jnp.float32
    shape = jax.ShapeDtypeStruct
    half = sizes[1] // sizes[2]
    return pl.pallas_call(
        functools.partial(attend_kernel, sizes),
        in_specs=[pl.BlockSpec(memory_space=pltpu.SMEM), VMEM, VMEM],
        out_specs=[VMEM, VMEM, VMEM, ANY],
        out_shape=[
            shape((tokens, width), low),
            shape((width // HDIM, tokens), wide),
            shape((2, tokens * sizes[2], width), low),
            shape((half * dy.shape[0], sizes[2] * dy.shape[1]), low),
        ],
        scratch_shapes=plane_sems(sizes) + [DMA, DMA, DMA],
        compiler_params=pltpu.CompilerParams(collective_id=1, has_side_effects=True),
        name="attend",
    )(prefix, qkv, dy)


def fold(column):
    return jnp.broadcast_to(column, (column.shape[0], 128))


def join_kernel(
    sizes, part, x, gain, hidden, normed_all, landing, mine, theirs, block,
    ssend, srecv, gsend, grecv, psend, precv,
):
    spot = here()
    dp, row, col = spot
    greet_plane(spot, sizes)
    scatter = Scatter(spot, sizes, part, landing, ssend, srecv)
    scatter.start()
    scatter.wait()
    total = x[...].astype(jnp.float32)
    for q in range(sizes[1]):
        total = total + landing[q].astype(jnp.float32)
    hidden[...] = total
    mine[...] = fold(jnp.sum(total * total, axis=1, keepdims=True))
    pair = remote(mine, theirs, psend, precv, (dp, row, 1 - col))
    pair.start()
    pair.wait()
    squares = mine[:, :1] + theirs[:, :1]
    scale = lax.rsqrt(squares / D + EPSILON)
    block[...] = (hidden[...] * scale * gain[...].astype(jnp.float32)).astype(jnp.bfloat16)
    gather = Gather(spot, sizes, block, normed_all, gsend, grecv)
    gather.start()
    scatter.wait_send()
    gather.wait()


def join(sizes, part, x, gain):
    tokens, width = x.shape
    rows = sizes[1]
    return pl.pallas_call(
        functools.partial(join_kernel, sizes),
        in_specs=[VMEM] * 3,
        out_specs=[VMEM, VMEM],
        out_shape=[
            jax.ShapeDtypeStruct((tokens, width), jnp.float32),
            jax.ShapeDtypeStruct(part.shape, jnp.bfloat16),
        ],
        scratch_shapes=[
            pltpu.VMEM((rows, tokens, width), jnp.bfloat16),
            pltpu.VMEM((tokens, 128), jnp.float32),
            pltpu.VMEM((tokens, 128), jnp.float32),
            pltpu.VMEM((tokens, width), jnp.bfloat16),
        ]
        + plane_sems(sizes) * 2
        + [DMA, DMA],
        compiler_params=pltpu.CompilerParams(collective_id=3, has_side_effects=True),
        name="join",
    )(part, x, gain[None])


def norm_back(sizes, spot, landing, base, above, gain, mine, theirs, psend, precv):
    dp, row, col = spot
    normed_grad = landing[0].astype(jnp.float32)
    for q in range(1, sizes[1]):
        normed_grad = normed_grad + landing[q].astype(jnp.float32)
    values = base[...].astype(jnp.float32)
    unit_grad = normed_grad * gain[...].astype(jnp.float32)
    mine[0] = fold(jnp.sum(values * values, axis=1, keepdims=True))
    mine[1] = fold(jnp.sum(unit_grad * values, axis=1, keepdims=True))
    pair = remote(mine, theirs, psend, precv, (dp, row, 1 - col))
    pair.start()
    pair.wait()
    scale = lax.rsqrt((mine[0, :, :1] + theirs[0, :, :1]) / D + EPSILON)
    inner = scale * (mine[1, :, :1] + theirs[1, :, :1]) / D
    unit = values * scale
    grad = above[...].astype(jnp.float32) + scale * (unit_grad - unit * inner)
    return grad, jnp.sum(normed_grad * unit, axis=0, keepdims=True)


def slab(ref, dim, index, count):
    size = ref.shape[dim] // count
    window = [slice(None)] * len(ref.shape)
    window[dim] = pl.ds(pl.multiple_of(index * size, size), size)
    return ref.at[tuple(window)]


def add_into(target, addend):
    target[...] = (target[...].astype(jnp.float32) + addend[...].astype(jnp.float32)).astype(
        target.dtype
    )


class PairSum:
    def __init__(self, spot, sizes, terms, dims, halves, landings, send, recv):
        self.col, self.cols = spot[2], sizes[2]
        self.terms, self.dims, self.halves, self.landings = terms, dims, halves, landings
        self.copies = [
            remote(
                slab(term, dim, 1 - spot[2], sizes[2]), landing, send.at[n], recv.at[n],
                (spot[0], spot[1], 1 - spot[2]),
            )
            for n, (term, dim, landing) in enumerate(zip(terms, dims, landings))
        ]

    def start(self):
        for copy in self.copies:
            copy.start()

    def finish(self):
        for copy, term, dim, half, landing in zip(
            self.copies, self.terms, self.dims, self.halves, self.landings
        ):
            copy.wait()
            own = slab(term, dim, self.col, self.cols)
            half[...] = (own[...].astype(jnp.float32) + landing[...].astype(jnp.float32)).astype(
                half.dtype
            )


class LineReduce:
    def __init__(self, spot, sizes, arrays, dims, below, above, sems):
        self.spot, self.count = spot, sizes[0]
        self.arrays, self.dims, self.below, self.above = arrays, dims, below, above
        self.up_send, self.up_recv, self.down_send, self.down_recv = sems

    def copy(self, n, k, up):
        dp, row, col = self.spot
        landing = self.below[n] if up else self.above[n]
        send, recv = (
            (self.up_send, self.up_recv) if up else (self.down_send, self.down_recv)
        )
        dim = self.dims[n]
        return remote(
            slab(self.arrays[n], dim, k, self.count),
            slab(landing, dim, k, self.count),
            send.at[n, k],
            recv.at[n, k],
            (jnp.clip(dp + (1 if up else -1), 0, self.count - 1), row, col),
        )

    def send(self, k, up):
        for n in range(len(self.arrays)):
            self.copy(n, k, up).start()

    def start(self):
        dp, last = self.spot[0], self.count - 1

        pl.when(dp == 0)(lambda: self.send(last, True))
        pl.when(dp == last)(lambda: self.send(0, False))

    def take(self, k, up):
        for n, (array, dim) in enumerate(zip(self.arrays, self.dims)):
            landing = slab((self.below if up else self.above)[n], dim, k, self.count)
            arrived(landing, (self.up_recv if up else self.down_recv).at[n, k])
            add_into(slab(array, dim, k, self.count), landing)

    def event(self, time):
        dp, last = self.spot[0], self.count - 1
        pl.when(jnp.logical_and(dp == 0, time < last))(lambda: self.send(last - time, True))
        pl.when(jnp.logical_and(dp == last, time < last))(lambda: self.send(time, False))

        @pl.when(jnp.logical_and(dp > 0, time >= dp))
        def _():
            k = dp + last - time
            self.take(k, True)
            pl.when(k > dp)(lambda: self.send(k, True))

        @pl.when(jnp.logical_and(dp < last, time >= last - dp))
        def _():
            k = time - (last - dp)
            self.take(k, False)
            pl.when(k < dp)(lambda: self.send(k, False))

    def events(self):
        lax.fori_loop(1, self.count, lambda time, c: (self.event(time), c)[1], 0)

    def finish(self):
        dp = self.spot[0]

        def one(k, carry):
            @pl.when(dp < k)
            def _():
                for n in range(len(self.arrays)):
                    self.copy(n, k, True).wait_send()

            @pl.when(dp > k)
            def _():
                for n in range(len(self.arrays)):
                    self.copy(n, k, False).wait_send()

            return carry

        lax.fori_loop(0, self.count, one, 0)


class LineGather:
    def __init__(self, spot, sizes, arrays, dims, sems):
        self.spot, self.count = spot, sizes[0]
        self.arrays, self.dims = arrays, dims
        self.up_send, self.down_send, self.recv = sems

    def copy(self, n, k, up):
        dp, row, col = self.spot
        part = slab(self.arrays[n], self.dims[n], k, self.count)
        return remote(
            part,
            part,
            (self.up_send if up else self.down_send).at[n, k],
            self.recv.at[n, k],
            (jnp.clip(dp + (1 if up else -1), 0, self.count - 1), row, col),
        )

    def send(self, k, up):
        dp = self.spot[0]

        @pl.when(dp < self.count - 1 if up else dp > 0)
        def _():
            for n in range(len(self.arrays)):
                self.copy(n, k, up).start()

    def start(self):
        self.send(self.spot[0], True)
        self.send(self.spot[0], False)

    def take(self, k):
        for n, (array, dim) in enumerate(zip(self.arrays, self.dims)):
            arrived(slab(array, dim, k, self.count), self.recv.at[n, k])

    def event(self, time):
        dp = self.spot[0]

        @pl.when(dp - time >= 0)
        def _():
            self.take(dp - time)
            self.send(dp - time, True)

        @pl.when(dp + time < self.count)
        def _():
            self.take(dp + time)
            self.send(dp + time, False)

    def events(self):
        lax.fori_loop(1, self.count, lambda time, c: (self.event(time), c)[1], 0)

    def finish(self):
        dp, last = self.spot[0], self.count - 1

        def one(k, carry):
            @pl.when(jnp.logical_and(k <= dp, dp < last))
            def _():
                for n in range(len(self.arrays)):
                    self.copy(n, k, True).wait_send()

            @pl.when(jnp.logical_and(k >= dp, dp > 0))
            def _():
                for n in range(len(self.arrays)):
                    self.copy(n, k, False).wait_send()

            return carry

        lax.fori_loop(0, self.count, one, 0)


def line_sems(sizes, arrays, kinds):
    return [DMA((arrays, sizes[0])) for _ in range(kinds)]


def greet_cross(spot, sizes):
    barrier = pltpu.get_barrier_semaphore()
    dp, row, col = spot
    dps, rows, cols = sizes
    for j in range(rows):
        for k in range(cols):
            if j + k > 0:
                pl.semaphore_signal(
                    barrier,
                    inc=1,
                    device_id=(dp, lax.rem(row + j, rows), lax.rem(col + k, cols)),
                    device_id_type=MESH,
                )
    for j in (1, dps - 1):
        pl.semaphore_signal(
            barrier, inc=1, device_id=(lax.rem(dp + j, dps), row, col), device_id_type=MESH
        )
    pl.semaphore_wait(barrier, rows * cols + 1)


FIRST_DIMS = (0, 0, 0)
FIRST_COLS = (0, 1, 0)
LAST_DIMS = (1, 0)
LAST_COLS = (1, 1)


def halved(shape, dim, cols):
    shape = list(shape)
    shape[dim] //= cols
    return tuple(shape)


def middle_kernel(sizes, *refs):
    part, hidden, dy, gain = refs[:4]
    terms = refs[4:7]
    grad, grad_all, gain_grad = refs[7:10]
    shards = refs[10:13]
    landing, mine, theirs, block = refs[13:17]
    halves, pair_land, below, above = refs[17:20], refs[20:23], refs[23:26], refs[26:29]
    ssend, srecv, gsend, grecv, psend, precv, hsend, hrecv, *line = refs[29:]
    spot = here()
    greet_cross(spot, sizes)
    scatter = Scatter(spot, sizes, part, landing, ssend, srecv)
    scatter.start()
    pair = PairSum(spot, sizes, terms, FIRST_COLS, halves, pair_land, hsend, hrecv)
    pair.start()
    pair.finish()
    reduce = LineReduce(spot, sizes, halves, FIRST_DIMS, below, above, line)
    reduce.start()
    reduce.event(1)
    scatter.wait()
    total, gains = norm_back(sizes, spot, landing, hidden, dy, gain, mine, theirs, psend, precv)
    gain_grad[...] = gains
    grad[...] = total
    block[...] = total.astype(jnp.bfloat16)
    gather = Gather(spot, sizes, block, grad_all, gsend, grecv)
    gather.start()
    lax.fori_loop(2, sizes[0], lambda time, c: (reduce.event(time), c)[1], 0)
    for half, dim, shard in zip(halves, FIRST_DIMS, shards):
        shard[...] = slab(half, dim, spot[0], sizes[0])[...]
    scatter.wait_send()
    gather.wait()
    reduce.finish()


def middle(sizes, part, hidden, dy, gain, terms):
    tokens, width = hidden.shape
    dps, rows, cols = sizes
    low, wide = jnp.bfloat16, jnp.float32
    halves = [halved(t.shape, d, cols) for t, d in zip(terms, FIRST_COLS)]
    shards = [halved(h, d, dps) for h, d in zip(halves, FIRST_DIMS)]
    return pl.pallas_call(
        functools.partial(middle_kernel, sizes),
        in_specs=[VMEM] * 7,
        out_specs=[VMEM] * 6,
        out_shape=[
            jax.ShapeDtypeStruct((tokens, width), wide),
            jax.ShapeDtypeStruct(part.shape, low),
            jax.ShapeDtypeStruct((1, width), wide),
        ]
        + [jax.ShapeDtypeStruct(s, low) for s in shards],
        scratch_shapes=[
            pltpu.VMEM((rows, tokens, width), low),
            pltpu.VMEM((2, tokens, 128), wide),
            pltpu.VMEM((2, tokens, 128), wide),
            pltpu.VMEM((tokens, width), low),
        ]
        + [pltpu.VMEM(h, low) for h in halves] * 4
        + plane_sems(sizes) * 2
        + [DMA, DMA, DMA((3,)), DMA((3,))]
        + line_sems(sizes, 3, 4),
        compiler_params=pltpu.CompilerParams(collective_id=4, has_side_effects=True),
        name="middle",
    )(part, hidden, dy, gain[None], *terms)


def last_kernel(sizes, *refs):
    part, x, above_grad, gain, other_gain = refs[:5]
    keys, shard, terms = refs[5], refs[6], refs[7:9]
    table, grads_all = refs[9:11]
    grad, gain_sums, row_grads, first = refs[11:15]
    lasts, keys_all = refs[15:17], refs[17]
    landing, mine, theirs, own_gain, gain_landing, tables, chunks, row_sums = refs[18:26]
    halves, pair_land, below, above = refs[26:28], refs[28:30], refs[30:32], refs[32:34]
    (
        ssend, srecv, psend, precv, bsend, brecv, hsend, hrecv, tsem, csem,
        xsend, xrecv, kxsend, kxrecv, *line
    ) = refs[34:]
    spot = here()
    dp, row, col = spot
    dps, rows, cols = sizes
    count = dps * rows * cols
    me = index_of(spot, sizes)
    loads = dps * cols
    block = grads_all.shape[-1]

    def load(index):
        slot = lax.rem(index, 2)
        where = (lax.div(index, cols), lax.rem(index, cols))
        return (
            pltpu.make_async_copy(table.at[where], tables.at[slot], tsem.at[slot]),
        ) + tuple(
            pltpu.make_async_copy(
                grads_all.at[where + (r,)],
                chunks.at[slot, :, pl.ds(r * block, block)],
                csem.at[slot, r],
            )
            for r in range(rows)
        )

    for copy in load(0):
        copy.start()
    greet_all(spot, sizes)
    scatter = Scatter(spot, sizes, part, landing, ssend, srecv)
    scatter.start()
    pair = PairSum(spot, sizes, terms, LAST_COLS, halves, pair_land, hsend, hrecv)
    pair.start()
    slab(first, 0, dp, dps)[...] = shard[...]
    gather = LineGather(spot, sizes, [first], [0], line[7:])
    gather.start()
    pair.finish()
    reduce = LineReduce(spot, sizes, halves, LAST_DIMS, below, above, line[:4])
    reduce.start()

    wide_strip = min(512, tables.shape[2])

    def product(index):
        slot = lax.rem(index, 2)
        for copy in load(index):
            copy.wait()

        @pl.when(index + 1 < loads)
        def _():
            for copy in load(index + 1):
                copy.start()

        def strip(n, carry):
            columns = pl.ds(pl.multiple_of(n * wide_strip, wide_strip), wide_strip)
            term = lax.dot_general(
                tables[slot, :, columns],
                chunks[slot],
                (((0,), (0,)), ((), ())),
                preferred_element_type=jnp.float32,
            )

            @pl.when(index == 0)
            def _():
                row_sums[columns] = term

            @pl.when(jnp.logical_and(index > 0, index < loads - 1))
            def _():
                row_sums[columns] = row_sums[columns] + term

            @pl.when(index == loads - 1)
            def _():
                row_grads[columns] = (row_sums[columns] + term).astype(jnp.bfloat16)

            return carry

        lax.fori_loop(0, tables.shape[2] // wide_strip, strip, 0)

    def products(first, end):
        lax.fori_loop(first, end, lambda index, c: (product(index), c)[1], 0)

    def sideways(k):
        return remote(
            keys, keys_all.at[row, col], xsend, xrecv.at[rows - k],
            (dp, lax.rem(row + k, rows), col),
        )

    def cross(src, k):
        there = keys_all.at[lax.rem(row + k, rows), col]
        return remote(src, there, kxsend, kxrecv, (dp, row, 1 - col))

    def both(time):
        reduce.event(time)
        gather.event(time)

    products(0, loads // 8)
    both(1)
    products(loads // 8, loads // 4)
    scatter.wait()
    total, gains = norm_back(sizes, spot, landing, x, above_grad, gain, mine, theirs, psend, precv)
    lines = gains.shape[1] // 128
    for line_index in range(lines):
        columns = slice(line_index * 128, (line_index + 1) * 128)
        own_gain[line_index : line_index + 1] = gains[:, columns]
        own_gain[lines + line_index : lines + line_index + 1] = other_gain[:, columns]

    def tell(device):
        remote(own_gain, gain_landing.at[me], bsend, brecv, device).start()

    each_other(spot, sizes, tell)
    gain_landing[me] = own_gain[...]
    grad[...] = total
    for k in range(1, rows):
        sideways(k).start()
    cross(keys, 0).start()
    keys_all[row, col] = keys[...]
    both(2)
    products(loads // 4, 3 * loads // 8)
    lax.fori_loop(3, dps, lambda time, c: (both(time), c)[1], 0)
    for first, half, dim in zip(lasts, halves, LAST_DIMS):
        slab(first, dim, dp, dps)[...] = slab(half, dim, dp, dps)[...]
    final = LineGather(spot, sizes, lasts, LAST_DIMS, line[4:7])
    final.start()
    products(3 * loads // 8, 5 * loads // 8)
    final.event(1)
    for k in range(1, rows):
        landed = keys_all.at[lax.rem(row + k, rows), col]
        arrived(landed, xrecv.at[k])
        cross(landed, k).start()
    products(5 * loads // 8, 7 * loads // 8)
    final.event(2)
    products(7 * loads // 8, loads)
    lax.fori_loop(3, dps, lambda time, c: (final.event(time), c)[1], 0)
    arrived(keys_all.at[:, 1 - col], kxrecv)
    scatter.wait_send()
    arrived(gain_landing.at[pl.ds(0, count - 1)], brecv)
    for c in range(cols):

        def add(index, sums):
            return sums + gain_landing[index * cols + c]

        gain_sums[c] = lax.fori_loop(0, dps * rows, add, jnp.zeros(own_gain.shape, jnp.float32))
    arrived(gain_landing.at[pl.ds(0, count - 1)], bsend)
    arrived(keys_all.at[:, col], kxsend)
    arrived(keys_all.at[pl.ds(0, rows - 1), col], xsend)
    gather.finish()
    reduce.finish()
    final.finish()


def last(sizes, part, x, above, gain, other_gain, keys, shard, terms, table, grads_all):
    tokens, width = x.shape
    dps, rows, cols = sizes
    lines = 2 * width // 128
    count = dps * rows * cols
    low, wide = jnp.bfloat16, jnp.float32
    shape = jax.ShapeDtypeStruct

    halves = [halved(t.shape, d, cols) for t, d in zip(terms, LAST_COLS)]
    rows_dev = table.shape[-1]
    features = grads_all.shape[-1] * rows
    chunk = table.shape[2]
    return pl.pallas_call(
        functools.partial(last_kernel, sizes),
        in_specs=[VMEM] * 9 + [ANY] * 2,
        out_specs=[VMEM] * 7,
        out_shape=[
            shape((tokens, width), wide),
            shape((cols, lines, 128), wide),
            shape((rows_dev, features), low),
            shape((shard.shape[0] * dps, shard.shape[1]), low),
        ]
        + [shape(s, low) for s in halves]
        + [shape((rows, cols) + keys.shape, low)],
        scratch_shapes=[
            pltpu.VMEM((rows, tokens, width), low),
            pltpu.VMEM((2, tokens, 128), wide),
            pltpu.VMEM((2, tokens, 128), wide),
            pltpu.VMEM((lines, 128), wide),
            pltpu.VMEM((count, lines, 128), wide),
            pltpu.VMEM((2, chunk, rows_dev), low),
            pltpu.VMEM((2, chunk, features), low),
            pltpu.VMEM((rows_dev, features), wide),
        ]
        + [pltpu.VMEM(h, low) for h in halves] * 4
        + plane_sems(sizes)
        + [DMA, DMA, DMA, DMA, DMA((2,)), DMA((2,)), DMA((2,)), DMA((2, rows))]
        + [DMA, DMA((rows,)), DMA, DMA]
        + line_sems(sizes, 2, 7)
        + line_sems(sizes, 1, 3),
        compiler_params=pltpu.CompilerParams(collective_id=5, has_side_effects=True),
        name="last",
    )(part, x, above, gain[None], other_gain, keys, shard, *terms, table, grads_all)


def turn_kernel(sizes, *refs):
    prefix, queries, kv, grad_out, log_sums, out_part, hidden = refs[:7]
    shards, term = refs[7:10], refs[10]
    grad_q, grad_kv, output = refs[11:14]
    firsts, term_shard = refs[14:17], refs[17]
    totals, kv_landing, out_landing, half, pair_land, below, above = refs[18:25]
    osend, orecv, ksend, krecv, hsend, hrecv, *line = refs[25:]
    spot = here()
    dp, row, col = spot
    dps = sizes[0]
    tokens, width = queries.shape
    keys = kv.shape[1]
    tile = tokens // 2
    greet_cross(spot, sizes)
    for first, dim, shard in zip(firsts, FIRST_DIMS, shards):
        slab(first, dim, dp, dps)[...] = shard[...]
    pair = PairSum(spot, sizes, [term], [0], [half], [pair_land], hsend, hrecv)
    pair.start()
    gather = LineGather(spot, sizes, firsts, FIRST_DIMS, line[:3])
    gather.start()
    out_scatter = Scatter(spot, sizes, out_part, out_landing, osend, orecv)
    out_scatter.start()
    pair.finish()
    reduce = LineReduce(spot, sizes, [half], [0], [below], [above], line[3:])
    reduce.start()

    def events(time):
        gather.event(time)
        reduce.event(time)

    limit = prefix[0]
    key_pos = lax.broadcasted_iota(jnp.int32, (keys, tile), 0)
    sides = lane_sides()

    def unit(index, carry):
        pair, part = lax.div(index, 2), lax.rem(index, 2)
        lanes = pl.ds(pl.multiple_of(pair * 2 * HDIM, 2 * HDIM), 2 * HDIM)
        lines = pl.ds(pl.multiple_of(part * tile, tile), tile)
        query_pos = col * tokens + part * tile + lax.broadcasted_iota(jnp.int32, (1, tile), 1)
        allowed = jnp.logical_or(key_pos <= query_pos, key_pos < limit)
        q2, g2 = queries[lines, lanes], grad_out[lines, lanes]
        k2, v2 = kv[0, :, lanes], kv[1, :, lanes]
        dq = jnp.zeros((tile, 2 * HDIM), jnp.float32)
        dk = jnp.zeros((keys, 2 * HDIM), jnp.float32)
        dv = jnp.zeros((keys, 2 * HDIM), jnp.float32)
        for a in range(2):
            ka = k2 * sides[a]
            scores = jnp.where(allowed, dense_nt(ka, q2) * HDIM ** (-0.5), -jnp.inf)
            probs = jnp.exp(scores - log_sums[pl.ds(2 * pair + a, 1), lines])
            grad_probs = dense_nt(v2 * sides[a], g2)
            inner = jnp.sum(probs * grad_probs, axis=0, keepdims=True)
            grad_scores = (probs * (grad_probs - inner)).astype(jnp.bfloat16)
            dq = dq + dense_tn(grad_scores, ka)
            dk = dk + dense(grad_scores, q2 * sides[a])
            dv = dv + dense(probs.astype(jnp.bfloat16), g2 * sides[a])
        grad_q[lines, lanes] = (dq * HDIM ** (-0.5)).astype(jnp.bfloat16)
        dk = dk * HDIM ** (-0.5)

        @pl.when(part == 0)
        def _():
            totals[0, :, lanes] = dk
            totals[1, :, lanes] = dv

        @pl.when(part > 0)
        def _():
            totals[0, :, lanes] = totals[0, :, lanes] + dk
            totals[1, :, lanes] = totals[1, :, lanes] + dv

        pl.when(index == 0)(lambda: events(1))
        pl.when(index == 2)(lambda: events(2))
        return carry

    lax.fori_loop(0, 2 * width // (2 * HDIM), unit, 0)
    size = kv_landing.shape[1]
    other = pl.multiple_of((1 - col) * size, size)
    away = remote(totals.at[:, pl.ds(other, size)], kv_landing, ksend, krecv, (dp, row, 1 - col))
    away.start()
    out_scatter.wait()
    result = hidden[...]
    for q in range(sizes[1]):
        result = result + out_landing[q].astype(jnp.float32)
    output[...] = result.astype(jnp.bfloat16)
    away.wait()
    own = totals[:, pl.ds(pl.multiple_of(col * size, size), size)]
    grad_kv[...] = (own + kv_landing[...]).astype(jnp.bfloat16)
    lax.fori_loop(3, dps, lambda time, c: (events(time), c)[1], 0)
    term_shard[...] = slab(half, 0, dp, dps)[...]
    out_scatter.wait_send()
    gather.finish()
    reduce.finish()


def turn(sizes, prefix, queries, kv, grad_out, log_sums, out_part, hidden, shards, term):
    tokens, width = queries.shape
    dps, rows, cols = sizes
    low, wide = jnp.bfloat16, jnp.float32
    shape = jax.ShapeDtypeStruct

    def grown(shard, dim):
        full = list(shard.shape)
        full[dim] *= dps
        return tuple(full)

    firsts = [grown(s, d) for s, d in zip(shards, FIRST_DIMS)]
    half = halved(term.shape, 0, cols)
    return pl.pallas_call(
        functools.partial(turn_kernel, sizes),
        in_specs=[pl.BlockSpec(memory_space=pltpu.SMEM)] + [VMEM] * 10,
        out_specs=[VMEM] * 7,
        out_shape=[
            shape((tokens, width), low),
            shape((2, tokens, width), low),
            shape(hidden.shape, low),
        ]
        + [shape(s, low) for s in firsts]
        + [shape(halved(half, 0, dps), low)],
        scratch_shapes=[
            pltpu.VMEM(kv.shape, wide),
            pltpu.VMEM((2, tokens, width), wide),
            pltpu.VMEM((rows,) + hidden.shape, low),
        ]
        + [pltpu.VMEM(half, low)] * 4
        + plane_sems(sizes)
        + [DMA, DMA, DMA((1,)), DMA((1,))]
        + line_sems(sizes, 3, 3)
        + line_sems(sizes, 1, 4),
        compiler_params=pltpu.CompilerParams(collective_id=2, has_side_effects=True),
        name="turn",
    )(prefix, queries, kv, grad_out, log_sums, out_part, hidden, *shards, term)


def flat_picks(picks_head):
    blocks = picks_head.shape[0] // FBLK
    return jnp.swapaxes(picks_head.reshape(blocks, FBLK, TOPK), 1, 2).reshape(blocks, TOPK * FBLK)


def one_hot(row_values, size):
    hot = lax.broadcasted_iota(jnp.int32, (size, row_values.shape[1]), 0) == row_values
    return jnp.where(hot, 1.0, 0.0).astype(jnp.bfloat16)


def route_block(picks, rows_dev, owners, cap):
    lane = lax.broadcasted_iota(jnp.int32, (FBLK, FBLK), 0)
    before = jnp.where(lane < lax.broadcasted_iota(jnp.int32, (FBLK, FBLK), 1), 1.0, 0.0).astype(
        jnp.bfloat16
    )
    owner = picks // rows_dev
    local = picks % rows_dev
    hot = one_hot(owner, owners)
    running = jnp.zeros((owners, 1), jnp.float32)
    ranks = []
    for chunk in range(picks.shape[1] // FBLK):
        part = hot[:, chunk * FBLK : (chunk + 1) * FBLK]
        earlier = jnp.dot(part, before, preferred_element_type=jnp.float32)
        wide = part.astype(jnp.float32)
        ranks.append(jnp.sum(wide * (earlier + running), axis=0, keepdims=True))
        running = running + jnp.sum(wide, axis=1, keepdims=True)
    rank = jnp.concatenate(ranks, axis=1).astype(jnp.int32)
    slot_hot = one_hot(rank, cap)
    token = lax.broadcasted_iota(jnp.int32, picks.shape, 1) % FBLK
    outs = []
    for payload in (local % SUBKEYS, local // SUBKEYS, token):
        scaled = hot * payload.astype(jnp.float32).astype(jnp.bfloat16)
        outs.append(
            lax.dot_general(
                scaled, slot_hot, (((1,), (1,)), ((), ())), preferred_element_type=jnp.float32
            ).astype(jnp.int32)
        )
    return rank, (outs[1] * FBLK + outs[2]) * SUBKEYS + outs[0]


def pick_rows(table, index):
    inner = index % 8
    outer = index // 8
    result = jnp.zeros(index.shape, jnp.float32)
    for group in range(SUBKEYS // 8):
        rows = table[group * 8 : (group + 1) * 8]
        found = [
            jnp.take_along_axis(rows, inner[n * 8 : (n + 1) * 8], axis=0)
            for n in range(index.shape[0] // 8)
        ]
        result = jnp.where(outer == group, jnp.concatenate(found, axis=0), result)
    return result


def weigh_kernel(
    rows_dev, owners, cap, query_ref, keys_ref, picks_ref, square_ref, rank_ref, weights_ref, slots_ref
):
    picks = picks_ref[0]
    square = square_ref[0]
    first = lax.dot_general(
        keys_ref[0], query_ref[:, :HALF], (((1,), (1,)), ((), ())), preferred_element_type=jnp.float32
    )
    second = lax.dot_general(
        keys_ref[1], query_ref[:, HALF:], (((1,), (1,)), ((), ())), preferred_element_type=jnp.float32
    )
    scores = pick_rows(first, square // SUBKEYS) + pick_rows(second, square % SUBKEYS)
    powers = jnp.exp(scores - jnp.max(scores, axis=0, keepdims=True))
    weights = powers / jnp.sum(powers, axis=0, keepdims=True)
    weights_ref[0] = weights
    flat = jnp.concatenate([weights[pick : pick + 1] for pick in range(TOPK)], axis=1)
    scaled = one_hot(picks // rows_dev, owners) * flat.astype(jnp.bfloat16)
    slots_ref[0] = lax.dot_general(
        one_hot(rank_ref[0], cap),
        scaled,
        (((1,), (1,)), ((), ())),
        preferred_element_type=jnp.float32,
    )


def weigh(query_rows, keys_head, flat, square, rank, rows_dev, owners, cap):
    blocks, count = flat.shape
    return pl.pallas_call(
        functools.partial(weigh_kernel, rows_dev, owners, cap),
        grid=(blocks,),
        in_specs=[
            pl.BlockSpec((FBLK, 2 * HALF), lambda i: (i, 0)),
            pl.BlockSpec((2, SUBKEYS, HALF), lambda i: (0, 0, 0)),
            pl.BlockSpec((1, 1, count), lambda i: (i, 0, 0)),
            pl.BlockSpec((1, TOPK, FBLK), lambda i: (i, 0, 0)),
            pl.BlockSpec((1, 1, count), lambda i: (i, 0, 0)),
        ],
        out_specs=[
            pl.BlockSpec((1, TOPK, FBLK), lambda i: (i, 0, 0)),
            pl.BlockSpec((1, cap, owners), lambda i: (i, 0, 0)),
        ],
        out_shape=[
            jax.ShapeDtypeStruct((blocks, TOPK, FBLK), jnp.float32),
            jax.ShapeDtypeStruct((blocks, cap, owners), jnp.float32),
        ],
        name="weigh",
    )(query_rows, keys_head, flat[:, None, :], square, rank)


def short_hot(row_values, size):
    short = jnp.int16
    hot = lax.broadcasted_iota(short, (size, row_values.shape[1]), 0) == row_values.astype(short)
    return jnp.where(hot, jnp.ones((), jnp.bfloat16), jnp.zeros((), jnp.bfloat16))


def send_rows(spot, sizes, src, landing, send, recv):
    me = index_of(spot, sizes)

    def one(device):
        remote(src.at[index_of(device, sizes)], landing.at[me], send, recv, device).start()

    each_other(spot, sizes, one)
    landing[me] = src[me]


def all_rows(landing, sem):
    return arrived(landing.at[pl.ds(0, landing.shape[0] - 1)], sem)


def slot_row(sizes, table, dp, col, block):
    pieces = []
    for row in range(sizes[1]):
        index = (dp * sizes[1] + row) * sizes[2] + col
        pieces.append(table[index, pl.ds(block, 1), :])
    return jnp.concatenate(pieces, axis=1)


def nth_place(dp, q, dps):
    twice = 2 * jnp.minimum(dp, dps - 1 - dp)
    inside = q <= twice
    distance = jnp.where(inside, lax.div(q + 1, 2), q - lax.div(twice, 2))
    below = jnp.logical_or(
        jnp.logical_and(inside, lax.rem(q, 2) == 1),
        jnp.logical_and(jnp.logical_not(inside), dp > dps - 1 - dp),
    )
    return dp + jnp.where(below, -distance, distance), below


def plane_neighbours(row, rows):
    across = row + 1 - 2 * lax.rem(row, 2)
    along = lax.rem(row + rows // 2, rows)
    return across, along, lax.rem(across + rows // 2, rows)


RING = 3


def memory_kernel(
    sizes, blocks, grads, meta, slots, values,
    grads_all, table, other_part, memory, back,
    meta_in, slots_in, values_t, tables, parts,
    chunks, found, sums, grids, theirs, acc, first_land, side_land, deep_land, total,
    msend, mrecv, ssend, srecv, zup, zdown, zrecv, wsend, wrecv, csend, crecv,
    local, tsem, qsend, qrecv,
    gsem, esem, hsend, hrecv, xsend, xrecv, dsend, drecv, fsend, frecv, flocal,
):
    spot = here()
    dp, row, col = spot
    dps, rows, cols = sizes
    tokens, width = grads.shape
    half = tokens // 2
    areas = values.shape[0] // SUBKEYS
    count = dps * rows * cols
    me = index_of(spot, sizes)
    across, along, opposite = plane_neighbours(row, rows)
    first_half, second_half = pl.ds(0, half), pl.ds(half, half)
    greet_all(spot, sizes)
    send_rows(spot, sizes, meta, meta_in, msend, mrecv)
    send_rows(spot, sizes, slots, slots_in, ssend, srecv)

    def place_of(u):
        return nth_place(dp, dps - 1 - u, dps)[0]

    def block_at(place, r, lines=slice(None)):
        return grads_all.at[place, col, r, lines]

    def cross(q, place, r, src=None):
        there = block_at(place, r)
        remote(there if src is None else src, there, csend, crecv.at[q], (dp, row, 1 - col)).start()

    def line_copy(place, up, src=None):
        there = block_at(place, row)
        return remote(
            there if src is None else src,
            there,
            (zup if up else zdown).at[place],
            zrecv.at[place],
            (jnp.clip(dp + (1 if up else -1), 0, dps - 1), row, col),
        )

    def sideways(q, place, src=None):
        there = block_at(place, row)
        for n, r in enumerate((across, along)):
            remote(
                there if src is None else src, there, wsend, wrecv.at[q, n], (dp, r, col)
            ).start()

    pl.when(dp < dps - 1)(lambda: line_copy(dp, True, grads).start())
    pl.when(dp > 0)(lambda: line_copy(dp, False, grads).start())
    sideways(0, dp, grads)
    cross(0, dp, row, grads)
    keep = pltpu.make_async_copy(grads, block_at(dp, row), local)
    keep.start()

    def from_line(q):
        place, below = nth_place(dp, q, dps)
        arrived(block_at(place, row), zrecv.at[place])
        pl.when(jnp.logical_and(below, dp < dps - 1))(lambda: line_copy(place, True).start())
        pl.when(jnp.logical_and(jnp.logical_not(below), dp > 0))(
            lambda: line_copy(place, False).start()
        )
        sideways(q, place)
        cross(q, place, row)

    def from_sides(q):
        place, _ = nth_place(dp, q, dps)
        for n, (r, other, lines) in enumerate(
            ((across, along, first_half), (along, across, second_half))
        ):
            arrived(block_at(place, r), wrecv.at[q, n])
            half = block_at(place, r, lines)
            remote(half, half, wsend, wrecv.at[q, 2 + n], (dp, other, col)).start()
            cross(q, place, r)

    def from_opposite(q):
        place, _ = nth_place(dp, q, dps)
        for n, lines in enumerate((first_half, second_half)):
            arrived(block_at(place, opposite, lines), wrecv.at[q, 2 + n])
        cross(q, place, opposite)

    def turn_rows(n, carry):
        lines = pl.ds(pl.multiple_of(n * 256, 256), 256)
        values_t[:, lines] = values[lines].T
        return carry

    lax.fori_loop(0, values.shape[0] // 256, turn_rows, 0)
    all_rows(meta_in, mrecv)
    all_rows(slots_in, srecv)

    def write_places(chunk):
        turn = lax.div(chunk, 2)
        slot = lax.rem(chunk, 2)
        return turn, slot, place_of(turn), jnp.where(slot == 0, 1 - col, col)

    def table_copy(chunk):
        _, slot, source_dp, source_col = write_places(chunk)
        return pltpu.make_async_copy(
            tables.at[slot], table.at[source_dp, source_col], tsem.at[slot]
        )

    def build(chunk):
        turn, slot, source_dp, source_col = write_places(chunk)
        pl.when(turn > 0)(lambda: table_copy(chunk).wait())
        def one(block, carry):
            row_meta = slot_row(sizes, meta_in, source_dp, source_col, block)
            key = row_meta // SUBKEYS
            low = row_meta % SUBKEYS
            weight = slot_row(sizes, slots_in, source_dp, source_col, block)
            short = jnp.int16
            at_key = lax.broadcasted_iota(short, (areas * FBLK, key.shape[1]), 0) == key.astype(short)
            left = jnp.where(at_key, weight.astype(jnp.bfloat16), jnp.zeros((), jnp.bfloat16))
            stacked = lax.dot_general(
                left,
                short_hot(low, SUBKEYS),
                (((1,), (1,)), ((), ())),
                preferred_element_type=jnp.float32,
            ).astype(jnp.bfloat16)
            for area in range(areas):
                tables[
                    slot,
                    pl.ds(pl.multiple_of(block * FBLK, FBLK), FBLK),
                    area * SUBKEYS : (area + 1) * SUBKEYS,
                ] = stacked[area * FBLK : (area + 1) * FBLK]
            return carry

        lax.fori_loop(0, blocks, one, 0)
        table_copy(chunk).start()

    def away(turn, source_dp):
        return remote(parts.at[0], other_part.at[source_dp], qsend, qrecv.at[turn], (dp, row, 1 - col))

    def multiply(chunk):
        turn, slot, source_dp, _ = write_places(chunk)
        later = turn > 0
        pl.when(jnp.logical_and(later, slot == 0))(lambda: away(turn, source_dp).wait_send())

        def strip(n, carry):
            columns = pl.ds(pl.multiple_of(n * 512, 512), 512)
            parts[slot, :, columns] = jnp.dot(
                tables[slot], values[:, columns], preferred_element_type=jnp.float32
            ).astype(jnp.bfloat16)
            return carry

        lax.fori_loop(0, values.shape[1] // 512, strip, 0)
        pl.when(slot == 0)(lambda: away(turn, source_dp).start())

    def load_part(u):
        return pltpu.make_async_copy(other_part.at[place_of(u)], theirs, esem)

    def strip(u, r, lines=slice(None)):
        return acc.at[lax.rem(u, RING), lines, pl.ds(pl.multiple_of(r * width, width), width)]

    lines_of = (pl.ds(0, half), pl.ds(half, half))

    def halves(u):
        return [
            remote(
                strip(u, opposite, lines_of[n]), first_land.at[u, n],
                hsend.at[lax.rem(u, RING), n], hrecv.at[u, n], (dp, r, col),
            )
            for n, r in enumerate((across, along))
        ]

    def wholes(u):
        return [
            remote(
                strip(u, r), side_land.at[u, n],
                xsend.at[lax.rem(u, RING), n], xrecv.at[u, n], (dp, r, col),
            )
            for n, r in enumerate((across, along))
        ]

    def sent(u):
        for copy in halves(u) + wholes(u):
            copy.wait_send()

    def fetch(u):
        arrived(other_part.at[place_of(u)], qrecv.at[u])
        load_part(u).start()

    def combine(u):
        pl.when(u >= RING)(lambda: sent(u - RING))
        load_part(u).wait()
        acc[lax.rem(u, RING)] = (
            parts[1].astype(jnp.float32) + theirs[...].astype(jnp.float32)
        ).astype(jnp.bfloat16)
        for copy in halves(u):
            copy.start()

    def relay(u):
        for n, r in enumerate((along, across)):
            arrived(first_land.at[u, n], hrecv.at[u, n])
            add_into(strip(u, r, lines_of[n]), first_land.at[u, n])
        for copy in wholes(u):
            copy.start()

    def deep_copy(u):
        place = place_of(u)
        up = place > dp
        target = jnp.where(up, dp + 1, dp - 1)
        there = jnp.where(jnp.logical_and(jnp.logical_not(up), target == place), dps, place)
        return remote(
            total.at[u], deep_land.at[there], dsend.at[u], drecv.at[there],
            (jnp.clip(target, 0, dps - 1), row, col),
        )

    def finish(u):
        for n in range(2):
            arrived(side_land.at[u, n], xrecv.at[u, n])
        place = place_of(u)
        result = (
            strip(u, row)[...].astype(jnp.float32)
            + side_land[u, 0].astype(jnp.float32)
            + side_land[u, 1].astype(jnp.float32)
        )
        memory[...] = result

        def more(index):
            arrived(deep_land.at[index], drecv.at[index])
            memory[...] = memory[...] + deep_land[index].astype(jnp.float32)

        below = jnp.logical_and(place >= dp, dp > 0)
        above = jnp.logical_and(place <= dp, dp < dps - 1)
        pl.when(jnp.logical_or(below, jnp.logical_and(above, place < dp)))(lambda: more(place))
        pl.when(jnp.logical_and(above, place == dp))(lambda: more(dps))

        @pl.when(u < dps - 1)
        def _():
            total[u] = memory[...].astype(jnp.bfloat16)
            deep_copy(u).start()

    def read_places(chunk):
        slot = lax.rem(chunk, 2)
        place = nth_place(dp, lax.div(chunk, 2), dps)[0]
        return slot, place, jnp.where(slot == 0, col, 1 - col)

    def load_chunk(chunk):
        slot, source_dp, source_col = read_places(chunk)
        return [
            pltpu.make_async_copy(
                grads_all.at[source_dp, source_col, r],
                chunks.at[slot, :, pl.ds(r * width, width)],
                gsem.at[slot, r],
            )
            for r in range(rows)
        ]

    def start_chunk(chunk):
        slot, source_dp, source_col = read_places(chunk)

        @pl.when(slot == 1)
        def _():
            arrived(grads_all.at[source_dp, source_col], crecv.at[lax.div(chunk, 2)])

        for copy in load_chunk(chunk):
            copy.start()

    wide_strip = min(2048, areas * SUBKEYS)
    per_strip = wide_strip // SUBKEYS

    def search(chunk, part):
        slot, source_dp, source_col = read_places(chunk)

        @pl.when(part == 0)
        def _():
            for copy in load_chunk(chunk):
                copy.wait()

            def strip(n, carry):
                columns = pl.ds(pl.multiple_of(n * wide_strip, wide_strip), wide_strip)
                grid = jnp.dot(
                    chunks[slot], values_t[:, columns], preferred_element_type=jnp.float32
                ).astype(jnp.bfloat16)
                for area in range(per_strip):
                    grids[n * per_strip + area] = grid[:, area * SUBKEYS : (area + 1) * SUBKEYS]
                return carry

            lax.fori_loop(0, areas // per_strip, strip, 0)

            @pl.when(chunk + 2 < dps * cols)
            def _():
                start_chunk(chunk + 2)

        @pl.when(part == 1)
        def _():
            def one(block, carry):
                row_meta = slot_row(sizes, meta_in, source_dp, source_col, block)
                lines = pl.ds(pl.multiple_of(block * FBLK, FBLK), FBLK)
                stacked = grids[:, lines, :].reshape(areas * FBLK, SUBKEYS)
                product = jnp.dot(
                    stacked, short_hot(row_meta % SUBKEYS, SUBKEYS), preferred_element_type=jnp.float32
                )
                spot_id = lax.broadcasted_iota(jnp.int32, product.shape, 0)
                sums[block] = jnp.sum(
                    jnp.where(spot_id == row_meta // SUBKEYS, product, 0.0), axis=0, keepdims=True
                )
                return carry

            lax.fori_loop(0, blocks, one, 0)

            for r in range(rows):
                index = (source_dp * rows + r) * cols + source_col
                for block in range(blocks):
                    found[index, block : block + 1, :] = sums[block, :, r * 128 : (r + 1) * 128]
                away = remote(found.at[index], back.at[me], fsend, frecv, (source_dp, r, source_col))
                own = jnp.logical_and(
                    jnp.logical_and(source_dp == dp, row == r), source_col == col
                )
                pl.when(jnp.logical_not(own))(away.start)
                pl.when(own)(pltpu.make_async_copy(found.at[index], back.at[me], flocal).start)

    writes = 4 * dps

    def poll(p, carry):
        phase = lax.rem(p, 2)
        writing = p < writes
        pl.when(jnp.logical_and(writing, phase == 0))(lambda: build(lax.div(p, 2)))
        pl.when(jnp.logical_and(writing, phase == 1))(lambda: multiply(lax.div(p, 2)))

        @pl.when(p == writes)
        def _():
            keep.wait()
            start_chunk(0)
            start_chunk(1)

        pl.when(p >= writes)(lambda: search(lax.div(p - writes, 2), phase))
        turn, third = lax.div(p, 3), lax.rem(p, 3)
        pl.when(jnp.logical_and(third == 2, turn + 1 < dps))(lambda: from_line(turn + 1))
        for event, delay in ((from_sides, 1), (from_opposite, 2)):
            now = jnp.logical_and(turn >= delay, turn < dps + delay)
            pl.when(jnp.logical_and(third == 0, now))(functools.partial(event, turn - delay))
        for event, delay in ((finish, FINISH_AT), (relay, RELAY_AT), (combine, COMBINE_AT), (fetch, FETCH_AT)):
            late = p - delay
            now = jnp.logical_and(
                jnp.logical_and(late >= 0, lax.rem(late, 4) == 0), late < 4 * dps
            )
            pl.when(now)(functools.partial(event, lax.div(late, 4)))
        return carry

    lax.fori_loop(0, 8 * dps, poll, 0)
    for slot in range(2):
        pltpu.make_async_copy(tables.at[slot], table.at[0, 0], tsem.at[slot]).wait()
    away(0, 0).wait_send()
    arrived(grads_all.at[:, 0], csend)
    arrived(grads_all.at[:, 0, pl.ds(0, rows - 1)], wsend)
    all_rows(meta_in, msend)
    all_rows(slots_in, ssend)

    def line_sent(k, carry):
        pl.when(jnp.logical_and(k <= dp, dp < dps - 1))(lambda: line_copy(k, True).wait_send())
        pl.when(jnp.logical_and(k >= dp, dp > 0))(lambda: line_copy(k, False).wait_send())
        return carry

    lax.fori_loop(0, dps, line_sent, 0)
    arrived(back.at[pl.ds(0, count - 1)], frecv)
    arrived(back.at[0], flocal)
    arrived(back.at[pl.ds(0, count - 1)], fsend)
    for u in range(max(0, dps - RING), dps):
        sent(u)
    lax.fori_loop(0, dps - 1, lambda u, c: (deep_copy(u).wait_send(), c)[1], 0)


FETCH_AT, COMBINE_AT, RELAY_AT, FINISH_AT = 5, 6, 10, 16


def use_memory(sizes, grads, meta, slots, values):
    dps, rows, cols = sizes
    tokens, width = grads.shape
    rows_dev, features = values.shape
    blocks = tokens // FBLK
    count = dps * rows * cols
    low, wide = jnp.bfloat16, jnp.float32
    shape = jax.ShapeDtypeStruct
    grads_all, table, _, memory, back = pl.pallas_call(
        functools.partial(memory_kernel, sizes, blocks),
        in_specs=[VMEM] * 4,
        out_specs=[ANY] * 3 + [VMEM] * 2,
        out_shape=[
            shape((dps, cols, rows, tokens, width), low),
            shape((dps, cols, tokens, rows_dev), low),
            shape((dps, tokens, features), low),
            shape((tokens, width), wide),
            shape((count, blocks, 128), wide),
        ],
        scratch_shapes=[
            pltpu.VMEM(meta.shape, meta.dtype),
            pltpu.VMEM(slots.shape, slots.dtype),
            pltpu.VMEM((features, rows_dev), low),
            pltpu.VMEM((2, tokens, rows_dev), low),
            pltpu.VMEM((2, tokens, features), low),
            pltpu.VMEM((2, tokens, features), low),
            pltpu.VMEM((count, blocks, 128), wide),
            pltpu.VMEM((blocks, 1, rows * 128), wide),
            pltpu.VMEM((rows_dev // SUBKEYS, tokens, SUBKEYS), low),
            pltpu.VMEM((tokens, features), low),
            pltpu.VMEM((RING, tokens, features), low),
            pltpu.VMEM((dps, 2, tokens // 2, width), low),
            pltpu.VMEM((dps, 2, tokens, width), low),
            pltpu.VMEM((dps + 1, tokens, width), low),
            pltpu.VMEM((dps, tokens, width), low),
            DMA, DMA, DMA, DMA,
            DMA((dps,)), DMA((dps,)), DMA((dps,)),
            DMA, DMA((dps, 4)),
            DMA, DMA((dps,)),
            DMA, DMA((2,)), DMA, DMA((dps,)),
            DMA((2, rows)), DMA,
            DMA((RING, 2)), DMA((dps, 2)),
            DMA((RING, 2)), DMA((dps, 2)),
            DMA((dps,)), DMA((dps + 1,)),
            DMA, DMA, DMA,
        ],
        compiler_params=pltpu.CompilerParams(collective_id=6, has_side_effects=True),
        name="use_memory",
    )(grads, meta, slots, values)
    return grads_all, table, memory, back


def unweigh_kernel(rows_dev, owners, back_ref, picks_ref, rank_ref, weights_ref, first_ref, second_ref):
    picks = picks_ref[0]
    hot = one_hot(picks // rows_dev, owners)
    back = back_ref[0]
    high = back.astype(jnp.bfloat16)
    rest = back - high.astype(jnp.float32)
    middle = rest.astype(jnp.bfloat16)
    lowest = (rest - middle.astype(jnp.float32)).astype(jnp.bfloat16)
    spread_back = jnp.dot(
        jnp.concatenate([high, middle, lowest], axis=1),
        jnp.concatenate([hot, hot, hot], axis=0),
        preferred_element_type=jnp.float32,
    )
    slot = lax.broadcasted_iota(jnp.int32, spread_back.shape, 0)
    flat = jnp.sum(jnp.where(slot == rank_ref[0], spread_back, 0.0), axis=0, keepdims=True)
    grads = jnp.concatenate(
        [flat[:, pick * FBLK : (pick + 1) * FBLK] for pick in range(TOPK)], axis=0
    )
    weights = weights_ref[0]
    grads = weights * (grads - jnp.sum(weights * grads, axis=0, keepdims=True))
    upper = picks // SUBKEYS
    lower = picks % SUBKEYS
    tile = 64

    def some_keys(index, carry):
        lines = pl.ds(pl.multiple_of(index * tile, tile), tile)
        key_id = lax.broadcasted_iota(jnp.int32, (tile, FBLK), 0) + index * tile
        first = jnp.zeros((tile, FBLK), jnp.float32)
        second = jnp.zeros((tile, FBLK), jnp.float32)
        for pick in range(TOPK):
            columns = slice(pick * FBLK, (pick + 1) * FBLK)
            value = grads[pick : pick + 1]
            first = first + jnp.where(key_id == upper[:, columns], value, 0.0)
            second = second + jnp.where(key_id == lower[:, columns], value, 0.0)
        first_ref[lines] = first.astype(jnp.bfloat16)
        second_ref[lines] = second.astype(jnp.bfloat16)
        return carry

    lax.fori_loop(0, SUBKEYS // tile, some_keys, 0)


def unweigh(back, flat, rank, weights, rows_dev, owners):
    blocks, count = flat.shape
    cap = back.shape[1]
    return pl.pallas_call(
        functools.partial(unweigh_kernel, rows_dev, owners),
        grid=(blocks,),
        in_specs=[
            pl.BlockSpec((1, cap, owners), lambda i: (i, 0, 0)),
            pl.BlockSpec((1, 1, count), lambda i: (i, 0, 0)),
            pl.BlockSpec((1, 1, count), lambda i: (i, 0, 0)),
            pl.BlockSpec((1, TOPK, FBLK), lambda i: (i, 0, 0)),
        ],
        out_specs=[
            pl.BlockSpec((SUBKEYS, FBLK), lambda i: (0, i)),
            pl.BlockSpec((SUBKEYS, FBLK), lambda i: (0, i)),
        ],
        out_shape=[jax.ShapeDtypeStruct((SUBKEYS, blocks * FBLK), jnp.bfloat16)] * 2,
        name="unweigh",
    )(back, flat[:, None, :], rank, weights)


def memory_all(query_rows, grad_memory, flat, rank, meta, subkeys, values):
    sizes = grid_sizes()
    owners = sizes[0] * sizes[1] * sizes[2]
    rows_dev = values.shape[0]
    cap = FBLK * TOPK // owners
    head_id = lax.axis_index("row")
    keys_head = lax.dynamic_index_in_dim(subkeys, head_id, 0, keepdims=False)
    square = flat.reshape(-1, TOPK, FBLK)
    weights, slots = weigh(query_rows, keys_head, flat, square, rank, rows_dev, owners, cap)
    spare = ((0, 0), (0, 0), (0, 128 - cap))
    meta = jnp.pad(jnp.swapaxes(meta, 0, 1), spare, constant_values=-1)
    slots = jnp.pad(jnp.transpose(slots, (2, 0, 1)), spare)
    grads_all, table, memory, back = use_memory(
        sizes, grad_memory, meta, slots, values
    )
    first_t, second_t = unweigh(
        jnp.transpose(back, (1, 2, 0))[:, :cap], flat, rank, weights, rows_dev, owners
    )
    grad_query = jnp.concatenate(
        [
            lax.dot_general(
                part, keys_head[i], (((0,), (0,)), ((), ())), preferred_element_type=jnp.float32
            )
            for i, part in enumerate((first_t, second_t))
        ],
        axis=1,
    ).astype(jnp.bfloat16)
    grad_keys = jnp.stack(
        [
            jnp.dot(first_t, query_rows[:, :HALF], preferred_element_type=jnp.float32),
            jnp.dot(second_t, query_rows[:, HALF:], preferred_element_type=jnp.float32),
        ]
    )
    return memory, grad_query, grad_keys, table, grads_all


def dense(left, right):
    return jnp.dot(left, right, preferred_element_type=jnp.float32)


def dense_nt(left, right):
    return lax.dot_general(left, right, (((1,), (1,)), ((), ())), preferred_element_type=jnp.float32)


def dense_tn(left, right):
    return lax.dot_general(left, right, (((0,), (0,)), ((), ())), preferred_element_type=jnp.float32)


def per_device(
    inputs,
    prefix,
    picks,
    gain_attn,
    w_qkv,
    w_attn_out,
    gain_mem,
    w_query,
    w_gate,
    w_proj,
    subkeys,
    values,
    cotangent,
):
    low = jnp.bfloat16
    sizes = grid_sizes()
    width_part = inputs.shape[1]
    col = lax.axis_index("col")
    col_first = col * width_part
    gain_one = lax.dynamic_slice_in_dim(gain_attn, col_first, width_part)
    gain_two = lax.dynamic_slice_in_dim(gain_mem, col_first, width_part)

    flat = flat_picks(lax.dynamic_index_in_dim(picks, lax.axis_index("row"), 1, keepdims=False))
    x_own, qkv_w, query_w, gate_w, proj_w, attn_w, rank, meta = start_all(
        sizes, values.shape[0], inputs, w_qkv, w_query, w_gate, w_proj, w_attn_out, flat
    )
    residual = x_own.astype(jnp.float32)
    scale_one = lax.rsqrt(jnp.sum(residual * residual, axis=1, keepdims=True) / D + EPSILON)
    normed_one = (residual * scale_one * gain_attn.astype(jnp.float32)).astype(low)
    qkv = jnp.einsum("tc,jcf->jtf", normed_one, qkv_w, preferred_element_type=jnp.float32).astype(low)
    attended, log_sums, kv_all, dy_own = attend(sizes, prefix, qkv, cotangent)
    hidden, normed_two = join(sizes, dense(attended, attn_w).astype(low), inputs, gain_two)
    query_rows = dense(normed_two, query_w).astype(low)
    gate_value = dense(normed_two, gate_w)
    sigmoid_gate = jax.nn.sigmoid(gate_value)
    silu_gate = gate_value * sigmoid_gate
    grad_gated = dense_nt(dy_own, proj_w)
    grad_memory = (grad_gated * silu_gate).astype(low)
    memory, grad_query, grad_keys, table, grads_all = memory_all(
        query_rows, grad_memory, flat, rank, meta, subkeys, values
    )
    gated_value = (memory * silu_gate).astype(low)
    out_part = dense(gated_value, proj_w).astype(low)
    grad_gate = (
        grad_gated * memory * sigmoid_gate * (1.0 + gate_value * (1.0 - sigmoid_gate))
    ).astype(low)
    grad_part = (dense_nt(grad_query, query_w) + dense_nt(grad_gate, gate_w)).astype(low)
    query_term = dense_tn(normed_two, grad_query).astype(low)
    first_terms = [
        dense_tn(normed_two, grad_gate).astype(low),
        dense_tn(gated_value, dy_own).astype(low),
        grad_keys.reshape(-1, HALF).astype(low),
    ]
    grad_hidden, grad_hidden_all, gain_two_grad, *shards = middle(
        sizes, grad_part, hidden, cotangent, gain_two, first_terms
    )
    grad_attended = dense_nt(grad_hidden_all, attn_w).astype(low)
    grad_q, grad_kv, output, grad_w_gate, grad_w_proj, grad_keys_half, query_shard = turn(
        sizes, prefix, qkv[0], kv_all, grad_attended, log_sums, out_part, hidden, shards, query_term
    )
    x_part = (
        dense_nt(grad_q, qkv_w[0]) + dense_nt(grad_kv[0], qkv_w[1]) + dense_nt(grad_kv[1], qkv_w[2])
    ).astype(low)
    last_terms = [
        jnp.stack([dense_tn(normed_one, part) for part in (grad_q, grad_kv[0], grad_kv[1])]).astype(low),
        dense_tn(attended, grad_hidden_all).astype(low),
    ]
    (
        grad_inputs, gain_sums, grad_values, grad_w_query, grad_w_qkv, grad_w_attn_out, grad_subkeys,
    ) = last(
        sizes, x_part, inputs, grad_hidden, gain_one, gain_two_grad, grad_keys_half, query_shard,
        last_terms, table, grads_all,
    )
    gain_rows = gain_sums.reshape(sizes[2], 2, width_part)
    grad_gain_one = gain_rows[:, 0].reshape(-1)
    grad_gain_two = gain_rows[:, 1].reshape(-1)

    return (
        output,
        grad_inputs,
        grad_gain_one,
        grad_w_qkv.astype(jnp.float32),
        grad_w_attn_out.astype(jnp.float32),
        grad_gain_two,
        grad_w_query.astype(jnp.float32),
        grad_w_gate.astype(jnp.float32),
        grad_w_proj.astype(jnp.float32),
        grad_subkeys.astype(jnp.float32),
        grad_values.astype(jnp.float32),
    )


def solution(mesh):
    placed = (
        P(("dp", "row"), "col"),
        P("dp"),
        P(("dp", "col"), None, None),
        P(),
        P(None, "col", "row"),
        P("row", "col"),
        P(),
        P("col", "row"),
        P("col", "row"),
        P("row", "col"),
        P(),
        P(("dp", "row", "col"), None),
        P(("dp", "row"), "col"),
    )
    return jax.shard_map(
        per_device,
        mesh=mesh,
        in_specs=placed,
        out_specs=(
            P(("dp", "row"), "col"),
            P(("dp", "row"), "col"),
            P(),
            P(None, "col", "row"),
            P("row", "col"),
            P(),
            P("col", "row"),
            P("col", "row"),
            P("row", "col"),
            P(),
            P(("dp", "row", "col"), None),
        ),
        check_vma=False,
    )
```
